32 devices in a mesh: section: 2 (over x), replica: 2 (over core), shard: 8 (over z, y).
Axes of the slice: x: 2, y: 2, z: 4, core: 2. Of those that a mesh axis runs over, the one named last changes fastest.
Arguments:
- tokens: int32 [32, 320], P('replica'), may hold values from 0 to 31999
- parents: int32 [32, 10], P('replica'), may hold values from 0 to 8, as said below
- loss_positions: int32 [32, 16], P('replica'), may hold values from 0 to 319
- targets: int32 [32, 16], P('replica'), may hold values from 0 to 31999
- teacher_index: int32 [32, 16, 64], P('replica'), may hold values from 0 to 31999
- teacher_probability: float32 [32, 16, 64], P('replica'), may hold values from 0.001 to 0.05
- step_count: int32 [], replicated, may hold values from 1 to 20
- embed_table: float32 [32000, 768], P(('replica', 'shard')), may hold values from -0.4330127 to 0.4330127
- table_first: float32 [32000, 768], P(('replica', 'shard')), may hold values from -9.1552734e-05 to 9.1552734e-05
- table_second: float32 [32000, 768], P(('replica', 'shard')), may hold values from 3.2273243e-13 to 3.2273243e-11
- attention_in: float32 [2, 768, 2304], P('section', 'shard'), may hold values from -0.21875 to 0.21875
- attention_in_first: float32 [2, 768, 2304], P('section', 'shard'), may hold values from -9.1552734e-05 to 9.1552734e-05
- attention_in_second: float32 [2, 768, 2304], P('section', 'shard'), may hold values from 3.2273243e-13 to 3.2273243e-11
- attention_out: float32 [2, 768, 768], P('section', 'shard'), may hold values from -0.4375 to 0.4375
- attention_out_first: float32 [2, 768, 768], P('section', 'shard'), may hold values from -9.1552734e-05 to 9.1552734e-05
- attention_out_second: float32 [2, 768, 768], P('section', 'shard'), may hold values from 3.2273243e-13 to 3.2273243e-11
- feedforward_in: float32 [2, 768, 4096], P('section', 'shard'), may hold values from -0.21875 to 0.21875
- feedforward_in_first: float32 [2, 768, 4096], P('section', 'shard'), may hold values from -9.1552734e-05 to 9.1552734e-05
- feedforward_in_second: float32 [2, 768, 4096], P('section', 'shard'), may hold values from 3.2273243e-13 to 3.2273243e-11
- feedforward_out: float32 [2, 2048, 768], P('section', 'shard'), may hold values from -0.125 to 0.125
- feedforward_out_first: float32 [2, 2048, 768], P('section', 'shard'), may hold values from -9.1552734e-05 to 9.1552734e-05
- feedforward_out_second: float32 [2, 2048, 768], P('section', 'shard'), may hold values from 3.2273243e-13 to 3.2273243e-11
- forget_gate: float32 [2, 769, 12], replicated
- forget_first: float32 [2, 769, 12], replicated, may hold values from -9.1552734e-05 to 9.1552734e-05
- forget_second: float32 [2, 769, 12], replicated, may hold values from 3.2273243e-13 to 3.2273243e-11
- norm_gains: float32 [5, 768], replicated, may hold values from 0.5 to 1.5
- gains_first: float32 [5, 768], replicated, may hold values from -9.1552734e-05 to 9.1552734e-05
- gains_second: float32 [5, 768], replicated, may hold values from 3.2273243e-13 to 3.2273243e-11
Outputs:
- new_table: float32 [32000, 768], P(('replica', 'shard'))
- new_table_first: float32 [32000, 768], P(('replica', 'shard'))
- new_table_second: float32 [32000, 768], P(('replica', 'shard'))
- new_attention_in: float32 [2, 768, 2304], P('section', 'shard')
- new_attention_in_first: float32 [2, 768, 2304], P('section', 'shard')
- new_attention_in_second: float32 [2, 768, 2304], P('section', 'shard')
- new_attention_out: float32 [2, 768, 768], P('section', 'shard')
- new_attention_out_first: float32 [2, 768, 768], P('section', 'shard')
- new_attention_out_second: float32 [2, 768, 768], P('section', 'shard')
- new_feedforward_in: float32 [2, 768, 4096], P('section', 'shard')
- new_feedforward_in_first: float32 [2, 768, 4096], P('section', 'shard')
- new_feedforward_in_second: float32 [2, 768, 4096], P('section', 'shard')
- new_feedforward_out: float32 [2, 2048, 768], P('section', 'shard')
- new_feedforward_out_first: float32 [2, 2048, 768], P('section', 'shard')
- new_feedforward_out_second: float32 [2, 2048, 768], P('section', 'shard')
- new_forget_gate: float32 [2, 769, 12], replicated
- new_forget_first: float32 [2, 769, 12], replicated
- new_forget_second: float32 [2, 769, 12], replicated
- new_gains: float32 [5, 768], replicated
- new_gains_first: float32 [5, 768], replicated
- new_gains_second: float32 [5, 768], replicated
- tensor_norms: float32 [16, 2], replicated
- grad_norm: float32 [], replicated
- loss: float32 [], replicated
The draws below stay inside these ranges and needn't reach their ends.
Inputs may be any that keep to these rules, and one draw needn't show every extreme that they name: parents[t, 0] = 0 marks the root; for s >= 1, parents[t, s] < s; parents[t, 9] = 8.
All inputs are finite; a program needn't handle non-finite values.
Results may differ from the reference program's by a relative error of at most 0.028.
Values may be sent and summed in bfloat16 or wider, within the bound.
A program may use at most 320 MiB of HBM per device.

```python
import math
from functools import partial
import jax
import jax.numpy as jnp
import numpy as np
from jax import lax

D = 768
HEADS = 12
HDIM = 64
FF = 2048
V = 32000
TOPK = 64
NSEG = 10
NPOS = 16
TREE = 320
SEQS = 32
POS_ALL = 512
PARAMS = 38731776


def draw_parents(key, part):
    segment_ids = jnp.arange(NSEG, dtype=jnp.int32)
    raw_draw = jax.random.randint(key, (SEQS, NSEG), 0, 1 << 20, dtype=jnp.int32)
    chosen = raw_draw % jnp.maximum(segment_ids, 1)[None, :]
    chosen = jnp.where(segment_ids[None, :] == 0, 0, chosen)
    chosen = jnp.where(segment_ids[None, :] == NSEG - 1, NSEG - 2, chosen)
    return chosen.astype(jnp.int32)


def draw_forget_gate(key, part):
    weight_key = jax.random.fold_in(key, 11)
    bias_key = jax.random.fold_in(key, 23)
    weights = jax.random.normal(weight_key, (2, D, HEADS), jnp.float32) * (0.5 / D ** 0.5)
    biases = jax.random.uniform(bias_key, (2, 1, HEADS), jnp.float32, 3.0, 8.0)
    return jnp.concatenate([weights, biases], axis=1)


def with_ends(result, rng, low, top_value):
    dims = result.shape
    place = [jax.random.randint(jax.random.fold_in(rng, axis), (), 0, dims[axis]) for axis in range(len(dims))]
    result = result.at[tuple(place)].set(low)
    longest = dims.index(max(dims))
    place[longest] = (place[longest] + 1) % dims[longest]
    return result.at[tuple(place)].set(top_value)


def steps_of(own_key, shape, cuts, smallest, high):
    factor_of = 1.0
    for axis_at, shards_of in cuts:
        draws = jax.random.uniform(jax.random.fold_in(jax.random.fold_in(own_key, 6), axis_at), (shards_of,), jnp.float32, smallest / len(cuts), high / len(cuts))
        factor_of = factor_of * jnp.repeat(jnp.exp(draws), shape[axis_at] // shards_of).reshape((-1,) + (1,) * (len(shape) - 1 - axis_at))
    return factor_of


def rank_bounds(amount, slope):
    weights = [(1 << 20) // math.isqrt(grade ** slope) + 1 for grade in range(1, amount + 1)]
    scale = 1 + sum(weights) // (1 << 30)
    return np.cumsum(np.array([max(1, weight // scale) for weight in weights]))


def skewed_ids(stream_key, dims, count, skew):
    table = rank_bounds(count, skew)
    ticket = jax.random.randint(jax.random.fold_in(stream_key, 1), dims, 0, int(table[count - 1]))
    grade = jnp.searchsorted(jnp.asarray(table, jnp.int32), ticket, side="right")
    return jax.random.permutation(jax.random.fold_in(stream_key, 2), count)[grade].astype(jnp.int32)


def noise(stream_key, shape, spread, reach, shards=(), kind=jnp.bfloat16):
    entries = jax.random.normal(stream_key, shape, jnp.float32) * spread
    if len(shards) > 0:
        entries = steps_of(stream_key, shape, shards, -0.22, 0.18) * entries
    return jnp.clip(entries, min=-reach, max=reach).astype(kind)


def setup_inputs(seed: int = 0) -> dict:
    keys = jax.random.split(jax.random.key(seed), 29)
    return {
        "tokens": with_ends(skewed_ids(keys[0], (SEQS, TREE), V, 2), jax.random.fold_in(keys[0], 3), 0, V - 1).astype(jnp.int32),
        "parents": draw_parents(jax.random.fold_in(keys[28], 71), 0),
        "loss_positions": with_ends(jax.random.randint(keys[2], (SEQS, NPOS), 0, TREE), jax.random.fold_in(keys[2], 1), 0, TREE - 1).astype(jnp.int32),
        "targets": with_ends(skewed_ids(keys[3], (SEQS, NPOS), V, 2), jax.random.fold_in(keys[3], 3), 0, V - 1).astype(jnp.int32),
        "teacher_index": with_ends(jax.random.randint(keys[4], (SEQS, NPOS, TOPK), 0, V), jax.random.fold_in(keys[4], 1), 0, V - 1).astype(jnp.int32),
        "teacher_probability": jnp.clip(jnp.exp(math.log(0.05) - 3.912023 * jax.random.uniform(keys[5], (SEQS, NPOS, TOPK), jnp.float32) ** steps_of(keys[5], (SEQS, NPOS, TOPK), ((0, 2),), -0.2, 0.2)), 0.001, 0.05),
        "step_count": jax.random.randint(keys[6], (), 1, 21).astype(jnp.int32),
        "embed_table": noise(keys[7], (V, D), (2.0 / D ** 0.5), 0.4330127, ((0, 16),), jnp.float32),
        "table_first": noise(keys[8], (V, D), (0.88 / (POS_ALL * PARAMS) ** 0.5), 9.1552734375e-05, ((0, 16),), jnp.float32),
        "table_second": jnp.clip(jnp.exp(math.log(3.227324310572932e-11) - 4.6051702 * jax.random.uniform(keys[9], (V, D), jnp.float32) ** steps_of(keys[9], (V, D), ((0, 16),), -0.2, 0.2)), 3.227324278046867e-13, 3.227324310572932e-11),
        "attention_in": noise(keys[10], (2, D, 3 * D), D ** -0.5, 0.21875, ((0, 2), (1, 8)), jnp.float32),
        "attention_in_first": noise(keys[11], (2, D, 3 * D), (0.88 / (POS_ALL * PARAMS) ** 0.5), 9.1552734375e-05, ((0, 2), (1, 8)), jnp.float32),
        "attention_in_second": jnp.clip(jnp.exp(math.log(3.227324310572932e-11) - 4.6051702 * jax.random.uniform(keys[12], (2, D, 3 * D), jnp.float32) ** steps_of(keys[12], (2, D, 3 * D), ((0, 2), (1, 8)), -0.2, 0.2)), 3.227324278046867e-13, 3.227324310572932e-11),
        "attention_out": noise(keys[13], (2, D, D), (D // 4) ** -0.5, 0.4375, ((0, 2), (1, 8)), jnp.float32),
        "attention_out_first": noise(keys[14], (2, D, D), (0.88 / (POS_ALL * PARAMS) ** 0.5), 9.1552734375e-05, ((0, 2), (1, 8)), jnp.float32),
        "attention_out_second": jnp.clip(jnp.exp(math.log(3.227324310572932e-11) - 4.6051702 * jax.random.uniform(keys[15], (2, D, D), jnp.float32) ** steps_of(keys[15], (2, D, D), ((0, 2), (1, 8)), -0.2, 0.2)), 3.227324278046867e-13, 3.227324310572932e-11),
        "feedforward_in": noise(keys[16], (2, D, 2 * FF), D ** -0.5, 0.21875, ((0, 2), (1, 8)), jnp.float32),
        "feedforward_in_first": noise(keys[17], (2, D, 2 * FF), (0.88 / (POS_ALL * PARAMS) ** 0.5), 9.1552734375e-05, ((0, 2), (1, 8)), jnp.float32),
        "feedforward_in_second": jnp.clip(jnp.exp(math.log(3.227324310572932e-11) - 4.6051702 * jax.random.uniform(keys[18], (2, D, 2 * FF), jnp.float32) ** steps_of(keys[18], (2, D, 2 * FF), ((0, 2), (1, 8)), -0.2, 0.2)), 3.227324278046867e-13, 3.227324310572932e-11),
        "feedforward_out": noise(keys[19], (2, FF, D), FF ** -0.5, 0.125, ((0, 2), (1, 8)), jnp.float32),
        "feedforward_out_first": noise(keys[20], (2, FF, D), (0.88 / (POS_ALL * PARAMS) ** 0.5), 9.1552734375e-05, ((0, 2), (1, 8)), jnp.float32),
        "feedforward_out_second": jnp.clip(jnp.exp(math.log(3.227324310572932e-11) - 4.6051702 * jax.random.uniform(keys[21], (2, FF, D), jnp.float32) ** steps_of(keys[21], (2, FF, D), ((0, 2), (1, 8)), -0.2, 0.2)), 3.227324278046867e-13, 3.227324310572932e-11),
        "forget_gate": draw_forget_gate(jax.random.fold_in(keys[28], 71), 0),
        "forget_first": noise(keys[23], (2, D + 1, HEADS), (0.88 / (POS_ALL * PARAMS) ** 0.5), 9.1552734375e-05, (), jnp.float32),
        "forget_second": jnp.clip(jnp.exp(jax.random.uniform(keys[24], (2, D + 1, HEADS), jnp.float32, math.log(3.227324278046867e-13), math.log(3.227324310572932e-11))), 3.227324278046867e-13, 3.227324310572932e-11),
        "norm_gains": jnp.clip(1.0 + 0.1 * jax.random.normal(keys[25], (5, D), jnp.float32), 0.5, 1.5),
        "gains_first": noise(keys[26], (5, D), (0.88 / (POS_ALL * PARAMS) ** 0.5), 9.1552734375e-05, (), jnp.float32),
        "gains_second": jnp.clip(jnp.exp(jax.random.uniform(keys[27], (5, D), jnp.float32, math.log(3.227324278046867e-13), math.log(3.227324310572932e-11))), 3.227324278046867e-13, 3.227324310572932e-11),
    }


@jax.custom_vjp
def low(v):
    return lax.optimization_barrier(v.astype(jnp.bfloat16)).astype(jnp.float32)

@jax.custom_vjp
def low_back(v):
    return v

def low_keep(v):
    return (low(v), None)

def low_pass(kept, grad):
    return (grad,)

def back_keep(v):
    return (v, None)

def back_low(kept, grad):
    return (low(grad),)
low.defvjp(low_keep, low_pass)
low_back.defvjp(back_keep, back_low)
eps_norm = 1e-06
beta_first = 0.9
beta_second = 0.999
adam_eps = 1e-10
decay_rate = 0.01
learn_rate = 0.2
clip_factor = 8.0
highest = lax.Precision.HIGHEST

def matmul(left, right):
    return jnp.dot(left, right, precision=highest)

def rms_scale(values, gain):
    return values * lax.rsqrt(lax.optimization_barrier(jnp.mean(values * values, axis=-1, keepdims=True)) + eps_norm) * gain

def path_mask(parent_row, tree_len):
    seg_count = parent_row.shape[0]
    seglen = tree_len // seg_count
    seg_order = jnp.arange(seg_count, dtype=jnp.int32)
    parent_hot = ((parent_row[:, None] == seg_order[None, :]) & (seg_order[:, None] >= 1)).astype(jnp.float32)
    identity = jnp.eye(seg_count, dtype=jnp.float32)

    def extend(step_index, reached):
        return jnp.minimum(1.0, identity + matmul(parent_hot, reached))
    reached = lax.fori_loop(0, seg_count, extend, identity)
    strict = reached - identity
    seg_of = jnp.arange(tree_len, dtype=jnp.int32) // seglen
    seg_hot = (seg_of[:, None] == seg_order[None, :]).astype(jnp.float32)
    ancestor = matmul(matmul(seg_hot, strict), seg_hot.T)
    places = jnp.arange(tree_len, dtype=jnp.int32)
    inside = (seg_of[:, None] == seg_of[None, :]) & (places[None, :] <= places[:, None])
    return ancestor + inside.astype(jnp.float32)

def layer_pass(values, allowed, weight_in, weight_out, weight_up, weight_down, forget_layer, gain_attention, gain_feedforward):
    tree_len, width = values.shape
    act_a = low(rms_scale(values, gain_attention))
    mixed = low(low_back(matmul(act_a, low(weight_in))))
    forget_logit = low_back(matmul(act_a, low(forget_layer[:width])) + forget_layer[width])
    cumul = matmul(allowed, jax.nn.log_sigmoid(forget_logit))
    queries = mixed[:, :width].reshape(tree_len, HEADS, HDIM)
    keys_all = mixed[:, width:2 * width].reshape(tree_len, HEADS, HDIM)
    values_all = mixed[:, 2 * width:].reshape(tree_len, HEADS, HDIM)
    scores = jnp.einsum('ihd,jhd->hij', queries, keys_all, precision=highest) * HDIM ** (-0.5)
    scores = low_back(scores + cumul.T[:, :, None] - cumul.T[:, None, :])
    scores = jnp.where(allowed[None] > 0, scores, -1e+30)
    probs = low(jax.nn.softmax(scores, axis=-1))
    attended = jnp.einsum('hij,jhd->ihd', probs, values_all, precision=highest).reshape(tree_len, width)
    attended = low(low_back(attended))
    middle = values + low_back(matmul(attended, low(weight_out)))
    act_b = low(rms_scale(middle, gain_feedforward))
    gate_up = low_back(matmul(act_b, low(weight_up)))
    hidden = low(jax.nn.silu(gate_up[:, :FF]) * gate_up[:, FF:])
    return middle + low_back(matmul(hidden, low(weight_down)))

def tree_loss(params, item):
    embed_table, attention_in, attention_out, feedforward_in, feedforward_out, forget_gate, norm_gains = params
    tokens, parents, positions, targets, teacher_index, teacher_probability = item
    allowed = path_mask(parents, tokens.shape[0])
    table_low = low(embed_table)
    hidden = low_back(table_low[tokens])
    for layer_index in range(2):
        if layer_index == 1:
            hidden = low_back(low(hidden))
        hidden = layer_pass(hidden, allowed, attention_in[layer_index], attention_out[layer_index], feedforward_in[layer_index], feedforward_out[layer_index], forget_gate[layer_index], norm_gains[2 * layer_index], norm_gains[2 * layer_index + 1])
    picked = low(rms_scale(hidden[positions], norm_gains[4]))
    logits = low_back(matmul(picked, table_low.T))
    log_norm = jax.nn.logsumexp(logits, axis=-1)
    target_logit = jnp.take_along_axis(logits, targets[:, None], axis=1)[:, 0]
    teacher_logit = jnp.take_along_axis(logits, teacher_index, axis=1)
    row_loss = log_norm - target_logit + lax.optimization_barrier(jnp.sum(teacher_probability * (jnp.log(teacher_probability) - teacher_logit + log_norm[:, None]), axis=-1))
    return jnp.sum(row_loss)

def reference(tokens, parents, loss_positions, targets, teacher_index, teacher_probability, step_count, embed_table, table_first, table_second, attention_in, attention_in_first, attention_in_second, attention_out, attention_out_first, attention_out_second, feedforward_in, feedforward_in_first, feedforward_in_second, feedforward_out, feedforward_out_first, feedforward_out_second, forget_gate, forget_first, forget_second, norm_gains, gains_first, gains_second):
    params = (embed_table, attention_in, attention_out, feedforward_in, feedforward_out, forget_gate, norm_gains)
    data = (tokens, parents, loss_positions, targets, teacher_index, teacher_probability)

    def total_loss(weights):
        per_tree = lax.map(jax.checkpoint(partial(tree_loss, weights)), data)
        return jnp.sum(per_tree) / POS_ALL
    loss_value, pullback = jax.vjp(total_loss, params)
    grads = pullback(jnp.ones((), loss_value.dtype))[0]
    grad_norm = jnp.sqrt(sum((jnp.sum(piece * piece) for piece in grads)))
    clip_scale = jnp.minimum(1.0, clip_factor / jnp.sqrt(jnp.float32(POS_ALL)) / grad_norm)
    count_float = step_count.astype(jnp.float32)
    correct_first = 1.0 - jnp.power(beta_first, count_float)
    correct_second = 1.0 - jnp.power(beta_second, count_float)
    firsts = (table_first, attention_in_first, attention_out_first, feedforward_in_first, feedforward_out_first, forget_first, gains_first)
    seconds = (table_second, attention_in_second, attention_out_second, feedforward_in_second, feedforward_out_second, forget_second, gains_second)
    axes_list = (None, (1, 2), (1, 2), (1, 2), (1, 2), (1, 2), (1,))
    results = []
    norm_rows = []
    for weight, grad, first, second, axes_here in zip(params, grads, firsts, seconds, axes_list):
        scaled = clip_scale * grad
        first_new = beta_first * first + (1.0 - beta_first) * scaled
        second_new = beta_second * second + (1.0 - beta_second) * scaled * scaled
        direction = first_new / correct_first / (jnp.sqrt(second_new / correct_second) + adam_eps) + decay_rate * weight
        weight_norm = jnp.sqrt(lax.optimization_barrier(jnp.sum(weight * weight, axis=axes_here)))
        update_norm = jnp.sqrt(lax.optimization_barrier(jnp.sum(direction * direction, axis=axes_here)))
        ratio = weight_norm / update_norm
        if axes_here is None:
            new_weight = weight - learn_rate * ratio * direction
        elif len(axes_here) == 2:
            new_weight = weight - learn_rate * ratio[:, None, None] * direction
        else:
            new_weight = weight - learn_rate * ratio[:, None] * direction
        results.extend([new_weight, first_new, second_new])
        norm_rows.append(jnp.stack([jnp.atleast_1d(weight_norm), jnp.atleast_1d(update_norm)], axis=1))
    tensor_norms = jnp.concatenate(norm_rows, axis=0)
    return (results[0], results[1], results[2], results[3], results[4], results[5], results[6], results[7], results[8], results[9], results[10], results[11], results[12], results[13], results[14], results[15], results[16], results[17], results[18], results[19], results[20], tensor_norms, grad_norm, loss_value)
```

```python
from functools import partial

import jax
import jax.numpy as jnp
from jax import lax
from jax.experimental import pallas as pl
from jax.experimental.pallas import tpu as pltpu
from jax.sharding import PartitionSpec as P

MESH = pl.DeviceIdType.MESH
VMEM = pl.BlockSpec(memory_space=pltpu.VMEM)
ANY = pl.BlockSpec(memory_space=pl.ANY)
DMA = pltpu.SemaphoreType.DMA
eps_norm = 1e-06
beta_first = 0.9
beta_second = 0.999
adam_eps = 1e-10
decay_rate = 0.01
learn_rate = 0.2
clip_factor = 8.0
highest = lax.Precision.HIGHEST
masked_score = -1e30
batch_rows = 40
every_axis = ("section", "replica", "shard")


class Place:
    def __init__(self):
        self.sections = lax.axis_size("section")
        self.replicas = lax.axis_size("replica")
        self.shards = lax.axis_size("shard")
        self.nz = min(4, self.shards)
        self.ny = self.shards // self.nz
        self.x = lax.axis_index("section")
        self.rep = lax.axis_index("replica")
        self.shard = lax.axis_index("shard")
        self.core = lax.rem(self.rep, 2)
        self.z = self.shard // self.ny
        self.y = lax.rem(self.shard, self.ny)

    def at(self, section=None, rep=None, z=None, y=None, shard=None):
        if shard is None:
            shard = (self.z if z is None else z) * self.ny + (self.y if y is None else y)
        return {
            "section": self.x if section is None else section,
            "replica": self.rep if rep is None else rep,
            "shard": shard,
        }

    def peer_x(self, i):
        return self.at(section=lax.rem(self.x + i, self.sections))

    def peer_y(self, j):
        return self.at(y=lax.rem(self.y + j, self.ny))

    def line(self, step):
        return self.at(z=self.z + step)

    def partner(self):
        return self.at(rep=self.rep + 1 - 2 * self.core)

    def group(self, p):
        count = self.replicas * self.shards
        place = lax.rem(self.rep * self.shards + self.shard + p, count)
        return place, self.at(rep=place // self.shards, shard=lax.rem(place, self.shards))

    def inside(self, k):
        if k == 0:
            return None
        return self.z + k < self.nz if k > 0 else self.z + k >= 0

    def greet(self, use_x=True):
        barrier = pltpu.get_barrier_semaphore()

        def signal(device):
            pl.semaphore_signal(barrier, inc=1, device_id=device, device_id_type=MESH)

        count = 1
        if use_x:
            for i in range(1, self.sections):
                signal(self.peer_x(i))
                count += 1
        for j in range(1, self.ny):
            signal(self.peer_y(j))
            count += 1
        signal(self.partner())
        up, down = self.inside(1), self.inside(-1)
        pl.when(up)(lambda: signal(self.line(1)))
        pl.when(down)(lambda: signal(self.line(-1)))
        ends = jnp.minimum(self.z, 1) + jnp.minimum(self.nz - 1 - self.z, 1)
        pl.semaphore_wait(barrier, count + ends)


def when(cond, fn):
    if cond is None:
        fn()
    else:
        pl.when(cond)(fn)


def both(a, b):
    if a is None:
        return b
    if b is None:
        return a
    return jnp.logical_and(a, b)


def remote(src, dst, send, recv, device):
    return pltpu.make_async_remote_copy(
        src_ref=src, dst_ref=dst, send_sem=send, recv_sem=recv, device_id=device, device_id_type=MESH
    )


def gather_kernel(count, pairs, split, orders, *refs):
    ins, refs = refs[:count], refs[count:]
    pair_ins, refs = refs[:pairs], refs[pairs:]
    outs, refs = refs[:count], refs[count:]
    pair_outs, refs = refs[:pairs], refs[pairs:]
    send_sem, recv_sem, cross_sem, pair_sem, local_sem = refs
    me = Place()
    nz, ny, nx = me.nz, me.ny, me.sections
    if "x" not in orders[0]:
        nx = 1
    me.greet(use_x=nx > 1)

    def slot(ref, k, j, i, half):
        section = lax.rem(me.x + i, nx) if nx > 1 else 0
        return ref.at[section, (me.z + k) * ny + lax.rem(me.y + j, ny), half]

    locals_ = []
    for a in range(count):
        if split:
            dst = outs[a].at[me.x if nx > 1 else 0, me.shard]
        else:
            dst = outs[a].at[me.x if nx > 1 else 0, me.shard, me.core]
        locals_.append(pltpu.make_async_copy(ins[a], dst, local_sem.at[a]))
    for p in range(pairs):
        locals_.append(
            pltpu.make_async_copy(pair_ins[p], pair_outs[p].at[me.core], local_sem.at[count + p])
        )
    for copy in locals_:
        copy.start()
    pair_copies = [
        remote(pair_ins[p], pair_outs[p].at[me.core], pair_sem.at[0, p], pair_sem.at[1, p], me.partner())
        for p in range(pairs)
    ]

    def run(core, order):
        sends = []

        def push(cond, src, dst, device, sem):
            copy = remote(src, dst, send_sem.at[len(sends)], sem, device)
            when(cond, copy.start)
            sends.append((cond, copy))

        def sem_of(a, k, j, i):
            return recv_sem.at[a, k + nz - 1, j, i]

        def spread(k, j, i, via):
            cond = me.inside(k)
            own = via is None
            later = order if own else order[order.index(via) + 1 :]
            for a in range(count):
                dst = slot(outs[a], k, j, i, core)
                src = dst
                if own:
                    src = ins[a].at[core] if split else ins[a]
                else:
                    arrival = remote(dst, dst, send_sem.at[0], sem_of(a, k, j, i), me.partner())
                    when(cond, arrival.wait_recv)
                steps = []
                if via == "z":
                    steps = [-1 if k > 0 else 1]
                elif "z" in later:
                    steps = [1, -1]
                for step in steps:
                    push(both(cond, me.inside(step)), src, dst, me.line(step), sem_of(a, k - step, j, i))
                if "y" in later:
                    for p in range(1, ny):
                        push(cond, src, dst, me.peer_y(p), sem_of(a, k, (j - p) % ny, i))
                if "x" in later:
                    for p in range(1, nx):
                        push(cond, src, dst, me.peer_x(p), sem_of(a, k, j, (i - p) % nx))
                if not (own and split):
                    push(cond, src, dst, me.partner(), cross_sem.at[a, k + nz - 1, j, i])

        events = []
        for k in range(1 - nz, nz):
            for j in range(ny):
                for i in range(nx):
                    via = [d for d in order if {"z": k, "y": j, "x": i}[d] != 0]
                    hops = abs(k) + (j != 0) + (i != 0)
                    stage = order.index(via[-1]) if via else -1
                    events.append((hops, stage, k, j, i, via[-1] if via else None))
        events.sort(key=lambda e: e[:5])
        for hops, stage, k, j, i, via in events:
            spread(k, j, i, via)
            if via is None:
                for copy in pair_copies:
                    copy.start()
        for hops, stage, k, j, i, via in events:
            if via is None and split:
                continue
            for a in range(count):
                dst = slot(outs[a], k, j, i, 1 - core)
                arrival = remote(dst, dst, send_sem.at[0], cross_sem.at[a, k + nz - 1, j, i], me.partner())
                when(me.inside(k), arrival.wait_recv)
        for cond, copy in sends:
            when(cond, copy.wait_send)

    for core, order in enumerate(orders):
        pl.when(me.core == core)(partial(run, core, order))
    for p in range(pairs):
        pair_copies[p].wait_send()
        remote(
            pair_ins[p], pair_outs[p].at[1 - me.core], pair_sem.at[0, p], pair_sem.at[1, p], me.partner()
        ).wait_recv()
    for copy in locals_:
        copy.wait()


def gather(parts, ident, pair_parts=(), split=False, orders=(("z", "y", "x"), ("x", "z", "y")), space=ANY):
    count, pairs = len(parts), len(pair_parts)
    shards = lax.axis_size("shard")
    nx = lax.axis_size("section") if "x" in orders[0] else 1
    nz = min(4, shards)
    ny = shards // nz
    lead = (nx, shards) if split else (nx, shards, 2)
    blocks = (2 * nz - 1) * ny * nx
    outs = pl.pallas_call(
        partial(gather_kernel, count, pairs, split, orders),
        out_shape=[jax.ShapeDtypeStruct(lead + p.shape, p.dtype) for p in parts]
        + [jax.ShapeDtypeStruct((2,) + p.shape, p.dtype) for p in pair_parts],
        in_specs=[VMEM] * (count + pairs),
        out_specs=[space] * (count + pairs),
        scratch_shapes=[
            DMA((blocks * count * 4,)),
            DMA((count, 2 * nz - 1, ny, nx)),
            DMA((count, 2 * nz - 1, ny, nx)),
            DMA((2, max(pairs, 1))),
            DMA((count + pairs,)),
        ],
        compiler_params=pltpu.CompilerParams(collective_id=ident, has_side_effects=True),
        name=f"gather_{ident}",
    )(*parts, *pair_parts)
    return outs[:count], outs[count:]


def exchange_kernel(relay, src_ref, out_ref, send_sem, recv_sem, relay_send, relay_recv, local_sem):
    me = Place()
    peers = me.replicas * me.shards
    barrier = pltpu.get_barrier_semaphore()
    for p in range(1, peers):
        pl.semaphore_signal(barrier, inc=1, device_id=me.group(p)[1], device_id_type=MESH)
    if relay:
        for i in range(1, me.sections):
            pl.semaphore_signal(barrier, inc=1, device_id=me.peer_x(i), device_id_type=MESH)
    pl.semaphore_wait(barrier, peers - 1 + (me.sections - 1 if relay else 0))
    mine = me.rep * me.shards + me.shard
    section = me.x if relay else 0
    own = pltpu.make_async_copy(src_ref.at[mine], out_ref.at[section, mine], local_sem.at[0])
    own.start()
    sends = []
    for p in range(1, peers):
        place, device = me.group(p)
        copy = remote(
            src_ref.at[place], out_ref.at[section, mine], send_sem.at[p], recv_sem.at[p], device
        )
        copy.start()
        sends.append(copy)
    relays = []

    def forward(p, src, dst):
        for i in range(1, me.sections):
            copy = remote(src, dst, relay_send.at[p, i], relay_recv.at[p, i], me.peer_x(i))
            copy.start()
            relays.append(copy)

    if relay:
        forward(0, src_ref.at[mine], out_ref.at[me.x, mine])
    for p in range(1, peers):
        source, device = me.group(peers - p)
        dst = out_ref.at[section, source]
        remote(dst, dst, send_sem.at[p], recv_sem.at[p], device).wait_recv()
        if relay:
            forward(p, dst, dst)
    if relay:
        for p in range(peers):
            source, _ = me.group(peers - p)
            for i in range(1, me.sections):
                dst = out_ref.at[lax.rem(me.x + me.sections - i, me.sections), source]
                remote(dst, dst, relay_send.at[p, i], relay_recv.at[p, i], me.peer_x(i)).wait_recv()
    for copy in sends + relays:
        copy.wait_send()
    own.wait()


def exchange(blocks, ident, relay=False):
    peers = blocks.shape[0]
    nx = lax.axis_size("section")
    return pl.pallas_call(
        partial(exchange_kernel, relay),
        out_shape=jax.ShapeDtypeStruct((nx if relay else 1,) + blocks.shape, blocks.dtype),
        in_specs=[VMEM],
        out_specs=VMEM,
        scratch_shapes=[DMA((peers,)), DMA((peers,)), DMA((peers, nx)), DMA((peers, nx)), DMA((1,))],
        compiler_params=pltpu.CompilerParams(collective_id=ident, has_side_effects=True),
        name=f"exchange_{ident}",
    )(blocks)


def total_kernel(value_ref, out_ref, held, send_sem, recv_sem):
    me = Place()
    steps = []
    for axis, size in (("replica", me.replicas), ("section", me.sections), ("shard", me.shards)):
        bit = 1
        while bit < size:
            steps.append((axis, bit))
            bit *= 2
    position = {"section": me.x, "replica": me.rep, "shard": me.shard}

    def other(axis, bit):
        index = position[axis]
        set_ = lax.rem(index // bit, 2)
        return {**position, axis: index + bit - 2 * bit * set_}

    barrier = pltpu.get_barrier_semaphore()
    for axis, bit in steps:
        pl.semaphore_signal(barrier, inc=1, device_id=other(axis, bit), device_id_type=MESH)
    pl.semaphore_wait(barrier, len(steps))
    held[0] = value_ref[...]
    copies = []
    for n, (axis, bit) in enumerate(steps):
        copy = remote(held.at[2 * n], held.at[2 * n + 1], send_sem.at[n], recv_sem.at[n], other(axis, bit))
        copy.start()
        copies.append(copy)
        copy.wait_recv()
        summed = held[2 * n] + held[2 * n + 1]
        if n + 1 < len(steps):
            held[2 * n + 2] = summed
        else:
            out_ref[...] = summed
    for copy in copies:
        copy.wait_send()


def total(value, ident):
    steps = sum((lax.axis_size(axis) - 1).bit_length() for axis in every_axis)
    return pl.pallas_call(
        total_kernel,
        out_shape=jax.ShapeDtypeStruct(value.shape, value.dtype),
        in_specs=[VMEM],
        out_specs=VMEM,
        scratch_shapes=[pltpu.VMEM((2 * steps,) + value.shape, value.dtype), DMA((steps,)), DMA((steps,))],
        compiler_params=pltpu.CompilerParams(collective_id=ident, has_side_effects=True),
        name=f"total_{ident}",
    )(value)


def add_rows(dst, src):
    rows = dst.shape[0]
    if rows % 16 != 0:
        dst[...] = (dst[...].astype(jnp.float32) + src[...].astype(jnp.float32)).astype(dst.dtype)
        return
    step = 16

    def body(n, carry):
        at = pl.ds(pl.multiple_of(n * step, step), step)
        dst[at, :] = (dst[at, :].astype(jnp.float32) + src[at, :].astype(jnp.float32)).astype(dst.dtype)
        return carry

    lax.fori_loop(0, rows // step, body, 0)


def reduce_kernel(count, *refs):
    ins, refs = refs[:count], refs[count:]
    outs, refs = refs[:count], refs[count:]
    acc, refs = refs[:count], refs[count:]
    from_core, refs = refs[:count], refs[count:]
    from_x, refs = refs[:count], refs[count:]
    from_y, refs = refs[:count], refs[count:]
    from_z, refs = refs[:count], refs[count:]
    load_sem, core_send, core_recv, send_sem, x_recv, y_recv, z_recv, last_sem = refs
    me = Place()
    nz, ny, nx = me.nz, me.ny, me.sections
    me.greet()
    far = sorted((k for k in range(1 - nz, nz)), key=lambda k: -abs(k))

    def block(k, j, i):
        return lax.rem(me.x + i, nx), (me.z + k) * ny + lax.rem(me.y + j, ny)

    def order_of(core):
        if core == 0:
            return [(k, j, i) for i in range(nx - 1, -1, -1) for j in range(ny - 1, -1, -1) for k in far]
        return [(k, j, i) for j in range(ny - 1, -1, -1) for k in far for i in range(nx - 1, -1, -1)]

    def run(core):
        other = 1 - core
        sends = []

        def start_core(k, j, i):
            x, s = block(k, j, i)

            def go():
                for a in range(count):
                    remote(
                        ins[a].at[x, s, other], from_core[a].at[x, s], core_send.at[a, x, s],
                        core_recv.at[a, x, s], me.partner(),
                    ).start()

            when(me.inside(k), go)

        def start_load(k, j, i):
            x, s = block(k, j, i)

            def go():
                for a in range(count):
                    pltpu.make_async_copy(ins[a].at[x, s, core], acc[a].at[x, s], load_sem.at[a, x, s]).start()

            when(me.inside(k), go)

        for b in order_of(other):
            start_core(*b)
        for b in order_of(core):
            start_load(*b)

        def push(cond, src, dst, sem, device):
            copy = remote(src, dst, send_sem.at[len(sends)], sem, device)
            when(cond, copy.start)
            sends.append((cond, copy))

        def take(cond, dst, src, sem):
            def go():
                remote(src, src, core_send.at[0, 0, 0], sem, me.partner()).wait_recv()
                add_rows(dst, src)

            when(cond, go)

        def join_core(a, k, j, i):
            x, s = block(k, j, i)

            def go():
                pltpu.make_async_copy(ins[a].at[x, s, core], acc[a].at[x, s], load_sem.at[a, x, s]).wait()

            when(me.inside(k), go)
            take(me.inside(k), acc[a].at[x, s], from_core[a].at[x, s], core_recv.at[a, x, s])

        def join_x(a, k, j):
            x, s = block(k, j, 0)
            for p in range(1, nx):
                take(me.inside(k), acc[a].at[x, s], from_x[a].at[p - 1, s], x_recv.at[a, p - 1, s])

        def join_y(a, k, i):
            x, s = block(k, 0, i)
            for p in range(1, ny):
                take(me.inside(k), acc[a].at[x, s], from_y[a].at[p - 1, x, me.z + k], y_recv.at[a, p - 1, x, me.z + k])

        def join_z(a, k, i):
            x, s = block(k, 0, i)
            if k >= 0:
                take(both(me.inside(k), me.inside(-1)), acc[a].at[x, s], from_z[a].at[x, me.z + k], z_recv.at[a, x, me.z + k])
            if k <= 0:
                place = nz if k == 0 else me.z + k
                take(both(me.inside(k), me.inside(1)), acc[a].at[x, s], from_z[a].at[x, place], z_recv.at[a, x, place])

        def send_x(a, k, j, i):
            x, s = block(k, j, i)
            push(me.inside(k), acc[a].at[x, s], from_x[a].at[i - 1, s], x_recv.at[a, i - 1, s], me.peer_x(i))

        def send_y(a, k, j, i):
            x, s = block(k, j, i)
            push(
                me.inside(k), acc[a].at[x, s], from_y[a].at[j - 1, x, me.z + k],
                y_recv.at[a, j - 1, x, me.z + k], me.peer_y(j),
            )

        def send_z(a, k, i):
            x, s = block(k, 0, i)
            place = nz if k == -1 else me.z + k
            push(
                me.inside(k), acc[a].at[x, s], from_z[a].at[x, place], z_recv.at[a, x, place],
                me.line(1 if k > 0 else -1),
            )

        each = range(count)
        if core == 0:
            for i in range(nx - 1, 0, -1):
                for j in range(ny - 1, -1, -1):
                    for k in far:
                        for a in each:
                            join_core(a, k, j, i)
                            send_x(a, k, j, i)
            for j in range(ny - 1, -1, -1):
                for k in far:
                    for a in each:
                        join_core(a, k, j, 0)
            for j in range(ny - 1, 0, -1):
                for k in far:
                    for a in each:
                        join_x(a, k, j)
                        send_y(a, k, j, 0)
            for k in far:
                for a in each:
                    join_x(a, k, 0)
                    join_y(a, k, 0)
                    join_z(a, k, 0)
                    if k != 0:
                        send_z(a, k, 0)
        else:
            for j in range(ny - 1, 0, -1):
                for k in far:
                    for i in range(nx - 1, -1, -1):
                        for a in each:
                            join_core(a, k, j, i)
                            send_y(a, k, j, i)
            for k in far:
                for i in range(nx - 1, -1, -1):
                    for a in each:
                        join_core(a, k, 0, i)
            for k in far:
                for i in range(nx - 1, -1, -1):
                    for a in each:
                        join_y(a, k, i)
                        join_z(a, k, i)
                        if k != 0:
                            send_z(a, k, i)
                        elif i != 0:
                            send_x(a, 0, 0, i)
                        else:
                            join_x(a, 0, 0)
        finals = []
        for a in each:
            copy = remote(
                acc[a].at[me.x, me.shard], outs[a].at[core], last_sem.at[0, a], last_sem.at[1, a], me.partner()
            )
            copy.start()
            finals.append(copy)
            outs[a][core] = acc[a][me.x, me.shard]
        for a in each:
            remote(outs[a].at[other], outs[a].at[other], last_sem.at[0, a], last_sem.at[1, a], me.partner()).wait_recv()
        for cond, copy in sends:
            when(cond, copy.wait_send)
        for copy in finals:
            copy.wait_send()
        for k, j, i in order_of(other):
            x, s = block(k, j, i)

            def finish():
                for a in each:
                    remote(
                        ins[a].at[x, s, other], from_core[a].at[x, s], core_send.at[a, x, s],
                        core_recv.at[a, x, s], me.partner(),
                    ).wait_send()

            when(me.inside(k), finish)

    pl.when(me.core == 0)(lambda: run(0))
    pl.when(me.core == 1)(lambda: run(1))


def reduce_shards(grads, ident):
    count = len(grads)
    nx, shards = lax.axis_size("section"), lax.axis_size("shard")
    nz = min(4, shards)
    ny = shards // nz
    blocks = (2 * nz - 1) * ny * nx

    def scratch(lead):
        return [pltpu.VMEM(lead + g.shape[3:], g.dtype) for g in grads]

    return pl.pallas_call(
        partial(reduce_kernel, count),
        out_shape=[jax.ShapeDtypeStruct(g.shape[2:], g.dtype) for g in grads],
        in_specs=[ANY] * count,
        out_specs=[VMEM] * count,
        scratch_shapes=scratch((nx, shards))
        + scratch((nx, shards))
        + scratch((max(nx - 1, 1), shards))
        + scratch((max(ny - 1, 1), nx, nz))
        + scratch((nx, nz + 1))
        + [
            DMA((count, nx, shards)),
            DMA((count, nx, shards)),
            DMA((count, nx, shards)),
            DMA((blocks * count * 2,)),
            DMA((count, max(nx - 1, 1), shards)),
            DMA((count, max(ny - 1, 1), nx, nz)),
            DMA((count, nx, nz + 1)),
            DMA((2, count)),
        ],
        compiler_params=pltpu.CompilerParams(
            collective_id=ident, has_side_effects=True, vmem_limit_bytes=67043328
        ),
        name=f"reduce_{ident}",
    )(*grads)


def reduce_parts(grads, ident):
    nx, shards = lax.axis_size("section"), lax.axis_size("shard")
    ny = shards // min(4, shards)
    slots = 2 * nx * shards + (nx - 1) * shards + (ny - 1) * nx * 4 + nx * 5 + 4
    groups, used = [[]], 0
    for n, grad in enumerate(grads):
        rows, columns = grad.shape[3:]
        size = slots * (-(-rows // 16) * 16) * columns * 2
        if used + size > 58 * 2**20 and groups[-1]:
            groups.append([])
            used = 0
        groups[-1].append(n)
        used += size
    out = [None] * len(grads)
    for g, group in enumerate(groups):
        for n, value in zip(group, reduce_shards([grads[n] for n in group], ident + g)):
            out[n] = value
    return out


def spread_kernel(columns_ref, weight_ref, out_ref):
    groups, entries = columns_ref.shape[0], columns_ref.shape[2]
    high = out_ref.shape[1] // 128
    each = entries // 8

    def body(g, carry):
        column = columns_ref[g]
        value = weight_ref[g]
        row = lax.broadcasted_iota(jnp.int32, (1, entries), 1) // each
        key = jnp.where(column >= 0, (column // 128) * 8 + row, -1)
        low_part = jnp.where(column >= 0, lax.rem(column, 128), -1)
        left = jnp.where(
            key == lax.broadcasted_iota(jnp.int32, (high * 8, entries), 0), value, 0.0
        )
        right = jnp.where(
            low_part == lax.broadcasted_iota(jnp.int32, (128, entries), 0), 1.0, 0.0
        ).astype(jnp.bfloat16)
        first = left.astype(jnp.bfloat16)
        second = (left - first.astype(jnp.float32)).astype(jnp.bfloat16)
        dims = (((1,), (1,)), ((), ()))
        placed = lax.dot_general(first, right, dims, preferred_element_type=jnp.float32)
        placed = placed + lax.dot_general(second, right, dims, preferred_element_type=jnp.float32)
        at = pl.ds(pl.multiple_of(g * 8, 8), 8)
        for h in range(high):
            out_ref[at, h * 128 : (h + 1) * 128] = placed[h * 8 : (h + 1) * 8]
        return carry

    lax.fori_loop(0, groups, body, 0)


def spread_entries(columns, values, width):
    rows, each = columns.shape
    return pl.pallas_call(
        spread_kernel,
        out_shape=jax.ShapeDtypeStruct((rows, width), jnp.float32),
        in_specs=[VMEM] * 2,
        out_specs=VMEM,
        name="spread_entries",
    )(columns.reshape(rows // 8, 1, 8 * each), values.reshape(rows // 8, 1, 8 * each))


def lower(values):
    return values.astype(jnp.bfloat16)


def product(left, right):
    return jnp.dot(left, right, preferred_element_type=jnp.float32)


def product_left(left, right):
    return lax.dot_general(left, right, (((0,), (0,)), ((), ())), preferred_element_type=jnp.float32)


def product_right(left, right):
    return lax.dot_general(left, right, (((1,), (1,)), ((), ())), preferred_element_type=jnp.float32)


def rms_forward(values, gain):
    inverse = lax.rsqrt(jnp.mean(values * values, axis=-1, keepdims=True) + eps_norm)
    normed = values * inverse
    return (normed * gain, normed, inverse)


def rms_backward(grad_out, normed, inverse, gain):
    grad_normed = grad_out * gain
    grad_in = inverse * (
        grad_normed - normed * jnp.mean(grad_normed * normed, axis=-1, keepdims=True)
    )
    return (grad_in, jnp.sum(grad_out * normed, axis=0))


def path_mask(parent_row, tree_len):
    seg_count = parent_row.shape[0]
    seglen = tree_len // seg_count
    seg_order = jnp.arange(seg_count, dtype=jnp.int32)
    parent_hot = ((parent_row[:, None] == seg_order[None, :]) & (seg_order[:, None] >= 1)).astype(
        jnp.float32
    )
    identity = jnp.eye(seg_count, dtype=jnp.float32)
    power, steps = parent_hot, 1
    reached = identity + parent_hot
    while steps < seg_count:
        reached = jnp.minimum(1.0, jnp.dot(reached, reached))
        steps *= 2
    strict = reached - identity
    seg_of = jnp.arange(tree_len, dtype=jnp.int32) // seglen
    seg_hot = (seg_of[:, None] == seg_order[None, :]).astype(jnp.float32)
    ancestor = jnp.dot(jnp.dot(seg_hot, strict), seg_hot.T)
    places = jnp.arange(tree_len, dtype=jnp.int32)
    inside = (seg_of[:, None] == seg_of[None, :]) & (places[None, :] <= places[:, None])
    return ancestor + inside.astype(jnp.float32)


def attention_scores(queries, keys_all, cumul):
    scale = queries.shape[-1] ** (-0.5)
    scores = (
        jnp.einsum("ihd,jhd->hij", queries, keys_all, preferred_element_type=jnp.float32) * scale
    )
    cumul_heads = cumul.T
    return scores + cumul_heads[:, :, None] - cumul_heads[:, None, :]


def layer_forward(values, allowed, weights):
    (
        weight_in,
        weight_out,
        weight_up,
        weight_down,
        forget_proj,
        forget_bias,
        gain_attention,
        gain_feedforward,
    ) = weights
    tree_len, width = values.shape
    head_count = forget_proj.shape[1]
    normed_out_a, normed_a, inverse_a = rms_forward(values, gain_attention)
    act_a = lower(normed_out_a)
    mixed = lower(product(act_a, weight_in))
    forget_logit = product(act_a, forget_proj) + forget_bias
    cumul = jnp.dot(allowed, jax.nn.log_sigmoid(forget_logit), precision=highest)
    parts = mixed.reshape(tree_len, 3, head_count, width // head_count)
    scores = attention_scores(parts[:, 0], parts[:, 1], cumul)
    scores = jnp.where(allowed[None] > 0, scores, masked_score)
    score_max = jnp.max(scores, axis=-1, keepdims=True)
    exp_scores = jnp.exp(scores - score_max)
    score_sum = jnp.sum(exp_scores, axis=-1, keepdims=True)
    probs = lower(exp_scores / score_sum)
    log_total = score_max + jnp.log(score_sum)
    attended = jnp.einsum("hij,jhd->ihd", probs, parts[:, 2], preferred_element_type=jnp.float32)
    attended = lower(attended.reshape(tree_len, width))
    middle = values + product(attended, weight_out)
    normed_out_b, normed_b, inverse_b = rms_forward(middle, gain_feedforward)
    act_b = lower(normed_out_b)
    gate_up = product(act_b, weight_up)
    half_width = gate_up.shape[1] // 2
    hidden = lower(jax.nn.silu(gate_up[:, :half_width]) * gate_up[:, half_width:])
    output = middle + product(hidden, weight_down)
    return (output, (values, mixed, forget_logit, log_total, attended, middle, gate_up))


def layer_backward(grad_out, allowed, saved, weights):
    (
        weight_in,
        weight_out,
        weight_up,
        weight_down,
        forget_proj,
        forget_bias,
        gain_attention,
        gain_feedforward,
    ) = weights
    values, mixed, forget_logit, log_total, attended, middle, gate_up = saved
    tree_len, width = values.shape
    head_count = forget_proj.shape[1]
    head_width = width // head_count
    half_width = gate_up.shape[1] // 2
    gate = gate_up[:, :half_width]
    upper = gate_up[:, half_width:]
    sigma = jax.nn.sigmoid(gate)
    silu_gate = gate * sigma
    hidden = lower(silu_gate * upper)
    normed_out_b, normed_b, inverse_b = rms_forward(middle, gain_feedforward)
    act_b = lower(normed_out_b)
    grad_branch = lower(grad_out)
    grad_down = lower(product_left(hidden, grad_branch))
    grad_hidden = product_right(grad_branch, weight_down)
    grad_gate = grad_hidden * upper * sigma * (1.0 + gate * (1.0 - sigma))
    grad_upper = grad_hidden * silu_gate
    grad_gate_up = lower(jnp.concatenate([grad_gate, grad_upper], axis=1))
    grad_up = lower(product_left(act_b, grad_gate_up))
    grad_norm_b, grad_gain_b = rms_backward(
        product_right(grad_gate_up, weight_up), normed_b, inverse_b, gain_feedforward
    )
    grad_middle = grad_out + grad_norm_b
    grad_attn_branch = lower(grad_middle)
    grad_out_weight = lower(product_left(attended, grad_attn_branch))
    grad_attended = lower(product_right(grad_attn_branch, weight_out)).reshape(
        tree_len, head_count, head_width
    )
    normed_out_a, normed_a, inverse_a = rms_forward(values, gain_attention)
    act_a = lower(normed_out_a)
    cumul = jnp.dot(allowed, jax.nn.log_sigmoid(forget_logit), precision=highest)
    parts = mixed.reshape(tree_len, 3, head_count, head_width)
    scale = head_width ** (-0.5)
    scores = attention_scores(parts[:, 0], parts[:, 1], cumul)
    scores = jnp.where(allowed[None] > 0, scores, masked_score)
    probs = jnp.exp(scores - log_total)
    grad_probs = jnp.einsum(
        "ihd,jhd->hij", grad_attended, parts[:, 2], preferred_element_type=jnp.float32
    )
    grad_values = jnp.einsum(
        "hij,ihd->jhd", lower(probs), grad_attended, preferred_element_type=jnp.float32
    )
    grad_scores = lower(probs * (grad_probs - jnp.sum(probs * grad_probs, axis=-1, keepdims=True)))
    grad_queries = (
        jnp.einsum("hij,jhd->ihd", grad_scores, parts[:, 1], preferred_element_type=jnp.float32)
        * scale
    )
    grad_keys = (
        jnp.einsum("hij,ihd->jhd", grad_scores, parts[:, 0], preferred_element_type=jnp.float32)
        * scale
    )
    grad_cumul = (
        jnp.sum(grad_scores, axis=2, dtype=jnp.float32)
        - jnp.sum(grad_scores, axis=1, dtype=jnp.float32)
    ).T
    grad_logit = lower(
        jnp.dot(allowed.T, grad_cumul, precision=highest) * jax.nn.sigmoid(-forget_logit)
    )
    grad_mixed = lower(
        jnp.stack([grad_queries, grad_keys, grad_values], axis=1).reshape(tree_len, 3 * width)
    )
    grad_in_weight = lower(product_left(act_a, grad_mixed))
    grad_forget = jnp.concatenate(
        [product_left(act_a, grad_logit), jnp.sum(grad_logit, axis=0, dtype=jnp.float32)[None]],
        axis=0,
    )
    grad_act_a = product_right(grad_mixed, weight_in) + product_right(grad_logit, forget_proj)
    grad_norm_a, grad_gain_a = rms_backward(grad_act_a, normed_a, inverse_a, gain_attention)
    grad_in = grad_middle + grad_norm_a
    return (
        grad_in,
        (grad_in_weight, grad_out_weight, grad_up, grad_down),
        grad_forget,
        jnp.stack([grad_gain_a, grad_gain_b]),
    )


def adam_step(weight, grad, first, second, clip_scale, correct_first, correct_second):
    scaled = clip_scale * grad
    first_new = beta_first * first + (1.0 - beta_first) * scaled
    second_new = beta_second * second + (1.0 - beta_second) * scaled * scaled
    direction = (
        first_new / correct_first / (jnp.sqrt(second_new / correct_second) + adam_eps)
        + decay_rate * weight
    )
    return (first_new, second_new, direction)


def square_sum(values):
    return jnp.sum(values * values)


def packed(parts):
    flat = jnp.concatenate([p.reshape(-1) for p in parts])
    rows = -(-flat.shape[0] // 1024) * 8
    return jnp.pad(flat, (0, rows * 128 - flat.shape[0])).reshape(rows, 128)


def unpacked(flat, like):
    flat, out, at = flat.reshape(-1), [], 0
    for p in like:
        out.append(flat[at : at + p.size].reshape(p.shape))
        at += p.size
    return out


def local(
    tokens,
    parents,
    loss_positions,
    targets,
    teacher_index,
    teacher_probability,
    step_count,
    embed_table,
    table_first,
    table_second,
    attention_in,
    attention_in_first,
    attention_in_second,
    attention_out,
    attention_out_first,
    attention_out_second,
    feedforward_in,
    feedforward_in_first,
    feedforward_in_second,
    feedforward_out,
    feedforward_out_first,
    feedforward_out_second,
    forget_gate,
    forget_first,
    forget_second,
    norm_gains,
    gains_first,
    gains_second,
):
    section_id = lax.axis_index("section")
    replica_id = lax.axis_index("replica")
    shard_id = lax.axis_index("shard")
    sections = lax.axis_size("section")
    replicas = lax.axis_size("replica")
    shards = lax.axis_size("shard")
    group_trees, tree_len = tokens.shape
    rows_each, width = embed_table.shape
    pos_count = loss_positions.shape[1]
    pos_all = group_trees * replicas * pos_count
    owners = replicas * shards
    owner_id = replica_id * shards + shard_id
    own_tree = section_id * shards + shard_id
    table_low = lower(embed_table)

    def own_row(values):
        return lax.dynamic_index_in_dim(values, own_tree, 0, keepdims=False)

    tree_tokens = own_row(tokens)
    token_owner = tree_tokens // rows_each
    token_row = tree_tokens % rows_each
    spots = jnp.arange(tree_len, dtype=jnp.int32)
    earlier = spots[None, :] < spots[:, None]
    same = tree_tokens[:, None] == tree_tokens[None, :]
    is_first = jnp.logical_not(jnp.any(same & earlier, axis=1))
    counted = earlier & (token_owner[:, None] == token_owner[None, :]) & is_first[None, :]
    number_first = jnp.sum(counted.astype(jnp.int32), axis=1)
    number = jnp.sum(jnp.where(same & is_first[None, :], number_first[None, :], 0), axis=1)
    most = jnp.max(number) + 1

    def asked(batch):
        slot = number - batch * batch_rows
        inside = (slot >= 0) & (slot < batch_rows)
        place = jnp.where(inside, token_owner * batch_rows + slot, -1)
        spot_of = jnp.arange(owners * batch_rows, dtype=jnp.int32)
        hot = place[None, :] == spot_of[:, None]
        rows = jnp.max(jnp.where(hot & is_first[None, :], token_row[None, :] + 1, 0), axis=1)
        return rows.reshape(owners, batch_rows), lower(hot)

    def all_devices(part, ident):
        if replicas != 2:
            out = part
            for axis in ("shard", "replica", "section"):
                out = lax.all_gather(out, axis)
            return out
        return jnp.swapaxes(gather([part], ident, space=VMEM)[0][0], 1, 2)

    def wanted(batch, ident):
        rows, hot = asked(batch)
        note = jnp.zeros((1, 128), jnp.int32) + most
        part = jnp.concatenate([jnp.pad(rows, ((0, 0), (0, 128 - batch_rows))), note], axis=0)
        part = jnp.pad(part, ((0, -part.shape[0] % 8), (0, 0)))
        every = all_devices(part, ident)
        mine = lax.dynamic_index_in_dim(every, owner_id, 3, keepdims=False)[..., :batch_rows]
        wish = mine.reshape(sections * owners * batch_rows) - 1
        row_of = jnp.arange(rows_each, dtype=jnp.int32)
        pick = lower(wish[:, None] == row_of[None, :])
        return hot, pick, jnp.max(every[:, :, :, owners, 0])

    def fetch(hot, pick, ident):
        own_pick = lax.dynamic_index_in_dim(
            pick.reshape(sections, owners * batch_rows, rows_each), section_id, 0, keepdims=False
        )
        sent = lower(product(own_pick, table_low)).reshape(owners, batch_rows, width)
        got = exchange(sent, ident)[0].reshape(owners * batch_rows, width)
        return product_left(hot, got)

    hot, pick, most_all = wanted(0, 0)
    batches = (most_all + batch_rows - 1) // batch_rows
    embeds = fetch(hot, pick, 1)

    def more_rows(state):
        batch, total_rows = state
        hot_more, pick_more, _ = wanted(batch, 0)
        return (batch + 1, total_rows + fetch(hot_more, pick_more, 1))

    _, embeds = lax.while_loop(lambda s: s[0] < batches, more_rows, (jnp.int32(1), embeds))

    def halves(weight):
        return lower(weight).reshape(2, weight.shape[1] // 2, weight.shape[2])

    layer_weights = (attention_in, attention_out, feedforward_in, feedforward_out)
    group_data = [targets, teacher_index.reshape(group_trees, -1), teacher_probability.reshape(group_trees, -1)]
    pair_parts = group_data if replicas == 2 else []
    gathered, group_all = gather([halves(w) for w in layer_weights], 2, pair_parts, split=True)
    if replicas != 2:
        group_all = [lax.all_gather(part, "replica") for part in group_data]
    forget_low = lower(forget_gate[:, :width])

    def weights_of(layer):
        mats = [g[layer].reshape(-1, g.shape[-1]) for g in gathered]
        return (
            *mats,
            forget_low[layer],
            forget_gate[layer, width],
            norm_gains[2 * layer],
            norm_gains[2 * layer + 1],
        )

    allowed = path_mask(own_row(parents), tree_len)
    out_0, saved_0 = layer_forward(embeds, allowed, weights_of(0))
    out_1, saved_1 = layer_forward(lower(out_0).astype(jnp.float32), allowed, weights_of(1))

    positions = own_row(loss_positions)
    position_hot = (positions[:, None] == spots[None, :]).astype(jnp.float32)
    picked = jnp.take(out_1, positions, axis=0)
    final_gain = norm_gains[4]
    head_out, head_normed, head_inverse = rms_forward(picked, final_gain)
    head_rows = jnp.swapaxes(all_devices(lower(head_out), 3), 0, 1).reshape(pos_all, width)

    flat = [part.reshape((replicas * group_trees * pos_count,) + (-1,) * (n > 0)) for n, part in enumerate(group_all)]
    target_all, index_all, prob_all = flat

    def owned(ids):
        column = ids - owner_id * rows_each
        return jnp.where((column >= 0) & (column < rows_each), column, -1)

    width_all = -(-rows_each // 128) * 128
    marks = spread_entries(owned(index_all), prob_all, width_all)[:, :rows_each]
    columns = jnp.arange(rows_each, dtype=jnp.int32)
    marks = marks + (owned(target_all)[:, None] == columns[None, :]).astype(jnp.float32)
    logits = product_right(head_rows, table_low)
    linear_part = jnp.sum(logits * marks)
    local_peak = jnp.max(logits, axis=1)
    local_total = jnp.sum(jnp.exp(logits - local_peak[:, None]), axis=1)
    stats = jnp.stack([local_peak, local_total]).reshape(2, -1, 128)
    if replicas == 2:
        stats_all = gather([stats], 4, orders=(("z", "y"), ("z", "y")), space=VMEM)[0][0]
    else:
        stats_all = lax.all_gather(lax.all_gather(stats, "replica"), "shard")
    stats_all = stats_all.reshape(owners, 2, pos_all)
    row_peak = jnp.max(stats_all[:, 0], axis=0)
    row_total = jnp.sum(stats_all[:, 1] * jnp.exp(stats_all[:, 0] - row_peak[None]), axis=0)
    log_norm = row_peak + jnp.log(row_total)
    prob_sum = jnp.sum(prob_all, axis=1)
    row_part = jnp.sum(log_norm * (1.0 + prob_sum) + jnp.sum(prob_all * jnp.log(prob_all), axis=1))
    grad_logits = lower(
        ((1.0 + prob_sum)[:, None] * jnp.exp(logits - log_norm[:, None]) - marks) / pos_all
    )
    own_rows = lax.dynamic_index_in_dim(
        grad_logits.reshape(replicas, sections, shards * pos_count, rows_each), section_id, 1, keepdims=False
    )
    grad_heads = lower(product(own_rows.reshape(-1, rows_each), table_low))
    grad_heads = exchange(grad_heads.reshape(owners, pos_count, width), 5)[0]
    grad_heads = jnp.sum(grad_heads.astype(jnp.float32), axis=0)
    head_table = product_left(grad_logits, head_rows)
    grad_picked, grad_final = rms_backward(grad_heads, head_normed, head_inverse, final_gain)
    grad_top = lax.dot_general(
        position_hot, grad_picked, (((0,), (0,)), ((), ())), precision=highest
    )

    grad_mid, grads_1, forget_1, gains_1 = layer_backward(grad_top, allowed, saved_1, weights_of(1))
    grad_low, grads_0, forget_0, gains_0 = layer_backward(
        lower(grad_mid).astype(jnp.float32), allowed, saved_0, weights_of(0)
    )
    embed_low = lower(grad_low)

    def deliver(hot, pick, ident):
        sent = lower(product(hot, embed_low)).reshape(owners, batch_rows, width)
        got = exchange(sent, ident, relay=True).reshape(sections * owners * batch_rows, width)
        return product_left(pick, got)

    embed_grad = deliver(hot, pick, 6)

    def more_grads(state):
        batch, total_rows = state
        hot_more, pick_more, _ = wanted(batch, 0)
        return (batch + 1, total_rows + deliver(hot_more, pick_more, 6))

    _, embed_grad = lax.while_loop(lambda s: s[0] < batches, more_grads, (jnp.int32(1), embed_grad))
    table_grad = embed_grad + head_table

    stacked = [
        jnp.stack([a, b]).reshape(sections, shards, 2, -1, a.shape[-1]) for a, b in zip(grads_0, grads_1)
    ]
    layer_grads = reduce_parts(stacked, 8)
    if replicas != 2:
        layer_grads = [lax.psum(g * jnp.bfloat16(0.5), "replica") for g in layer_grads]
    layer_grads = [
        g.astype(jnp.float32).reshape(w.shape) for g, w in zip(layer_grads, layer_weights)
    ]

    small = [
        jnp.zeros((8,), jnp.float32),
        jnp.stack([forget_0, forget_1]),
        jnp.concatenate([gains_0, gains_1, grad_final[None]], axis=0),
    ]
    first_section = section_id == 0
    first_replica = replica_id == 0
    square = jnp.where(first_section, square_sum(table_grad), 0.0) + jnp.where(
        first_replica, sum(square_sum(g) for g in layer_grads), 0.0
    )
    linear_once = jnp.where(first_section, linear_part, 0.0)
    small[0] = jnp.stack([square, linear_once] + [jnp.float32(0)] * 6)
    scalars, forget_total, gains_total = unpacked(total(packed(small), 15), small)
    loss_total = (row_part - scalars[1]) / pos_all
    grad_norm = jnp.sqrt(scalars[0] + square_sum(forget_total) + square_sum(gains_total))
    clip_scale = jnp.minimum(1.0, clip_factor / jnp.sqrt(jnp.float32(pos_all)) / grad_norm)
    count_float = step_count.astype(jnp.float32)
    correct_first = 1.0 - jnp.power(beta_first, count_float)
    correct_second = 1.0 - jnp.power(beta_second, count_float)
    adam = partial(
        adam_step, clip_scale=clip_scale, correct_first=correct_first, correct_second=correct_second
    )
    table_first_new, table_second_new, table_direction = adam(
        embed_table, table_grad, table_first, table_second
    )
    layer_firsts = (
        attention_in_first,
        attention_out_first,
        feedforward_in_first,
        feedforward_out_first,
    )
    layer_seconds = (
        attention_in_second,
        attention_out_second,
        feedforward_in_second,
        feedforward_out_second,
    )
    layer_steps = [
        adam(weight, grad, first, second)
        for weight, grad, first, second in zip(
            layer_weights, layer_grads, layer_firsts, layer_seconds
        )
    ]
    section_slot = (jnp.arange(sections, dtype=jnp.int32) == section_id).astype(jnp.float32)
    table_parts = jnp.where(
        first_section, jnp.stack([square_sum(embed_table), square_sum(table_direction)]), 0.0
    )
    layer_parts = jnp.stack(
        [
            jnp.stack([square_sum(weight), square_sum(stepped[2])])
            for weight, stepped in zip(layer_weights, layer_steps)
        ]
    )
    layer_parts = jnp.where(first_replica, layer_parts, 0.0)
    layer_spread = layer_parts[:, None, :] * section_slot[None, :, None]
    norm_parts = [table_parts, layer_spread]
    norm_totals = unpacked(total(packed(norm_parts), 16), norm_parts)
    table_norms = jnp.sqrt(norm_totals[0])
    layer_norms = jnp.sqrt(norm_totals[1])
    new_table = embed_table - learn_rate * (table_norms[0] / table_norms[1]) * table_direction
    mine = jnp.sum(layer_norms * section_slot[None, :, None], axis=1)
    new_layers = []
    for mat_index in range(4):
        ratio = mine[mat_index, 0] / mine[mat_index, 1]
        stepped = layer_steps[mat_index]
        new_layers.append(
            (layer_weights[mat_index] - learn_rate * ratio * stepped[2], stepped[0], stepped[1])
        )
    forget_first_new, forget_second_new, forget_direction = adam(
        forget_gate, forget_total, forget_first, forget_second
    )
    forget_weight_norm = jnp.sqrt(jnp.sum(forget_gate * forget_gate, axis=(1, 2)))
    forget_update_norm = jnp.sqrt(jnp.sum(forget_direction * forget_direction, axis=(1, 2)))
    new_forget = (
        forget_gate
        - learn_rate * (forget_weight_norm / forget_update_norm)[:, None, None] * forget_direction
    )
    gains_first_new, gains_second_new, gains_direction = adam(
        norm_gains, gains_total, gains_first, gains_second
    )
    gains_weight_norm = jnp.sqrt(jnp.sum(norm_gains * norm_gains, axis=1))
    gains_update_norm = jnp.sqrt(jnp.sum(gains_direction * gains_direction, axis=1))
    new_gains = (
        norm_gains - learn_rate * (gains_weight_norm / gains_update_norm)[:, None] * gains_direction
    )
    tensor_norms = jnp.concatenate(
        [
            table_norms[None],
            layer_norms.reshape(4 * sections, 2),
            jnp.stack([forget_weight_norm, forget_update_norm], axis=1),
            jnp.stack([gains_weight_norm, gains_update_norm], axis=1),
        ],
        axis=0,
    )
    return (
        new_table,
        table_first_new,
        table_second_new,
        *new_layers[0],
        *new_layers[1],
        *new_layers[2],
        *new_layers[3],
        new_forget,
        forget_first_new,
        forget_second_new,
        new_gains,
        gains_first_new,
        gains_second_new,
        tensor_norms,
        grad_norm,
        loss_total,
    )


def solution(mesh):
    group = P("replica", None)
    table = P(("replica", "shard"), None)
    layer = P("section", "shard", None)
    in_specs = (
        (group,) * 4
        + (P("replica", None, None),) * 2
        + (P(),)
        + (table,) * 3
        + (layer,) * 12
        + (P(),) * 6
    )
    out_specs = (table,) * 3 + (layer,) * 12 + (P(),) * 9
    return jax.shard_map(local, mesh=mesh, in_specs=in_specs, out_specs=out_specs, check_vma=False)
```

```python
from functools import partial

import jax
import jax.numpy as jnp
from jax import lax
from jax.experimental import pallas as pl
from jax.experimental.pallas import tpu as pltpu
from jax.sharding import PartitionSpec as P

MESH = pl.DeviceIdType.MESH
VMEM = pl.BlockSpec(memory_space=pltpu.VMEM)
ANY = pl.BlockSpec(memory_space=pl.ANY)
DMA = pltpu.SemaphoreType.DMA
eps_norm = 1e-06
beta_first = 0.9
beta_second = 0.999
adam_eps = 1e-10
decay_rate = 0.01
learn_rate = 0.2
clip_factor = 8.0
highest = lax.Precision.HIGHEST
masked_score = -1e30
batch_rows = 32
every_axis = ("section", "replica", "shard")


class Place:
    def __init__(self):
        self.sections = lax.axis_size("section")
        self.replicas = lax.axis_size("replica")
        self.shards = lax.axis_size("shard")
        self.nz = min(4, self.shards)
        self.ny = self.shards // self.nz
        self.x = lax.axis_index("section")
        self.rep = lax.axis_index("replica")
        self.shard = lax.axis_index("shard")
        self.core = lax.rem(self.rep, 2)
        self.z = self.shard // self.ny
        self.y = lax.rem(self.shard, self.ny)

    def at(self, section=None, rep=None, z=None, y=None, shard=None):
        if shard is None:
            shard = (self.z if z is None else z) * self.ny + (self.y if y is None else y)
        return {
            "section": self.x if section is None else section,
            "replica": self.rep if rep is None else rep,
            "shard": shard,
        }

    def peer_x(self, i):
        return self.at(section=lax.rem(self.x + i, self.sections))

    def peer_y(self, j):
        return self.at(y=lax.rem(self.y + j, self.ny))

    def line(self, step):
        return self.at(z=self.z + step)

    def partner(self):
        return self.at(rep=self.rep + 1 - 2 * self.core)

    def group(self, p):
        count = self.replicas * self.shards
        place = lax.rem(self.rep * self.shards + self.shard + p, count)
        return place, self.at(rep=place // self.shards, shard=lax.rem(place, self.shards))

    def device(self, i, p):
        place, _ = self.group(p)
        section = lax.rem(self.x + i, self.sections)
        return place, self.at(section=section, rep=place // self.shards, shard=lax.rem(place, self.shards))

    def greet_all(self):
        barrier = pltpu.get_barrier_semaphore()
        peers = self.replicas * self.shards
        for i in range(self.sections):
            for p in range(peers):
                if i or p:
                    pl.semaphore_signal(barrier, inc=1, device_id=self.device(i, p)[1], device_id_type=MESH)
        pl.semaphore_wait(barrier, self.sections * peers - 1)

    def greet_group(self):
        barrier = pltpu.get_barrier_semaphore()
        peers = self.replicas * self.shards
        for p in range(1, peers):
            pl.semaphore_signal(barrier, inc=1, device_id=self.group(p)[1], device_id_type=MESH)
        for i in range(1, self.sections):
            pl.semaphore_signal(barrier, inc=1, device_id=self.peer_x(i), device_id_type=MESH)
        pl.semaphore_wait(barrier, peers + self.sections - 2)

    def inside(self, k):
        if k == 0:
            return None
        return self.z + k < self.nz if k > 0 else self.z + k >= 0

    def greet(self, use_x=True):
        barrier = pltpu.get_barrier_semaphore()

        def signal(device):
            pl.semaphore_signal(barrier, inc=1, device_id=device, device_id_type=MESH)

        count = 1
        if use_x:
            for i in range(1, self.sections):
                signal(self.peer_x(i))
                count += 1
        for j in range(1, self.ny):
            signal(self.peer_y(j))
            count += 1
        signal(self.partner())
        up, down = self.inside(1), self.inside(-1)
        pl.when(up)(lambda: signal(self.line(1)))
        pl.when(down)(lambda: signal(self.line(-1)))
        ends = jnp.minimum(self.z, 1) + jnp.minimum(self.nz - 1 - self.z, 1)
        pl.semaphore_wait(barrier, count + ends)


def when(cond, fn):
    if cond is None:
        fn()
    else:
        pl.when(cond)(fn)


def both(a, b):
    if a is None:
        return b
    if b is None:
        return a
    return jnp.logical_and(a, b)


def remote(src, dst, send, recv, device):
    return pltpu.make_async_remote_copy(
        src_ref=src, dst_ref=dst, send_sem=send, recv_sem=recv, device_id=device, device_id_type=MESH
    )


def rows_errand(me, ask_ref, table_ref, asked_ref, got_ref, hot, found, ask_sem, row_sem, own_sem):
    peers = me.replicas * me.shards
    mine = me.rep * me.shards + me.shard
    width = table_ref.shape[1]
    asks = []
    for i in range(me.sections):
        for p in range(peers):
            place, device = me.device(i, p)
            if i or p:
                asks.append(remote(ask_ref.at[place], asked_ref.at[me.x, mine], ask_sem.at[0, i, p], ask_sem.at[1, i, p], device))
    for copy in asks:
        copy.start()
    own_ask = pltpu.make_async_copy(ask_ref.at[mine], asked_ref.at[me.x, mine], own_sem.at[0])
    own_ask.start()
    rows = [
        remote(found.at[me.group(p)[0]], got_ref.at[mine], row_sem.at[0, p], row_sem.at[1, p], me.group(p)[1])
        for p in range(1, peers)
    ]
    own_rows = pltpu.make_async_copy(found.at[mine], got_ref.at[mine], own_sem.at[1])

    def look_up():
        own_ask.wait()
        for i in range(me.sections):
            for p in range(peers):
                if i or p:
                    source = lax.rem(mine + peers - p, peers)
                    dst = asked_ref.at[lax.rem(me.x + me.sections - i, me.sections), source]
                    remote(dst, dst, ask_sem.at[0, i, p], ask_sem.at[1, i, p], me.partner()).wait_recv()
        wish = asked_ref[me.x].reshape(peers, 128).astype(jnp.float32).T
        column = lax.broadcasted_iota(jnp.int32, (batch_rows, table_ref.shape[0]), 1).astype(jnp.float32) + 1.0
        for s in range(peers):
            ours = wish[0:batch_rows, s : s + 1] == column
            hot[s * batch_rows : (s + 1) * batch_rows, :] = jnp.where(ours, 1.0, 0.0).astype(jnp.bfloat16)

        def take(n, carry):
            at = pl.ds(pl.multiple_of(n * 256, 256), 256)
            values = jnp.dot(hot[...], table_ref[:, at], preferred_element_type=jnp.float32)
            found[:, :, at] = values.reshape(peers, batch_rows, 256).astype(jnp.bfloat16)
            return carry

        lax.fori_loop(0, width // 256, take, 0)
        own_rows.start()
        for copy in rows:
            copy.start()

    def finish():
        for p in range(1, peers):
            source = lax.rem(mine + peers - p, peers)
            dst = got_ref.at[source]
            remote(dst, dst, row_sem.at[0, p], row_sem.at[1, p], me.partner()).wait_recv()
        own_rows.wait()
        for copy in asks + rows:
            copy.wait_send()

    return {1: look_up, "end": finish}


def gather_kernel(count, pairs, split, orders, errand, *refs):
    ins, refs = refs[:count], refs[count:]
    pair_ins, refs = refs[:pairs], refs[pairs:]
    errand_in, refs = refs[: 2 * errand], refs[2 * errand :]
    outs, refs = refs[:count], refs[count:]
    pair_outs, refs = refs[:pairs], refs[pairs:]
    errand_out, refs = refs[: 2 * errand], refs[2 * errand :]
    errand_refs = errand_in + errand_out
    send_sem, recv_sem, cross_sem, pair_sem, local_sem = refs[:5]
    me = Place()
    nz, ny, nx = me.nz, me.ny, me.sections
    if "x" not in orders[0][0][0]:
        nx = 1
    hooks = {}
    if errand:
        me.greet_all()
        hooks = rows_errand(me, *errand_refs, *refs[5:])
    else:
        me.greet(use_x=nx > 1)

    def slot(ref, k, j, i, half):
        section = lax.rem(me.x + i, nx) if nx > 1 else 0
        return ref.at[section, (me.z + k) * ny + lax.rem(me.y + j, ny), half]

    locals_ = []
    for a in range(count):
        if split:
            dst = outs[a].at[me.x if nx > 1 else 0, me.shard]
        else:
            dst = outs[a].at[me.x if nx > 1 else 0, me.shard, me.core]
        locals_.append(pltpu.make_async_copy(ins[a], dst, local_sem.at[a]))
    for p in range(pairs):
        locals_.append(
            pltpu.make_async_copy(pair_ins[p], pair_outs[p].at[me.core], local_sem.at[count + p])
        )
    for copy in locals_:
        copy.start()
    pair_copies = [
        remote(pair_ins[p], pair_outs[p].at[me.core], pair_sem.at[0, p], pair_sem.at[1, p], me.partner())
        for p in range(pairs)
    ]

    def run(core, plan):
        sends = []

        def push(cond, src, dst, device, sem):
            copy = remote(src, dst, send_sem.at[len(sends)], sem, device)
            when(cond, copy.start)
            sends.append((cond, copy))

        def sem_of(a, k, j, i):
            return recv_sem.at[a, k + nz - 1, j, i]

        def spread(order, arrays, k, j, i, via):
            cond = me.inside(k)
            own = via is None
            later = order if own else order[order.index(via) + 1 :]
            for a in arrays:
                dst = slot(outs[a], k, j, i, core)
                src = dst
                if own:
                    src = ins[a].at[core] if split else ins[a]
                else:
                    arrival = remote(dst, dst, send_sem.at[0], sem_of(a, k, j, i), me.partner())
                    when(cond, arrival.wait_recv)
                steps = []
                if via == "z":
                    steps = [-1 if k > 0 else 1]
                elif "z" in later:
                    steps = [1, -1]
                for step in steps:
                    push(both(cond, me.inside(step)), src, dst, me.line(step), sem_of(a, k - step, j, i))
                if "y" in later:
                    for p in range(1, ny):
                        push(cond, src, dst, me.peer_y(p), sem_of(a, k, (j - p) % ny, i))
                if "x" in later:
                    for p in range(1, nx):
                        push(cond, src, dst, me.peer_x(p), sem_of(a, k, j, (i - p) % nx))
                if not (own and split):
                    push(cond, src, dst, me.partner(), cross_sem.at[a, k + nz - 1, j, i])

        events = []
        for order, arrays in plan:
            for k in range(1 - nz, nz):
                for j in range(ny):
                    for i in range(nx):
                        via = [d for d in order if {"z": k, "y": j, "x": i}[d] != 0]
                        hops = abs(k) + (j != 0) + (i != 0)
                        stage = order.index(via[-1]) if via else -1
                        events.append((hops, stage, k, j, i, order, arrays, via[-1] if via else None))
        events.sort(key=lambda e: e[:5])
        for n, (hops, stage, k, j, i, order, arrays, via) in enumerate(events):
            spread(order, arrays, k, j, i, via)
            if n + 1 < len(events) and events[n + 1][0] == hops:
                continue
            if hops == 0:
                for copy in pair_copies:
                    copy.start()
            if hops in hooks:
                hooks[hops]()
        for hops, stage, k, j, i, order, arrays, via in events:
            if via is None and split:
                continue
            for a in arrays:
                dst = slot(outs[a], k, j, i, 1 - core)
                arrival = remote(dst, dst, send_sem.at[0], cross_sem.at[a, k + nz - 1, j, i], me.partner())
                when(me.inside(k), arrival.wait_recv)
        for cond, copy in sends:
            when(cond, copy.wait_send)

    for core, plan in enumerate(orders):
        pl.when(me.core == core)(partial(run, core, plan))
    if errand:
        hooks["end"]()
    for p in range(pairs):
        pair_copies[p].wait_send()
        remote(
            pair_ins[p], pair_outs[p].at[1 - me.core], pair_sem.at[0, p], pair_sem.at[1, p], me.partner()
        ).wait_recv()
    for copy in locals_:
        copy.wait()


def gather(parts, ident, pair_parts=(), split=False, use_x=True, space=ANY, errand=()):
    count, pairs = len(parts), len(pair_parts)
    every = list(range(count))
    if not use_x:
        orders = [[(("z", "y"), every)]] * 2
    elif split:
        orders = [[(("z", "y", "x"), every)], [(("x", "z", "y"), every[:-1]), (("x", "y", "z"), every[-1:])]]
    else:
        orders = [[(("z", "y", "x"), every)], [(("x", "z", "y"), every)]]
    shards = lax.axis_size("shard")
    nx = lax.axis_size("section") if use_x else 1
    nz = min(4, shards)
    ny = shards // nz
    lead = (nx, shards) if split else (nx, shards, 2)
    blocks = (2 * nz - 1) * ny * nx
    errand_shapes, errand_scratch = [], []
    if errand:
        asks, table = errand
        peers, wide = asks.shape[0], table.shape[1]
        errand_shapes = [
            jax.ShapeDtypeStruct((nx, peers) + asks.shape[1:], asks.dtype),
            jax.ShapeDtypeStruct((peers, batch_rows, wide), table.dtype),
        ]
        errand_scratch = [
            pltpu.VMEM((peers * batch_rows, table.shape[0]), table.dtype),
            pltpu.VMEM((peers, batch_rows, wide), table.dtype),
            DMA((2, nx, peers)),
            DMA((2, peers)),
            DMA((2,)),
        ]
    outs = pl.pallas_call(
        partial(gather_kernel, count, pairs, split, orders, bool(errand)),
        out_shape=[jax.ShapeDtypeStruct(lead + p.shape, p.dtype) for p in parts]
        + [jax.ShapeDtypeStruct((2,) + p.shape, p.dtype) for p in pair_parts]
        + errand_shapes,
        in_specs=[VMEM] * (count + pairs + len(errand)),
        out_specs=[space] * (count + pairs) + [VMEM] * len(errand_shapes),
        scratch_shapes=[
            DMA((blocks * count * 4,)),
            DMA((count, 2 * nz - 1, ny, nx)),
            DMA((count, 2 * nz - 1, ny, nx)),
            DMA((2, max(pairs, 1))),
            DMA((count + pairs,)),
        ]
        + errand_scratch,
        compiler_params=pltpu.CompilerParams(collective_id=ident, has_side_effects=True),
        name=f"gather_{ident}",
    )(*parts, *pair_parts, *errand)
    return outs[:count], outs[count : count + pairs], outs[count + pairs :]


def exchange_kernel(relay, src_ref, out_ref, send_sem, recv_sem, relay_send, relay_recv, local_sem):
    me = Place()
    peers = me.replicas * me.shards
    barrier = pltpu.get_barrier_semaphore()
    for p in range(1, peers):
        pl.semaphore_signal(barrier, inc=1, device_id=me.group(p)[1], device_id_type=MESH)
    if relay:
        for i in range(1, me.sections):
            pl.semaphore_signal(barrier, inc=1, device_id=me.peer_x(i), device_id_type=MESH)
    pl.semaphore_wait(barrier, peers - 1 + (me.sections - 1 if relay else 0))
    mine = me.rep * me.shards + me.shard
    section = me.x if relay else 0
    own = pltpu.make_async_copy(
        src_ref.at[mine if src_ref.shape[0] > 1 else 0], out_ref.at[section, mine], local_sem.at[0]
    )
    own.start()
    sends = []
    for p in range(1, peers):
        place, device = me.group(p)
        copy = remote(
            src_ref.at[place if src_ref.shape[0] > 1 else 0], out_ref.at[section, mine], send_sem.at[p], recv_sem.at[p], device
        )
        copy.start()
        sends.append(copy)
    relays = []

    def forward(p, src, dst):
        for i in range(1, me.sections):
            copy = remote(src, dst, relay_send.at[p, i], relay_recv.at[p, i], me.peer_x(i))
            copy.start()
            relays.append(copy)

    if relay:
        forward(0, src_ref.at[mine], out_ref.at[me.x, mine])
    for p in range(1, peers):
        source, device = me.group(peers - p)
        dst = out_ref.at[section, source]
        remote(dst, dst, send_sem.at[p], recv_sem.at[p], device).wait_recv()
        if relay:
            forward(p, dst, dst)
    if relay:
        for p in range(peers):
            source, _ = me.group(peers - p)
            for i in range(1, me.sections):
                dst = out_ref.at[lax.rem(me.x + me.sections - i, me.sections), source]
                remote(dst, dst, relay_send.at[p, i], relay_recv.at[p, i], me.peer_x(i)).wait_recv()
    for copy in sends + relays:
        copy.wait_send()
    own.wait()


def exchange(blocks, ident, relay=False):
    peers = lax.axis_size("replica") * lax.axis_size("shard")
    nx = lax.axis_size("section")
    return pl.pallas_call(
        partial(exchange_kernel, relay),
        out_shape=jax.ShapeDtypeStruct((nx if relay else 1, peers) + blocks.shape[1:], blocks.dtype),
        in_specs=[VMEM],
        out_specs=VMEM,
        scratch_shapes=[DMA((peers,)), DMA((peers,)), DMA((peers, nx)), DMA((peers, nx)), DMA((1,))],
        compiler_params=pltpu.CompilerParams(collective_id=ident, has_side_effects=True),
        name=f"exchange_{ident}",
    )(blocks)


def total_steps(me):
    steps = []
    for axis, size in (("replica", me.replicas), ("section", me.sections), ("shard", me.shards)):
        bit = 1
        while bit < size:
            steps.append((axis, bit))
            bit *= 2
    return steps


def total_kernel(count, *refs):
    ins, refs = refs[:count], refs[count:]
    outs, refs = refs[:count], refs[count:]
    held, refs = refs[:count], refs[count:]
    send_sem, recv_sem = refs
    me = Place()
    steps = total_steps(me)
    position = {"section": me.x, "replica": me.rep, "shard": me.shard}

    def other(axis, bit):
        index = position[axis]
        return {**position, axis: index + bit - 2 * bit * lax.rem(index // bit, 2)}

    barrier = pltpu.get_barrier_semaphore()
    for axis, bit in steps:
        pl.semaphore_signal(barrier, inc=1, device_id=other(axis, bit), device_id_type=MESH)
    pl.semaphore_wait(barrier, len(steps))
    for a in range(count):
        held[a][0] = ins[a][...]
    copies = []
    for n, (axis, bit) in enumerate(steps):
        step_copies = [
            remote(held[a].at[2 * n], held[a].at[2 * n + 1], send_sem.at[n, a], recv_sem.at[n, a], other(axis, bit))
            for a in range(count)
        ]
        for copy in step_copies:
            copy.start()
        copies += step_copies
        for a in range(count):
            step_copies[a].wait_recv()
            summed = held[a][2 * n] + held[a][2 * n + 1]
            if n + 1 < len(steps):
                held[a][2 * n + 2] = summed
            else:
                outs[a][...] = summed
    for copy in copies:
        copy.wait_send()


def total(values, ident):
    count = len(values)
    steps = sum((lax.axis_size(axis) - 1).bit_length() for axis in every_axis)
    return pl.pallas_call(
        partial(total_kernel, count),
        out_shape=[jax.ShapeDtypeStruct(v.shape, v.dtype) for v in values],
        in_specs=[VMEM] * count,
        out_specs=[VMEM] * count,
        scratch_shapes=[pltpu.VMEM((2 * steps,) + v.shape, v.dtype) for v in values]
        + [DMA((steps, count)), DMA((steps, count))],
        compiler_params=pltpu.CompilerParams(collective_id=ident, has_side_effects=True),
        name=f"total_{ident}",
    )(*values)


def add_rows(dst, src):
    rows = dst.shape[0]
    if rows % 16 != 0:
        dst[...] = (dst[...].astype(jnp.float32) + src[...].astype(jnp.float32)).astype(dst.dtype)
        return
    step = 16

    def body(n, carry):
        at = pl.ds(pl.multiple_of(n * step, step), step)
        dst[at, :] = (dst[at, :].astype(jnp.float32) + src[at, :].astype(jnp.float32)).astype(dst.dtype)
        return carry

    lax.fori_loop(0, rows // step, body, 0)


def grads_errand(me, sent, got, sum_in, sum_out, *refs):
    n_sums = len(sum_in)
    held, refs = refs[:n_sums], refs[n_sums:]
    row_sem, relay_sem, own_sem, sum_sem = refs
    peers = me.replicas * me.shards
    mine = me.rep * me.shards + me.shard
    direct = [
        remote(sent.at[me.group(p)[0]], got.at[me.x, mine], row_sem.at[0, p], row_sem.at[1, p], me.group(p)[1])
        for p in range(1, peers)
    ]
    own = pltpu.make_async_copy(sent.at[mine], got.at[me.x, mine], own_sem.at[0])
    relays = []

    def source(p):
        return lax.rem(mine + peers - p, peers)

    def begin():
        own.start()
        for copy in direct:
            copy.start()
        for i in range(1, me.sections):
            copy = remote(sent.at[mine], got.at[me.x, mine], relay_sem.at[0, 0, i], relay_sem.at[1, 0, i], me.peer_x(i))
            copy.start()
            relays.append(copy)

    steps = total_steps(me)
    position = {"section": me.x, "replica": me.rep, "shard": me.shard}

    def other(axis, bit):
        index = position[axis]
        return {**position, axis: index + bit - 2 * bit * lax.rem(index // bit, 2)}

    def sum_copies(n):
        axis, bit = steps[n]
        return [
            remote(held[a].at[2 * n], held[a].at[2 * n + 1], sum_sem.at[0, n, a], sum_sem.at[1, n, a], other(axis, bit))
            for a in range(n_sums)
        ]

    def sum_step(n):
        if n == 0:
            for a in range(n_sums):
                held[a][0] = sum_in[a][...]
        else:
            for a, copy in enumerate(sum_copies(n - 1)):
                copy.wait_recv()
                summed = held[a][2 * n - 2] + held[a][2 * n - 1]
                if n < len(steps):
                    held[a][2 * n] = summed
                else:
                    sum_out[a][...] = summed
        if n < len(steps):
            for copy in sum_copies(n):
                copy.start()

    def relay(first, last):
        for p in range(first, last):
            dst = got.at[me.x, source(p)]
            remote(dst, dst, row_sem.at[0, p], row_sem.at[1, p], me.partner()).wait_recv()
            for i in range(1, me.sections):
                copy = remote(dst, dst, relay_sem.at[0, p, i], relay_sem.at[1, p, i], me.peer_x(i))
                copy.start()
                relays.append(copy)

    def finish():
        for p in range(peers):
            for i in range(1, me.sections):
                dst = got.at[lax.rem(me.x + me.sections - i, me.sections), source(p)]
                remote(dst, dst, relay_sem.at[0, p, i], relay_sem.at[1, p, i], me.partner()).wait_recv()
        for p in range(peers):
            for i in range(1, me.sections):
                dst = got.at[me.x, source(p)]
                remote(dst, dst, relay_sem.at[0, p, i], relay_sem.at[1, p, i], me.peer_x(i)).wait_send()
        for copy in direct:
            copy.wait_send()
        for n in range(len(steps)):
            for copy in sum_copies(n):
                copy.wait_send()
        own.wait()

    hooks = [begin, partial(sum_step, 0)]
    middle = (peers + 1) // 2
    pieces = [partial(relay, 1, middle), partial(relay, middle, peers)]
    sums = [partial(sum_step, n) for n in range(1, len(steps) + 1)]
    hooks += [sums[0], pieces[0], sums[1], pieces[1]] + sums[2:] + [finish]
    return hooks


def reduce_kernel(count, sections, sums, *refs):
    ins, refs = [refs[a * sections : (a + 1) * sections] for a in range(count)], refs[count * sections :]
    sum_in, refs = refs[:sums], refs[sums:]
    sent = None
    if sums:
        sent, refs = refs[0], refs[1:]
    outs, refs = refs[:count], refs[count:]
    sum_out, refs = refs[:sums], refs[sums:]
    if sums:
        got, refs = refs[0], refs[1:]
    acc, refs = refs[:count], refs[count:]
    from_core, refs = refs[:count], refs[count:]
    from_x, refs = refs[:count], refs[count:]
    from_y, refs = refs[:count], refs[count:]
    from_z, refs = refs[:count], refs[count:]
    load_sem, core_send, core_recv, send_sem, x_recv, y_recv, z_recv, last_sem = refs[:8]
    me = Place()
    nz, ny, nx = me.nz, me.ny, me.sections
    hooks = []
    if sums:
        me.greet_group()
        hooks = grads_errand(me, sent, got, sum_in, sum_out, *refs[8 : 8 + sums], *refs[8 + sums :])
    else:
        me.greet()

    far = sorted((k for k in range(1 - nz, nz)), key=lambda k: -abs(k))

    def block(k, j, i):
        return lax.rem(me.x + i, nx), (me.z + k) * ny + lax.rem(me.y + j, ny)

    def order_of(core):
        if core == 0:
            return [(k, j, i) for i in range(nx - 1, -1, -1) for j in range(ny - 1, -1, -1) for k in far]
        return [(k, j, i) for j in range(ny - 1, -1, -1) for k in far for i in range(nx - 1, -1, -1)]

    def run(core):
        other = 1 - core
        sends = []

        def start_core(k, j, i):
            x, s = block(k, j, i)

            def go(layer):
                for a in range(count):
                    remote(
                        ins[a][layer].at[s, other], from_core[a].at[x, s], core_send.at[a, x, s],
                        core_recv.at[a, x, s], me.partner(),
                    ).start()

            for layer in range(nx):
                when(both(me.inside(k), x == layer), partial(go, layer))

        def start_load(k, j, i):
            x, s = block(k, j, i)

            def go(layer):
                for a in range(count):
                    pltpu.make_async_copy(ins[a][layer].at[s, core], acc[a].at[x, s], load_sem.at[a, x, s]).start()

            for layer in range(nx):
                when(both(me.inside(k), x == layer), partial(go, layer))

        for b in order_of(other):
            start_core(*b)
        for b in order_of(core):
            start_load(*b)
        todo = list(hooks)

        def errand(last=False):
            while todo and (last or len(todo) > 1):
                todo.pop(0)()
                if not last:
                    break

        errand()

        def push(cond, src, dst, sem, device):
            copy = remote(src, dst, send_sem.at[len(sends)], sem, device)
            when(cond, copy.start)
            sends.append((cond, copy))

        def take(cond, dst, src, sem):
            def go():
                remote(src, src, core_send.at[0, 0, 0], sem, me.partner()).wait_recv()
                add_rows(dst, src)

            when(cond, go)

        def join_core(a, k, j, i):
            x, s = block(k, j, i)

            def go():
                pltpu.make_async_copy(ins[a][0].at[s, core], acc[a].at[x, s], load_sem.at[a, x, s]).wait()

            when(me.inside(k), go)
            take(me.inside(k), acc[a].at[x, s], from_core[a].at[x, s], core_recv.at[a, x, s])

        def join_x(a, k, j):
            x, s = block(k, j, 0)
            for p in range(1, nx):
                take(me.inside(k), acc[a].at[x, s], from_x[a].at[p - 1, s], x_recv.at[a, p - 1, s])

        def join_y(a, k, i):
            x, s = block(k, 0, i)
            for p in range(1, ny):
                take(me.inside(k), acc[a].at[x, s], from_y[a].at[p - 1, x, me.z + k], y_recv.at[a, p - 1, x, me.z + k])

        def join_z(a, k, i):
            x, s = block(k, 0, i)
            if k >= 0:
                take(both(me.inside(k), me.inside(-1)), acc[a].at[x, s], from_z[a].at[x, me.z + k], z_recv.at[a, x, me.z + k])
            if k <= 0:
                place = nz if k == 0 else me.z + k
                take(both(me.inside(k), me.inside(1)), acc[a].at[x, s], from_z[a].at[x, place], z_recv.at[a, x, place])

        def send_x(a, k, j, i):
            x, s = block(k, j, i)
            push(me.inside(k), acc[a].at[x, s], from_x[a].at[i - 1, s], x_recv.at[a, i - 1, s], me.peer_x(i))

        def send_y(a, k, j, i):
            x, s = block(k, j, i)
            push(
                me.inside(k), acc[a].at[x, s], from_y[a].at[j - 1, x, me.z + k],
                y_recv.at[a, j - 1, x, me.z + k], me.peer_y(j),
            )

        def send_z(a, k, i):
            x, s = block(k, 0, i)
            place = nz if k == -1 else me.z + k
            push(
                me.inside(k), acc[a].at[x, s], from_z[a].at[x, place], z_recv.at[a, x, place],
                me.line(1 if k > 0 else -1),
            )

        each = range(count)
        if core == 0:
            for i in range(nx - 1, 0, -1):
                for j in range(ny - 1, -1, -1):
                    for k in far:
                        for a in each:
                            join_core(a, k, j, i)
                            send_x(a, k, j, i)
                        errand()
            for j in range(ny - 1, -1, -1):
                for k in far:
                    for a in each:
                        join_core(a, k, j, 0)
            for j in range(ny - 1, 0, -1):
                for k in far:
                    for a in each:
                        join_x(a, k, j)
                        send_y(a, k, j, 0)
            for k in far:
                for a in each:
                    join_x(a, k, 0)
                    join_y(a, k, 0)
                    join_z(a, k, 0)
                    if k != 0:
                        send_z(a, k, 0)
        else:
            for j in range(ny - 1, 0, -1):
                for k in far:
                    for i in range(nx - 1, -1, -1):
                        for a in each:
                            join_core(a, k, j, i)
                            send_y(a, k, j, i)
                        errand()
            for k in far:
                for i in range(nx - 1, -1, -1):
                    for a in each:
                        join_core(a, k, 0, i)
            for k in far:
                for i in range(nx - 1, -1, -1):
                    for a in each:
                        join_y(a, k, i)
                        join_z(a, k, i)
                        if k != 0:
                            send_z(a, k, i)
                        elif i != 0:
                            send_x(a, 0, 0, i)
                        else:
                            join_x(a, 0, 0)
        errand(last=True)
        finals = []
        for a in each:
            copy = remote(
                acc[a].at[me.x, me.shard], outs[a].at[core], last_sem.at[0, a], last_sem.at[1, a], me.partner()
            )
            copy.start()
            finals.append(copy)
            outs[a][core] = acc[a][me.x, me.shard]
        for a in each:
            remote(outs[a].at[other], outs[a].at[other], last_sem.at[0, a], last_sem.at[1, a], me.partner()).wait_recv()
        for cond, copy in sends:
            when(cond, copy.wait_send)
        for copy in finals:
            copy.wait_send()
        for k, j, i in order_of(other):
            x, s = block(k, j, i)

            def finish():
                for a in each:
                    remote(
                        ins[a][0].at[s, other], from_core[a].at[x, s], core_send.at[a, x, s],
                        core_recv.at[a, x, s], me.partner(),
                    ).wait_send()

            when(me.inside(k), finish)

    pl.when(me.core == 0)(lambda: run(0))
    pl.when(me.core == 1)(lambda: run(1))


def reduce_shards(grads, ident, errand=None):
    count = len(grads)
    nx, shards = lax.axis_size("section"), lax.axis_size("shard")
    nz = min(4, shards)
    ny = shards // nz
    blocks = (2 * nz - 1) * ny * nx

    def scratch(lead):
        return [pltpu.VMEM(lead + g[0].shape[2:], g[0].dtype) for g in grads]

    extra_in, extra_shapes, extra_scratch, sums = [], [], [], 0
    if errand:
        values, sent = errand
        sums, peers = len(values), sent.shape[0]
        steps = sum((lax.axis_size(axis) - 1).bit_length() for axis in every_axis)
        extra_in = [*values, sent]
        extra_shapes = [jax.ShapeDtypeStruct(v.shape, v.dtype) for v in values] + [
            jax.ShapeDtypeStruct((nx,) + sent.shape, sent.dtype)
        ]
        extra_scratch = [pltpu.VMEM((2 * steps,) + v.shape, v.dtype) for v in values] + [
            DMA((2, peers)),
            DMA((2, peers, nx)),
            DMA((1,)),
            DMA((2, steps, sums)),
        ]
    return pl.pallas_call(
        partial(reduce_kernel, count, nx, sums),
        out_shape=[jax.ShapeDtypeStruct(g[0].shape[1:], g[0].dtype) for g in grads] + extra_shapes,
        in_specs=[ANY] * (count * nx) + [VMEM] * sums + [ANY] * bool(sums),
        out_specs=[VMEM] * (count + sums) + [ANY] * bool(sums),
        scratch_shapes=scratch((nx, shards))
        + scratch((nx, shards))
        + scratch((max(nx - 1, 1), shards))
        + scratch((max(ny - 1, 1), nx, nz))
        + scratch((nx, nz + 1))
        + [
            DMA((count, nx, shards)),
            DMA((count, nx, shards)),
            DMA((count, nx, shards)),
            DMA((blocks * count * 2,)),
            DMA((count, max(nx - 1, 1), shards)),
            DMA((count, max(ny - 1, 1), nx, nz)),
            DMA((count, nx, nz + 1)),
            DMA((2, count)),
        ]
        + extra_scratch,
        compiler_params=pltpu.CompilerParams(
            collective_id=ident, has_side_effects=True, vmem_limit_bytes=67043328
        ),
        name=f"reduce_{ident}",
    )(*[layer for g in grads for layer in g], *extra_in)


def reduce_parts(grads, ident, errand):
    nx, shards = lax.axis_size("section"), lax.axis_size("shard")
    ny = shards // min(4, shards)
    slots = 2 * nx * shards + (nx - 1) * shards + (ny - 1) * nx * 4 + nx * 5 + 4
    groups, used = [[]], 0
    for n, grad in enumerate(grads):
        rows, columns = grad[0].shape[2:]
        size = slots * (-(-rows // 16) * 16) * columns * 2
        if used + size > 58 * 2**20 and groups[-1]:
            groups.append([])
            used = 0
        groups[-1].append(n)
        used += size
    out = [None] * len(grads)
    for g, group in enumerate(groups):
        done = reduce_shards([grads[n] for n in group], ident + g, errand if g == 0 else None)
        for n, value in zip(group, done):
            out[n] = value
        if g == 0:
            extra = done[len(group) :]
    return out, extra


def spread_kernel(columns_ref, weight_ref, target_ref, out_ref):
    groups, entries = columns_ref.shape[0], columns_ref.shape[2]
    high = out_ref.shape[1] // 128
    each = entries // 8

    def body(g, carry):
        column = columns_ref[g]
        value = weight_ref[g]
        row = lax.broadcasted_iota(jnp.int32, (1, entries), 1) // each
        key = jnp.where(column >= 0, (column // 128) * 8 + row, -1)
        low_part = jnp.where(column >= 0, lax.rem(column, 128), -1)
        left = jnp.where(
            key == lax.broadcasted_iota(jnp.int32, (high * 8, entries), 0), value, 0.0
        ).astype(jnp.bfloat16)
        right = jnp.where(
            low_part == lax.broadcasted_iota(jnp.int32, (128, entries), 0), 1.0, 0.0
        ).astype(jnp.bfloat16)
        dims = (((1,), (1,)), ((), ()))
        placed = lax.dot_general(left, right, dims, preferred_element_type=jnp.float32)
        at = pl.ds(pl.multiple_of(g * 8, 8), 8)
        target = target_ref[at, :]
        for h in range(high):
            one = jnp.where(lax.broadcasted_iota(jnp.int32, (8, 128), 1) + 128 * h == target, 1.0, 0.0)
            out_ref[at, h * 128 : (h + 1) * 128] = placed[h * 8 : (h + 1) * 8] + one
        return carry

    lax.fori_loop(0, groups, body, 0)


def spread_entries(columns, values, targets, width):
    rows, each = columns.shape
    return pl.pallas_call(
        spread_kernel,
        out_shape=jax.ShapeDtypeStruct((rows, width), jnp.float32),
        in_specs=[VMEM] * 3,
        out_specs=VMEM,
        name="spread_entries",
    )(columns.reshape(rows // 8, 1, 8 * each), values.reshape(rows // 8, 1, 8 * each), targets[:, None])


def ask_kernel(owners, token_row, token_col, owner_row, owner_col, row_col, hot_ref, ask_ref):
    count = token_row.shape[1]
    i = lax.broadcasted_iota(jnp.int32, (count, count), 0)
    j = lax.broadcasted_iota(jnp.int32, (count, count), 1)
    same = token_col[...] == token_row[...]
    kin = owner_col[...] == owner_row[...]
    first_col = 1.0 - jnp.max(jnp.where(same & (j < i), 1.0, 0.0), axis=1, keepdims=True)
    first_row = 1.0 - jnp.max(jnp.where(same & (i < j), 1.0, 0.0), axis=0, keepdims=True)
    place_col = jnp.sum(jnp.where(kin & (j < i), first_row, 0.0), axis=1, keepdims=True)
    place_row = jnp.sum(jnp.where(kin & (i < j), first_col, 0.0), axis=0, keepdims=True)
    number_col = jnp.sum(jnp.where(same, first_row * place_row, 0.0), axis=1, keepdims=True)
    number_row = jnp.sum(jnp.where(same, first_col * place_col, 0.0), axis=0, keepdims=True)
    size = float(batch_rows)
    slot_row = jnp.where(number_row < size, owner_row[...].astype(jnp.float32) * size + number_row, -1.0)
    slot_col = jnp.where(number_col < size, owner_col[...].astype(jnp.float32) * size + number_col, -1.0)
    spots = owners * batch_rows
    part = 512 if spots % 512 == 0 else spots
    for at in range(0, spots, part):
        line = lax.broadcasted_iota(jnp.int32, (part, count), 0).astype(jnp.float32) + float(at)
        hot_ref[at : at + part, :] = jnp.where(slot_row == line, 1.0, 0.0).astype(jnp.bfloat16)
    most = jnp.max(number_col) + 1.0
    wanted = first_col * (row_col[...].astype(jnp.float32) + 1.0)
    lane = lax.broadcasted_iota(jnp.int32, (1, 128), 1)
    for at in range(0, spots, 128):
        line = lax.broadcasted_iota(jnp.int32, (count, 128), 1).astype(jnp.float32) + float(at)
        rows = jnp.max(jnp.where(slot_col == line, wanted, 0.0), axis=0, keepdims=True)
        for n in range(128 // batch_rows):
            shifted = pltpu.roll(rows, (128 - n * batch_rows) % 128, 1) if n else rows
            values = jnp.where(lane < batch_rows, shifted, jnp.where(lane == 127, most, 0.0))
            ask_ref[at // batch_rows + n] = values.astype(jnp.int32)


def ask_rows(tokens, owner, row, owners):
    count = tokens.shape[0]
    return pl.pallas_call(
        partial(ask_kernel, owners),
        out_shape=[
            jax.ShapeDtypeStruct((owners * batch_rows, count), jnp.bfloat16),
            jax.ShapeDtypeStruct((owners, 1, 128), jnp.int32),
        ],
        in_specs=[VMEM] * 5,
        out_specs=[VMEM] * 2,
        name="ask_rows",
    )(tokens[None], tokens[:, None], owner[None], owner[:, None], row[:, None])


def table_kernel(asked_ref, got_ref, head_ref, *refs):
    layers, table_ref, square_ref = refs[:-2], refs[-2], refs[-1]
    sections, peers = asked_ref.shape[:2]
    each = 128 // batch_rows
    lane = lax.broadcasted_iota(jnp.int32, (1, 128), 1)
    lists = []
    for at in range(0, sections * peers, each):
        wish = jnp.zeros((1, 128), jnp.int32)
        for n in range(each):
            part = asked_ref[(at + n) // peers, (at + n) % peers]
            part = pltpu.roll(part, n * batch_rows, 1) if n else part
            wish = jnp.where((lane >= n * batch_rows) & (lane < (n + 1) * batch_rows), part, wish)
        lists.append(wish)
    wish = jnp.concatenate(lists, axis=1)
    rows = table_ref.shape[0]
    step = 400 if rows % 400 == 0 else rows

    def body(n, square):
        at = pl.ds(pl.multiple_of(n * step, 8), step) if step != rows else slice(0, rows)
        row = lax.broadcasted_iota(jnp.int32, (step, wish.shape[1]), 0) + 1 + n * step
        hot = jnp.where(row == wish, 1.0, 0.0).astype(jnp.bfloat16)
        values = head_ref[at, :] + jnp.dot(hot, got_ref[...], preferred_element_type=jnp.float32)
        table_ref[at, :] = values
        return square + jnp.sum(values * values, axis=0, keepdims=True)

    zero = jnp.zeros((1, table_ref.shape[1]), jnp.float32)
    square = jnp.sum(lax.fori_loop(0, rows // step, body, zero)) if step != rows else jnp.sum(body(0, zero))
    square = jnp.where(lax.axis_index("section") == 0, square, 0.0)
    others = jnp.float32(0)
    for layer in layers:
        for half in range(2):
            values = layer[half].astype(jnp.float32)
            others = others + jnp.sum(values * values)
    square = square + jnp.where(lax.axis_index("replica") == 0, others, 0.0)
    corner = lax.broadcasted_iota(jnp.int32, (8, 128), 0) + lax.broadcasted_iota(jnp.int32, (8, 128), 1)
    square_ref[...] = jnp.where(corner == 0, square, 0.0)


def table_gradient(rows_each, asked, got, head_table, layer_grads):
    width = head_table.shape[1]
    return pl.pallas_call(
        table_kernel,
        out_shape=[
            jax.ShapeDtypeStruct((rows_each, width), jnp.float32),
            jax.ShapeDtypeStruct((8, 128), jnp.float32),
        ],
        in_specs=[VMEM] * (3 + len(layer_grads)),
        out_specs=[VMEM] * 2,
        compiler_params=pltpu.CompilerParams(vmem_limit_bytes=56 * 2**20),
        name="table_gradient",
    )(asked, got, head_table, *layer_grads)
def dims_nt(left, right):
    return lax.dot_general(left, right, (((1,), (1,)), ((), ())), preferred_element_type=jnp.float32)


def dims_tn(left, right):
    return lax.dot_general(left, right, (((0,), (0,)), ((), ())), preferred_element_type=jnp.float32)


def three_parts(values):
    first = lower(values)
    rest = values - first.astype(jnp.float32)
    second = lower(rest)
    return first, second, lower(rest - second.astype(jnp.float32))


def log_sigmoid(values):
    return jnp.minimum(values, 0.0) - jnp.log1p(jnp.exp(-jnp.abs(values)))


def norm_parts(values, gain):
    inverse = lax.rsqrt(jnp.mean(values * values, axis=-1, keepdims=True) + eps_norm)
    normed = values * inverse
    return normed, inverse, lower(normed * gain)


class HeadPair:
    def __init__(self, tree_len, cumul):
        self.lane = lax.broadcasted_iota(jnp.int32, (tree_len, 128), 1)
        self.parts = jnp.concatenate(three_parts(cumul), axis=1)
        self.row = lax.broadcasted_iota(jnp.int32, (384, 128), 0)
        self.column = lax.broadcasted_iota(jnp.int32, (384, 128), 1)

    def augmented(self, head, side, query, key):
        start = 64 - 64 * side
        mine = (self.lane >= 64 * side) & (self.lane < 64 * side + 64)
        wanted = (self.row - 128 * (self.row // 128) == head) & (self.column == self.row // 128 + start)
        placed = product(self.parts, lower(jnp.where(wanted, 1.0, 0.0)))
        wanted = (self.row - 128 * (self.row // 128) == head) & (self.column == self.row // 128 + start + 3)
        negative = product(self.parts, lower(jnp.where(wanted, -1.0, 0.0)))
        ones_q = jnp.where((self.lane >= start + 3) & (self.lane < start + 6), 1.0, 0.0)
        ones_k = jnp.where((self.lane >= start) & (self.lane < start + 3), 1.0, 0.0)
        query = lower(jnp.where(mine, query.astype(jnp.float32) * 0.125, placed + ones_q))
        key = lower(jnp.where(mine, key.astype(jnp.float32), negative + ones_k))
        return query, key, mine


def forward_kernel(layer, round_input, x_ref, allowed_ref, w_in, w_out, w_up, w_down, forget_ref, bias_ref, gain_ref,
                   y_ref, qkv_ref, logit_ref, lse_ref, att_ref, mid_ref, gu_ref,
                   b_in, b_out, b_up, b_down, gu_buf, hidden, mask, sem, gu_sem):
    tree_len, width = x_ref.shape
    heads = width // 64
    half = hidden.shape[1]
    loads = [
        pltpu.make_async_copy(src.at[layer], dst, sem.at[n])
        for n, (src, dst) in enumerate(((w_in, b_in), (w_out, b_out), (w_up, b_up), (w_down, b_down)))
    ]
    for copy in loads:
        copy.start()
    x = x_ref[...]
    if round_input:
        x = lower(x).astype(jnp.float32)
    _, _, act = norm_parts(x, gain_ref[0:1, :])
    allowed = allowed_ref[...]
    mask[...] = jnp.where(allowed > 0, 0.0, masked_score)
    logit = product(act, forget_ref[...]) + bias_ref[...]
    logit_ref[...] = logit
    cumul = sum(product(allowed, part) for part in three_parts(log_sigmoid(logit)))
    loads[0].wait()

    def project(n, carry):
        at = pl.ds(pl.multiple_of(n * 256, 256), 256)
        qkv_ref[:, at] = lower(product(act, b_in[:, at]))
        return carry

    lax.fori_loop(0, 3 * width // 256, project, 0)
    pair = HeadPair(tree_len, cumul)
    lse_ref[...] = jnp.zeros_like(lse_ref)

    def attend(p, carry):
        base = pl.multiple_of(p * 128, 128)
        query = qkv_ref[:, pl.ds(base, 128)]
        key = qkv_ref[:, pl.ds(base + width, 128)]
        value = qkv_ref[:, pl.ds(base + 2 * width, 128)]
        outs = []
        for side in range(2):
            q_side, k_side, mine = pair.augmented(2 * p + side, side, query, key)
            scores = dims_nt(q_side, k_side) + mask[...]
            peak = jnp.max(scores, axis=1, keepdims=True)
            probs = jnp.exp(scores - peak)
            count = jnp.sum(probs, axis=1, keepdims=True)
            outs.append(product(lower(probs * (1.0 / count)), value))
            lse_ref[...] = jnp.where(pair.lane == 2 * p + side, peak + jnp.log(count), lse_ref[...])
        att_ref[:, pl.ds(base, 128)] = lower(jnp.where(pair.lane < 64, outs[0], outs[1]))
        return carry

    lax.fori_loop(0, heads // 2, attend, 0)
    loads[1].wait()
    middle = x + product(att_ref[...], b_out[...])
    mid_ref[...] = middle
    _, _, act_b = norm_parts(middle, gain_ref[1:2, :])
    loads[2].wait()

    def stores(n):
        return [
            pltpu.make_async_copy(
                gu_buf.at[:, pl.ds(n * 512 + s * half, 512)], gu_ref.at[:, pl.ds(n * 512 + s * half, 512)], gu_sem.at[n, s]
            )
            for s in range(2)
        ]

    for n in range(half // 512):
        def expand(h, carry):
            at = pl.ds(pl.multiple_of(n * 512 + h * 256, 256), 256)
            at_up = pl.ds(pl.multiple_of(half + n * 512 + h * 256, 256), 256)
            gate = product(act_b, b_up[:, at])
            upper = product(act_b, b_up[:, at_up])
            gu_buf[:, at] = gate
            gu_buf[:, at_up] = upper
            hidden[:, at] = lower(gate / (1.0 + jnp.exp(-gate)) * upper)
            return carry

        lax.fori_loop(0, 2, expand, 0)
        for copy in stores(n):
            copy.start()
    loads[3].wait()

    def contract(n, carry):
        at = pl.ds(pl.multiple_of(n * 256, 256), 256)
        y_ref[:, at] = mid_ref[:, at] + product(hidden[...], b_down[:, at])
        return carry

    lax.fori_loop(0, width // 256, contract, 0)
    for n in range(half // 512):
        for copy in stores(n):
            copy.wait()


def layer_forward(layer, round_input, values, allowed, mats, forget_w, forget_b, gains):
    tree_len, width = values.shape
    w_in, w_out, w_up, w_down = mats
    half = w_down.shape[1]
    f32, b16 = jnp.float32, jnp.bfloat16
    shape = jax.ShapeDtypeStruct
    return pl.pallas_call(
        partial(forward_kernel, layer, round_input),
        out_shape=[
            shape((tree_len, width), f32),
            shape((tree_len, 3 * width), b16),
            shape((tree_len, 128), f32),
            shape((tree_len, 128), f32),
            shape((tree_len, width), b16),
            shape((tree_len, width), f32),
            shape((tree_len, 2 * half), f32),
        ],
        in_specs=[VMEM] * 2 + [ANY] * 4 + [VMEM] * 3,
        out_specs=[VMEM] * 6 + [ANY],
        scratch_shapes=[pltpu.VMEM(w.shape[1:], b16) for w in mats]
        + [
            pltpu.VMEM((tree_len, 2 * half), f32),
            pltpu.VMEM((tree_len, half), b16),
            pltpu.VMEM((tree_len, tree_len), f32),
            DMA((4,)),
            DMA((half // 512, 2)),
        ],
        compiler_params=pltpu.CompilerParams(vmem_limit_bytes=56 * 2**20),
        name=f"forward_{layer}",
    )(values, allowed, *mats, forget_w, forget_b, gains)


def backward_kernel(layer, round_input, round_grad, dy_ref, x_ref, allowed_ref, qkv_ref, logit_ref, lse_ref, att_ref,
                    mid_ref, forget_ref, gain_ref, gu_hbm, w_in, w_out, w_up, w_down,
                    dx_ref, dforget_ref, dgain_ref, dw_in, dw_out, dw_up, dw_down,
                    b_in, b_out, b_up, b_down, gu, dqkv, act_t, grad_b, mask, dcum,
                    g_in, g_out, g_up, g_down, sem, gu_sem, store_sem):
    tree_len, width = x_ref.shape
    heads = width // 64
    half = b_down.shape[0]
    chunk = 256
    gu_loads = [
        [
            pltpu.make_async_copy(
                gu_hbm.at[:, pl.ds(n * chunk + s * half, chunk)], gu.at[:, pl.ds(n * chunk + s * half, chunk)], gu_sem.at[n, s]
            )
            for s in range(2)
        ]
        for n in range(half // chunk)
    ]
    loads = [
        pltpu.make_async_copy(src.at[layer], dst, sem.at[n])
        for n, (src, dst) in enumerate(((w_in, b_in), (w_out, b_out), (w_up, b_up), (w_down, b_down)))
    ]
    loads[3].start()
    for pair_copies in gu_loads:
        for copy in pair_copies:
            copy.start()
    for n in (2, 1, 0):
        loads[n].start()
    dy = dy_ref[...]
    if round_grad:
        dy = lower(dy).astype(jnp.float32)
    branch = lower(dy)
    normed_b, inverse_b, act_b = norm_parts(mid_ref[...], gain_ref[1:2, :])
    act_t[...] = lower((normed_b * gain_ref[1:2, :]).T)
    grad_b[...] = jnp.zeros_like(grad_b)
    loads[3].wait()
    for copies in gu_loads:
        for copy in copies:
            copy.wait()
    loads[2].wait()

    def feed(n, carry):
        at = pl.ds(pl.multiple_of(n * chunk, chunk), chunk)
        at_up = pl.ds(pl.multiple_of(half + n * chunk, chunk), chunk)
        gate, upper = gu[:, at], gu[:, at_up]
        sigma = 1.0 / (1.0 + jnp.exp(-gate))
        silu = gate * sigma
        hidden = lower(silu * upper)
        grad_hidden = dims_nt(branch, b_down[at, :])
        g_down[at, :] = lower(dims_tn(hidden, branch))
        grad_gate = lower(grad_hidden * upper * sigma * (1.0 + gate * (1.0 - sigma)))
        grad_upper = lower(grad_hidden * silu)
        g_up[:, at] = lower(product(act_t[...], grad_gate))
        g_up[:, at_up] = lower(product(act_t[...], grad_upper))
        grad_b[...] += dims_nt(grad_gate, b_up[:, at]) + dims_nt(grad_upper, b_up[:, at_up])
        return carry

    lax.fori_loop(0, half // chunk, feed, 0)
    stores = [
        pltpu.make_async_copy(src, dst, store_sem.at[n])
        for n, (src, dst) in enumerate(((g_down, dw_down), (g_up, dw_up), (g_out, dw_out), (g_in, dw_in)))
    ]
    stores[0].start()
    stores[1].start()

    def norm_backward(grad, normed, inverse, gain):
        grad_normed = grad * gain
        back = inverse * (grad_normed - normed * jnp.mean(grad_normed * normed, axis=-1, keepdims=True))
        return back, jnp.sum(grad * normed, axis=0, keepdims=True)

    back_b, dgain_b = norm_backward(grad_b[...], normed_b, inverse_b, gain_ref[1:2, :])
    grad_mid = dy + back_b
    branch_a = lower(grad_mid)
    g_out[...] = lower(dims_tn(att_ref[...], branch_a))
    stores[2].start()
    loads[1].wait()
    att_ref_grad = lower(dims_nt(branch_a, b_out[...]))
    x = x_ref[...]
    if round_input:
        x = lower(x).astype(jnp.float32)
    normed_a, inverse_a, act_a = norm_parts(x, gain_ref[0:1, :])
    act_t[...] = lower((normed_a * gain_ref[0:1, :]).T)
    allowed = allowed_ref[...]
    mask[...] = jnp.where(allowed > 0, 0.0, masked_score)
    logit = logit_ref[...]
    cumul = sum(product(allowed, part) for part in three_parts(log_sigmoid(logit)))
    pair = HeadPair(tree_len, cumul)
    dcum[...] = jnp.zeros_like(dcum)
    grad_att = grad_b
    grad_att[...] = att_ref_grad.astype(jnp.float32)

    def attend(p, carry):
        base = pl.multiple_of(p * 128, 128)
        query = qkv_ref[:, pl.ds(base, 128)]
        key = qkv_ref[:, pl.ds(base + width, 128)]
        value = qkv_ref[:, pl.ds(base + 2 * width, 128)]
        grad_out = grad_att[:, pl.ds(base, 128)]
        grad_low = lower(grad_out)
        results = []
        for side in range(2):
            head = 2 * p + side
            start = 64 - 64 * side
            q_side, k_side, mine = pair.augmented(head, side, query, key)
            lse = jnp.sum(jnp.where(pair.lane == head, lse_ref[...], 0.0), axis=1, keepdims=True)
            probs = jnp.exp(dims_nt(q_side, k_side) + (mask[...] - lse))
            grad_probs = dims_nt(lower(jnp.where(mine, grad_out, 0.0)), value)
            weighted = probs * grad_probs
            row = jnp.sum(weighted, axis=1, keepdims=True)
            grad_scores = lower(weighted - probs * row)
            grad_value = dims_tn(lower(probs), grad_low)
            grad_query = product(grad_scores, k_side)
            grad_key = dims_tn(grad_scores, q_side)
            taken = jnp.sum(
                jnp.where(pair.lane == start, grad_query, 0.0) - jnp.where(pair.lane == start + 3, grad_key, 0.0),
                axis=1, keepdims=True,
            )
            dcum[...] = jnp.where(pair.lane == head, taken, dcum[...])
            results.append((grad_query * 0.125, grad_key, grad_value))
        for part in range(3):
            merged = jnp.where(pair.lane < 64, results[0][part], results[1][part])
            dqkv[:, pl.ds(base + part * width, 128)] = lower(merged)
        return carry

    lax.fori_loop(0, heads // 2, attend, 0)
    rising = sum(dims_tn(allowed, part) for part in three_parts(dcum[...]))
    grad_logit = rising / (1.0 + jnp.exp(logit))
    lane = lax.broadcasted_iota(jnp.int32, grad_logit.shape, 1)
    grad_logit = lower(jnp.where(lane < heads, grad_logit, 0.0))
    dforget_ref[0:128, :] = dims_tn(grad_logit, act_a)
    bias = jnp.sum(grad_logit.astype(jnp.float32), axis=0, keepdims=True)
    dforget_ref[128:136, :] = jnp.concatenate(
        [jnp.broadcast_to(bias, (8, 128)), jnp.zeros((8, width - 128), jnp.float32)], axis=1
    )

    def weigh(n, carry):
        at = pl.ds(pl.multiple_of(n * 256, 256), 256)
        g_in[:, at] = lower(product(act_t[...], dqkv[:, at]))
        return carry

    lax.fori_loop(0, 3 * width // 256, weigh, 0)
    stores[3].start()
    loads[0].wait()
    grad_b[...] = dims_nt(grad_logit, forget_ref[...])

    def gather_back(n, carry):
        at = pl.ds(pl.multiple_of(n * 256, 256), 256)
        grad_b[...] += dims_nt(dqkv[:, at], b_in[:, at])
        return carry

    lax.fori_loop(0, 3 * width // 256, gather_back, 0)
    back_a, dgain_a = norm_backward(grad_b[...], normed_a, inverse_a, gain_ref[0:1, :])
    dx_ref[...] = grad_mid + back_a
    dgain_ref[...] = jnp.concatenate([dgain_a, dgain_b, jnp.zeros((6, width), jnp.float32)], axis=0)
    for copy in stores:
        copy.wait()


def layer_backward(layer, round_input, round_grad, grad, values, allowed, saved, mats, forget_w, gains):
    tree_len, width = values.shape
    qkv, logit, lse, att, middle, gate_up = saved
    w_in, w_out, w_up, w_down = mats
    half = w_down.shape[1]
    f32, b16 = jnp.float32, jnp.bfloat16
    shape = jax.ShapeDtypeStruct
    return pl.pallas_call(
        partial(backward_kernel, layer, round_input, round_grad),
        out_shape=[
            shape((tree_len, width), f32),
            shape((136, width), f32),
            shape((8, width), f32),
        ]
        + [shape(w.shape[1:], b16) for w in mats],
        in_specs=[VMEM] * 10 + [ANY] * 5,
        out_specs=[VMEM] * 3 + [ANY] * 4,
        scratch_shapes=[pltpu.VMEM(w.shape[1:], b16) for w in mats]
        + [
            pltpu.VMEM((tree_len, 2 * half), f32),
            pltpu.VMEM((tree_len, 3 * width), b16),
            pltpu.VMEM((width, tree_len), b16),
            pltpu.VMEM((tree_len, width), f32),
            pltpu.VMEM((tree_len, tree_len), f32),
            pltpu.VMEM((tree_len, 128), f32),
        ]
        + [pltpu.VMEM(w.shape[1:], b16) for w in mats]
        + [DMA((4,)), DMA((half // 256, 2)), DMA((4,))],
        compiler_params=pltpu.CompilerParams(vmem_limit_bytes=60 * 2**20),
        name=f"backward_{layer}",
    )(grad, values, allowed, qkv, logit, lse, att, middle, forget_w, gains, gate_up, *mats)
def head_forward_kernel(rows_each, z_ref, table_ref, marks_ref, logits_ref, stats_ref):
    rows = z_ref.shape[0]
    chunk = 256 if table_ref.shape[0] % 256 == 0 else 128
    z = z_ref[...]

    def body(n, carry):
        peak, count, linear = carry
        at = pl.ds(pl.multiple_of(n * chunk, chunk), chunk)
        logits = dims_nt(z, table_ref[at, :])
        column = lax.broadcasted_iota(jnp.int32, (rows, chunk), 1) + n * chunk
        linear = linear + jnp.sum(logits * marks_ref[:, at], axis=1, keepdims=True)
        logits = jnp.where(column < rows_each, logits, masked_score)
        logits_ref[:, at] = logits
        new_peak = jnp.maximum(peak, jnp.max(logits, axis=1, keepdims=True))
        count = count * jnp.exp(peak - new_peak) + jnp.sum(jnp.exp(logits - new_peak), axis=1, keepdims=True)
        return new_peak, count, linear

    start = jnp.full((rows, 1), masked_score, jnp.float32)
    zero = jnp.zeros((rows, 1), jnp.float32)
    peak, count, linear = lax.fori_loop(0, table_ref.shape[0] // chunk, body, (start, zero, zero))
    lane = lax.broadcasted_iota(jnp.int32, (rows, 128), 1)
    stats = jnp.where(lane == 0, peak, jnp.where(lane == 1, count, jnp.where(lane == 2, linear, 0.0)))
    stats_ref[...] = stats.T[0:4, :]


def head_forward(rows_each, z, table, marks):
    rows, width = z.shape[0], table.shape[0]
    return pl.pallas_call(
        partial(head_forward_kernel, rows_each),
        out_shape=[jax.ShapeDtypeStruct((rows, width), jnp.float32), jax.ShapeDtypeStruct((4, rows), jnp.float32)],
        in_specs=[VMEM] * 3,
        out_specs=[VMEM] * 2,
        name="head_forward",
    )(z, table, marks)


def head_backward_kernel(sections, span, pos_all, z_ref, table_ref, marks_ref, logits_ref, stats_ref,
                         prob_ref, dz_ref, dtable_ref, row_ref, grads):
    rows, width = logits_ref.shape
    peak = jnp.max(stats_ref[:, 0, :], axis=0, keepdims=True)
    count = jnp.sum(stats_ref[:, 1, :] * jnp.exp(stats_ref[:, 0, :] - peak), axis=0, keepdims=True)
    log_norm = peak + jnp.log(count)
    prob = prob_ref[...]
    prob_sum = jnp.sum(prob, axis=1, keepdims=True)
    entropy = jnp.sum(prob * jnp.log(prob), axis=1, keepdims=True)
    log_norm = jnp.broadcast_to(log_norm, (128, rows)).T[:, 0:1]
    whole = jnp.sum(log_norm * (1.0 + prob_sum) + entropy) - jnp.sum(stats_ref[:, 2, :])
    row_ref[...] = jnp.full((8, 128), whole)
    chunk = 256 if width % 256 == 0 else 128
    weight = 1.0 + prob_sum

    def body(n, carry):
        at = pl.ds(pl.multiple_of(n * chunk, chunk), chunk)
        grad = (weight * jnp.exp(logits_ref[:, at] - log_norm) - marks_ref[:, at]) * (1.0 / pos_all)
        grads[:, at] = lower(grad)
        dtable_ref[at, :] = dims_tn(lower(grad), z_ref[...])
        return carry

    lax.fori_loop(0, width // chunk, body, 0)
    section = lax.axis_index("section")
    for r in range(rows // (sections * span)):
        at = pl.ds(pl.multiple_of((r * sections + section) * span, span), span)
        dz_ref[r * span : (r + 1) * span, :] = lower(product(grads[at, :], table_ref[...]))


def head_backward(z, table, marks, logits, stats_all, prob, span, pos_all):
    rows, width = logits.shape
    sections = lax.axis_size("section")
    return pl.pallas_call(
        partial(head_backward_kernel, sections, span, pos_all),
        out_shape=[
            jax.ShapeDtypeStruct((rows // sections, z.shape[1]), jnp.bfloat16),
            jax.ShapeDtypeStruct((width, z.shape[1]), jnp.float32),
            jax.ShapeDtypeStruct((8, 128), jnp.float32),
        ],
        in_specs=[VMEM] * 6,
        out_specs=[VMEM] * 3,
        scratch_shapes=[pltpu.VMEM((rows, width), jnp.bfloat16)],
        name="head_backward",
    )(z, table, marks, logits, stats_all, prob)
def pieces_of(rows):
    part = 400 if rows % 400 == 0 else rows
    return [(at, part) for at in range(0, rows, part)]


def each_tile(rows, columns, fn, carry):
    step = 16
    wide = 256 if columns % 256 == 0 else columns

    def body(n, carry):
        at = pl.ds(pl.multiple_of(n * step, step), step)
        for c in range(0, columns, wide):
            carry = fn(at, slice(c, c + wide), carry)
        return carry

    carry = lax.fori_loop(0, rows // step, body, carry)
    if rows % step:
        at = slice(rows // step * step, rows)
        tail = [jnp.zeros((rows % step, wide), jnp.float32)] * 2
        for c in range(0, columns, wide):
            tail = fn(at, slice(c, c + wide), tail)
        carry = [carry[0], carry[1]] + [jnp.sum(t) for t in tail]
    return carry


def step_kernel(shapes, scalar_ref, sums_ref, forget_sum_ref, gains_sum_ref, *refs):
    n = len(shapes)
    small_in, refs = refs[:6], refs[6:]
    grads, refs = refs[:n], refs[n:]
    weights, refs = refs[:n], refs[n:]
    firsts, refs = refs[:n], refs[n:]
    seconds, refs = refs[:n], refs[n:]
    out_first, refs = refs[:n], refs[n:]
    out_second, refs = refs[:n], refs[n:]
    out_dir, refs = refs[:n], refs[n:]
    small_out, refs = refs[:6], refs[6:]
    norm_ref, small_norm_ref, refs = refs[0], refs[1], refs[2:]
    g_buf, refs = refs[:n], refs[n:]
    w_buf, refs = refs[:n], refs[n:]
    m_buf, refs = refs[:n], refs[n:]
    v_buf, refs = refs[:n], refs[n:]
    d_buf, refs = refs[:n], refs[n:]
    load_sem, store_sem = refs
    work = []
    for a in range(n):
        for at, part in pieces_of(shapes[a][0]):
            rows = pl.ds(at, part)
            p = len(work)
            loads = [
                pltpu.make_async_copy(src.at[rows], dst.at[rows], load_sem.at[p, q])
                for q, (src, dst) in enumerate(
                    ((grads[a], g_buf[a]), (weights[a], w_buf[a]), (firsts[a], m_buf[a]), (seconds[a], v_buf[a]))
                )
            ]
            stores = [
                pltpu.make_async_copy(src.at[rows], dst.at[rows], store_sem.at[p, q])
                for q, (src, dst) in enumerate(
                    ((m_buf[a], out_first[a]), (v_buf[a], out_second[a]), (d_buf[a], out_dir[a]))
                )
            ]
            work.append((a, at, part, loads, stores))
    for _, _, _, loads, _ in work:
        for copy in loads:
            copy.start()
    lane = lax.broadcasted_iota(jnp.int32, (8, 128), 1)
    row = lax.broadcasted_iota(jnp.int32, (8, 128), 0)

    def scalar_at(values, r, c):
        return jnp.sum(jnp.where((row == r) & (lane == c), values, 0.0))

    forget_sum, gains_sum = forget_sum_ref[...], gains_sum_ref[...]
    norm = jnp.sqrt(
        jnp.full((1, 1), scalar_at(sums_ref[...], 0, 0) + square_sum(forget_sum) + square_sum(gains_sum))
    )
    clip = jnp.minimum(1.0, scalar_ref[2] / norm)
    inverse_first = scalar_ref[0]
    inverse_second = scalar_ref[1]

    def adam(weight, grad, first, second):
        scaled = clip * grad
        first_new = beta_first * first + (1.0 - beta_first) * scaled
        second_new = beta_second * second + (1.0 - beta_second) * scaled * scaled
        direction = (first_new * inverse_first) / (
            jnp.sqrt(second_new * inverse_second) + adam_eps
        ) + decay_rate * weight
        return first_new, second_new, direction

    small_norms = []
    for s, (grad, group) in enumerate(((forget_sum, scalar_heads(forget_sum)), (gains_sum, 1))):
        w_ref, m_ref, v_ref = small_in[3 * s : 3 * s + 3]
        weight = w_ref[...]
        first_new, second_new, direction = adam(weight, grad, m_ref[...], v_ref[...])
        w_norm = jnp.sum(weight * weight, axis=1, keepdims=True)
        d_norm = jnp.sum(direction * direction, axis=1, keepdims=True)
        rows = weight.shape[0]
        owner = lax.broadcasted_iota(jnp.int32, (rows, 1), 0) // group
        ratio = jnp.zeros((rows, 1), jnp.float32)
        for t in range(-(-rows // group)):
            ours = owner == t
            w_total = jnp.sqrt(jnp.full((1, 1), jnp.sum(jnp.where(ours, w_norm, 0.0))))
            d_total = jnp.sqrt(jnp.full((1, 1), jnp.sum(jnp.where(ours, d_norm, 0.0))))
            ratio = jnp.where(ours, w_total / d_total, ratio)
            small_norms += [w_total, d_total]
        small_out[3 * s][...] = weight - learn_rate * ratio * direction
        small_out[3 * s + 1][...] = first_new
        small_out[3 * s + 2][...] = second_new
    table = jnp.where((row == 0) & (lane == 0), norm, 0.0)
    for t, value in enumerate(small_norms):
        table = jnp.where((row == 1) & (lane == t), value, table)
    small_norm_ref[...] = table

    sums = [[jnp.float32(0), jnp.float32(0)] for _ in range(n)]
    for a, at, part, loads, stores in work:
        for copy in loads:
            copy.wait()
        g, w, m, v, d = (buf[a].at[pl.ds(at, part)] for buf in (g_buf, w_buf, m_buf, v_buf, d_buf))
        columns = shapes[a][1]
        wide = 256 if columns % 256 == 0 else columns

        def tile(rows, cols, carry):
            weight = w[rows, cols]
            first_new, second_new, direction = adam(
                weight, g[rows, cols].astype(jnp.float32), m[rows, cols], v[rows, cols]
            )
            m[rows, cols] = first_new
            v[rows, cols] = second_new
            d[rows, cols] = direction
            return [carry[0] + weight * weight, carry[1] + direction * direction]

        zero = jnp.zeros((16, wide), jnp.float32)
        done = each_tile(part, columns, tile, [zero, zero])
        for copy in stores:
            copy.start()
        for q in range(2):
            sums[a][q] = sums[a][q] + jnp.sum(done[q])
            if len(done) > 2:
                sums[a][q] = sums[a][q] + done[2 + q]
    section = lax.axis_index("section")
    table = jnp.zeros((8, 128), jnp.float32)
    for a in range(n):
        here = (section if a == 0 else lax.axis_index("replica")) == 0
        place = 0 if a == 0 else 2 * section
        for q in range(2):
            value = jnp.where(here, sums[a][q], 0.0)
            table = jnp.where((row == a) & (lane == place + q), value, table)
    norm_ref[...] = table
    for _, _, _, _, stores in work:
        for copy in stores:
            copy.wait()


def scalar_heads(forget_sum):
    return forget_sum.shape[0] // 2


def optimizer_step(scalars, sums, forget_sum, gains_sum, small, grads, weights, firsts, seconds):
    n = len(grads)
    shapes = [w.shape for w in weights]
    flat = [jax.ShapeDtypeStruct(s, jnp.float32) for s in shapes]
    buffers = lambda kinds: [pltpu.VMEM(s, k) for s, k in zip(shapes, kinds)]
    parts = sum(len(pieces_of(s[0])) for s in shapes)
    out = pl.pallas_call(
        partial(step_kernel, shapes),
        out_shape=flat * 3
        + [jax.ShapeDtypeStruct(s.shape, jnp.float32) for s in small]
        + [jax.ShapeDtypeStruct((8, 128), jnp.float32)] * 2,
        in_specs=[pl.BlockSpec(memory_space=pltpu.SMEM)] + [VMEM] * 9 + [ANY] * (4 * n),
        out_specs=[ANY] * (3 * n) + [VMEM] * 8,
        scratch_shapes=buffers([g.dtype for g in grads])
        + buffers([jnp.float32] * n) * 4
        + [DMA((parts, 4)), DMA((parts, 3))],
        compiler_params=pltpu.CompilerParams(vmem_limit_bytes=60 * 2**20),
        name="optimizer_step",
    )(scalars, sums, forget_sum, gains_sum, *small, *grads, *weights, *firsts, *seconds)
    return out[:n], out[n : 2 * n], out[2 * n : 3 * n], out[3 * n : 3 * n + 6], out[-2], out[-1]


def apply_kernel(shapes, ratio_ref, *refs):
    n = len(shapes)
    weights, directions, outs = refs[:n], refs[n : 2 * n], refs[2 * n : 3 * n]
    w_buf, d_buf = refs[3 * n : 4 * n], refs[4 * n : 5 * n]
    load_sem, store_sem = refs[5 * n :]
    work = []
    for a in range(n):
        for at, part in pieces_of(shapes[a][0]):
            rows = pl.ds(at, part)
            p = len(work)
            loads = [
                pltpu.make_async_copy(weights[a].at[rows], w_buf[a].at[rows], load_sem.at[p, 0]),
                pltpu.make_async_copy(directions[a].at[rows], d_buf[a].at[rows], load_sem.at[p, 1]),
            ]
            store = pltpu.make_async_copy(w_buf[a].at[rows], outs[a].at[rows], store_sem.at[p])
            work.append((a, at, part, loads, store))
    for _, _, _, loads, _ in work:
        for copy in loads:
            copy.start()
    for a, at, part, loads, store in work:
        for copy in loads:
            copy.wait()
        w, d = w_buf[a].at[pl.ds(at, part)], d_buf[a].at[pl.ds(at, part)]
        rate = ratio_ref[a]

        def tile(rows, cols, carry):
            w[rows, cols] = w[rows, cols] - rate * d[rows, cols]
            return carry

        each_tile(part, shapes[a][1], tile, [jnp.float32(0), jnp.float32(0)])
        store.start()
    for _, _, _, _, store in work:
        store.wait()


def apply_step(rates, weights, directions):
    n = len(weights)
    shapes = [w.shape for w in weights]
    parts = sum(len(pieces_of(s[0])) for s in shapes)
    return pl.pallas_call(
        partial(apply_kernel, shapes),
        out_shape=[jax.ShapeDtypeStruct(s, jnp.float32) for s in shapes],
        in_specs=[pl.BlockSpec(memory_space=pltpu.SMEM)] + [ANY] * (2 * n),
        out_specs=[ANY] * n,
        scratch_shapes=[pltpu.VMEM(s, jnp.float32) for s in shapes] * 2 + [DMA((parts, 2)), DMA((parts,))],
        compiler_params=pltpu.CompilerParams(vmem_limit_bytes=40 * 2**20),
        name="apply_step",
    )(rates, *weights, *directions)


def lower(values):
    return values.astype(jnp.bfloat16)


def product(left, right):
    return jnp.dot(left, right, preferred_element_type=jnp.float32)


def product_left(left, right):
    return lax.dot_general(left, right, (((0,), (0,)), ((), ())), preferred_element_type=jnp.float32)


def product_right(left, right):
    return lax.dot_general(left, right, (((1,), (1,)), ((), ())), preferred_element_type=jnp.float32)


def rms_forward(values, gain):
    inverse = lax.rsqrt(jnp.mean(values * values, axis=-1, keepdims=True) + eps_norm)
    normed = values * inverse
    return (normed * gain, normed, inverse)


def rms_backward(grad_out, normed, inverse, gain):
    grad_normed = grad_out * gain
    grad_in = inverse * (
        grad_normed - normed * jnp.mean(grad_normed * normed, axis=-1, keepdims=True)
    )
    return (grad_in, jnp.sum(grad_out * normed, axis=0))


def path_mask(parent_row, tree_len):
    seg_count = parent_row.shape[0]
    seglen = tree_len // seg_count
    seg_order = jnp.arange(seg_count, dtype=jnp.int32)
    parent_hot = ((parent_row[:, None] == seg_order[None, :]) & (seg_order[:, None] >= 1)).astype(
        jnp.float32
    )
    identity = jnp.eye(seg_count, dtype=jnp.float32)
    power, steps = parent_hot, 1
    reached = identity + parent_hot
    while steps < seg_count:
        reached = jnp.minimum(1.0, jnp.dot(reached, reached))
        steps *= 2
    strict = reached - identity
    seg_of = jnp.arange(tree_len, dtype=jnp.int32) // seglen
    seg_hot = (seg_of[:, None] == seg_order[None, :]).astype(jnp.float32)
    ancestor = jnp.dot(jnp.dot(seg_hot, strict), seg_hot.T)
    places = jnp.arange(tree_len, dtype=jnp.int32)
    inside = (seg_of[:, None] == seg_of[None, :]) & (places[None, :] <= places[:, None])
    return ancestor + inside.astype(jnp.float32)


def square_sum(values):
    return jnp.sum(values * values)


def local(
    tokens,
    parents,
    loss_positions,
    targets,
    teacher_index,
    teacher_probability,
    step_count,
    embed_table,
    table_first,
    table_second,
    attention_in,
    attention_in_first,
    attention_in_second,
    attention_out,
    attention_out_first,
    attention_out_second,
    feedforward_in,
    feedforward_in_first,
    feedforward_in_second,
    feedforward_out,
    feedforward_out_first,
    feedforward_out_second,
    forget_gate,
    forget_first,
    forget_second,
    norm_gains,
    gains_first,
    gains_second,
):
    section_id = lax.axis_index("section")
    replica_id = lax.axis_index("replica")
    shard_id = lax.axis_index("shard")
    sections = lax.axis_size("section")
    replicas = lax.axis_size("replica")
    shards = lax.axis_size("shard")
    group_trees, tree_len = tokens.shape
    rows_each, width = embed_table.shape
    pos_count = loss_positions.shape[1]
    pos_all = group_trees * replicas * pos_count
    owners = replicas * shards
    owner_id = replica_id * shards + shard_id
    own_tree = section_id * shards + shard_id
    table_low = lower(embed_table)

    def own_row(values):
        return lax.dynamic_index_in_dim(values, own_tree, 0, keepdims=False)

    tree_tokens = own_row(tokens)
    token_owner = tree_tokens // rows_each
    token_row = tree_tokens % rows_each
    spots = jnp.arange(tree_len, dtype=jnp.int32)

    def asked(batch):
        earlier = spots[None, :] < spots[:, None]
        same = tree_tokens[:, None] == tree_tokens[None, :]
        is_first = jnp.logical_not(jnp.any(same & earlier, axis=1))
        counted = earlier & (token_owner[:, None] == token_owner[None, :]) & is_first[None, :]
        number_first = jnp.sum(counted.astype(jnp.int32), axis=1)
        number = jnp.sum(jnp.where(same & is_first[None, :], number_first[None, :], 0), axis=1)
        slot = number - batch * batch_rows
        inside = (slot >= 0) & (slot < batch_rows)
        place = jnp.where(inside, token_owner * batch_rows + slot, -1)
        spot_of = jnp.arange(owners * batch_rows, dtype=jnp.int32)
        hot = place[None, :] == spot_of[:, None]
        rows = jnp.max(jnp.where(hot & is_first[None, :], token_row[None, :] + 1, 0), axis=1)
        return rows.reshape(owners, batch_rows), lower(hot)

    def all_devices(part, ident):
        if replicas != 2:
            out = part
            for axis in ("shard", "replica", "section"):
                out = lax.all_gather(out, axis)
            return out
        return jnp.swapaxes(gather([part], ident, space=VMEM)[0][0], 1, 2)

    def wanted(batch):
        rows, hot = asked(batch)
        every = all_devices(jnp.pad(rows, ((0, 0), (0, 128 - batch_rows))), 0)
        mine = lax.dynamic_index_in_dim(every, owner_id, 3, keepdims=False)[..., :batch_rows]
        wish = mine.reshape(sections * owners * batch_rows) - 1
        row_of = jnp.arange(rows_each, dtype=jnp.int32)
        return hot, lower(wish[:, None] == row_of[None, :])

    def more_rows(state):
        batch, total_rows = state
        hot_more, pick = wanted(batch)
        own_pick = lax.dynamic_index_in_dim(
            pick.reshape(sections, owners * batch_rows, rows_each), section_id, 0, keepdims=False
        )
        sent = lower(product(own_pick, table_low)).reshape(owners, batch_rows, width)
        got_more = exchange(sent, 1)[0].reshape(owners * batch_rows, width)
        return (batch + 1, total_rows + product_left(hot_more, got_more))

    def more_grads(state):
        batch, total_rows = state
        hot_more, pick = wanted(batch)
        sent = lower(product(hot_more, embed_low)).reshape(owners, batch_rows, width)
        got_more = exchange(sent, 6, relay=True).reshape(sections * owners * batch_rows, width)
        return (batch + 1, total_rows + product_left(pick, got_more))

    def halves(weight):
        return lower(weight).reshape(2, weight.shape[1] // 2, weight.shape[2])

    width_all = -(-rows_each // 128) * 128
    table_wide = jnp.pad(table_low, ((0, width_all - rows_each), (0, 0)))
    layer_weights = (attention_in, attention_out, feedforward_in, feedforward_out)
    group_data = [targets, teacher_index.reshape(group_trees, -1), teacher_probability.reshape(group_trees, -1)]
    pair_parts = group_data if replicas == 2 else []
    hot, asks = ask_rows(tree_tokens, token_owner, token_row, owners)
    gathered, group_all, (asked_all, got) = gather(
        [halves(w) for w in layer_weights], 2, pair_parts, split=True, errand=(asks, table_wide)
    )
    if replicas != 2:
        group_all = [lax.all_gather(part, "replica") for part in group_data]
    batches = (jnp.max(asked_all[:, :, 0, 127]) + batch_rows - 1) // batch_rows
    embeds = product_left(hot, got.reshape(owners * batch_rows, width))
    _, embeds = lax.while_loop(lambda s: s[0] < batches, more_rows, (jnp.int32(1), embeds))
    mats = [g.reshape(sections, -1, g.shape[-1]) for g in gathered]
    heads = forget_gate.shape[2]
    forget_low = jnp.pad(lower(forget_gate[:, :width]), ((0, 0), (0, 0), (0, 128 - heads)))
    forget_bias = jnp.pad(forget_gate[:, width:], ((0, 0), (0, 0), (0, 128 - heads)))
    gains_of = [jnp.pad(norm_gains[2 * n : 2 * n + 2], ((0, 6), (0, 0))) for n in range(2)]

    allowed = lower(path_mask(own_row(parents), tree_len))
    out_0, *saved_0 = layer_forward(0, False, embeds, allowed, mats, forget_low[0], forget_bias[0], gains_of[0])
    out_1, *saved_1 = layer_forward(1, True, out_0, allowed, mats, forget_low[1], forget_bias[1], gains_of[1])

    positions = own_row(loss_positions)
    position_hot = (positions[:, None] == spots[None, :]).astype(jnp.float32)
    picked = jnp.take(out_1, positions, axis=0)
    final_gain = norm_gains[4]
    head_out, head_normed, head_inverse = rms_forward(picked, final_gain)
    head_rows = jnp.swapaxes(all_devices(lower(head_out), 3), 0, 1).reshape(pos_all, width)

    target_all, index_all, prob_all = [
        part.reshape((pos_all,) + (-1,) * (n > 0)) for n, part in enumerate(group_all)
    ]

    def owned(ids):
        column = ids - owner_id * rows_each
        return jnp.where((column >= 0) & (column < rows_each), column, -1)

    marks = spread_entries(owned(index_all), prob_all, owned(target_all), width_all)
    logits, stats = head_forward(rows_each, head_rows, table_wide, marks)
    if replicas == 2:
        stats_all = exchange(stats[None], 4)[0]
    else:
        stats_all = lax.all_gather(lax.all_gather(stats, "replica"), "shard")
    grad_heads, head_table, loss_sum = head_backward(
        head_rows, table_wide, marks, logits, stats_all.reshape(owners, 4, pos_all), prob_all, shards * pos_count, pos_all
    )
    grad_heads = exchange(grad_heads.reshape(owners, pos_count, width), 5)[0]
    grad_heads = jnp.sum(grad_heads.astype(jnp.float32), axis=0)
    grad_picked, grad_final = rms_backward(grad_heads, head_normed, head_inverse, final_gain)
    grad_top = lax.dot_general(
        position_hot, grad_picked, (((0,), (0,)), ((), ())), precision=highest
    )

    grad_mid, forget_1, gains_1, *grads_1 = layer_backward(
        1, True, False, grad_top, out_0, allowed, saved_1, mats, forget_low[1], gains_of[1]
    )
    grad_low, forget_0, gains_0, *grads_0 = layer_backward(
        0, False, True, grad_mid, embeds, allowed, saved_0, mats, forget_low[0], gains_of[0]
    )
    embed_low = lower(grad_low)

    stacked = [
        [g.reshape(shards, 2, -1, g.shape[-1]) for g in pair] for pair in zip(grads_0, grads_1)
    ]
    def forget_form(values):
        return jnp.pad(jnp.swapaxes(values, 1, 2).reshape(-1, values.shape[1]), ((0, 0), (0, -values.shape[1] % 128)))

    def forget_terms(values):
        bias = jnp.swapaxes(values[128:129, :heads], 0, 1)
        return jnp.concatenate([values[:heads], jnp.pad(bias, ((0, 0), (0, -(width + 1) % 128)))], axis=1)

    def forget_back(values):
        return jnp.swapaxes(values[:, : width + 1].reshape(forget_gate.shape[0], -1, width + 1), 1, 2)

    def gains_form(values):
        return jnp.pad(values, ((0, 8 - values.shape[0]), (0, 0)))

    sent = lower(product(hot, embed_low)).reshape(owners, batch_rows, width)
    small_sums = [
        jnp.concatenate([forget_terms(forget_0), forget_terms(forget_1)], axis=0),
        gains_form(jnp.concatenate([gains_0[:2], gains_1[:2], grad_final[None]], axis=0)),
    ]
    layer_grads, (forget_total, gains_total, got_grads) = reduce_parts(stacked, 8, (small_sums, sent))
    if replicas != 2:
        layer_grads = [lax.psum(g * jnp.bfloat16(0.5), "replica") for g in layer_grads]
    _, head_table = lax.while_loop(lambda s: s[0] < batches, more_grads, (jnp.int32(1), head_table[:rows_each]))
    table_grad, square = table_gradient(
        rows_each, asked_all, got_grads.reshape(-1, width), head_table, layer_grads
    )
    layer_grads = [g.reshape(w.shape[1:]) for g, w in zip(layer_grads, layer_weights)]
    (scalars,) = total([square], 15)
    loss_total = loss_sum[0, 0] / pos_all
    count_float = step_count.astype(jnp.float32)
    rates = jnp.stack(
        [
            1.0 / (1.0 - jnp.power(beta_first, count_float)),
            1.0 / (1.0 - jnp.power(beta_second, count_float)),
            clip_factor / jnp.sqrt(jnp.float32(pos_all)),
        ]
    )
    small = [forget_form(v) for v in (forget_gate, forget_first, forget_second)] + [
        gains_form(v) for v in (norm_gains, gains_first, gains_second)
    ]
    weights = [embed_table] + [w[0] for w in layer_weights]
    firsts = [table_first] + [
        m[0] for m in (attention_in_first, attention_out_first, feedforward_in_first, feedforward_out_first)
    ]
    seconds = [table_second] + [
        m[0] for m in (attention_in_second, attention_out_second, feedforward_in_second, feedforward_out_second)
    ]
    firsts_new, seconds_new, directions, small_new, norms, small_norms = optimizer_step(
        rates, scalars, forget_total, gains_total, small, [table_grad, *layer_grads], weights, firsts, seconds
    )
    norms = jnp.sqrt(total([norms], 16)[0])
    table_norms = norms[0, :2]
    layer_norms = norms[1:5, : 2 * sections].reshape(4, sections, 2)
    mine = lax.dynamic_index_in_dim(layer_norms, section_id, 1, keepdims=False)
    both_norms = jnp.concatenate([table_norms[None], mine], axis=0)
    weights_new = apply_step(learn_rate * both_norms[:, 0] / both_norms[:, 1], weights, directions)
    new_table, table_first_new, table_second_new = weights_new[0], firsts_new[0], seconds_new[0]
    new_layers = [(weights_new[n][None], firsts_new[n][None], seconds_new[n][None]) for n in range(1, 5)]
    new_forget, forget_first_new, forget_second_new = [forget_back(v) for v in small_new[:3]]
    gain_count = norm_gains.shape[0]
    new_gains, gains_first_new, gains_second_new = [v[:gain_count] for v in small_new[3:]]
    layer_count = forget_gate.shape[0]
    grad_norm = small_norms[0, 0]
    tensor_norms = jnp.concatenate(
        [
            table_norms[None],
            layer_norms.reshape(4 * sections, 2),
            small_norms[1, : 2 * (layer_count + gain_count)].reshape(-1, 2),
        ],
        axis=0,
    )
    return (
        new_table,
        table_first_new,
        table_second_new,
        *new_layers[0],
        *new_layers[1],
        *new_layers[2],
        *new_layers[3],
        new_forget,
        forget_first_new,
        forget_second_new,
        new_gains,
        gains_first_new,
        gains_second_new,
        tensor_norms,
        grad_norm,
        loss_total,
    )


def solution(mesh):
    group = P("replica", None)
    table = P(("replica", "shard"), None)
    layer = P("section", "shard", None)
    in_specs = (
        (group,) * 4
        + (P("replica", None, None),) * 2
        + (P(),)
        + (table,) * 3
        + (layer,) * 12
        + (P(),) * 6
    )
    out_specs = (table,) * 3 + (layer,) * 12 + (P(),) * 9
    return jax.shard_map(local, mesh=mesh, in_specs=in_specs, out_specs=out_specs, check_vma=False)
```

```python
from functools import partial

import jax
import jax.numpy as jnp
from jax import lax
from jax.experimental import pallas as pl
from jax.experimental.pallas import tpu as pltpu
from jax.sharding import PartitionSpec as P

MESH = pl.DeviceIdType.MESH
VMEM = pl.BlockSpec(memory_space=pltpu.VMEM)
ANY = pl.BlockSpec(memory_space=pl.ANY)
DMA = pltpu.SemaphoreType.DMA
eps_norm = 1e-06
beta_first = 0.9
beta_second = 0.999
adam_eps = 1e-10
decay_rate = 0.01
learn_rate = 0.2
clip_factor = 8.0
highest = lax.Precision.HIGHEST
masked_score = -1e30
batch_rows = 32
every_axis = ("section", "replica", "shard")


class Place:
    def __init__(self):
        self.sections = lax.axis_size("section")
        self.replicas = lax.axis_size("replica")
        self.shards = lax.axis_size("shard")
        self.nz = min(4, self.shards)
        self.ny = self.shards // self.nz
        self.x = lax.axis_index("section")
        self.rep = lax.axis_index("replica")
        self.shard = lax.axis_index("shard")
        self.core = lax.rem(self.rep, 2)
        self.z = self.shard // self.ny
        self.y = lax.rem(self.shard, self.ny)

    def at(self, section=None, rep=None, z=None, y=None, shard=None):
        if shard is None:
            shard = (self.z if z is None else z) * self.ny + (self.y if y is None else y)
        return {
            "section": self.x if section is None else section,
            "replica": self.rep if rep is None else rep,
            "shard": shard,
        }

    def peer_x(self, i):
        return self.at(section=lax.rem(self.x + i, self.sections))

    def peer_y(self, j):
        return self.at(y=lax.rem(self.y + j, self.ny))

    def line(self, step):
        return self.at(z=self.z + step)

    def partner(self):
        return self.at(rep=self.rep + 1 - 2 * self.core)

    def group(self, p):
        count = self.replicas * self.shards
        place = lax.rem(self.rep * self.shards + self.shard + p, count)
        return place, self.at(rep=place // self.shards, shard=lax.rem(place, self.shards))

    def device(self, i, p):
        place, _ = self.group(p)
        section = lax.rem(self.x + i, self.sections)
        return place, self.at(section=section, rep=place // self.shards, shard=lax.rem(place, self.shards))

    def greet_all(self):
        barrier = pltpu.get_barrier_semaphore()
        peers = self.replicas * self.shards
        for i in range(self.sections):
            for p in range(peers):
                if i or p:
                    pl.semaphore_signal(barrier, inc=1, device_id=self.device(i, p)[1], device_id_type=MESH)
        pl.semaphore_wait(barrier, self.sections * peers - 1)

    def greet_group(self):
        barrier = pltpu.get_barrier_semaphore()
        peers = self.replicas * self.shards
        for p in range(1, peers):
            pl.semaphore_signal(barrier, inc=1, device_id=self.group(p)[1], device_id_type=MESH)
        for i in range(1, self.sections):
            pl.semaphore_signal(barrier, inc=1, device_id=self.peer_x(i), device_id_type=MESH)
        pl.semaphore_wait(barrier, peers + self.sections - 2)

    def inside(self, k):
        if k == 0:
            return None
        return self.z + k < self.nz if k > 0 else self.z + k >= 0

    def greet(self, use_x=True):
        barrier = pltpu.get_barrier_semaphore()

        def signal(device):
            pl.semaphore_signal(barrier, inc=1, device_id=device, device_id_type=MESH)

        count = 1
        if use_x:
            for i in range(1, self.sections):
                signal(self.peer_x(i))
                count += 1
        for j in range(1, self.ny):
            signal(self.peer_y(j))
            count += 1
        signal(self.partner())
        up, down = self.inside(1), self.inside(-1)
        pl.when(up)(lambda: signal(self.line(1)))
        pl.when(down)(lambda: signal(self.line(-1)))
        ends = jnp.minimum(self.z, 1) + jnp.minimum(self.nz - 1 - self.z, 1)
        pl.semaphore_wait(barrier, count + ends)


def when(cond, fn):
    if cond is None:
        fn()
    else:
        pl.when(cond)(fn)


def both(a, b):
    if a is None:
        return b
    if b is None:
        return a
    return jnp.logical_and(a, b)


def remote(src, dst, send, recv, device):
    return pltpu.make_async_remote_copy(
        src_ref=src, dst_ref=dst, send_sem=send, recv_sem=recv, device_id=device, device_id_type=MESH
    )


def rows_errand(me, ask_ref, table_ref, asked_ref, got_ref, hot, found, ask_sem, row_sem, own_sem):
    peers = me.replicas * me.shards
    mine = me.rep * me.shards + me.shard
    width = table_ref.shape[1]
    asks = []
    for i in range(me.sections):
        for p in range(peers):
            place, device = me.device(i, p)
            if i or p:
                asks.append(remote(ask_ref.at[place], asked_ref.at[me.x, mine], ask_sem.at[0, i, p], ask_sem.at[1, i, p], device))
    for copy in asks:
        copy.start()
    own_ask = pltpu.make_async_copy(ask_ref.at[mine], asked_ref.at[me.x, mine], own_sem.at[0])
    own_ask.start()
    rows = [
        remote(found.at[me.group(p)[0]], got_ref.at[mine], row_sem.at[0, p], row_sem.at[1, p], me.group(p)[1])
        for p in range(1, peers)
    ]
    own_rows = pltpu.make_async_copy(found.at[mine], got_ref.at[mine], own_sem.at[1])

    def look_up():
        own_ask.wait()
        for i in range(me.sections):
            for p in range(peers):
                if i or p:
                    source = lax.rem(mine + peers - p, peers)
                    dst = asked_ref.at[lax.rem(me.x + me.sections - i, me.sections), source]
                    remote(dst, dst, ask_sem.at[0, i, p], ask_sem.at[1, i, p], me.partner()).wait_recv()
        wish = asked_ref[me.x].reshape(peers, 128).astype(jnp.float32).T
        column = lax.broadcasted_iota(jnp.int32, (batch_rows, table_ref.shape[0]), 1).astype(jnp.float32) + 1.0
        for s in range(peers):
            ours = wish[0:batch_rows, s : s + 1] == column
            hot[s * batch_rows : (s + 1) * batch_rows, :] = jnp.where(ours, 1.0, 0.0).astype(jnp.bfloat16)

        def take(n, carry):
            at = pl.ds(pl.multiple_of(n * 256, 256), 256)
            values = jnp.dot(hot[...], table_ref[:, at], preferred_element_type=jnp.float32)
            found[:, :, at] = values.reshape(peers, batch_rows, 256).astype(jnp.bfloat16)
            return carry

        lax.fori_loop(0, width // 256, take, 0)
        own_rows.start()
        for copy in rows:
            copy.start()

    def finish():
        for p in range(1, peers):
            source = lax.rem(mine + peers - p, peers)
            dst = got_ref.at[source]
            remote(dst, dst, row_sem.at[0, p], row_sem.at[1, p], me.partner()).wait_recv()
        own_rows.wait()
        for copy in asks + rows:
            copy.wait_send()

    return {1: look_up, "end": finish}


def gather_kernel(count, pairs, split, orders, errand, *refs):
    ins, refs = refs[:count], refs[count:]
    pair_ins, refs = refs[:pairs], refs[pairs:]
    asked = 2 if errand else 0
    errand_in, refs = refs[:asked], refs[asked:]
    outs, refs = refs[:count], refs[count:]
    pair_outs, refs = refs[:pairs], refs[pairs:]
    errand_out, refs = refs[:asked], refs[asked:]
    if errand and pairs:
        marks_ref, refs = refs[0], refs[1:]
    errand_refs = errand_in + errand_out
    send_sem, recv_sem, cross_sem, pair_sem, local_sem = refs[:5]
    me = Place()
    nz, ny, nx = me.nz, me.ny, me.sections
    if "x" not in orders[0][0][0]:
        nx = 1
    hooks = {}
    if errand:
        me.greet_all()
        hooks = rows_errand(me, *errand_refs, *refs[5:])
    else:
        me.greet(use_x=nx > 1)

    def slot(ref, k, j, i, half):
        section = lax.rem(me.x + i, nx) if nx > 1 else 0
        return ref.at[section, (me.z + k) * ny + lax.rem(me.y + j, ny), half]

    locals_ = []
    for a in range(count):
        if split:
            dst = outs[a].at[me.x if nx > 1 else 0, me.shard]
        else:
            dst = outs[a].at[me.x if nx > 1 else 0, me.shard, me.core]
        locals_.append(pltpu.make_async_copy(ins[a], dst, local_sem.at[a]))
    for p in range(pairs):
        locals_.append(
            pltpu.make_async_copy(pair_ins[p], pair_outs[p].at[me.core], local_sem.at[count + p])
        )
    for copy in locals_:
        copy.start()
    pair_copies = [
        remote(pair_ins[p], pair_outs[p].at[me.core], pair_sem.at[0, p], pair_sem.at[1, p], me.partner())
        for p in range(pairs)
    ]

    def run(core, plan):
        sends = []

        def push(cond, src, dst, device, sem):
            copy = remote(src, dst, send_sem.at[len(sends)], sem, device)
            when(cond, copy.start)
            sends.append((cond, copy))

        def sem_of(a, k, j, i):
            return recv_sem.at[a, k + nz - 1, j, i]

        def spread(order, arrays, k, j, i, via):
            cond = me.inside(k)
            own = via is None
            later = order if own else order[order.index(via) + 1 :]
            for a in arrays:
                dst = slot(outs[a], k, j, i, core)
                src = dst
                if own:
                    src = ins[a].at[core] if split else ins[a]
                else:
                    arrival = remote(dst, dst, send_sem.at[0], sem_of(a, k, j, i), me.partner())
                    when(cond, arrival.wait_recv)
                steps = []
                if via == "z":
                    steps = [-1 if k > 0 else 1]
                elif "z" in later:
                    steps = [1, -1]
                for step in steps:
                    push(both(cond, me.inside(step)), src, dst, me.line(step), sem_of(a, k - step, j, i))
                if "y" in later:
                    for p in range(1, ny):
                        push(cond, src, dst, me.peer_y(p), sem_of(a, k, (j - p) % ny, i))
                if "x" in later:
                    for p in range(1, nx):
                        push(cond, src, dst, me.peer_x(p), sem_of(a, k, j, (i - p) % nx))
                if not (own and split):
                    push(cond, src, dst, me.partner(), cross_sem.at[a, k + nz - 1, j, i])

        events = []
        for order, arrays in plan:
            for k in range(1 - nz, nz):
                for j in range(ny):
                    for i in range(nx):
                        via = [d for d in order if {"z": k, "y": j, "x": i}[d] != 0]
                        hops = abs(k) + (j != 0) + (i != 0)
                        stage = order.index(via[-1]) if via else -1
                        events.append((hops, stage, k, j, i, order, arrays, via[-1] if via else None))
        events.sort(key=lambda e: e[:5])
        for n, (hops, stage, k, j, i, order, arrays, via) in enumerate(events):
            spread(order, arrays, k, j, i, via)
            if n + 1 < len(events) and events[n + 1][0] == hops:
                continue
            if hops == 0:
                for copy in pair_copies:
                    copy.start()
            if hops in hooks:
                hooks[hops]()
        for hops, stage, k, j, i, order, arrays, via in events:
            if via is None and split:
                continue
            for a in arrays:
                dst = slot(outs[a], k, j, i, 1 - core)
                arrival = remote(dst, dst, send_sem.at[0], cross_sem.at[a, k + nz - 1, j, i], me.partner())
                when(me.inside(k), arrival.wait_recv)
        for cond, copy in sends:
            when(cond, copy.wait_send)

    if errand and pairs:
        groups = 2 * pair_ins[0].shape[0]
        shift = (me.rep * me.shards + me.shard) * errand
        far_hops = [hops for hops in range(2, nz + 2)]

        def spread_some(n):
            if n == 0:
                for copy in locals_[count:]:
                    copy.wait()
                for p in range(pairs):
                    pair_copies[p].wait_send()
                    remote(
                        pair_ins[p], pair_outs[p].at[1 - me.core], pair_sem.at[0, p], pair_sem.at[1, p], me.partner()
                    ).wait_recv()
            edges = [groups * t // len(far_hops) for t in range(len(far_hops) + 1)]
            spread_range(edges[n], edges[n + 1], shift, errand, *pair_outs, marks_ref)

        for n, hops in enumerate(far_hops):
            hooks[hops] = partial(spread_some, n)

    for core, plan in enumerate(orders):
        pl.when(me.core == core)(partial(run, core, plan))
    if errand:
        hooks["end"]()
    for copy in locals_[:count]:
        copy.wait()


def gather(parts, ident, pair_parts=(), split=False, use_x=True, space=ANY, errand=(), rows_each=0):
    count, pairs = len(parts), len(pair_parts)
    every = list(range(count))
    if not use_x:
        orders = [[(("z", "y"), every)]] * 2
    elif split:
        orders = [[(("z", "y", "x"), every)], [(("x", "z", "y"), every[:-1]), (("x", "y", "z"), every[-1:])]]
    else:
        orders = [[(("z", "y", "x"), every)], [(("x", "z", "y"), every)]]
    shards = lax.axis_size("shard")
    nx = lax.axis_size("section") if use_x else 1
    nz = min(4, shards)
    ny = shards // nz
    lead = (nx, shards) if split else (nx, shards, 2)
    blocks = (2 * nz - 1) * ny * nx
    errand_shapes, errand_scratch = [], []
    if errand:
        asks, table = errand
        peers, wide = asks.shape[0], table.shape[1]
        errand_shapes = [
            jax.ShapeDtypeStruct((nx, peers) + asks.shape[1:], asks.dtype),
            jax.ShapeDtypeStruct((peers, batch_rows, wide), table.dtype),
        ]
        if pairs:
            rows = 2 * pair_parts[2].shape[0]
            errand_shapes.append(jax.ShapeDtypeStruct((rows, table.shape[0]), jnp.float32))
        errand_scratch = [
            pltpu.VMEM((peers * batch_rows, table.shape[0]), table.dtype),
            pltpu.VMEM((peers, batch_rows, wide), table.dtype),
            DMA((2, nx, peers)),
            DMA((2, peers)),
            DMA((2,)),
        ]
    outs = pl.pallas_call(
        partial(gather_kernel, count, pairs, split, orders, rows_each),
        out_shape=[jax.ShapeDtypeStruct(lead + p.shape, p.dtype) for p in parts]
        + [jax.ShapeDtypeStruct((2,) + p.shape, p.dtype) for p in pair_parts]
        + errand_shapes,
        in_specs=[VMEM] * (count + pairs + len(errand)),
        out_specs=[space] * count + [VMEM] * pairs + [VMEM] * len(errand_shapes),
        scratch_shapes=[
            DMA((blocks * count * 4,)),
            DMA((count, 2 * nz - 1, ny, nx)),
            DMA((count, 2 * nz - 1, ny, nx)),
            DMA((2, max(pairs, 1))),
            DMA((count + pairs,)),
        ]
        + errand_scratch,
        compiler_params=pltpu.CompilerParams(collective_id=ident, has_side_effects=True),
        name=f"gather_{ident}",
    )(*parts, *pair_parts, *errand)
    return outs[:count], outs[count : count + pairs], outs[count + pairs :]


def exchange_kernel(relay, src_ref, out_ref, send_sem, recv_sem, relay_send, relay_recv, local_sem):
    me = Place()
    peers = me.replicas * me.shards
    barrier = pltpu.get_barrier_semaphore()
    for p in range(1, peers):
        pl.semaphore_signal(barrier, inc=1, device_id=me.group(p)[1], device_id_type=MESH)
    if relay:
        for i in range(1, me.sections):
            pl.semaphore_signal(barrier, inc=1, device_id=me.peer_x(i), device_id_type=MESH)
    pl.semaphore_wait(barrier, peers - 1 + (me.sections - 1 if relay else 0))
    mine = me.rep * me.shards + me.shard
    section = me.x if relay else 0
    own = pltpu.make_async_copy(
        src_ref.at[mine if src_ref.shape[0] > 1 else 0], out_ref.at[section, mine], local_sem.at[0]
    )
    own.start()
    sends = []
    for p in range(1, peers):
        place, device = me.group(p)
        copy = remote(
            src_ref.at[place if src_ref.shape[0] > 1 else 0], out_ref.at[section, mine], send_sem.at[p], recv_sem.at[p], device
        )
        copy.start()
        sends.append(copy)
    relays = []

    def forward(p, src, dst):
        for i in range(1, me.sections):
            copy = remote(src, dst, relay_send.at[p, i], relay_recv.at[p, i], me.peer_x(i))
            copy.start()
            relays.append(copy)

    if relay:
        forward(0, src_ref.at[mine if src_ref.shape[0] > 1 else 0], out_ref.at[me.x, mine])
    for p in range(1, peers):
        source, device = me.group(peers - p)
        dst = out_ref.at[section, source]
        remote(dst, dst, send_sem.at[p], recv_sem.at[p], device).wait_recv()
        if relay:
            forward(p, dst, dst)
    if relay:
        for p in range(peers):
            source, _ = me.group(peers - p)
            for i in range(1, me.sections):
                dst = out_ref.at[lax.rem(me.x + me.sections - i, me.sections), source]
                remote(dst, dst, relay_send.at[p, i], relay_recv.at[p, i], me.peer_x(i)).wait_recv()
    for copy in sends + relays:
        copy.wait_send()
    own.wait()


def exchange(blocks, ident, relay=False):
    peers = lax.axis_size("replica") * lax.axis_size("shard")
    nx = lax.axis_size("section")
    return pl.pallas_call(
        partial(exchange_kernel, relay),
        out_shape=jax.ShapeDtypeStruct((nx if relay else 1, peers) + blocks.shape[1:], blocks.dtype),
        in_specs=[VMEM],
        out_specs=VMEM,
        scratch_shapes=[DMA((peers,)), DMA((peers,)), DMA((peers, nx)), DMA((peers, nx)), DMA((1,))],
        compiler_params=pltpu.CompilerParams(collective_id=ident, has_side_effects=True),
        name=f"exchange_{ident}",
    )(blocks)


def total_steps(me):
    steps = []
    for axis, size in (("replica", me.replicas), ("section", me.sections), ("shard", me.shards)):
        bit = 1
        while bit < size:
            steps.append((axis, bit))
            bit *= 2
    return steps


def total_kernel(count, *refs):
    ins, refs = refs[:count], refs[count:]
    outs, refs = refs[:count], refs[count:]
    held, refs = refs[:count], refs[count:]
    send_sem, recv_sem = refs
    me = Place()
    steps = total_steps(me)
    position = {"section": me.x, "replica": me.rep, "shard": me.shard}

    def other(axis, bit):
        index = position[axis]
        return {**position, axis: index + bit - 2 * bit * lax.rem(index // bit, 2)}

    barrier = pltpu.get_barrier_semaphore()
    for axis, bit in steps:
        pl.semaphore_signal(barrier, inc=1, device_id=other(axis, bit), device_id_type=MESH)
    pl.semaphore_wait(barrier, len(steps))
    for a in range(count):
        held[a][0] = ins[a][...]
    copies = []
    for n, (axis, bit) in enumerate(steps):
        step_copies = [
            remote(held[a].at[2 * n], held[a].at[2 * n + 1], send_sem.at[n, a], recv_sem.at[n, a], other(axis, bit))
            for a in range(count)
        ]
        for copy in step_copies:
            copy.start()
        copies += step_copies
        for a in range(count):
            step_copies[a].wait_recv()
            summed = held[a][2 * n] + held[a][2 * n + 1]
            if n + 1 < len(steps):
                held[a][2 * n + 2] = summed
            else:
                outs[a][...] = summed
    for copy in copies:
        copy.wait_send()


def total(values, ident):
    count = len(values)
    steps = sum((lax.axis_size(axis) - 1).bit_length() for axis in every_axis)
    return pl.pallas_call(
        partial(total_kernel, count),
        out_shape=[jax.ShapeDtypeStruct(v.shape, v.dtype) for v in values],
        in_specs=[VMEM] * count,
        out_specs=[VMEM] * count,
        scratch_shapes=[pltpu.VMEM((2 * steps,) + v.shape, v.dtype) for v in values]
        + [DMA((steps, count)), DMA((steps, count))],
        compiler_params=pltpu.CompilerParams(collective_id=ident, has_side_effects=True),
        name=f"total_{ident}",
    )(*values)


def add_rows(dst, src):
    rows = dst.shape[0]
    if rows % 16 != 0:
        dst[...] = (dst[...].astype(jnp.float32) + src[...].astype(jnp.float32)).astype(dst.dtype)
        return
    step = 16

    def body(n, carry):
        at = pl.ds(pl.multiple_of(n * step, step), step)
        dst[at, :] = (dst[at, :].astype(jnp.float32) + src[at, :].astype(jnp.float32)).astype(dst.dtype)
        return carry

    lax.fori_loop(0, rows // step, body, 0)


def grads_errand(me, sent, got, sum_in, sum_out, *refs):
    n_sums = len(sum_in)
    held, refs = refs[:n_sums], refs[n_sums:]
    row_sem, relay_sem, own_sem, sum_sem = refs
    peers = me.replicas * me.shards
    mine = me.rep * me.shards + me.shard
    direct = [
        remote(sent.at[me.group(p)[0]], got.at[me.x, mine], row_sem.at[0, p], row_sem.at[1, p], me.group(p)[1])
        for p in range(1, peers)
    ]
    own = pltpu.make_async_copy(sent.at[mine], got.at[me.x, mine], own_sem.at[0])
    relays = []

    def source(p):
        return lax.rem(mine + peers - p, peers)

    def begin():
        own.start()
        for copy in direct:
            copy.start()
        for i in range(1, me.sections):
            copy = remote(sent.at[mine], got.at[me.x, mine], relay_sem.at[0, 0, i], relay_sem.at[1, 0, i], me.peer_x(i))
            copy.start()
            relays.append(copy)

    steps = total_steps(me)
    position = {"section": me.x, "replica": me.rep, "shard": me.shard}

    def other(axis, bit):
        index = position[axis]
        return {**position, axis: index + bit - 2 * bit * lax.rem(index // bit, 2)}

    def sum_copies(n):
        axis, bit = steps[n]
        return [
            remote(held[a].at[2 * n], held[a].at[2 * n + 1], sum_sem.at[0, n, a], sum_sem.at[1, n, a], other(axis, bit))
            for a in range(n_sums)
        ]

    def sum_step(n):
        if n == 0:
            for a in range(n_sums):
                held[a][0] = sum_in[a][...]
        else:
            for a, copy in enumerate(sum_copies(n - 1)):
                copy.wait_recv()
                summed = held[a][2 * n - 2] + held[a][2 * n - 1]
                if n < len(steps):
                    held[a][2 * n] = summed
                else:
                    sum_out[a][...] = summed
        if n < len(steps):
            for copy in sum_copies(n):
                copy.start()

    def relay(first, last):
        for p in range(first, last):
            dst = got.at[me.x, source(p)]
            remote(dst, dst, row_sem.at[0, p], row_sem.at[1, p], me.partner()).wait_recv()
            for i in range(1, me.sections):
                copy = remote(dst, dst, relay_sem.at[0, p, i], relay_sem.at[1, p, i], me.peer_x(i))
                copy.start()
                relays.append(copy)

    def finish():
        for p in range(peers):
            for i in range(1, me.sections):
                dst = got.at[lax.rem(me.x + me.sections - i, me.sections), source(p)]
                remote(dst, dst, relay_sem.at[0, p, i], relay_sem.at[1, p, i], me.partner()).wait_recv()
        for p in range(peers):
            for i in range(1, me.sections):
                dst = got.at[me.x, source(p)]
                remote(dst, dst, relay_sem.at[0, p, i], relay_sem.at[1, p, i], me.peer_x(i)).wait_send()
        for copy in direct:
            copy.wait_send()
        for n in range(len(steps)):
            for copy in sum_copies(n):
                copy.wait_send()
        own.wait()

    early = [begin] + [partial(sum_step, n) for n in range(len(steps) + 1)]
    return early, [partial(relay, 1, peers)], [finish]


def reduce_kernel(count, sections, sums, *refs):
    ins, refs = [refs[a * sections : (a + 1) * sections] for a in range(count)], refs[count * sections :]
    sum_in, refs = refs[:sums], refs[sums:]
    sent = None
    if sums:
        sent, refs = refs[0], refs[1:]
    outs, refs = refs[:count], refs[count:]
    sum_out, refs = refs[:sums], refs[sums:]
    if sums:
        got, refs = refs[0], refs[1:]
    acc, refs = refs[:count], refs[count:]
    from_core, refs = refs[:count], refs[count:]
    from_x, refs = refs[:count], refs[count:]
    from_y, refs = refs[:count], refs[count:]
    from_z, refs = refs[:count], refs[count:]
    load_sem, core_send, core_recv, send_sem, x_recv, y_recv, z_recv, last_sem = refs[:8]
    me = Place()
    nz, ny, nx = me.nz, me.ny, me.sections
    hooks = []
    if sums:
        me.greet_group()
        hooks = grads_errand(me, sent, got, sum_in, sum_out, *refs[8 : 8 + sums], *refs[8 + sums :])
    else:
        me.greet()

    far = sorted((k for k in range(1 - nz, nz)), key=lambda k: -abs(k))

    def block(k, j, i):
        return lax.rem(me.x + i, nx), (me.z + k) * ny + lax.rem(me.y + j, ny)

    def order_of(core):
        if core == 0:
            return [(k, j, i) for i in range(nx - 1, -1, -1) for j in range(ny - 1, -1, -1) for k in far]
        return [(k, j, i) for j in range(ny - 1, -1, -1) for k in far for i in range(nx - 1, -1, -1)]

    def run(core):
        other = 1 - core
        sends = []

        def start_core(k, j, i):
            x, s = block(k, j, i)

            def go(layer):
                for a in range(count):
                    remote(
                        ins[a][layer].at[s, other], from_core[a].at[x, s], core_send.at[a, x, s],
                        core_recv.at[a, x, s], me.partner(),
                    ).start()

            for layer in range(nx):
                when(both(me.inside(k), x == layer), partial(go, layer))

        def start_load(k, j, i):
            x, s = block(k, j, i)

            def go(layer):
                for a in range(count):
                    pltpu.make_async_copy(ins[a][layer].at[s, core], acc[a].at[x, s], load_sem.at[a, x, s]).start()

            for layer in range(nx):
                when(both(me.inside(k), x == layer), partial(go, layer))

        for b in order_of(other):
            start_core(*b)
        for b in order_of(core):
            start_load(*b)
        early, late, final = [list(part) for part in hooks] if hooks else ([], [], [])

        def errand(todo, every=False):
            while todo:
                todo.pop(0)()
                if not every:
                    break

        errand(early)

        def push(cond, src, dst, sem, device):
            copy = remote(src, dst, send_sem.at[len(sends)], sem, device)
            when(cond, copy.start)
            sends.append((cond, copy))

        def take(cond, dst, src, sem):
            def go():
                remote(src, src, core_send.at[0, 0, 0], sem, me.partner()).wait_recv()
                add_rows(dst, src)

            when(cond, go)

        def join_core(a, k, j, i):
            x, s = block(k, j, i)

            def go():
                pltpu.make_async_copy(ins[a][0].at[s, core], acc[a].at[x, s], load_sem.at[a, x, s]).wait()

            when(me.inside(k), go)
            take(me.inside(k), acc[a].at[x, s], from_core[a].at[x, s], core_recv.at[a, x, s])

        def join_x(a, k, j):
            x, s = block(k, j, 0)
            for p in range(1, nx):
                take(me.inside(k), acc[a].at[x, s], from_x[a].at[p - 1, s], x_recv.at[a, p - 1, s])

        def join_y(a, k, i):
            x, s = block(k, 0, i)
            for p in range(1, ny):
                take(me.inside(k), acc[a].at[x, s], from_y[a].at[p - 1, x, me.z + k], y_recv.at[a, p - 1, x, me.z + k])

        def join_z(a, k, i):
            x, s = block(k, 0, i)
            if k >= 0:
                take(both(me.inside(k), me.inside(-1)), acc[a].at[x, s], from_z[a].at[x, me.z + k], z_recv.at[a, x, me.z + k])
            if k <= 0:
                place = nz if k == 0 else me.z + k
                take(both(me.inside(k), me.inside(1)), acc[a].at[x, s], from_z[a].at[x, place], z_recv.at[a, x, place])

        def send_x(a, k, j, i):
            x, s = block(k, j, i)
            push(me.inside(k), acc[a].at[x, s], from_x[a].at[i - 1, s], x_recv.at[a, i - 1, s], me.peer_x(i))

        def send_y(a, k, j, i):
            x, s = block(k, j, i)
            push(
                me.inside(k), acc[a].at[x, s], from_y[a].at[j - 1, x, me.z + k],
                y_recv.at[a, j - 1, x, me.z + k], me.peer_y(j),
            )

        def send_z(a, k, i):
            x, s = block(k, 0, i)
            place = nz if k == -1 else me.z + k
            push(
                me.inside(k), acc[a].at[x, s], from_z[a].at[x, place], z_recv.at[a, x, place],
                me.line(1 if k > 0 else -1),
            )

        each = range(count)

        def x_first(arrays):
            first, second, third = [], [], []

            def cross_x(k, j, i):
                for a in arrays:
                    join_core(a, k, j, i)
                    send_x(a, k, j, i)

            def join_own(k, j):
                for a in arrays:
                    join_core(a, k, j, 0)

            def cross_y(k, j):
                for a in arrays:
                    join_x(a, k, j)
                    send_y(a, k, j, 0)

            def along_z(k):
                for a in arrays:
                    join_x(a, k, 0)
                    join_y(a, k, 0)
                    join_z(a, k, 0)
                    if k != 0:
                        send_z(a, k, 0)

            for i in range(nx - 1, 0, -1):
                for j in range(ny - 1, -1, -1):
                    first += [partial(cross_x, k, j, i) for k in far]
            for j in range(ny - 1, -1, -1):
                second += [partial(join_own, k, j) for k in far]
            for j in range(ny - 1, 0, -1):
                second += [partial(cross_y, k, j) for k in far]
            third += [partial(along_z, k) for k in far]
            return first, second, third

        def y_first(arrays):
            def cross_y(k, j, i):
                for a in arrays:
                    join_core(a, k, j, i)
                    send_y(a, k, j, i)

            def join_own(k, i):
                for a in arrays:
                    join_core(a, k, 0, i)

            def along_z(k, i):
                for a in arrays:
                    join_y(a, k, i)
                    join_z(a, k, i)
                    if k != 0:
                        send_z(a, k, i)
                    elif i != 0:
                        send_x(a, 0, 0, i)
                    else:
                        join_x(a, 0, 0)

            slots = range(nx - 1, -1, -1)
            first = [partial(cross_y, k, j, i) for j in range(ny - 1, 0, -1) for k in far for i in slots]
            second = [partial(join_own, k, i) for k in far for i in slots]
            third = [partial(along_z, k, i) for k in far for i in slots]
            return first, second, third

        plans = [x_first(list(each)) if core == 0 else y_first(list(each))]
        for stage in range(3):
            lists = [plan[stage] for plan in plans if plan[stage]]
            longest = max(len(steps) for steps in lists)
            if stage == 1:
                errand(early, every=True)
                errand(late, every=True)
            for n in range(longest):
                for steps in lists:
                    for step in steps[len(steps) * n // longest : len(steps) * (n + 1) // longest]:
                        step()
                errand(early)
        errand(final, every=True)
        finals = []
        for a in each:
            copy = remote(
                acc[a].at[me.x, me.shard], outs[a].at[core], last_sem.at[0, a], last_sem.at[1, a], me.partner()
            )
            copy.start()
            finals.append(copy)
            outs[a][core] = acc[a][me.x, me.shard]
        for a in each:
            remote(outs[a].at[other], outs[a].at[other], last_sem.at[0, a], last_sem.at[1, a], me.partner()).wait_recv()
        for cond, copy in sends:
            when(cond, copy.wait_send)
        for copy in finals:
            copy.wait_send()
        for k, j, i in order_of(other):
            x, s = block(k, j, i)

            def finish():
                for a in each:
                    remote(
                        ins[a][0].at[s, other], from_core[a].at[x, s], core_send.at[a, x, s],
                        core_recv.at[a, x, s], me.partner(),
                    ).wait_send()

            when(me.inside(k), finish)

    pl.when(me.core == 0)(lambda: run(0))
    pl.when(me.core == 1)(lambda: run(1))


def reduce_shards(grads, ident, errand=None):
    count = len(grads)
    nx, shards = lax.axis_size("section"), lax.axis_size("shard")
    nz = min(4, shards)
    ny = shards // nz
    blocks = (2 * nz - 1) * ny * nx

    def scratch(lead):
        return [pltpu.VMEM(lead + g[0].shape[2:], g[0].dtype) for g in grads]

    extra_in, extra_shapes, extra_scratch, sums = [], [], [], 0
    if errand:
        values, sent = errand
        sums, peers = len(values), sent.shape[0]
        steps = sum((lax.axis_size(axis) - 1).bit_length() for axis in every_axis)
        extra_in = [*values, sent]
        extra_shapes = [jax.ShapeDtypeStruct(v.shape, v.dtype) for v in values] + [
            jax.ShapeDtypeStruct((nx,) + sent.shape, sent.dtype)
        ]
        extra_scratch = [pltpu.VMEM((2 * steps,) + v.shape, v.dtype) for v in values] + [
            DMA((2, peers)),
            DMA((2, peers, nx)),
            DMA((1,)),
            DMA((2, steps, sums)),
        ]
    return pl.pallas_call(
        partial(reduce_kernel, count, nx, sums),
        out_shape=[jax.ShapeDtypeStruct(g[0].shape[1:], g[0].dtype) for g in grads] + extra_shapes,
        in_specs=[ANY] * (count * nx) + [VMEM] * sums + [ANY] * bool(sums),
        out_specs=[VMEM] * (count + sums) + [ANY] * bool(sums),
        scratch_shapes=scratch((nx, shards))
        + scratch((nx, shards))
        + scratch((max(nx - 1, 1), shards))
        + scratch((max(ny - 1, 1), nx, nz))
        + scratch((nx, nz + 1))
        + [
            DMA((count, nx, shards)),
            DMA((count, nx, shards)),
            DMA((count, nx, shards)),
            DMA((blocks * count * 2,)),
            DMA((count, max(nx - 1, 1), shards)),
            DMA((count, max(ny - 1, 1), nx, nz)),
            DMA((count, nx, nz + 1)),
            DMA((2, count)),
        ]
        + extra_scratch,
        compiler_params=pltpu.CompilerParams(
            collective_id=ident, has_side_effects=True, vmem_limit_bytes=67043328
        ),
        name=f"reduce_{ident}",
    )(*[layer for g in grads for layer in g], *extra_in)


def reduce_parts(grads, ident, errand):
    nx, shards = lax.axis_size("section"), lax.axis_size("shard")
    ny = shards // min(4, shards)
    slots = 2 * nx * shards + (nx - 1) * shards + (ny - 1) * nx * 4 + nx * 5 + 4
    groups, used = [[]], 0
    for n, grad in enumerate(grads):
        rows, columns = grad[0].shape[2:]
        size = slots * (-(-rows // 16) * 16) * columns * 2
        if used + size > 58 * 2**20 and groups[-1]:
            groups.append([])
            used = 0
        groups[-1].append(n)
        used += size
    out = [None] * len(grads)
    for g, group in enumerate(groups):
        done = reduce_shards([grads[n] for n in group], ident + g, errand if g == 0 else None)
        for n, value in zip(group, done):
            out[n] = value
        if g == 0:
            extra = done[len(group) :]
    return out, extra


def spread_group(columns, values, target, high):
    entries = columns.shape[1]
    each = entries // 8
    row = lax.broadcasted_iota(jnp.int32, (1, entries), 1) // each
    key = jnp.where(columns >= 0, (columns // 128) * 8 + row, -1)
    low_part = jnp.where(columns >= 0, lax.rem(columns, 128), -1)
    left = jnp.where(key == lax.broadcasted_iota(jnp.int32, (high * 8, entries), 0), values, 0.0).astype(jnp.bfloat16)
    right = jnp.where(low_part == lax.broadcasted_iota(jnp.int32, (128, entries), 0), 1.0, 0.0).astype(jnp.bfloat16)
    placed = lax.dot_general(left, right, (((1,), (1,)), ((), ())), preferred_element_type=jnp.float32)
    pieces = []
    for h in range(high):
        one = jnp.where(lax.broadcasted_iota(jnp.int32, (8, 128), 1) + 128 * h == target, 1.0, 0.0)
        pieces.append(placed[h * 8 : (h + 1) * 8] + one)
    return pieces


def spread_range(first, last, shift, rows_each, columns_ref, weight_ref, target_ref, out_ref):
    high = out_ref.shape[1] // 128
    per = columns_ref.shape[1]

    def local_of(ids):
        column = ids - shift
        return jnp.where((column >= 0) & (column < rows_each), column, -1)

    def body(g, carry):
        pair, place = g // per, lax.rem(g, per)
        target = target_ref[pair, pl.ds(pl.multiple_of(place * 8, 8), 8), :]
        pieces = spread_group(local_of(columns_ref[pair, place]), weight_ref[pair, place], local_of(target), high)
        at = pl.ds(pl.multiple_of(g * 8, 8), 8)
        for h in range(high):
            out_ref[at, h * 128 : (h + 1) * 128] = pieces[h]
        return carry

    lax.fori_loop(first, last, body, 0)


def spread_kernel(rows_each, shift_ref, columns_ref, weight_ref, target_ref, out_ref):
    spread_range(
        0, columns_ref.shape[0] * columns_ref.shape[1], shift_ref[0], rows_each, columns_ref, weight_ref, target_ref, out_ref
    )


def spread_entries(shift, columns, values, targets, rows_each, width):
    rows = targets.shape[0] * targets.shape[1]
    return pl.pallas_call(
        partial(spread_kernel, rows_each),
        out_shape=jax.ShapeDtypeStruct((rows, width), jnp.float32),
        in_specs=[pl.BlockSpec(memory_space=pltpu.SMEM)] + [VMEM] * 3,
        out_specs=VMEM,
        name="spread_entries",
    )(shift, columns, values, targets)


def ask_kernel(owners, token_row, token_col, owner_row, owner_col, row_col, hot_ref, ask_ref):
    count = token_row.shape[1]
    i = lax.broadcasted_iota(jnp.int32, (count, count), 0)
    j = lax.broadcasted_iota(jnp.int32, (count, count), 1)
    same = token_col[...] == token_row[...]
    kin = owner_col[...] == owner_row[...]
    first_col = 1.0 - jnp.max(jnp.where(same & (j < i), 1.0, 0.0), axis=1, keepdims=True)
    first_row = 1.0 - jnp.max(jnp.where(same & (i < j), 1.0, 0.0), axis=0, keepdims=True)
    place_col = jnp.sum(jnp.where(kin & (j < i), first_row, 0.0), axis=1, keepdims=True)
    place_row = jnp.sum(jnp.where(kin & (i < j), first_col, 0.0), axis=0, keepdims=True)
    number_col = jnp.sum(jnp.where(same, first_row * place_row, 0.0), axis=1, keepdims=True)
    number_row = jnp.sum(jnp.where(same, first_col * place_col, 0.0), axis=0, keepdims=True)
    size = float(batch_rows)
    slot_row = jnp.where(number_row < size, owner_row[...].astype(jnp.float32) * size + number_row, -1.0)
    slot_col = jnp.where(number_col < size, owner_col[...].astype(jnp.float32) * size + number_col, -1.0)
    spots = owners * batch_rows
    part = 512 if spots % 512 == 0 else spots
    for at in range(0, spots, part):
        line = lax.broadcasted_iota(jnp.int32, (part, count), 0).astype(jnp.float32) + float(at)
        hot_ref[at : at + part, :] = jnp.where(slot_row == line, 1.0, 0.0).astype(jnp.bfloat16)
    most = jnp.max(number_col) + 1.0
    wanted = first_col * (row_col[...].astype(jnp.float32) + 1.0)
    lane = lax.broadcasted_iota(jnp.int32, (1, 128), 1)
    for at in range(0, spots, 128):
        line = lax.broadcasted_iota(jnp.int32, (count, 128), 1).astype(jnp.float32) + float(at)
        rows = jnp.max(jnp.where(slot_col == line, wanted, 0.0), axis=0, keepdims=True)
        for n in range(128 // batch_rows):
            shifted = pltpu.roll(rows, (128 - n * batch_rows) % 128, 1) if n else rows
            values = jnp.where(lane < batch_rows, shifted, jnp.where(lane == 127, most, 0.0))
            ask_ref[at // batch_rows + n] = values.astype(jnp.int32)


def ask_rows(tokens, owner, row, owners):
    count = tokens.shape[0]
    return pl.pallas_call(
        partial(ask_kernel, owners),
        out_shape=[
            jax.ShapeDtypeStruct((owners * batch_rows, count), jnp.bfloat16),
            jax.ShapeDtypeStruct((owners, 1, 128), jnp.int32),
        ],
        in_specs=[VMEM] * 5,
        out_specs=[VMEM] * 2,
        name="ask_rows",
    )(tokens[None], tokens[:, None], owner[None], owner[:, None], row[:, None])


def table_kernel(asked_ref, got_ref, head_ref, *refs):
    layers, table_ref, square_ref = refs[:-2], refs[-2], refs[-1]
    sections, peers = asked_ref.shape[:2]
    each = 128 // batch_rows
    lane = lax.broadcasted_iota(jnp.int32, (1, 128), 1)
    lists = []
    for at in range(0, sections * peers, each):
        wish = jnp.zeros((1, 128), jnp.int32)
        for n in range(each):
            part = asked_ref[(at + n) // peers, (at + n) % peers]
            part = pltpu.roll(part, n * batch_rows, 1) if n else part
            wish = jnp.where((lane >= n * batch_rows) & (lane < (n + 1) * batch_rows), part, wish)
        lists.append(wish)
    wish = jnp.concatenate(lists, axis=1)
    rows = table_ref.shape[0]
    step = 400 if rows % 400 == 0 else rows

    def body(n, square):
        at = pl.ds(pl.multiple_of(n * step, 8), step) if step != rows else slice(0, rows)
        row = lax.broadcasted_iota(jnp.int32, (step, wish.shape[1]), 0) + 1 + n * step
        hot = jnp.where(row == wish, 1.0, 0.0).astype(jnp.bfloat16)
        values = head_ref[at, :] + jnp.dot(hot, got_ref[...], preferred_element_type=jnp.float32)
        table_ref[at, :] = values
        return square + jnp.sum(values * values, axis=0, keepdims=True)

    zero = jnp.zeros((1, table_ref.shape[1]), jnp.float32)
    square = jnp.sum(lax.fori_loop(0, rows // step, body, zero)) if step != rows else jnp.sum(body(0, zero))
    square = jnp.where(lax.axis_index("section") == 0, square, 0.0)
    others = jnp.float32(0)
    for layer in layers:
        for half in range(2):
            values = layer[half].astype(jnp.float32)
            others = others + jnp.sum(values * values)
    square = square + jnp.where(lax.axis_index("replica") == 0, others, 0.0)
    corner = lax.broadcasted_iota(jnp.int32, (8, 128), 0) + lax.broadcasted_iota(jnp.int32, (8, 128), 1)
    square_ref[...] = jnp.where(corner == 0, square, 0.0)


def table_gradient(rows_each, asked, got, head_table, layer_grads):
    width = head_table.shape[1]
    return pl.pallas_call(
        table_kernel,
        out_shape=[
            jax.ShapeDtypeStruct((rows_each, width), jnp.float32),
            jax.ShapeDtypeStruct((8, 128), jnp.float32),
        ],
        in_specs=[VMEM] * (3 + len(layer_grads)),
        out_specs=[VMEM] * 2,
        compiler_params=pltpu.CompilerParams(vmem_limit_bytes=56 * 2**20),
        name="table_gradient",
    )(asked, got, head_table, *layer_grads)
def dims_nt(left, right):
    return lax.dot_general(left, right, (((1,), (1,)), ((), ())), preferred_element_type=jnp.float32)


def dims_tn(left, right):
    return lax.dot_general(left, right, (((0,), (0,)), ((), ())), preferred_element_type=jnp.float32)


def three_parts(values):
    first = lower(values)
    rest = values - first.astype(jnp.float32)
    second = lower(rest)
    return first, second, lower(rest - second.astype(jnp.float32))


def log_sigmoid(values):
    return jnp.minimum(values, 0.0) - jnp.log1p(jnp.exp(-jnp.abs(values)))


def norm_parts(values, gain):
    inverse = lax.rsqrt(jnp.mean(values * values, axis=-1, keepdims=True) + eps_norm)
    normed = values * inverse
    return normed, inverse, lower(normed * gain)


class HeadPair:
    def __init__(self, tree_len, cumul):
        self.lane = lax.broadcasted_iota(jnp.int32, (tree_len, 128), 1)
        self.parts = jnp.concatenate(three_parts(cumul), axis=1)
        self.row = lax.broadcasted_iota(jnp.int32, (384, 128), 0)
        self.column = lax.broadcasted_iota(jnp.int32, (384, 128), 1)

    def augmented(self, head, side, query, key):
        start = 64 - 64 * side
        mine = (self.lane >= 64 * side) & (self.lane < 64 * side + 64)
        wanted = (self.row - 128 * (self.row // 128) == head) & (self.column == self.row // 128 + start)
        placed = product(self.parts, lower(jnp.where(wanted, 1.0, 0.0)))
        wanted = (self.row - 128 * (self.row // 128) == head) & (self.column == self.row // 128 + start + 3)
        negative = product(self.parts, lower(jnp.where(wanted, -1.0, 0.0)))
        ones_q = jnp.where((self.lane >= start + 3) & (self.lane < start + 6), 1.0, 0.0)
        ones_k = jnp.where((self.lane >= start) & (self.lane < start + 3), 1.0, 0.0)
        query = lower(jnp.where(mine, query.astype(jnp.float32) * 0.125, placed + ones_q))
        key = lower(jnp.where(mine, key.astype(jnp.float32), negative + ones_k))
        return query, key, mine


def forward_kernel(layer, round_input, x_ref, allowed_ref, w_in, w_out, w_up, w_down, forget_ref, bias_ref, gain_ref,
                   y_ref, qkv_ref, logit_ref, lse_ref, att_ref, mid_ref, gu_ref,
                   b_in, b_out, b_up, b_down, gu_buf, hidden, mask, sem, gu_sem, in_sem):
    tree_len, width = x_ref.shape
    heads = width // 64
    half = hidden.shape[1]
    loads = [None] + [
        pltpu.make_async_copy(src.at[layer], dst, sem.at[n])
        for n, (src, dst) in enumerate(((w_out, b_out), (w_up, b_up), (w_down, b_down)))
    ]

    def first_load(n):
        at = pl.ds(pl.multiple_of(n * 256, 256), 256)
        return pltpu.make_async_copy(w_in.at[layer, :, at], b_in.at[:, at], in_sem.at[n])

    for n in range(3 * width // 256):
        first_load(n).start()
    for copy in loads[1:]:
        copy.start()
    x = x_ref[...]
    if round_input:
        x = lower(x).astype(jnp.float32)
    _, _, act = norm_parts(x, gain_ref[0:1, :])
    allowed = allowed_ref[...]
    mask[...] = jnp.where(allowed > 0, 0.0, masked_score)
    logit = product(act, forget_ref[...]) + bias_ref[...]
    logit_ref[...] = logit
    cumul = sum(product(allowed, part) for part in three_parts(log_sigmoid(logit)))
    def project(n, carry):
        first_load(n).wait()
        at = pl.ds(pl.multiple_of(n * 256, 256), 256)
        qkv_ref[:, at] = lower(product(act, b_in[:, at]))
        return carry

    lax.fori_loop(0, 3 * width // 256, project, 0)
    pair = HeadPair(tree_len, cumul)
    lse_ref[...] = jnp.zeros_like(lse_ref)

    def attend(p, carry):
        base = pl.multiple_of(p * 128, 128)
        query = qkv_ref[:, pl.ds(base, 128)]
        key = qkv_ref[:, pl.ds(base + width, 128)]
        value = qkv_ref[:, pl.ds(base + 2 * width, 128)]
        outs = []
        for side in range(2):
            q_side, k_side, mine = pair.augmented(2 * p + side, side, query, key)
            scores = dims_nt(q_side, k_side) + mask[...]
            peak = jnp.max(scores, axis=1, keepdims=True)
            probs = jnp.exp(scores - peak)
            count = jnp.sum(probs, axis=1, keepdims=True)
            outs.append(product(lower(probs * (1.0 / count)), value))
            lse_ref[...] = jnp.where(pair.lane == 2 * p + side, peak + jnp.log(count), lse_ref[...])
        att_ref[:, pl.ds(base, 128)] = lower(jnp.where(pair.lane < 64, outs[0], outs[1]))
        return carry

    lax.fori_loop(0, heads // 2, attend, 0)
    loads[1].wait()
    middle = x + product(att_ref[...], b_out[...])
    mid_ref[...] = middle
    _, _, act_b = norm_parts(middle, gain_ref[1:2, :])
    loads[2].wait()

    def stores(n):
        return [
            pltpu.make_async_copy(
                gu_buf.at[:, pl.ds(n * 512 + s * half, 512)], gu_ref.at[:, pl.ds(n * 512 + s * half, 512)], gu_sem.at[n, s]
            )
            for s in range(2)
        ]

    for n in range(half // 512):
        def expand(h, carry):
            at = pl.ds(pl.multiple_of(n * 512 + h * 256, 256), 256)
            at_up = pl.ds(pl.multiple_of(half + n * 512 + h * 256, 256), 256)
            gate = product(act_b, b_up[:, at])
            upper = product(act_b, b_up[:, at_up])
            gu_buf[:, at] = gate
            gu_buf[:, at_up] = upper
            hidden[:, at] = lower(gate / (1.0 + jnp.exp(-gate)) * upper)
            return carry

        lax.fori_loop(0, 2, expand, 0)
        for copy in stores(n):
            copy.start()
    loads[3].wait()

    def contract(n, carry):
        at = pl.ds(pl.multiple_of(n * 256, 256), 256)
        y_ref[:, at] = mid_ref[:, at] + product(hidden[...], b_down[:, at])
        return carry

    lax.fori_loop(0, width // 256, contract, 0)
    for n in range(half // 512):
        for copy in stores(n):
            copy.wait()


def layer_forward(layer, round_input, values, allowed, mats, forget_w, forget_b, gains):
    tree_len, width = values.shape
    w_in, w_out, w_up, w_down = mats
    half = w_down.shape[1]
    f32, b16 = jnp.float32, jnp.bfloat16
    shape = jax.ShapeDtypeStruct
    return pl.pallas_call(
        partial(forward_kernel, layer, round_input),
        out_shape=[
            shape((tree_len, width), f32),
            shape((tree_len, 3 * width), b16),
            shape((tree_len, 128), f32),
            shape((tree_len, 128), f32),
            shape((tree_len, width), b16),
            shape((tree_len, width), f32),
            shape((tree_len, 2 * half), f32),
        ],
        in_specs=[VMEM] * 2 + [ANY] * 4 + [VMEM] * 3,
        out_specs=[VMEM] * 6 + [ANY],
        scratch_shapes=[pltpu.VMEM(w.shape[1:], b16) for w in mats]
        + [
            pltpu.VMEM((tree_len, 2 * half), f32),
            pltpu.VMEM((tree_len, half), b16),
            pltpu.VMEM((tree_len, tree_len), f32),
            DMA((4,)),
            DMA((half // 512, 2)),
            DMA((3 * width // 256,)),
        ],
        compiler_params=pltpu.CompilerParams(vmem_limit_bytes=56 * 2**20),
        name=f"forward_{layer}",
    )(values, allowed, *mats, forget_w, forget_b, gains)


def backward_kernel(layer, round_input, round_grad, dy_ref, x_ref, allowed_ref, qkv_ref, logit_ref, lse_ref, att_ref,
                    mid_ref, forget_ref, gain_ref, gu_hbm, w_in, w_out, w_up, w_down,
                    dx_ref, dforget_ref, dgain_ref, dw_in, dw_out, dw_up, dw_down,
                    b_in, b_out, b_up, b_down, gu, dqkv, act_t, grad_b, mask, dcum,
                    g_in, g_out, g_up, g_down, sem, gu_sem, store_sem):
    tree_len, width = x_ref.shape
    heads = width // 64
    half = b_down.shape[0]
    chunk = 256
    loads = [
        pltpu.make_async_copy(src.at[layer], dst, sem.at[n]) for n, (src, dst) in enumerate(((w_in, b_in), (w_out, b_out)))
    ]
    def feed_loads(n):
        at = pl.ds(pl.multiple_of(n * chunk, chunk), chunk)
        at_up = pl.ds(pl.multiple_of(half + n * chunk, chunk), chunk)
        pairs = ((gu_hbm.at[:, at], gu.at[:, at]), (gu_hbm.at[:, at_up], gu.at[:, at_up]),
                 (w_down.at[layer, at], b_down.at[at]), (w_up.at[layer, :, at], b_up.at[:, at]),
                 (w_up.at[layer, :, at_up], b_up.at[:, at_up]))
        return [pltpu.make_async_copy(src, dst, gu_sem.at[n, s]) for s, (src, dst) in enumerate(pairs)]

    for n in range(half // chunk):
        for copy in feed_loads(n):
            copy.start()
    for n in (1, 0):
        loads[n].start()
    dy = dy_ref[...]
    if round_grad:
        dy = lower(dy).astype(jnp.float32)
    branch = lower(dy)
    normed_b, inverse_b, act_b = norm_parts(mid_ref[...], gain_ref[1:2, :])
    act_t[...] = lower((normed_b * gain_ref[1:2, :]).T)
    grad_b[...] = jnp.zeros_like(grad_b)

    def feed(n, carry):
        for copy in feed_loads(n):
            copy.wait()
        at = pl.ds(pl.multiple_of(n * chunk, chunk), chunk)
        at_up = pl.ds(pl.multiple_of(half + n * chunk, chunk), chunk)
        gate, upper = gu[:, at], gu[:, at_up]
        sigma = 1.0 / (1.0 + jnp.exp(-gate))
        silu = gate * sigma
        hidden = lower(silu * upper)
        grad_hidden = dims_nt(branch, b_down[at, :])
        g_down[at, :] = lower(dims_tn(hidden, branch))
        grad_gate = lower(grad_hidden * upper * sigma * (1.0 + gate * (1.0 - sigma)))
        grad_upper = lower(grad_hidden * silu)
        g_up[:, at] = lower(product(act_t[...], grad_gate))
        g_up[:, at_up] = lower(product(act_t[...], grad_upper))
        grad_b[...] += dims_nt(grad_gate, b_up[:, at]) + dims_nt(grad_upper, b_up[:, at_up])
        return carry

    lax.fori_loop(0, half // chunk, feed, 0)
    stores = [
        pltpu.make_async_copy(src, dst, store_sem.at[n])
        for n, (src, dst) in enumerate(((g_down, dw_down), (g_up, dw_up), (g_out, dw_out), (g_in, dw_in)))
    ]
    stores[0].start()
    stores[1].start()

    def norm_backward(grad, normed, inverse, gain):
        grad_normed = grad * gain
        back = inverse * (grad_normed - normed * jnp.mean(grad_normed * normed, axis=-1, keepdims=True))
        return back, jnp.sum(grad * normed, axis=0, keepdims=True)

    back_b, dgain_b = norm_backward(grad_b[...], normed_b, inverse_b, gain_ref[1:2, :])
    grad_mid = dy + back_b
    branch_a = lower(grad_mid)
    g_out[...] = lower(dims_tn(att_ref[...], branch_a))
    stores[2].start()
    loads[1].wait()
    att_ref_grad = lower(dims_nt(branch_a, b_out[...]))
    x = x_ref[...]
    if round_input:
        x = lower(x).astype(jnp.float32)
    normed_a, inverse_a, act_a = norm_parts(x, gain_ref[0:1, :])
    act_t[...] = lower((normed_a * gain_ref[0:1, :]).T)
    allowed = allowed_ref[...]
    mask[...] = jnp.where(allowed > 0, 0.0, masked_score)
    logit = logit_ref[...]
    cumul = sum(product(allowed, part) for part in three_parts(log_sigmoid(logit)))
    pair = HeadPair(tree_len, cumul)
    dcum[...] = jnp.zeros_like(dcum)
    grad_att = grad_b
    grad_att[...] = att_ref_grad.astype(jnp.float32)

    def attend(p, carry):
        base = pl.multiple_of(p * 128, 128)
        query = qkv_ref[:, pl.ds(base, 128)]
        key = qkv_ref[:, pl.ds(base + width, 128)]
        value = qkv_ref[:, pl.ds(base + 2 * width, 128)]
        grad_out = grad_att[:, pl.ds(base, 128)]
        grad_low = lower(grad_out)
        results = []
        for side in range(2):
            head = 2 * p + side
            start = 64 - 64 * side
            q_side, k_side, mine = pair.augmented(head, side, query, key)
            lse = jnp.sum(jnp.where(pair.lane == head, lse_ref[...], 0.0), axis=1, keepdims=True)
            probs = jnp.exp(dims_nt(q_side, k_side) + (mask[...] - lse))
            grad_probs = dims_nt(lower(jnp.where(mine, grad_out, 0.0)), value)
            weighted = probs * grad_probs
            row = jnp.sum(weighted, axis=1, keepdims=True)
            grad_scores = lower(weighted - probs * row)
            grad_value = dims_tn(lower(probs), grad_low)
            grad_query = product(grad_scores, k_side)
            grad_key = dims_tn(grad_scores, q_side)
            taken = jnp.sum(
                jnp.where(pair.lane == start, grad_query, 0.0) - jnp.where(pair.lane == start + 3, grad_key, 0.0),
                axis=1, keepdims=True,
            )
            dcum[...] = jnp.where(pair.lane == head, taken, dcum[...])
            results.append((grad_query * 0.125, grad_key, grad_value))
        for part in range(3):
            merged = jnp.where(pair.lane < 64, results[0][part], results[1][part])
            dqkv[:, pl.ds(base + part * width, 128)] = lower(merged)
        return carry

    lax.fori_loop(0, heads // 2, attend, 0)
    rising = sum(dims_tn(allowed, part) for part in three_parts(dcum[...]))
    grad_logit = rising / (1.0 + jnp.exp(logit))
    lane = lax.broadcasted_iota(jnp.int32, grad_logit.shape, 1)
    grad_logit = lower(jnp.where(lane < heads, grad_logit, 0.0))
    dforget_ref[:, 0:width] = dims_tn(grad_logit, act_a)[0:16, :]
    bias = dims_tn(grad_logit, jnp.ones((tree_len, 128), jnp.bfloat16))[0:16, :]
    dforget_ref[:, width : width + 128] = jnp.where(
        lax.broadcasted_iota(jnp.int32, (16, 128), 1) == 0, bias, 0.0
    )

    def weigh(n, carry):
        at = pl.ds(pl.multiple_of(n * 256, 256), 256)
        g_in[:, at] = lower(product(act_t[...], dqkv[:, at]))
        return carry

    lax.fori_loop(0, 3 * width // 256, weigh, 0)
    stores[3].start()
    loads[0].wait()
    grad_b[...] = dims_nt(grad_logit, forget_ref[...])

    def gather_back(n, carry):
        at = pl.ds(pl.multiple_of(n * 256, 256), 256)
        grad_b[...] += dims_nt(dqkv[:, at], b_in[:, at])
        return carry

    lax.fori_loop(0, 3 * width // 256, gather_back, 0)
    back_a, dgain_a = norm_backward(grad_b[...], normed_a, inverse_a, gain_ref[0:1, :])
    dx_ref[...] = grad_mid + back_a
    dgain_ref[...] = jnp.concatenate([dgain_a, dgain_b, jnp.zeros((6, width), jnp.float32)], axis=0)
    for copy in stores:
        copy.wait()


def layer_backward(layer, round_input, round_grad, grad, values, allowed, saved, mats, forget_w, gains):
    tree_len, width = values.shape
    qkv, logit, lse, att, middle, gate_up = saved
    w_in, w_out, w_up, w_down = mats
    half = w_down.shape[1]
    f32, b16 = jnp.float32, jnp.bfloat16
    shape = jax.ShapeDtypeStruct
    return pl.pallas_call(
        partial(backward_kernel, layer, round_input, round_grad),
        out_shape=[
            shape((tree_len, width), f32),
            shape((16, width + 128), f32),
            shape((8, width), f32),
        ]
        + [shape(w.shape[1:], b16) for w in mats],
        in_specs=[VMEM] * 10 + [ANY] * 5,
        out_specs=[VMEM] * 3 + [ANY] * 4,
        scratch_shapes=[pltpu.VMEM(w.shape[1:], b16) for w in mats]
        + [
            pltpu.VMEM((tree_len, 2 * half), f32),
            pltpu.VMEM((tree_len, 3 * width), b16),
            pltpu.VMEM((width, tree_len), b16),
            pltpu.VMEM((tree_len, width), f32),
            pltpu.VMEM((tree_len, tree_len), f32),
            pltpu.VMEM((tree_len, 128), f32),
        ]
        + [pltpu.VMEM(w.shape[1:], b16) for w in mats]
        + [DMA((4,)), DMA((half // 256, 5)), DMA((4,))],
        compiler_params=pltpu.CompilerParams(vmem_limit_bytes=60 * 2**20),
        name=f"backward_{layer}",
    )(grad, values, allowed, qkv, logit, lse, att, middle, forget_w, gains, gate_up, *mats)
def head_forward_kernel(rows_each, z_ref, table_ref, marks_ref, logits_ref, stats_ref):
    rows = z_ref.shape[0]
    chunk = 256 if table_ref.shape[0] % 256 == 0 else 128
    z = z_ref[...]

    def body(n, carry):
        peak, count, linear = carry
        at = pl.ds(pl.multiple_of(n * chunk, chunk), chunk)
        logits = dims_nt(z, table_ref[at, :])
        column = lax.broadcasted_iota(jnp.int32, (rows, chunk), 1) + n * chunk
        linear = linear + jnp.sum(logits * marks_ref[:, at], axis=1, keepdims=True)
        logits = jnp.where(column < rows_each, logits, masked_score)
        logits_ref[:, at] = logits
        new_peak = jnp.maximum(peak, jnp.max(logits, axis=1, keepdims=True))
        count = count * jnp.exp(peak - new_peak) + jnp.sum(jnp.exp(logits - new_peak), axis=1, keepdims=True)
        return new_peak, count, linear

    start = jnp.full((rows, 1), masked_score, jnp.float32)
    zero = jnp.zeros((rows, 1), jnp.float32)
    peak, count, linear = lax.fori_loop(0, table_ref.shape[0] // chunk, body, (start, zero, zero))
    lane = lax.broadcasted_iota(jnp.int32, (rows, 128), 1)
    stats = jnp.where(lane == 0, peak, jnp.where(lane == 1, count, jnp.where(lane == 2, linear, 0.0)))
    stats_ref[...] = stats.T[0:4, :]


def head_forward(rows_each, z, table, marks):
    rows, width = z.shape[0], table.shape[0]
    return pl.pallas_call(
        partial(head_forward_kernel, rows_each),
        out_shape=[jax.ShapeDtypeStruct((rows, width), jnp.float32), jax.ShapeDtypeStruct((4, rows), jnp.float32)],
        in_specs=[VMEM] * 3,
        out_specs=[VMEM] * 2,
        name="head_forward",
    )(z, table, marks)


def head_backward_kernel(sections, span, pos_all, z_ref, table_ref, marks_ref, logits_ref, stats_ref,
                         prob_ref, dz_ref, dtable_ref, row_ref, grads):
    rows, width = logits_ref.shape
    peak = jnp.max(stats_ref[:, 0, :], axis=0, keepdims=True)
    count = jnp.sum(stats_ref[:, 1, :] * jnp.exp(stats_ref[:, 0, :] - peak), axis=0, keepdims=True)
    log_norm = peak + jnp.log(count)
    prob = prob_ref[...]
    prob_sum = jnp.sum(prob, axis=1, keepdims=True)
    entropy = jnp.sum(prob * jnp.log(prob), axis=1, keepdims=True)
    log_norm = jnp.broadcast_to(log_norm, (128, rows)).T[:, 0:1]
    whole = jnp.sum(log_norm * (1.0 + prob_sum) + entropy) - jnp.sum(stats_ref[:, 2, :])
    row_ref[...] = jnp.full((8, 128), whole)
    chunk = 256 if width % 256 == 0 else 128
    weight = 1.0 + prob_sum

    def body(n, carry):
        at = pl.ds(pl.multiple_of(n * chunk, chunk), chunk)
        grad = (weight * jnp.exp(logits_ref[:, at] - log_norm) - marks_ref[:, at]) * (1.0 / pos_all)
        grads[:, at] = lower(grad)
        dtable_ref[at, :] = dims_tn(lower(grad), z_ref[...])
        return carry

    lax.fori_loop(0, width // chunk, body, 0)
    section = lax.axis_index("section")
    for r in range(rows // (sections * span)):
        at = pl.ds(pl.multiple_of((r * sections + section) * span, span), span)
        dz_ref[r * span : (r + 1) * span, :] = lower(product(grads[at, :], table_ref[...]))


def head_backward(z, table, marks, logits, stats_all, prob, span, pos_all):
    rows, width = logits.shape
    sections = lax.axis_size("section")
    return pl.pallas_call(
        partial(head_backward_kernel, sections, span, pos_all),
        out_shape=[
            jax.ShapeDtypeStruct((rows // sections, z.shape[1]), jnp.bfloat16),
            jax.ShapeDtypeStruct((width, z.shape[1]), jnp.float32),
            jax.ShapeDtypeStruct((8, 128), jnp.float32),
        ],
        in_specs=[VMEM] * 6,
        out_specs=[VMEM] * 3,
        scratch_shapes=[pltpu.VMEM((rows, width), jnp.bfloat16)],
        name="head_backward",
    )(z, table, marks, logits, stats_all, prob)
def pieces_of(rows):
    part = 400 if rows % 400 == 0 else rows
    return [(at, part) for at in range(0, rows, part)]


def each_tile(rows, columns, fn, carry):
    step = 16
    wide = 256 if columns % 256 == 0 else columns

    def body(n, carry):
        at = pl.ds(pl.multiple_of(n * step, step), step)
        for c in range(0, columns, wide):
            carry = fn(at, slice(c, c + wide), carry)
        return carry

    carry = lax.fori_loop(0, rows // step, body, carry)
    if rows % step:
        at = slice(rows // step * step, rows)
        tail = [jnp.zeros((rows % step, wide), jnp.float32)] * 2
        for c in range(0, columns, wide):
            tail = fn(at, slice(c, c + wide), tail)
        carry = [carry[0], carry[1]] + [jnp.sum(t) for t in tail]
    return carry


def step_kernel(shapes, scalar_ref, sums_ref, *refs):
    n = len(shapes)
    small_sums, refs = refs[:5], refs[5:]
    small_in, refs = refs[:6], refs[6:]
    grads, refs = refs[:n], refs[n:]
    weights, refs = refs[:n], refs[n:]
    firsts, refs = refs[:n], refs[n:]
    seconds, refs = refs[:n], refs[n:]
    out_first, refs = refs[:n], refs[n:]
    out_second, refs = refs[:n], refs[n:]
    out_dir, refs = refs[:n], refs[n:]
    small_out, refs = refs[:6], refs[6:]
    norm_ref, small_norm_ref, refs = refs[0], refs[1], refs[2:]
    g_buf, refs = refs[:n], refs[n:]
    w_buf, refs = refs[:n], refs[n:]
    m_buf, refs = refs[:n], refs[n:]
    v_buf, refs = refs[:n], refs[n:]
    d_buf, refs = refs[:n], refs[n:]
    load_sem, store_sem = refs
    work = []
    for a in range(n):
        for at, part in pieces_of(shapes[a][0]):
            rows = pl.ds(at, part)
            p = len(work)
            loads = [
                pltpu.make_async_copy(src.at[rows], dst.at[rows], load_sem.at[p, q])
                for q, (src, dst) in enumerate(
                    ((grads[a], g_buf[a]), (weights[a], w_buf[a]), (firsts[a], m_buf[a]), (seconds[a], v_buf[a]))
                )
            ]
            stores = [
                pltpu.make_async_copy(src.at[rows], dst.at[rows], store_sem.at[p, q])
                for q, (src, dst) in enumerate(
                    ((m_buf[a], out_first[a]), (v_buf[a], out_second[a]), (d_buf[a], out_dir[a]))
                )
            ]
            work.append((a, at, part, loads, stores))
    for _, _, _, loads, _ in work:
        for copy in loads:
            copy.start()
    lane = lax.broadcasted_iota(jnp.int32, (8, 128), 1)
    row = lax.broadcasted_iota(jnp.int32, (8, 128), 0)

    def scalar_at(values, r, c):
        return jnp.sum(jnp.where((row == r) & (lane == c), values, 0.0))

    smalls = [ref[...] for ref in small_sums]
    norm = jnp.sqrt(
        jnp.full((1, 1), scalar_at(sums_ref[...], 0, 0) + sum(square_sum(v) for v in smalls))
    )
    clip = jnp.minimum(1.0, scalar_ref[2] / norm)
    inverse_first = scalar_ref[0]
    inverse_second = scalar_ref[1]

    def adam(weight, grad, first, second):
        scaled = clip * grad
        first_new = beta_first * first + (1.0 - beta_first) * scaled
        second_new = beta_second * second + (1.0 - beta_second) * scaled * scaled
        direction = (first_new * inverse_first) / (
            jnp.sqrt(second_new * inverse_second) + adam_eps
        ) + decay_rate * weight
        return first_new, second_new, direction

    def small_step(group, part, grad):
        w_ref, m_ref, v_ref = small_in[3 * group : 3 * group + 3]
        weight = w_ref[part]
        first_new, second_new, direction = adam(weight, grad, m_ref[part], v_ref[part])
        norms = [jnp.sqrt(jnp.full((1, 1), square_sum(v))) for v in (weight, direction)]
        small_out[3 * group][part] = weight - learn_rate * (norms[0] / norms[1]) * direction
        small_out[3 * group + 1][part] = first_new
        small_out[3 * group + 2][part] = second_new
        return norms

    features, heads = small_in[0].shape[1:]
    small_norms = []
    for layer in range(2):
        small_norms += small_step(0, layer, smalls[layer].T[0:features, 0:heads])
    for t in range(5):
        grad = smalls[2 + t // 2][t % 2 : t % 2 + 1, :]
        small_norms += small_step(1, slice(t, t + 1), grad)
    table = jnp.where((row == 0) & (lane == 0), norm, 0.0)
    for t, value in enumerate(small_norms):
        table = jnp.where((row == 1) & (lane == t), value, table)
    small_norm_ref[...] = table

    sums = [[jnp.float32(0), jnp.float32(0)] for _ in range(n)]
    for a, at, part, loads, stores in work:
        for copy in loads:
            copy.wait()
        g, w, m, v, d = (buf[a].at[pl.ds(at, part)] for buf in (g_buf, w_buf, m_buf, v_buf, d_buf))
        columns = shapes[a][1]
        wide = 256 if columns % 256 == 0 else columns

        def tile(rows, cols, carry):
            weight = w[rows, cols]
            first_new, second_new, direction = adam(
                weight, g[rows, cols].astype(jnp.float32), m[rows, cols], v[rows, cols]
            )
            m[rows, cols] = first_new
            v[rows, cols] = second_new
            d[rows, cols] = direction
            return [carry[0] + weight * weight, carry[1] + direction * direction]

        zero = jnp.zeros((16, wide), jnp.float32)
        done = each_tile(part, columns, tile, [zero, zero])
        for copy in stores:
            copy.start()
        for q in range(2):
            sums[a][q] = sums[a][q] + jnp.sum(done[q])
            if len(done) > 2:
                sums[a][q] = sums[a][q] + done[2 + q]
    section = lax.axis_index("section")
    table = jnp.zeros((8, 128), jnp.float32)
    for a in range(n):
        here = (section if a == 0 else lax.axis_index("replica")) == 0
        place = 0 if a == 0 else 2 * section
        for q in range(2):
            value = jnp.where(here, sums[a][q], 0.0)
            table = jnp.where((row == a) & (lane == place + q), value, table)
    norm_ref[...] = table
    for _, _, _, _, stores in work:
        for copy in stores:
            copy.wait()


def optimizer_step(scalars, sums, small_sums, small, grads, weights, firsts, seconds):
    n = len(grads)
    shapes = [w.shape for w in weights]
    flat = [jax.ShapeDtypeStruct(s, jnp.float32) for s in shapes]
    buffers = lambda kinds: [pltpu.VMEM(s, k) for s, k in zip(shapes, kinds)]
    parts = sum(len(pieces_of(s[0])) for s in shapes)
    out = pl.pallas_call(
        partial(step_kernel, shapes),
        out_shape=flat * 3
        + [jax.ShapeDtypeStruct(s.shape, jnp.float32) for s in small]
        + [jax.ShapeDtypeStruct((8, 128), jnp.float32)] * 2,
        in_specs=[pl.BlockSpec(memory_space=pltpu.SMEM)] + [VMEM] * 12 + [ANY] * (4 * n),
        out_specs=[ANY] * (3 * n) + [VMEM] * 8,
        scratch_shapes=buffers([g.dtype for g in grads])
        + buffers([jnp.float32] * n) * 4
        + [DMA((parts, 4)), DMA((parts, 3))],
        compiler_params=pltpu.CompilerParams(vmem_limit_bytes=60 * 2**20),
        name="optimizer_step",
    )(scalars, sums, *small_sums, *small, *grads, *weights, *firsts, *seconds)
    return out[:n], out[n : 2 * n], out[2 * n : 3 * n], out[3 * n : 3 * n + 6], out[-2], out[-1]


def apply_kernel(shapes, norm_ref, *refs):
    n = len(shapes)
    norms = jnp.sqrt(norm_ref[...])
    lane = lax.broadcasted_iota(jnp.int32, (8, 128), 1)
    row = lax.broadcasted_iota(jnp.int32, (8, 128), 0)

    def norm_at(a, q):
        place = q if a == 0 else 2 * lax.axis_index("section") + q
        return jnp.full((1, 1), jnp.sum(jnp.where((row == a) & (lane == place), norms, 0.0)))

    weights, directions, outs = refs[:n], refs[n : 2 * n], refs[2 * n : 3 * n]
    w_buf, d_buf = refs[3 * n : 4 * n], refs[4 * n : 5 * n]
    load_sem, store_sem = refs[5 * n :]
    work = []
    for a in range(n):
        for at, part in pieces_of(shapes[a][0]):
            rows = pl.ds(at, part)
            p = len(work)
            loads = [
                pltpu.make_async_copy(weights[a].at[rows], w_buf[a].at[rows], load_sem.at[p, 0]),
                pltpu.make_async_copy(directions[a].at[rows], d_buf[a].at[rows], load_sem.at[p, 1]),
            ]
            store = pltpu.make_async_copy(w_buf[a].at[rows], outs[a].at[rows], store_sem.at[p])
            work.append((a, at, part, loads, store))
    for _, _, _, loads, _ in work:
        for copy in loads:
            copy.start()
    for a, at, part, loads, store in work:
        for copy in loads:
            copy.wait()
        w, d = w_buf[a].at[pl.ds(at, part)], d_buf[a].at[pl.ds(at, part)]
        rate = learn_rate * (norm_at(a, 0) / norm_at(a, 1))

        def tile(rows, cols, carry):
            w[rows, cols] = w[rows, cols] - rate * d[rows, cols]
            return carry

        each_tile(part, shapes[a][1], tile, [jnp.float32(0), jnp.float32(0)])
        store.start()
    for _, _, _, _, store in work:
        store.wait()


def apply_step(norms, weights, directions):
    n = len(weights)
    shapes = [w.shape for w in weights]
    parts = sum(len(pieces_of(s[0])) for s in shapes)
    return pl.pallas_call(
        partial(apply_kernel, shapes),
        out_shape=[jax.ShapeDtypeStruct(s, jnp.float32) for s in shapes],
        in_specs=[VMEM] + [ANY] * (2 * n),
        out_specs=[ANY] * n,
        scratch_shapes=[pltpu.VMEM(s, jnp.float32) for s in shapes] * 2 + [DMA((parts, 2)), DMA((parts,))],
        compiler_params=pltpu.CompilerParams(vmem_limit_bytes=62 * 2**20),
        name="apply_step",
    )(norms, *weights, *directions)


def lower(values):
    return values.astype(jnp.bfloat16)


def product(left, right):
    return jnp.dot(left, right, preferred_element_type=jnp.float32)


def product_left(left, right):
    return lax.dot_general(left, right, (((0,), (0,)), ((), ())), preferred_element_type=jnp.float32)


def product_right(left, right):
    return lax.dot_general(left, right, (((1,), (1,)), ((), ())), preferred_element_type=jnp.float32)


def rms_forward(values, gain):
    inverse = lax.rsqrt(jnp.mean(values * values, axis=-1, keepdims=True) + eps_norm)
    normed = values * inverse
    return (normed * gain, normed, inverse)


def rms_backward(grad_out, normed, inverse, gain):
    grad_normed = grad_out * gain
    grad_in = inverse * (
        grad_normed - normed * jnp.mean(grad_normed * normed, axis=-1, keepdims=True)
    )
    return (grad_in, jnp.sum(grad_out * normed, axis=0))


def path_mask(parent_row, tree_len):
    seg_count = parent_row.shape[0]
    seglen = tree_len // seg_count
    seg_order = jnp.arange(seg_count, dtype=jnp.int32)
    parent_hot = ((parent_row[:, None] == seg_order[None, :]) & (seg_order[:, None] >= 1)).astype(
        jnp.float32
    )
    identity = jnp.eye(seg_count, dtype=jnp.float32)
    power, steps = parent_hot, 1
    reached = identity + parent_hot
    while steps < seg_count:
        reached = jnp.minimum(1.0, jnp.dot(reached, reached))
        steps *= 2
    strict = reached - identity
    seg_of = jnp.arange(tree_len, dtype=jnp.int32) // seglen
    seg_hot = (seg_of[:, None] == seg_order[None, :]).astype(jnp.float32)
    ancestor = jnp.dot(jnp.dot(seg_hot, strict), seg_hot.T)
    places = jnp.arange(tree_len, dtype=jnp.int32)
    inside = (seg_of[:, None] == seg_of[None, :]) & (places[None, :] <= places[:, None])
    return ancestor + inside.astype(jnp.float32)


def square_sum(values):
    return jnp.sum(values * values)


def local(
    tokens,
    parents,
    loss_positions,
    targets,
    teacher_index,
    teacher_probability,
    step_count,
    embed_table,
    table_first,
    table_second,
    attention_in,
    attention_in_first,
    attention_in_second,
    attention_out,
    attention_out_first,
    attention_out_second,
    feedforward_in,
    feedforward_in_first,
    feedforward_in_second,
    feedforward_out,
    feedforward_out_first,
    feedforward_out_second,
    forget_gate,
    forget_first,
    forget_second,
    norm_gains,
    gains_first,
    gains_second,
):
    section_id = lax.axis_index("section")
    replica_id = lax.axis_index("replica")
    shard_id = lax.axis_index("shard")
    sections = lax.axis_size("section")
    replicas = lax.axis_size("replica")
    shards = lax.axis_size("shard")
    group_trees, tree_len = tokens.shape
    rows_each, width = embed_table.shape
    pos_count = loss_positions.shape[1]
    pos_all = group_trees * replicas * pos_count
    owners = replicas * shards
    owner_id = replica_id * shards + shard_id
    own_tree = section_id * shards + shard_id
    table_low = lower(embed_table)

    def own_row(values):
        return lax.dynamic_index_in_dim(values, own_tree, 0, keepdims=False)

    tree_tokens = own_row(tokens)
    token_owner = tree_tokens // rows_each
    token_row = tree_tokens % rows_each
    spots = jnp.arange(tree_len, dtype=jnp.int32)

    def asked(batch):
        earlier = spots[None, :] < spots[:, None]
        same = tree_tokens[:, None] == tree_tokens[None, :]
        is_first = jnp.logical_not(jnp.any(same & earlier, axis=1))
        counted = earlier & (token_owner[:, None] == token_owner[None, :]) & is_first[None, :]
        number_first = jnp.sum(counted.astype(jnp.int32), axis=1)
        number = jnp.sum(jnp.where(same & is_first[None, :], number_first[None, :], 0), axis=1)
        slot = number - batch * batch_rows
        inside = (slot >= 0) & (slot < batch_rows)
        place = jnp.where(inside, token_owner * batch_rows + slot, -1)
        spot_of = jnp.arange(owners * batch_rows, dtype=jnp.int32)
        hot = place[None, :] == spot_of[:, None]
        rows = jnp.max(jnp.where(hot & is_first[None, :], token_row[None, :] + 1, 0), axis=1)
        return rows.reshape(owners, batch_rows), lower(hot)

    def all_devices(part, ident):
        return exchange(part[None], ident, relay=True).reshape((sections, replicas, shards) + part.shape)

    def wanted(batch):
        rows, hot = asked(batch)
        every = all_devices(jnp.pad(rows, ((0, 0), (0, 128 - batch_rows))), 0)
        mine = lax.dynamic_index_in_dim(every, owner_id, 3, keepdims=False)[..., :batch_rows]
        wish = mine.reshape(sections * owners * batch_rows) - 1
        row_of = jnp.arange(rows_each, dtype=jnp.int32)
        return hot, lower(wish[:, None] == row_of[None, :])

    def more_rows(state):
        batch, total_rows = state
        hot_more, pick = wanted(batch)
        own_pick = lax.dynamic_index_in_dim(
            pick.reshape(sections, owners * batch_rows, rows_each), section_id, 0, keepdims=False
        )
        sent = lower(product(own_pick, table_low)).reshape(owners, batch_rows, width)
        got_more = exchange(sent, 1)[0].reshape(owners * batch_rows, width)
        return (batch + 1, total_rows + product_left(hot_more, got_more))

    def more_grads(state):
        batch, total_rows = state
        hot_more, pick = wanted(batch)
        sent = lower(product(hot_more, embed_low)).reshape(owners, batch_rows, width)
        got_more = exchange(sent, 6, relay=True).reshape(sections * owners * batch_rows, width)
        more = product_left(pick, got_more)
        return (batch + 1, total_rows + jnp.pad(more, ((0, width_all - rows_each), (0, 0))))

    def halves(weight):
        return lower(weight).reshape(2, weight.shape[1] // 2, weight.shape[2])

    width_all = -(-rows_each // 128) * 128
    table_wide = jnp.pad(table_low, ((0, width_all - rows_each), (0, 0)))
    layer_weights = (attention_in, attention_out, feedforward_in, feedforward_out)
    entries = 8 * teacher_index.shape[2]
    group_data = [
        teacher_index.reshape(-1, 1, entries),
        teacher_probability.reshape(-1, 1, entries),
        targets.reshape(-1, 1),
    ]
    pair_parts = group_data if replicas == 2 else []
    hot, asks = ask_rows(tree_tokens, token_owner, token_row, owners)
    gathered, group_all, (asked_all, got, *marks) = gather(
        [halves(w) for w in layer_weights], 2, pair_parts, split=True, errand=(asks, table_wide), rows_each=rows_each
    )
    if replicas != 2:
        group_all = [lax.all_gather(part, "replica") for part in group_data]
        marks = [spread_entries((owner_id * rows_each)[None], *group_all, rows_each, width_all)]
    batches = (jnp.max(asked_all[:, :, 0, 127]) + batch_rows - 1) // batch_rows
    embeds = product_left(hot, got.reshape(owners * batch_rows, width))
    _, embeds = lax.while_loop(lambda s: s[0] < batches, more_rows, (jnp.int32(1), embeds))
    mats = [g.reshape(sections, -1, g.shape[-1]) for g in gathered]
    heads = forget_gate.shape[2]
    forget_low = jnp.pad(lower(forget_gate[:, :width]), ((0, 0), (0, 0), (0, 128 - heads)))
    forget_bias = jnp.pad(forget_gate[:, width:], ((0, 0), (0, 0), (0, 128 - heads)))
    gains_of = [jnp.pad(norm_gains[2 * n : 2 * n + 2], ((0, 6), (0, 0))) for n in range(2)]

    allowed = lower(path_mask(own_row(parents), tree_len))
    out_0, *saved_0 = layer_forward(0, False, embeds, allowed, mats, forget_low[0], forget_bias[0], gains_of[0])
    out_1, *saved_1 = layer_forward(1, True, out_0, allowed, mats, forget_low[1], forget_bias[1], gains_of[1])

    positions = own_row(loss_positions)
    position_hot = (positions[:, None] == spots[None, :]).astype(jnp.float32)
    picked = jnp.take(out_1, positions, axis=0)
    final_gain = norm_gains[4]
    head_out, head_normed, head_inverse = rms_forward(picked, final_gain)
    head_rows = jnp.swapaxes(all_devices(lower(head_out), 3), 0, 1).reshape(pos_all, width)

    prob_all = group_all[1].reshape(pos_all, -1)
    marks = marks[0]
    logits, stats = head_forward(rows_each, head_rows, table_wide, marks)
    if replicas == 2:
        stats_all = exchange(stats[None], 4)[0]
    else:
        stats_all = lax.all_gather(lax.all_gather(stats, "replica"), "shard")
    grad_heads, head_table, loss_sum = head_backward(
        head_rows, table_wide, marks, logits, stats_all.reshape(owners, 4, pos_all), prob_all, shards * pos_count, pos_all
    )
    grad_heads = exchange(grad_heads.reshape(owners, pos_count, width), 5)[0]
    grad_heads = jnp.sum(grad_heads.astype(jnp.float32), axis=0)
    grad_picked, grad_final = rms_backward(grad_heads, head_normed, head_inverse, final_gain)
    grad_top = lax.dot_general(
        position_hot, grad_picked, (((0,), (0,)), ((), ())), precision=highest
    )

    grad_mid, forget_1, gains_1, *grads_1 = layer_backward(
        1, True, False, grad_top, out_0, allowed, saved_1, mats, forget_low[1], gains_of[1]
    )
    grad_low, forget_0, gains_0, *grads_0 = layer_backward(
        0, False, True, grad_mid, embeds, allowed, saved_0, mats, forget_low[0], gains_of[0]
    )
    embed_low = lower(grad_low)

    stacked = [
        [g.reshape(shards, 2, -1, g.shape[-1]) for g in pair] for pair in zip(grads_0, grads_1)
    ]
    sent = lower(product(hot, embed_low)).reshape(owners, batch_rows, width)
    small_sums = [forget_0, forget_1, gains_0, gains_1, grad_final[None]]
    layer_grads, (*small_sums, got_grads) = reduce_parts(stacked, 8, (small_sums, sent))
    if replicas != 2:
        layer_grads = [lax.psum(g * jnp.bfloat16(0.5), "replica") for g in layer_grads]
    _, head_table = lax.while_loop(lambda s: s[0] < batches, more_grads, (jnp.int32(1), head_table))
    table_grad, square = table_gradient(
        rows_each, asked_all, got_grads.reshape(-1, width), head_table, layer_grads
    )
    layer_grads = [g.reshape(w.shape[1:]) for g, w in zip(layer_grads, layer_weights)]
    (scalars,) = total([square], 15)
    loss_total = loss_sum[0, 0] / pos_all
    count_float = step_count.astype(jnp.float32)
    rates = jnp.stack(
        [
            1.0 / (1.0 - jnp.power(beta_first, count_float)),
            1.0 / (1.0 - jnp.power(beta_second, count_float)),
            clip_factor / jnp.sqrt(jnp.float32(pos_all)),
        ]
    )
    small = [forget_gate, forget_first, forget_second, norm_gains, gains_first, gains_second]
    weights = [embed_table] + [w[0] for w in layer_weights]
    firsts = [table_first] + [
        m[0] for m in (attention_in_first, attention_out_first, feedforward_in_first, feedforward_out_first)
    ]
    seconds = [table_second] + [
        m[0] for m in (attention_in_second, attention_out_second, feedforward_in_second, feedforward_out_second)
    ]
    firsts_new, seconds_new, directions, small_new, norms, small_norms = optimizer_step(
        rates, scalars, small_sums, small, [table_grad, *layer_grads], weights, firsts, seconds
    )
    (norms,) = total([norms], 16)
    weights_new = apply_step(norms, weights, directions)
    norms = jnp.sqrt(norms)
    table_norms = norms[0, :2]
    layer_norms = norms[1:5, : 2 * sections].reshape(4 * sections, 2)
    new_table, table_first_new, table_second_new = weights_new[0], firsts_new[0], seconds_new[0]
    new_layers = [(weights_new[n][None], firsts_new[n][None], seconds_new[n][None]) for n in range(1, 5)]
    new_forget, forget_first_new, forget_second_new, new_gains, gains_first_new, gains_second_new = small_new
    layer_count, gain_count = forget_gate.shape[0], norm_gains.shape[0]
    grad_norm = small_norms[0, 0]
    tensor_norms = jnp.concatenate(
        [
            table_norms[None],
            layer_norms,
            small_norms[1, : 2 * (layer_count + gain_count)].reshape(-1, 2),
        ],
        axis=0,
    )
    return (
        new_table,
        table_first_new,
        table_second_new,
        *new_layers[0],
        *new_layers[1],
        *new_layers[2],
        *new_layers[3],
        new_forget,
        forget_first_new,
        forget_second_new,
        new_gains,
        gains_first_new,
        gains_second_new,
        tensor_norms,
        grad_norm,
        loss_total,
    )


def solution(mesh):
    group = P("replica", None)
    table = P(("replica", "shard"), None)
    layer = P("section", "shard", None)
    in_specs = (
        (group,) * 4
        + (P("replica", None, None),) * 2
        + (P(),)
        + (table,) * 3
        + (layer,) * 12
        + (P(),) * 6
    )
    out_specs = (table,) * 3 + (layer,) * 12 + (P(),) * 9
    return jax.shard_map(local, mesh=mesh, in_specs=in_specs, out_specs=out_specs, check_vma=False)
```

```python
from functools import partial

import jax
import jax.numpy as jnp
from jax import lax
from jax.experimental import pallas as pl
from jax.experimental.pallas import tpu as pltpu
from jax.sharding import PartitionSpec as P

MESH = pl.DeviceIdType.MESH
VMEM = pl.BlockSpec(memory_space=pltpu.VMEM)
ANY = pl.BlockSpec(memory_space=pl.ANY)
DMA = pltpu.SemaphoreType.DMA
eps_norm = 1e-06
beta_first = 0.9
beta_second = 0.999
adam_eps = 1e-10
decay_rate = 0.01
learn_rate = 0.2
clip_factor = 8.0
highest = lax.Precision.HIGHEST
masked_score = -1e30
batch_rows = 32
every_axis = ("section", "replica", "shard")


class Place:
    def __init__(self):
        self.sections = lax.axis_size("section")
        self.replicas = lax.axis_size("replica")
        self.shards = lax.axis_size("shard")
        self.nz = min(4, self.shards)
        self.ny = self.shards // self.nz
        self.x = lax.axis_index("section")
        self.rep = lax.axis_index("replica")
        self.shard = lax.axis_index("shard")
        self.core = lax.rem(self.rep, 2)
        self.z = self.shard // self.ny
        self.y = lax.rem(self.shard, self.ny)

    def at(self, section=None, rep=None, z=None, y=None, shard=None):
        if shard is None:
            shard = (self.z if z is None else z) * self.ny + (self.y if y is None else y)
        return {
            "section": self.x if section is None else section,
            "replica": self.rep if rep is None else rep,
            "shard": shard,
        }

    def peer_x(self, i):
        return self.at(section=lax.rem(self.x + i, self.sections))

    def peer_y(self, j):
        return self.at(y=lax.rem(self.y + j, self.ny))

    def line(self, step):
        return self.at(z=self.z + step)

    def partner(self):
        return self.at(rep=self.rep + 1 - 2 * self.core)

    def group(self, p):
        count = self.replicas * self.shards
        place = lax.rem(self.rep * self.shards + self.shard + p, count)
        return place, self.at(rep=place // self.shards, shard=lax.rem(place, self.shards))

    def device(self, i, p):
        place, _ = self.group(p)
        section = lax.rem(self.x + i, self.sections)
        return place, self.at(section=section, rep=place // self.shards, shard=lax.rem(place, self.shards))

    def greet_all(self):
        barrier = pltpu.get_barrier_semaphore()
        peers = self.replicas * self.shards
        for i in range(self.sections):
            for p in range(peers):
                if i or p:
                    pl.semaphore_signal(barrier, inc=1, device_id=self.device(i, p)[1], device_id_type=MESH)
        pl.semaphore_wait(barrier, self.sections * peers - 1)

    def greet_group(self):
        barrier = pltpu.get_barrier_semaphore()
        peers = self.replicas * self.shards
        for p in range(1, peers):
            pl.semaphore_signal(barrier, inc=1, device_id=self.group(p)[1], device_id_type=MESH)
        for i in range(1, self.sections):
            pl.semaphore_signal(barrier, inc=1, device_id=self.peer_x(i), device_id_type=MESH)
        pl.semaphore_wait(barrier, peers + self.sections - 2)

    def inside(self, k):
        if k == 0:
            return None
        return self.z + k < self.nz if k > 0 else self.z + k >= 0

    def greet(self, use_x=True):
        barrier = pltpu.get_barrier_semaphore()

        def signal(device):
            pl.semaphore_signal(barrier, inc=1, device_id=device, device_id_type=MESH)

        count = 1
        if use_x:
            for i in range(1, self.sections):
                signal(self.peer_x(i))
                count += 1
        for j in range(1, self.ny):
            signal(self.peer_y(j))
            count += 1
        signal(self.partner())
        up, down = self.inside(1), self.inside(-1)
        pl.when(up)(lambda: signal(self.line(1)))
        pl.when(down)(lambda: signal(self.line(-1)))
        ends = jnp.minimum(self.z, 1) + jnp.minimum(self.nz - 1 - self.z, 1)
        pl.semaphore_wait(barrier, count + ends)


def when(cond, fn):
    if cond is None:
        fn()
    else:
        pl.when(cond)(fn)


def both(a, b):
    if a is None:
        return b
    if b is None:
        return a
    return jnp.logical_and(a, b)


def remote(src, dst, send, recv, device):
    return pltpu.make_async_remote_copy(
        src_ref=src, dst_ref=dst, send_sem=send, recv_sem=recv, device_id=device, device_id_type=MESH
    )


def rows_errand(me, ask_ref, table_ref, asked_ref, got_ref, hot, found, ask_sem, row_sem, own_sem):
    peers = me.replicas * me.shards
    mine = me.rep * me.shards + me.shard
    width = table_ref.shape[1]
    asks = []
    for i in range(me.sections):
        for p in range(peers):
            place, device = me.device(i, p)
            if i or p:
                asks.append(remote(ask_ref.at[place], asked_ref.at[me.x, mine], ask_sem.at[0, i, p], ask_sem.at[1, i, p], device))
    for copy in asks:
        copy.start()
    own_ask = pltpu.make_async_copy(ask_ref.at[mine], asked_ref.at[me.x, mine], own_sem.at[0])
    own_ask.start()
    rows = [
        remote(found.at[me.group(p)[0]], got_ref.at[mine], row_sem.at[0, p], row_sem.at[1, p], me.group(p)[1])
        for p in range(1, peers)
    ]
    own_rows = pltpu.make_async_copy(found.at[mine], got_ref.at[mine], own_sem.at[1])

    def look_up():
        own_ask.wait()
        for i in range(me.sections):
            for p in range(peers):
                if i or p:
                    source = lax.rem(mine + peers - p, peers)
                    dst = asked_ref.at[lax.rem(me.x + me.sections - i, me.sections), source]
                    remote(dst, dst, ask_sem.at[0, i, p], ask_sem.at[1, i, p], me.partner()).wait_recv()
        wish = asked_ref[me.x].reshape(peers, 128).astype(jnp.float32).T
        column = lax.broadcasted_iota(jnp.int32, (batch_rows, table_ref.shape[0]), 1).astype(jnp.float32) + 1.0
        for s in range(peers):
            ours = wish[0:batch_rows, s : s + 1] == column
            hot[s * batch_rows : (s + 1) * batch_rows, :] = jnp.where(ours, 1.0, 0.0).astype(jnp.bfloat16)

        def take(n, carry):
            at = pl.ds(pl.multiple_of(n * 256, 256), 256)
            values = jnp.dot(hot[...], table_ref[:, at], preferred_element_type=jnp.float32)
            found[:, :, at] = values.reshape(peers, batch_rows, 256).astype(jnp.bfloat16)
            return carry

        lax.fori_loop(0, width // 256, take, 0)
        own_rows.start()
        for copy in rows:
            copy.start()

    def finish():
        for p in range(1, peers):
            source = lax.rem(mine + peers - p, peers)
            dst = got_ref.at[source]
            remote(dst, dst, row_sem.at[0, p], row_sem.at[1, p], me.partner()).wait_recv()
        own_rows.wait()
        for copy in asks + rows:
            copy.wait_send()

    return {1: look_up, "end": finish}


def gather_kernel(count, pairs, split, orders, errand, *refs):
    ins, refs = refs[:count], refs[count:]
    pair_ins, refs = refs[:pairs], refs[pairs:]
    asked = 2 if errand else 0
    errand_in, refs = refs[:asked], refs[asked:]
    outs, refs = refs[:count], refs[count:]
    pair_outs, refs = refs[:pairs], refs[pairs:]
    errand_out, refs = refs[:asked], refs[asked:]
    if errand and pairs:
        marks_ref, refs = refs[0], refs[1:]
    errand_refs = errand_in + errand_out
    send_sem, recv_sem, cross_sem, pair_sem, local_sem = refs[:5]
    me = Place()
    nz, ny, nx = me.nz, me.ny, me.sections
    if "x" not in orders[0][0][0]:
        nx = 1
    hooks = {}
    if errand:
        me.greet_all()
        hooks = rows_errand(me, *errand_refs, *refs[5:])
    else:
        me.greet(use_x=nx > 1)

    def slot(ref, k, j, i, half):
        section = lax.rem(me.x + i, nx) if nx > 1 else 0
        return ref.at[section, (me.z + k) * ny + lax.rem(me.y + j, ny), half]

    locals_ = []
    for a in range(count):
        if split:
            dst = outs[a].at[me.x if nx > 1 else 0, me.shard]
        else:
            dst = outs[a].at[me.x if nx > 1 else 0, me.shard, me.core]
        locals_.append(pltpu.make_async_copy(ins[a], dst, local_sem.at[a]))
    for p in range(pairs):
        locals_.append(
            pltpu.make_async_copy(pair_ins[p], pair_outs[p].at[me.core], local_sem.at[count + p])
        )
    for copy in locals_:
        copy.start()
    pair_copies = [
        remote(pair_ins[p], pair_outs[p].at[me.core], pair_sem.at[0, p], pair_sem.at[1, p], me.partner())
        for p in range(pairs)
    ]

    def run(core, plan):
        sends = []

        def push(cond, src, dst, device, sem):
            copy = remote(src, dst, send_sem.at[len(sends)], sem, device)
            when(cond, copy.start)
            sends.append((cond, copy))

        def sem_of(a, k, j, i):
            return recv_sem.at[a, k + nz - 1, j, i]

        def spread(order, arrays, k, j, i, via):
            cond = me.inside(k)
            own = via is None
            later = order if own else order[order.index(via) + 1 :]
            for a in arrays:
                dst = slot(outs[a], k, j, i, core)
                src = dst
                if own:
                    src = ins[a].at[core] if split else ins[a]
                else:
                    arrival = remote(dst, dst, send_sem.at[0], sem_of(a, k, j, i), me.partner())
                    when(cond, arrival.wait_recv)
                steps = []
                if via == "z":
                    steps = [-1 if k > 0 else 1]
                elif "z" in later:
                    steps = [1, -1]
                for step in steps:
                    push(both(cond, me.inside(step)), src, dst, me.line(step), sem_of(a, k - step, j, i))
                if "y" in later:
                    for p in range(1, ny):
                        push(cond, src, dst, me.peer_y(p), sem_of(a, k, (j - p) % ny, i))
                if "x" in later:
                    for p in range(1, nx):
                        push(cond, src, dst, me.peer_x(p), sem_of(a, k, j, (i - p) % nx))
                if not (own and split):
                    push(cond, src, dst, me.partner(), cross_sem.at[a, k + nz - 1, j, i])

        events = []
        for order, arrays in plan:
            for k in range(1 - nz, nz):
                for j in range(ny):
                    for i in range(nx):
                        via = [d for d in order if {"z": k, "y": j, "x": i}[d] != 0]
                        hops = abs(k) + (j != 0) + (i != 0)
                        stage = order.index(via[-1]) if via else -1
                        events.append((hops, stage, k, j, i, order, arrays, via[-1] if via else None))
        events.sort(key=lambda e: e[:5])
        for n, (hops, stage, k, j, i, order, arrays, via) in enumerate(events):
            spread(order, arrays, k, j, i, via)
            if n + 1 < len(events) and events[n + 1][0] == hops:
                continue
            if hops == 0:
                for copy in pair_copies:
                    copy.start()
            if hops in hooks:
                hooks[hops]()
        for hops, stage, k, j, i, order, arrays, via in events:
            if via is None and split:
                continue
            for a in arrays:
                dst = slot(outs[a], k, j, i, 1 - core)
                arrival = remote(dst, dst, send_sem.at[0], cross_sem.at[a, k + nz - 1, j, i], me.partner())
                when(me.inside(k), arrival.wait_recv)
        for cond, copy in sends:
            when(cond, copy.wait_send)

    if errand and pairs:
        groups = 2 * pair_ins[0].shape[0]
        shift = (me.rep * me.shards + me.shard) * errand
        far_hops = [hops for hops in range(2, nz + 2)]

        def spread_some(n):
            if n == 0:
                for copy in locals_[count:]:
                    copy.wait()
                for p in range(pairs):
                    pair_copies[p].wait_send()
                    remote(
                        pair_ins[p], pair_outs[p].at[1 - me.core], pair_sem.at[0, p], pair_sem.at[1, p], me.partner()
                    ).wait_recv()
            edges = [groups * t // len(far_hops) for t in range(len(far_hops) + 1)]
            spread_range(edges[n], edges[n + 1], shift, errand, *pair_outs, marks_ref)

        for n, hops in enumerate(far_hops):
            hooks[hops] = partial(spread_some, n)

    for core, plan in enumerate(orders):
        pl.when(me.core == core)(partial(run, core, plan))
    if errand:
        hooks["end"]()
    for copy in locals_[:count]:
        copy.wait()


def gather(parts, ident, pair_parts=(), split=False, use_x=True, space=ANY, errand=(), rows_each=0):
    count, pairs = len(parts), len(pair_parts)
    every = list(range(count))
    if not use_x:
        orders = [[(("z", "y"), every)]] * 2
    elif split:
        orders = [[(("z", "y", "x"), every)], [(("x", "z", "y"), every[:-1]), (("x", "y", "z"), every[-1:])]]
    else:
        orders = [[(("z", "y", "x"), every)], [(("x", "z", "y"), every)]]
    shards = lax.axis_size("shard")
    nx = lax.axis_size("section") if use_x else 1
    nz = min(4, shards)
    ny = shards // nz
    lead = (nx, shards) if split else (nx, shards, 2)
    blocks = (2 * nz - 1) * ny * nx
    errand_shapes, errand_scratch = [], []
    if errand:
        asks, table = errand
        peers, wide = asks.shape[0], table.shape[1]
        errand_shapes = [
            jax.ShapeDtypeStruct((nx, peers) + asks.shape[1:], asks.dtype),
            jax.ShapeDtypeStruct((peers, batch_rows, wide), table.dtype),
        ]
        if pairs:
            rows = 2 * pair_parts[2].shape[0]
            errand_shapes.append(jax.ShapeDtypeStruct((rows, table.shape[0]), jnp.float32))
        errand_scratch = [
            pltpu.VMEM((peers * batch_rows, table.shape[0]), table.dtype),
            pltpu.VMEM((peers, batch_rows, wide), table.dtype),
            DMA((2, nx, peers)),
            DMA((2, peers)),
            DMA((2,)),
        ]
    outs = pl.pallas_call(
        partial(gather_kernel, count, pairs, split, orders, rows_each),
        out_shape=[jax.ShapeDtypeStruct(lead + p.shape, p.dtype) for p in parts]
        + [jax.ShapeDtypeStruct((2,) + p.shape, p.dtype) for p in pair_parts]
        + errand_shapes,
        in_specs=[VMEM] * (count + pairs + len(errand)),
        out_specs=[space] * count + [VMEM] * pairs + [VMEM] * len(errand_shapes),
        scratch_shapes=[
            DMA((blocks * count * 4,)),
            DMA((count, 2 * nz - 1, ny, nx)),
            DMA((count, 2 * nz - 1, ny, nx)),
            DMA((2, max(pairs, 1))),
            DMA((count + pairs,)),
        ]
        + errand_scratch,
        compiler_params=pltpu.CompilerParams(collective_id=ident, has_side_effects=True),
        name=f"gather_{ident}",
    )(*parts, *pair_parts, *errand)
    return outs[:count], outs[count : count + pairs], outs[count + pairs :]


def exchange_kernel(relay, src_ref, out_ref, send_sem, recv_sem, relay_send, relay_recv, local_sem):
    me = Place()
    peers = me.replicas * me.shards
    barrier = pltpu.get_barrier_semaphore()
    for p in range(1, peers):
        pl.semaphore_signal(barrier, inc=1, device_id=me.group(p)[1], device_id_type=MESH)
    if relay:
        for i in range(1, me.sections):
            pl.semaphore_signal(barrier, inc=1, device_id=me.peer_x(i), device_id_type=MESH)
    pl.semaphore_wait(barrier, peers - 1 + (me.sections - 1 if relay else 0))
    mine = me.rep * me.shards + me.shard
    section = me.x if relay else 0
    own = pltpu.make_async_copy(
        src_ref.at[mine if src_ref.shape[0] > 1 else 0], out_ref.at[section, mine], local_sem.at[0]
    )
    own.start()
    sends = []
    for p in range(1, peers):
        place, device = me.group(p)
        copy = remote(
            src_ref.at[place if src_ref.shape[0] > 1 else 0], out_ref.at[section, mine], send_sem.at[p], recv_sem.at[p], device
        )
        copy.start()
        sends.append(copy)
    relays = []

    def forward(p, src, dst):
        for i in range(1, me.sections):
            copy = remote(src, dst, relay_send.at[p, i], relay_recv.at[p, i], me.peer_x(i))
            copy.start()
            relays.append(copy)

    if relay:
        forward(0, src_ref.at[mine if src_ref.shape[0] > 1 else 0], out_ref.at[me.x, mine])
    for p in range(1, peers):
        source, device = me.group(peers - p)
        dst = out_ref.at[section, source]
        remote(dst, dst, send_sem.at[p], recv_sem.at[p], device).wait_recv()
        if relay:
            forward(p, dst, dst)
    if relay:
        for p in range(peers):
            source, _ = me.group(peers - p)
            for i in range(1, me.sections):
                dst = out_ref.at[lax.rem(me.x + me.sections - i, me.sections), source]
                remote(dst, dst, relay_send.at[p, i], relay_recv.at[p, i], me.peer_x(i)).wait_recv()
    for copy in sends + relays:
        copy.wait_send()
    own.wait()


def exchange(blocks, ident, relay=False):
    peers = lax.axis_size("replica") * lax.axis_size("shard")
    nx = lax.axis_size("section")
    return pl.pallas_call(
        partial(exchange_kernel, relay),
        out_shape=jax.ShapeDtypeStruct((nx if relay else 1, peers) + blocks.shape[1:], blocks.dtype),
        in_specs=[VMEM],
        out_specs=VMEM,
        scratch_shapes=[DMA((peers,)), DMA((peers,)), DMA((peers, nx)), DMA((peers, nx)), DMA((1,))],
        compiler_params=pltpu.CompilerParams(collective_id=ident, has_side_effects=True),
        name=f"exchange_{ident}",
    )(blocks)


def total_steps(me):
    steps = []
    for axis, size in (("replica", me.replicas), ("section", me.sections), ("shard", me.shards)):
        bit = 1
        while bit < size:
            steps.append((axis, bit))
            bit *= 2
    return steps


def total_kernel(count, *refs):
    ins, refs = refs[:count], refs[count:]
    outs, refs = refs[:count], refs[count:]
    held, refs = refs[:count], refs[count:]
    send_sem, recv_sem = refs
    me = Place()
    steps = total_steps(me)
    position = {"section": me.x, "replica": me.rep, "shard": me.shard}

    def other(axis, bit):
        index = position[axis]
        return {**position, axis: index + bit - 2 * bit * lax.rem(index // bit, 2)}

    barrier = pltpu.get_barrier_semaphore()
    for axis, bit in steps:
        pl.semaphore_signal(barrier, inc=1, device_id=other(axis, bit), device_id_type=MESH)
    pl.semaphore_wait(barrier, len(steps))
    for a in range(count):
        held[a][0] = ins[a][...]
    copies = []
    for n, (axis, bit) in enumerate(steps):
        step_copies = [
            remote(held[a].at[2 * n], held[a].at[2 * n + 1], send_sem.at[n, a], recv_sem.at[n, a], other(axis, bit))
            for a in range(count)
        ]
        for copy in step_copies:
            copy.start()
        copies += step_copies
        for a in range(count):
            step_copies[a].wait_recv()
            summed = (held[a][2 * n].astype(jnp.float32) + held[a][2 * n + 1].astype(jnp.float32)).astype(held[a].dtype)
            if n + 1 < len(steps):
                held[a][2 * n + 2] = summed
            else:
                outs[a][...] = summed
    for copy in copies:
        copy.wait_send()


def total(values, ident):
    count = len(values)
    steps = sum((lax.axis_size(axis) - 1).bit_length() for axis in every_axis)
    return pl.pallas_call(
        partial(total_kernel, count),
        out_shape=[jax.ShapeDtypeStruct(v.shape, v.dtype) for v in values],
        in_specs=[VMEM] * count,
        out_specs=[VMEM] * count,
        scratch_shapes=[pltpu.VMEM((2 * steps,) + v.shape, v.dtype) for v in values]
        + [DMA((steps, count)), DMA((steps, count))],
        compiler_params=pltpu.CompilerParams(collective_id=ident, has_side_effects=True),
        name=f"total_{ident}",
    )(*values)


def add_rows(dst, src):
    rows = dst.shape[0]
    if rows % 16 != 0:
        dst[...] = (dst[...].astype(jnp.float32) + src[...].astype(jnp.float32)).astype(dst.dtype)
        return
    step = 16

    def body(n, carry):
        at = pl.ds(pl.multiple_of(n * step, step), step)
        dst[at, :] = (dst[at, :].astype(jnp.float32) + src[at, :].astype(jnp.float32)).astype(dst.dtype)
        return carry

    lax.fori_loop(0, rows // step, body, 0)


def grads_errand(me, sent, got, sum_in, sum_out, *refs):
    n_sums = len(sum_in)
    held, refs = refs[:n_sums], refs[n_sums:]
    row_sem, relay_sem, own_sem, sum_sem = refs
    peers = me.replicas * me.shards
    mine = me.rep * me.shards + me.shard
    direct = [
        remote(sent.at[me.group(p)[0]], got.at[me.x, mine], row_sem.at[0, p], row_sem.at[1, p], me.group(p)[1])
        for p in range(1, peers)
    ]
    own = pltpu.make_async_copy(sent.at[mine], got.at[me.x, mine], own_sem.at[0])
    relays = []

    def source(p):
        return lax.rem(mine + peers - p, peers)

    def begin():
        own.start()
        for copy in direct:
            copy.start()
        for i in range(1, me.sections):
            copy = remote(sent.at[mine], got.at[me.x, mine], relay_sem.at[0, 0, i], relay_sem.at[1, 0, i], me.peer_x(i))
            copy.start()
            relays.append(copy)

    steps = total_steps(me)
    position = {"section": me.x, "replica": me.rep, "shard": me.shard}

    def other(axis, bit):
        index = position[axis]
        return {**position, axis: index + bit - 2 * bit * lax.rem(index // bit, 2)}

    def sum_copies(n):
        axis, bit = steps[n]
        return [
            remote(held[a].at[2 * n], held[a].at[2 * n + 1], sum_sem.at[0, n, a], sum_sem.at[1, n, a], other(axis, bit))
            for a in range(n_sums)
        ]

    def sum_step(n):
        if n == 0:
            for a in range(n_sums):
                held[a][0] = sum_in[a][...]
        else:
            for a, copy in enumerate(sum_copies(n - 1)):
                copy.wait_recv()
                summed = held[a][2 * n - 2] + held[a][2 * n - 1]
                if n < len(steps):
                    held[a][2 * n] = summed
                else:
                    sum_out[a][...] = summed
        if n < len(steps):
            for copy in sum_copies(n):
                copy.start()

    def relay(first, last):
        for p in range(first, last):
            dst = got.at[me.x, source(p)]
            remote(dst, dst, row_sem.at[0, p], row_sem.at[1, p], me.partner()).wait_recv()
            for i in range(1, me.sections):
                copy = remote(dst, dst, relay_sem.at[0, p, i], relay_sem.at[1, p, i], me.peer_x(i))
                copy.start()
                relays.append(copy)

    def finish():
        for p in range(peers):
            for i in range(1, me.sections):
                dst = got.at[lax.rem(me.x + me.sections - i, me.sections), source(p)]
                remote(dst, dst, relay_sem.at[0, p, i], relay_sem.at[1, p, i], me.partner()).wait_recv()
        for p in range(peers):
            for i in range(1, me.sections):
                dst = got.at[me.x, source(p)]
                remote(dst, dst, relay_sem.at[0, p, i], relay_sem.at[1, p, i], me.peer_x(i)).wait_send()
        for copy in direct:
            copy.wait_send()
        for n in range(len(steps)):
            for copy in sum_copies(n):
                copy.wait_send()
        own.wait()

    early = [begin] + [partial(sum_step, n) for n in range(len(steps) + 1) if n_sums]
    return early, [partial(relay, 1, peers)], [finish]


def reduce_kernel(count, sections, sums, extra, *refs):
    ins, refs = [refs[a * sections : (a + 1) * sections] for a in range(count)], refs[count * sections :]
    sum_in, refs = refs[:sums], refs[sums:]
    if extra:
        sent, refs = refs[0], refs[1:]
    outs, refs = refs[:count], refs[count:]
    sum_out, refs = refs[:sums], refs[sums:]
    if extra:
        got, refs = refs[0], refs[1:]
    acc, refs = refs[:count], refs[count:]
    from_core, refs = refs[:count], refs[count:]
    from_x, refs = refs[:count], refs[count:]
    from_y, refs = refs[:count], refs[count:]
    from_z, refs = refs[:count], refs[count:]
    load_sem, core_send, core_recv, send_sem, x_recv, y_recv, z_recv, last_sem = refs[:8]
    me = Place()
    nz, ny, nx = me.nz, me.ny, me.sections
    hooks = []
    if extra:
        me.greet_group()
        hooks = grads_errand(me, sent, got, sum_in, sum_out, *refs[8 : 8 + sums], *refs[8 + sums :])
    else:
        me.greet()

    far = sorted((k for k in range(1 - nz, nz)), key=lambda k: -abs(k))

    def block(k, j, i):
        return lax.rem(me.x + i, nx), (me.z + k) * ny + lax.rem(me.y + j, ny)

    def order_of(core):
        if core == 0:
            return [(k, j, i) for i in range(nx - 1, -1, -1) for j in range(ny - 1, -1, -1) for k in far]
        return [(k, j, i) for j in range(ny - 1, -1, -1) for k in far for i in range(nx - 1, -1, -1)]

    def run(core):
        other = 1 - core
        sends = []

        def start_core(k, j, i):
            x, s = block(k, j, i)

            def go(layer):
                for a in range(count):
                    remote(
                        ins[a][layer].at[s, other], from_core[a].at[x, s], core_send.at[a, x, s],
                        core_recv.at[a, x, s], me.partner(),
                    ).start()

            for layer in range(nx):
                when(both(me.inside(k), x == layer), partial(go, layer))

        def start_load(k, j, i):
            x, s = block(k, j, i)

            def go(layer):
                for a in range(count):
                    pltpu.make_async_copy(ins[a][layer].at[s, core], acc[a].at[x, s], load_sem.at[a, x, s]).start()

            for layer in range(nx):
                when(both(me.inside(k), x == layer), partial(go, layer))

        for b in order_of(other):
            start_core(*b)
        for b in order_of(core):
            start_load(*b)
        early, late, final = [list(part) for part in hooks] if hooks else ([], [], [])

        def errand(todo, every=False):
            while todo:
                todo.pop(0)()
                if not every:
                    break

        errand(early)

        def push(cond, src, dst, sem, device):
            copy = remote(src, dst, send_sem.at[len(sends)], sem, device)
            when(cond, copy.start)
            sends.append((cond, copy))

        def take(cond, dst, src, sem):
            def go():
                remote(src, src, core_send.at[0, 0, 0], sem, me.partner()).wait_recv()
                add_rows(dst, src)

            when(cond, go)

        def join_core(a, k, j, i):
            x, s = block(k, j, i)

            def go():
                pltpu.make_async_copy(ins[a][0].at[s, core], acc[a].at[x, s], load_sem.at[a, x, s]).wait()

            when(me.inside(k), go)
            take(me.inside(k), acc[a].at[x, s], from_core[a].at[x, s], core_recv.at[a, x, s])

        def join_x(a, k, j):
            x, s = block(k, j, 0)
            for p in range(1, nx):
                take(me.inside(k), acc[a].at[x, s], from_x[a].at[p - 1, s], x_recv.at[a, p - 1, s])

        def join_y(a, k, i):
            x, s = block(k, 0, i)
            for p in range(1, ny):
                take(me.inside(k), acc[a].at[x, s], from_y[a].at[p - 1, x, me.z + k], y_recv.at[a, p - 1, x, me.z + k])

        def join_z(a, k, i):
            x, s = block(k, 0, i)
            if k >= 0:
                take(both(me.inside(k), me.inside(-1)), acc[a].at[x, s], from_z[a].at[x, me.z + k], z_recv.at[a, x, me.z + k])
            if k <= 0:
                place = nz if k == 0 else me.z + k
                take(both(me.inside(k), me.inside(1)), acc[a].at[x, s], from_z[a].at[x, place], z_recv.at[a, x, place])

        def send_x(a, k, j, i):
            x, s = block(k, j, i)
            push(me.inside(k), acc[a].at[x, s], from_x[a].at[i - 1, s], x_recv.at[a, i - 1, s], me.peer_x(i))

        def send_y(a, k, j, i):
            x, s = block(k, j, i)
            push(
                me.inside(k), acc[a].at[x, s], from_y[a].at[j - 1, x, me.z + k],
                y_recv.at[a, j - 1, x, me.z + k], me.peer_y(j),
            )

        def send_z(a, k, i):
            x, s = block(k, 0, i)
            place = nz if k == -1 else me.z + k
            push(
                me.inside(k), acc[a].at[x, s], from_z[a].at[x, place], z_recv.at[a, x, place],
                me.line(1 if k > 0 else -1),
            )

        each = range(count)

        def x_first(arrays):
            first, second, third = [], [], []

            def cross_x(k, j, i):
                for a in arrays:
                    join_core(a, k, j, i)
                    send_x(a, k, j, i)

            def join_own(k, j):
                for a in arrays:
                    join_core(a, k, j, 0)

            def cross_y(k, j):
                for a in arrays:
                    join_x(a, k, j)
                    send_y(a, k, j, 0)

            def along_z(k):
                for a in arrays:
                    join_x(a, k, 0)
                    join_y(a, k, 0)
                    join_z(a, k, 0)
                    if k != 0:
                        send_z(a, k, 0)

            for i in range(nx - 1, 0, -1):
                for j in range(ny - 1, -1, -1):
                    first += [partial(cross_x, k, j, i) for k in far]
            for j in range(ny - 1, -1, -1):
                second += [partial(join_own, k, j) for k in far]
            for j in range(ny - 1, 0, -1):
                second += [partial(cross_y, k, j) for k in far]
            third += [partial(along_z, k) for k in far]
            return first, second, third

        def y_first(arrays):
            def cross_y(k, j, i):
                for a in arrays:
                    join_core(a, k, j, i)
                    send_y(a, k, j, i)

            def join_own(k, i):
                for a in arrays:
                    join_core(a, k, 0, i)

            def along_z(k, i):
                for a in arrays:
                    join_y(a, k, i)
                    join_z(a, k, i)
                    if k != 0:
                        send_z(a, k, i)
                    elif i != 0:
                        send_x(a, 0, 0, i)
                    else:
                        join_x(a, 0, 0)

            slots = range(nx - 1, -1, -1)
            first = [partial(cross_y, k, j, i) for j in range(ny - 1, 0, -1) for k in far for i in slots]
            second = [partial(join_own, k, i) for k in far for i in slots]
            third = [partial(along_z, k, i) for k in far for i in slots]
            return first, second, third

        plans = [x_first(list(each)) if core == 0 else y_first(list(each))]
        for stage in range(3):
            lists = [plan[stage] for plan in plans if plan[stage]]
            longest = max(len(steps) for steps in lists)
            if stage == 1:
                errand(early, every=True)
                errand(late, every=True)
            for n in range(longest):
                for steps in lists:
                    for step in steps[len(steps) * n // longest : len(steps) * (n + 1) // longest]:
                        step()
                errand(early)
        errand(final, every=True)
        finals = []
        for a in each:
            copy = remote(
                acc[a].at[me.x, me.shard], outs[a].at[core], last_sem.at[0, a], last_sem.at[1, a], me.partner()
            )
            copy.start()
            finals.append(copy)
            outs[a][core] = acc[a][me.x, me.shard]
        for a in each:
            remote(outs[a].at[other], outs[a].at[other], last_sem.at[0, a], last_sem.at[1, a], me.partner()).wait_recv()
        for cond, copy in sends:
            when(cond, copy.wait_send)
        for copy in finals:
            copy.wait_send()
        for k, j, i in order_of(other):
            x, s = block(k, j, i)

            def finish():
                for a in each:
                    remote(
                        ins[a][0].at[s, other], from_core[a].at[x, s], core_send.at[a, x, s],
                        core_recv.at[a, x, s], me.partner(),
                    ).wait_send()

            when(me.inside(k), finish)

    pl.when(me.core == 0)(lambda: run(0))
    pl.when(me.core == 1)(lambda: run(1))


def reduce_shards(grads, ident, errand=None):
    count = len(grads)
    nx, shards = lax.axis_size("section"), lax.axis_size("shard")
    nz = min(4, shards)
    ny = shards // nz
    blocks = (2 * nz - 1) * ny * nx

    def scratch(lead):
        return [pltpu.VMEM(lead + g[0].shape[2:], g[0].dtype) for g in grads]

    extra_in, extra_shapes, extra_scratch, sums = [], [], [], 0
    if errand:
        values, sent = errand
        sums, peers = len(values), sent.shape[0]
        steps = sum((lax.axis_size(axis) - 1).bit_length() for axis in every_axis)
        extra_in = [*values, sent]
        extra_shapes = [jax.ShapeDtypeStruct(v.shape, v.dtype) for v in values] + [
            jax.ShapeDtypeStruct((nx,) + sent.shape, sent.dtype)
        ]
        extra_scratch = [pltpu.VMEM((2 * steps,) + v.shape, v.dtype) for v in values] + [
            DMA((2, peers)),
            DMA((2, peers, nx)),
            DMA((1,)),
            DMA((2, steps, max(sums, 1))),
        ]
    return pl.pallas_call(
        partial(reduce_kernel, count, nx, sums, bool(errand)),
        out_shape=[jax.ShapeDtypeStruct(g[0].shape[1:], g[0].dtype) for g in grads] + extra_shapes,
        in_specs=[ANY] * (count * nx) + [VMEM] * sums + [ANY] * bool(errand),
        out_specs=[VMEM] * (count + sums) + [ANY] * bool(errand),
        scratch_shapes=scratch((nx, shards))
        + scratch((nx, shards))
        + scratch((max(nx - 1, 1), shards))
        + scratch((max(ny - 1, 1), nx, nz))
        + scratch((nx, nz + 1))
        + [
            DMA((count, nx, shards)),
            DMA((count, nx, shards)),
            DMA((count, nx, shards)),
            DMA((blocks * count * 2,)),
            DMA((count, max(nx - 1, 1), shards)),
            DMA((count, max(ny - 1, 1), nx, nz)),
            DMA((count, nx, nz + 1)),
            DMA((2, count)),
        ]
        + extra_scratch,
        compiler_params=pltpu.CompilerParams(
            collective_id=ident, has_side_effects=True, vmem_limit_bytes=67043328
        ),
        name=f"reduce_{ident}",
    )(*[layer for g in grads for layer in g], *extra_in)


def reduce_parts(grads, ident, errand):
    nx, shards = lax.axis_size("section"), lax.axis_size("shard")
    ny = shards // min(4, shards)
    slots = 2 * nx * shards + (nx - 1) * shards + (ny - 1) * nx * 4 + nx * 5 + 4
    groups, used = [[]], 0
    for n, grad in enumerate(grads):
        rows, columns = grad[0].shape[2:]
        size = slots * (-(-rows // 16) * 16) * columns * 2
        if used + size > 58 * 2**20 and groups[-1]:
            groups.append([])
            used = 0
        groups[-1].append(n)
        used += size
    out = [None] * len(grads)
    for g, group in enumerate(groups):
        done = reduce_shards([grads[n] for n in group], ident + g, errand if g == 0 else None)
        for n, value in zip(group, done):
            out[n] = value
        if g == 0:
            extra = done[len(group) :]
    return out, extra


def spread_group(columns, values, target, high):
    entries = columns.shape[1]
    each = entries // 8
    row = lax.broadcasted_iota(jnp.int32, (1, entries), 1) // each
    key = jnp.where(columns >= 0, (columns // 128) * 8 + row, -1)
    low_part = jnp.where(columns >= 0, lax.rem(columns, 128), -1)
    left = jnp.where(key == lax.broadcasted_iota(jnp.int32, (high * 8, entries), 0), values, 0.0).astype(jnp.bfloat16)
    right = jnp.where(low_part == lax.broadcasted_iota(jnp.int32, (128, entries), 0), 1.0, 0.0).astype(jnp.bfloat16)
    placed = lax.dot_general(left, right, (((1,), (1,)), ((), ())), preferred_element_type=jnp.float32)
    pieces = []
    for h in range(high):
        one = jnp.where(lax.broadcasted_iota(jnp.int32, (8, 128), 1) + 128 * h == target, 1.0, 0.0)
        pieces.append(placed[h * 8 : (h + 1) * 8] + one)
    return pieces


def spread_range(first, last, shift, rows_each, columns_ref, weight_ref, target_ref, out_ref):
    high = out_ref.shape[1] // 128
    per = columns_ref.shape[1]

    def local_of(ids):
        column = ids - shift
        return jnp.where((column >= 0) & (column < rows_each), column, -1)

    def body(g, carry):
        pair, place = g // per, lax.rem(g, per)
        target = target_ref[pair, pl.ds(pl.multiple_of(place * 8, 8), 8), :]
        pieces = spread_group(local_of(columns_ref[pair, place]), weight_ref[pair, place], local_of(target), high)
        at = pl.ds(pl.multiple_of(g * 8, 8), 8)
        for h in range(high):
            out_ref[at, h * 128 : (h + 1) * 128] = pieces[h]
        return carry

    lax.fori_loop(first, last, body, 0)


def spread_kernel(rows_each, shift_ref, columns_ref, weight_ref, target_ref, out_ref):
    spread_range(
        0, columns_ref.shape[0] * columns_ref.shape[1], shift_ref[0], rows_each, columns_ref, weight_ref, target_ref, out_ref
    )


def spread_entries(shift, columns, values, targets, rows_each, width):
    rows = targets.shape[0] * targets.shape[1]
    return pl.pallas_call(
        partial(spread_kernel, rows_each),
        out_shape=jax.ShapeDtypeStruct((rows, width), jnp.float32),
        in_specs=[pl.BlockSpec(memory_space=pltpu.SMEM)] + [VMEM] * 3,
        out_specs=VMEM,
        name="spread_entries",
    )(shift, columns, values, targets)


def ask_kernel(owners, token_row, token_col, owner_row, owner_col, row_col, hot_ref, ask_ref):
    count = token_row.shape[1]
    i = lax.broadcasted_iota(jnp.int32, (count, count), 0)
    j = lax.broadcasted_iota(jnp.int32, (count, count), 1)
    same = token_col[...] == token_row[...]
    kin = owner_col[...] == owner_row[...]
    first_col = 1.0 - jnp.max(jnp.where(same & (j < i), 1.0, 0.0), axis=1, keepdims=True)
    first_row = 1.0 - jnp.max(jnp.where(same & (i < j), 1.0, 0.0), axis=0, keepdims=True)
    place_col = jnp.sum(jnp.where(kin & (j < i), first_row, 0.0), axis=1, keepdims=True)
    place_row = jnp.sum(jnp.where(kin & (i < j), first_col, 0.0), axis=0, keepdims=True)
    number_col = jnp.sum(jnp.where(same, first_row * place_row, 0.0), axis=1, keepdims=True)
    number_row = jnp.sum(jnp.where(same, first_col * place_col, 0.0), axis=0, keepdims=True)
    size = float(batch_rows)
    slot_row = jnp.where(number_row < size, owner_row[...].astype(jnp.float32) * size + number_row, -1.0)
    slot_col = jnp.where(number_col < size, owner_col[...].astype(jnp.float32) * size + number_col, -1.0)
    spots = owners * batch_rows
    part = 512 if spots % 512 == 0 else spots
    for at in range(0, spots, part):
        line = lax.broadcasted_iota(jnp.int32, (part, count), 0).astype(jnp.float32) + float(at)
        hot_ref[at : at + part, :] = jnp.where(slot_row == line, 1.0, 0.0).astype(jnp.bfloat16)
    most = jnp.max(number_col) + 1.0
    wanted = first_col * (row_col[...].astype(jnp.float32) + 1.0)
    lane = lax.broadcasted_iota(jnp.int32, (1, 128), 1)
    for at in range(0, spots, 128):
        line = lax.broadcasted_iota(jnp.int32, (count, 128), 1).astype(jnp.float32) + float(at)
        rows = jnp.max(jnp.where(slot_col == line, wanted, 0.0), axis=0, keepdims=True)
        for n in range(128 // batch_rows):
            shifted = pltpu.roll(rows, (128 - n * batch_rows) % 128, 1) if n else rows
            values = jnp.where(lane < batch_rows, shifted, jnp.where(lane == 127, most, 0.0))
            ask_ref[at // batch_rows + n] = values.astype(jnp.int32)


def ask_rows(tokens, owner, row, owners):
    count = tokens.shape[0]
    return pl.pallas_call(
        partial(ask_kernel, owners),
        out_shape=[
            jax.ShapeDtypeStruct((owners * batch_rows, count), jnp.bfloat16),
            jax.ShapeDtypeStruct((owners, 1, 128), jnp.int32),
        ],
        in_specs=[VMEM] * 5,
        out_specs=[VMEM] * 2,
        name="ask_rows",
    )(tokens[None], tokens[:, None], owner[None], owner[:, None], row[:, None])


def table_kernel(asked_ref, got_ref, head_ref, *refs):
    layers, table_ref, square_ref = refs[:-2], refs[-2], refs[-1]
    sections, peers = asked_ref.shape[:2]
    each = 128 // batch_rows
    lane = lax.broadcasted_iota(jnp.int32, (1, 128), 1)
    lists = []
    for at in range(0, sections * peers, each):
        wish = jnp.zeros((1, 128), jnp.int32)
        for n in range(each):
            part = asked_ref[(at + n) // peers, (at + n) % peers]
            part = pltpu.roll(part, n * batch_rows, 1) if n else part
            wish = jnp.where((lane >= n * batch_rows) & (lane < (n + 1) * batch_rows), part, wish)
        lists.append(wish)
    wish = jnp.concatenate(lists, axis=1)
    rows = table_ref.shape[0]
    step = 400 if rows % 400 == 0 else rows

    def body(n, square):
        at = pl.ds(pl.multiple_of(n * step, 8), step) if step != rows else slice(0, rows)
        row = lax.broadcasted_iota(jnp.int32, (step, wish.shape[1]), 0) + 1 + n * step
        hot = jnp.where(row == wish, 1.0, 0.0).astype(jnp.bfloat16)
        values = head_ref[at, :] + jnp.dot(hot, got_ref[...], preferred_element_type=jnp.float32)
        table_ref[at, :] = values
        return square + jnp.sum(values * values, axis=0, keepdims=True)

    zero = jnp.zeros((1, table_ref.shape[1]), jnp.float32)
    square = jnp.sum(lax.fori_loop(0, rows // step, body, zero)) if step != rows else jnp.sum(body(0, zero))
    square = jnp.where(lax.axis_index("section") == 0, square, 0.0)
    others = jnp.float32(0)
    for layer in layers:
        for half in range(2):
            values = layer[half].astype(jnp.float32)
            others = others + jnp.sum(values * values)
    square = square + jnp.where(lax.axis_index("replica") == 0, others, 0.0)
    corner = lax.broadcasted_iota(jnp.int32, (8, 128), 0) + lax.broadcasted_iota(jnp.int32, (8, 128), 1)
    square_ref[...] = jnp.where(corner == 0, square, 0.0)


def table_gradient(rows_each, asked, got, head_table, layer_grads):
    width = head_table.shape[1]
    return pl.pallas_call(
        table_kernel,
        out_shape=[
            jax.ShapeDtypeStruct((rows_each, width), jnp.float32),
            jax.ShapeDtypeStruct((8, 128), jnp.float32),
        ],
        in_specs=[VMEM] * (3 + len(layer_grads)),
        out_specs=[VMEM] * 2,
        compiler_params=pltpu.CompilerParams(vmem_limit_bytes=56 * 2**20),
        name="table_gradient",
    )(asked, got, head_table, *layer_grads)
def dims_nt(left, right):
    return lax.dot_general(left, right, (((1,), (1,)), ((), ())), preferred_element_type=jnp.float32)


def dims_tn(left, right):
    return lax.dot_general(left, right, (((0,), (0,)), ((), ())), preferred_element_type=jnp.float32)


def three_parts(values):
    first = lower(values)
    rest = values - first.astype(jnp.float32)
    second = lower(rest)
    return first, second, lower(rest - second.astype(jnp.float32))


def log_sigmoid(values):
    return jnp.minimum(values, 0.0) - jnp.log1p(jnp.exp(-jnp.abs(values)))


def norm_parts(values, gain):
    inverse = lax.rsqrt(jnp.mean(values * values, axis=-1, keepdims=True) + eps_norm)
    normed = values * inverse
    return normed, inverse, lower(normed * gain)


class HeadPair:
    def __init__(self, tree_len, cumul):
        self.lane = lax.broadcasted_iota(jnp.int32, (tree_len, 128), 1)
        self.parts = jnp.concatenate(three_parts(cumul), axis=1)
        self.row = lax.broadcasted_iota(jnp.int32, (384, 128), 0)
        self.column = lax.broadcasted_iota(jnp.int32, (384, 128), 1)

    def augmented(self, head, side, query, key):
        start = 64 - 64 * side
        mine = (self.lane >= 64 * side) & (self.lane < 64 * side + 64)
        wanted = (self.row - 128 * (self.row // 128) == head) & (self.column == self.row // 128 + start)
        placed = product(self.parts, lower(jnp.where(wanted, 1.0, 0.0)))
        wanted = (self.row - 128 * (self.row // 128) == head) & (self.column == self.row // 128 + start + 3)
        negative = product(self.parts, lower(jnp.where(wanted, -1.0, 0.0)))
        ones_q = jnp.where((self.lane >= start + 3) & (self.lane < start + 6), 1.0, 0.0)
        ones_k = jnp.where((self.lane >= start) & (self.lane < start + 3), 1.0, 0.0)
        query = lower(jnp.where(mine, query.astype(jnp.float32) * 0.125, placed + ones_q))
        key = lower(jnp.where(mine, key.astype(jnp.float32), negative + ones_k))
        return query, key, mine


def forward_kernel(layer, round_input, x_ref, allowed_ref, w_in, w_out, w_up, w_down, forget_ref, bias_ref, gain_ref,
                   y_ref, qkv_ref, logit_ref, lse_ref, att_ref, mid_ref, gu_ref,
                   b_in, b_out, b_up, b_down, gu_buf, hidden, mask, sem, gu_sem, in_sem):
    tree_len, width = x_ref.shape
    heads = width // 64
    half = hidden.shape[1]
    loads = [None] + [
        pltpu.make_async_copy(src.at[layer], dst, sem.at[n])
        for n, (src, dst) in enumerate(((w_out, b_out), (w_up, b_up), (w_down, b_down)))
    ]

    def first_load(n):
        at = pl.ds(pl.multiple_of(n * 256, 256), 256)
        return pltpu.make_async_copy(w_in.at[layer, :, at], b_in.at[:, at], in_sem.at[n])

    for n in range(3 * width // 256):
        first_load(n).start()
    for copy in loads[1:]:
        copy.start()
    x = x_ref[...]
    if round_input:
        x = lower(x).astype(jnp.float32)
    _, _, act = norm_parts(x, gain_ref[0:1, :])
    allowed = allowed_ref[...]
    mask[...] = jnp.where(allowed > 0, 0.0, masked_score)
    logit = product(act, forget_ref[...]) + bias_ref[...]
    logit_ref[...] = logit
    cumul = sum(product(allowed, part) for part in three_parts(log_sigmoid(logit)))
    def project(n, carry):
        first_load(n).wait()
        at = pl.ds(pl.multiple_of(n * 256, 256), 256)
        qkv_ref[:, at] = lower(product(act, b_in[:, at]))
        return carry

    lax.fori_loop(0, 3 * width // 256, project, 0)
    pair = HeadPair(tree_len, cumul)
    lse_ref[...] = jnp.zeros_like(lse_ref)

    def attend(p, carry):
        base = pl.multiple_of(p * 128, 128)
        query = qkv_ref[:, pl.ds(base, 128)]
        key = qkv_ref[:, pl.ds(base + width, 128)]
        value = qkv_ref[:, pl.ds(base + 2 * width, 128)]
        outs = []
        for side in range(2):
            q_side, k_side, mine = pair.augmented(2 * p + side, side, query, key)
            scores = dims_nt(q_side, k_side) + mask[...]
            peak = jnp.max(scores, axis=1, keepdims=True)
            probs = jnp.exp(scores - peak)
            count = jnp.sum(probs, axis=1, keepdims=True)
            outs.append(product(lower(probs * (1.0 / count)), value))
            lse_ref[...] = jnp.where(pair.lane == 2 * p + side, peak + jnp.log(count), lse_ref[...])
        att_ref[:, pl.ds(base, 128)] = lower(jnp.where(pair.lane < 64, outs[0], outs[1]))
        return carry

    lax.fori_loop(0, heads // 2, attend, 0)
    loads[1].wait()
    middle = x + product(att_ref[...], b_out[...])
    mid_ref[...] = middle
    _, _, act_b = norm_parts(middle, gain_ref[1:2, :])
    loads[2].wait()

    def stores(n):
        return [
            pltpu.make_async_copy(
                gu_buf.at[:, pl.ds(n * 512 + s * half, 512)], gu_ref.at[:, pl.ds(n * 512 + s * half, 512)], gu_sem.at[n, s]
            )
            for s in range(2)
        ]

    for n in range(half // 512):
        def expand(h, carry):
            at = pl.ds(pl.multiple_of(n * 512 + h * 256, 256), 256)
            at_up = pl.ds(pl.multiple_of(half + n * 512 + h * 256, 256), 256)
            gate = product(act_b, b_up[:, at])
            upper = product(act_b, b_up[:, at_up])
            gu_buf[:, at] = gate
            gu_buf[:, at_up] = upper
            hidden[:, at] = lower(gate / (1.0 + jnp.exp(-gate)) * upper)
            return carry

        lax.fori_loop(0, 2, expand, 0)
        for copy in stores(n):
            copy.start()
    loads[3].wait()

    def contract(n, carry):
        at = pl.ds(pl.multiple_of(n * 256, 256), 256)
        y_ref[:, at] = mid_ref[:, at] + product(hidden[...], b_down[:, at])
        return carry

    lax.fori_loop(0, width // 256, contract, 0)
    for n in range(half // 512):
        for copy in stores(n):
            copy.wait()


def layer_forward(layer, round_input, values, allowed, mats, forget_w, forget_b, gains):
    tree_len, width = values.shape
    w_in, w_out, w_up, w_down = mats
    half = w_down.shape[1]
    f32, b16 = jnp.float32, jnp.bfloat16
    shape = jax.ShapeDtypeStruct
    return pl.pallas_call(
        partial(forward_kernel, layer, round_input),
        out_shape=[
            shape((tree_len, width), f32),
            shape((tree_len, 3 * width), b16),
            shape((tree_len, 128), f32),
            shape((tree_len, 128), f32),
            shape((tree_len, width), b16),
            shape((tree_len, width), f32),
            shape((tree_len, 2 * half), f32),
        ],
        in_specs=[VMEM] * 2 + [ANY] * 4 + [VMEM] * 3,
        out_specs=[VMEM] * 6 + [ANY],
        scratch_shapes=[pltpu.VMEM(w.shape[1:], b16) for w in mats]
        + [
            pltpu.VMEM((tree_len, 2 * half), f32),
            pltpu.VMEM((tree_len, half), b16),
            pltpu.VMEM((tree_len, tree_len), f32),
            DMA((4,)),
            DMA((half // 512, 2)),
            DMA((3 * width // 256,)),
        ],
        compiler_params=pltpu.CompilerParams(vmem_limit_bytes=56 * 2**20),
        name=f"forward_{layer}",
    )(values, allowed, *mats, forget_w, forget_b, gains)


def backward_kernel(layer, round_input, round_grad, dy_ref, x_ref, allowed_ref, qkv_ref, logit_ref, lse_ref, att_ref,
                    mid_ref, forget_ref, gain_ref, gu_hbm, w_in, w_out, w_up, w_down,
                    dx_ref, dforget_ref, dgain_ref, dw_in, dw_out, dw_up, dw_down,
                    b_in, b_out, b_up, b_down, gu, dqkv, act_t, grad_b, mask, dcum,
                    g_in, g_out, g_up, g_down, sem, gu_sem, store_sem):
    tree_len, width = x_ref.shape
    heads = width // 64
    half = b_down.shape[0]
    chunk = 256
    loads = [
        pltpu.make_async_copy(src.at[layer], dst, sem.at[n]) for n, (src, dst) in enumerate(((w_in, b_in), (w_out, b_out)))
    ]
    def feed_loads(n):
        at = pl.ds(pl.multiple_of(n * chunk, chunk), chunk)
        at_up = pl.ds(pl.multiple_of(half + n * chunk, chunk), chunk)
        pairs = ((gu_hbm.at[:, at], gu.at[:, at]), (gu_hbm.at[:, at_up], gu.at[:, at_up]),
                 (w_down.at[layer, at], b_down.at[at]), (w_up.at[layer, :, at], b_up.at[:, at]),
                 (w_up.at[layer, :, at_up], b_up.at[:, at_up]))
        return [pltpu.make_async_copy(src, dst, gu_sem.at[n, s]) for s, (src, dst) in enumerate(pairs)]

    for n in range(half // chunk):
        for copy in feed_loads(n):
            copy.start()
    for n in (1, 0):
        loads[n].start()
    dy = dy_ref[...]
    if round_grad:
        dy = lower(dy).astype(jnp.float32)
    branch = lower(dy)
    normed_b, inverse_b, act_b = norm_parts(mid_ref[...], gain_ref[1:2, :])
    act_t[...] = lower((normed_b * gain_ref[1:2, :]).T)
    grad_b[...] = jnp.zeros_like(grad_b)

    def feed(n, carry):
        for copy in feed_loads(n):
            copy.wait()
        at = pl.ds(pl.multiple_of(n * chunk, chunk), chunk)
        at_up = pl.ds(pl.multiple_of(half + n * chunk, chunk), chunk)
        gate, upper = gu[:, at], gu[:, at_up]
        sigma = 1.0 / (1.0 + jnp.exp(-gate))
        silu = gate * sigma
        hidden = lower(silu * upper)
        grad_hidden = dims_nt(branch, b_down[at, :])
        g_down[at, :] = lower(dims_tn(hidden, branch))
        grad_gate = lower(grad_hidden * upper * sigma * (1.0 + gate * (1.0 - sigma)))
        grad_upper = lower(grad_hidden * silu)
        g_up[:, at] = lower(product(act_t[...], grad_gate))
        g_up[:, at_up] = lower(product(act_t[...], grad_upper))
        grad_b[...] += dims_nt(grad_gate, b_up[:, at]) + dims_nt(grad_upper, b_up[:, at_up])
        return carry

    lax.fori_loop(0, half // chunk, feed, 0)
    stores = [
        pltpu.make_async_copy(src, dst, store_sem.at[n])
        for n, (src, dst) in enumerate(((g_down, dw_down), (g_up, dw_up), (g_out, dw_out), (g_in, dw_in)))
    ]
    stores[0].start()
    stores[1].start()

    def norm_backward(grad, normed, inverse, gain):
        grad_normed = grad * gain
        back = inverse * (grad_normed - normed * jnp.mean(grad_normed * normed, axis=-1, keepdims=True))
        return back, jnp.sum(grad * normed, axis=0, keepdims=True)

    back_b, dgain_b = norm_backward(grad_b[...], normed_b, inverse_b, gain_ref[1:2, :])
    grad_mid = dy + back_b
    branch_a = lower(grad_mid)
    g_out[...] = lower(dims_tn(att_ref[...], branch_a))
    stores[2].start()
    loads[1].wait()
    att_ref_grad = lower(dims_nt(branch_a, b_out[...]))
    x = x_ref[...]
    if round_input:
        x = lower(x).astype(jnp.float32)
    normed_a, inverse_a, act_a = norm_parts(x, gain_ref[0:1, :])
    act_t[...] = lower((normed_a * gain_ref[0:1, :]).T)
    allowed = allowed_ref[...]
    mask[...] = jnp.where(allowed > 0, 0.0, masked_score)
    logit = logit_ref[...]
    cumul = sum(product(allowed, part) for part in three_parts(log_sigmoid(logit)))
    pair = HeadPair(tree_len, cumul)
    dcum[...] = jnp.zeros_like(dcum)
    grad_att = grad_b
    grad_att[...] = att_ref_grad.astype(jnp.float32)

    def attend(p, carry):
        base = pl.multiple_of(p * 128, 128)
        query = qkv_ref[:, pl.ds(base, 128)]
        key = qkv_ref[:, pl.ds(base + width, 128)]
        value = qkv_ref[:, pl.ds(base + 2 * width, 128)]
        grad_out = grad_att[:, pl.ds(base, 128)]
        grad_low = lower(grad_out)
        results = []
        for side in range(2):
            head = 2 * p + side
            start = 64 - 64 * side
            q_side, k_side, mine = pair.augmented(head, side, query, key)
            lse = jnp.sum(jnp.where(pair.lane == head, lse_ref[...], 0.0), axis=1, keepdims=True)
            probs = jnp.exp(dims_nt(q_side, k_side) + (mask[...] - lse))
            grad_probs = dims_nt(lower(jnp.where(mine, grad_out, 0.0)), value)
            weighted = probs * grad_probs
            row = jnp.sum(weighted, axis=1, keepdims=True)
            grad_scores = lower(weighted - probs * row)
            grad_value = dims_tn(lower(probs), grad_low)
            grad_query = product(grad_scores, k_side)
            grad_key = dims_tn(grad_scores, q_side)
            taken = jnp.sum(
                jnp.where(pair.lane == start, grad_query, 0.0) - jnp.where(pair.lane == start + 3, grad_key, 0.0),
                axis=1, keepdims=True,
            )
            dcum[...] = jnp.where(pair.lane == head, taken, dcum[...])
            results.append((grad_query * 0.125, grad_key, grad_value))
        for part in range(3):
            merged = jnp.where(pair.lane < 64, results[0][part], results[1][part])
            dqkv[:, pl.ds(base + part * width, 128)] = lower(merged)
        return carry

    lax.fori_loop(0, heads // 2, attend, 0)
    rising = sum(dims_tn(allowed, part) for part in three_parts(dcum[...]))
    grad_logit = rising / (1.0 + jnp.exp(logit))
    lane = lax.broadcasted_iota(jnp.int32, grad_logit.shape, 1)
    grad_logit = lower(jnp.where(lane < heads, grad_logit, 0.0))
    dforget_ref[:, 0:width] = lower(dims_tn(grad_logit, act_a)[0:16, :])
    bias = dims_tn(grad_logit, jnp.ones((tree_len, 128), jnp.bfloat16))[0:16, :]
    bias = jnp.where(lax.broadcasted_iota(jnp.int32, (16, 128), 1) == 0, bias, 0.0)
    dforget_ref[:, width : width + 128] = lower(bias)

    def weigh(n, carry):
        at = pl.ds(pl.multiple_of(n * 256, 256), 256)
        g_in[:, at] = lower(product(act_t[...], dqkv[:, at]))
        return carry

    lax.fori_loop(0, 3 * width // 256, weigh, 0)
    stores[3].start()
    loads[0].wait()
    grad_b[...] = dims_nt(grad_logit, forget_ref[...])

    def gather_back(n, carry):
        at = pl.ds(pl.multiple_of(n * 256, 256), 256)
        grad_b[...] += dims_nt(dqkv[:, at], b_in[:, at])
        return carry

    lax.fori_loop(0, 3 * width // 256, gather_back, 0)
    back_a, dgain_a = norm_backward(grad_b[...], normed_a, inverse_a, gain_ref[0:1, :])
    dx_ref[...] = grad_mid + back_a
    dgain_ref[...] = jnp.concatenate([dgain_a, dgain_b], axis=0)
    for copy in stores:
        copy.wait()


def layer_backward(layer, round_input, round_grad, grad, values, allowed, saved, mats, forget_w, gains):
    tree_len, width = values.shape
    qkv, logit, lse, att, middle, gate_up = saved
    w_in, w_out, w_up, w_down = mats
    half = w_down.shape[1]
    f32, b16 = jnp.float32, jnp.bfloat16
    shape = jax.ShapeDtypeStruct
    return pl.pallas_call(
        partial(backward_kernel, layer, round_input, round_grad),
        out_shape=[
            shape((tree_len, width), f32),
            shape((16, width + 128), b16),
            shape((2, width), f32),
        ]
        + [shape(w.shape[1:], b16) for w in mats],
        in_specs=[VMEM] * 10 + [ANY] * 5,
        out_specs=[VMEM] * 3 + [ANY] * 4,
        scratch_shapes=[pltpu.VMEM(w.shape[1:], b16) for w in mats]
        + [
            pltpu.VMEM((tree_len, 2 * half), f32),
            pltpu.VMEM((tree_len, 3 * width), b16),
            pltpu.VMEM((width, tree_len), b16),
            pltpu.VMEM((tree_len, width), f32),
            pltpu.VMEM((tree_len, tree_len), f32),
            pltpu.VMEM((tree_len, 128), f32),
        ]
        + [pltpu.VMEM(w.shape[1:], b16) for w in mats]
        + [DMA((4,)), DMA((half // 256, 5)), DMA((4,))],
        compiler_params=pltpu.CompilerParams(vmem_limit_bytes=60 * 2**20),
        name=f"backward_{layer}",
    )(grad, values, allowed, qkv, logit, lse, att, middle, forget_w, gains, gate_up, *mats)
def head_forward_kernel(rows_each, z_ref, table_ref, marks_ref, logits_ref, stats_ref):
    rows = z_ref.shape[0]
    chunk = 256 if table_ref.shape[0] % 256 == 0 else 128
    z = z_ref[...]

    def body(n, carry):
        peak, count, linear = carry
        at = pl.ds(pl.multiple_of(n * chunk, chunk), chunk)
        logits = dims_nt(z, table_ref[at, :])
        column = lax.broadcasted_iota(jnp.int32, (rows, chunk), 1) + n * chunk
        linear = linear + jnp.sum(logits * marks_ref[:, at], axis=1, keepdims=True)
        logits = jnp.where(column < rows_each, logits, masked_score)
        logits_ref[:, at] = logits
        new_peak = jnp.maximum(peak, jnp.max(logits, axis=1, keepdims=True))
        count = count * jnp.exp(peak - new_peak) + jnp.sum(jnp.exp(logits - new_peak), axis=1, keepdims=True)
        return new_peak, count, linear

    start = jnp.full((rows, 1), masked_score, jnp.float32)
    zero = jnp.zeros((rows, 1), jnp.float32)
    peak, count, linear = lax.fori_loop(0, table_ref.shape[0] // chunk, body, (start, zero, zero))
    lane = lax.broadcasted_iota(jnp.int32, (rows, 128), 1)
    stats = jnp.where(lane == 0, peak, jnp.where(lane == 1, count, jnp.where(lane == 2, linear, 0.0)))
    stats_ref[...] = stats.T[0:4, :]


def head_forward(rows_each, z, table, marks):
    rows, width = z.shape[0], table.shape[0]
    return pl.pallas_call(
        partial(head_forward_kernel, rows_each),
        out_shape=[jax.ShapeDtypeStruct((rows, width), jnp.float32), jax.ShapeDtypeStruct((4, rows), jnp.float32)],
        in_specs=[VMEM] * 3,
        out_specs=[VMEM] * 2,
        name="head_forward",
    )(z, table, marks)


def head_backward_kernel(sections, span, pos_all, z_ref, table_ref, marks_ref, logits_ref, stats_ref,
                         prob_ref, dz_ref, dtable_ref, row_ref, grads):
    rows, width = logits_ref.shape
    peak = jnp.max(stats_ref[:, 0, :], axis=0, keepdims=True)
    count = jnp.sum(stats_ref[:, 1, :] * jnp.exp(stats_ref[:, 0, :] - peak), axis=0, keepdims=True)
    log_norm = peak + jnp.log(count)
    prob = prob_ref[...]
    prob_sum = jnp.sum(prob, axis=1, keepdims=True)
    entropy = jnp.sum(prob * jnp.log(prob), axis=1, keepdims=True)
    log_norm = jnp.broadcast_to(log_norm, (128, rows)).T[:, 0:1]
    whole = jnp.sum(log_norm * (1.0 + prob_sum) + entropy) - jnp.sum(stats_ref[:, 2, :])
    row_ref[...] = jnp.full((8, 128), whole)
    chunk = 256 if width % 256 == 0 else 128
    weight = 1.0 + prob_sum

    def body(n, carry):
        at = pl.ds(pl.multiple_of(n * chunk, chunk), chunk)
        grad = (weight * jnp.exp(logits_ref[:, at] - log_norm) - marks_ref[:, at]) * (1.0 / pos_all)
        grads[:, at] = lower(grad)
        dtable_ref[at, :] = dims_tn(lower(grad), z_ref[...])
        return carry

    lax.fori_loop(0, width // chunk, body, 0)
    section = lax.axis_index("section")
    for r in range(rows // (sections * span)):
        at = pl.ds(pl.multiple_of((r * sections + section) * span, span), span)
        dz_ref[r * span : (r + 1) * span, :] = lower(product(grads[at, :], table_ref[...]))


def head_backward(z, table, marks, logits, stats_all, prob, span, pos_all):
    rows, width = logits.shape
    sections = lax.axis_size("section")
    return pl.pallas_call(
        partial(head_backward_kernel, sections, span, pos_all),
        out_shape=[
            jax.ShapeDtypeStruct((rows // sections, z.shape[1]), jnp.bfloat16),
            jax.ShapeDtypeStruct((width, z.shape[1]), jnp.float32),
            jax.ShapeDtypeStruct((8, 128), jnp.float32),
        ],
        in_specs=[VMEM] * 6,
        out_specs=[VMEM] * 3,
        scratch_shapes=[pltpu.VMEM((rows, width), jnp.bfloat16)],
        name="head_backward",
    )(z, table, marks, logits, stats_all, prob)
def pieces_of(rows):
    part = 400 if rows % 400 == 0 else rows
    return [(at, part) for at in range(0, rows, part)]


def each_tile(rows, columns, fn, carry):
    step = 16
    wide = 256 if columns % 256 == 0 else columns

    def body(n, carry):
        at = pl.ds(pl.multiple_of(n * step, step), step)
        for c in range(0, columns, wide):
            carry = fn(at, slice(c, c + wide), carry)
        return carry

    carry = lax.fori_loop(0, rows // step, body, carry)
    if rows % step:
        at = slice(rows // step * step, rows)
        tail = [jnp.zeros((rows % step, wide), jnp.float32)] * 2
        for c in range(0, columns, wide):
            tail = fn(at, slice(c, c + wide), tail)
        carry = [carry[0], carry[1]] + [jnp.sum(t) for t in tail]
    return carry


def step_kernel(shapes, scalar_ref, sums_ref, *refs):
    n = len(shapes)
    small_sums, refs = refs[:5], refs[5:]
    small_in, refs = refs[:6], refs[6:]
    grads, refs = refs[:n], refs[n:]
    weights, refs = refs[:n], refs[n:]
    firsts, refs = refs[:n], refs[n:]
    seconds, refs = refs[:n], refs[n:]
    out_first, refs = refs[:n], refs[n:]
    out_second, refs = refs[:n], refs[n:]
    out_dir, refs = refs[:n], refs[n:]
    small_out, refs = refs[:6], refs[6:]
    norm_ref, small_norm_ref, refs = refs[0], refs[1], refs[2:]
    g_buf, refs = refs[:n], refs[n:]
    w_buf, refs = refs[:n], refs[n:]
    m_buf, refs = refs[:n], refs[n:]
    v_buf, refs = refs[:n], refs[n:]
    d_buf, refs = refs[:n], refs[n:]
    load_sem, store_sem = refs
    work = []
    for a in range(n):
        for at, part in pieces_of(shapes[a][0]):
            rows = pl.ds(at, part)
            p = len(work)
            loads = [
                pltpu.make_async_copy(src.at[rows], dst.at[rows], load_sem.at[p, q])
                for q, (src, dst) in enumerate(
                    ((grads[a], g_buf[a]), (weights[a], w_buf[a]), (firsts[a], m_buf[a]), (seconds[a], v_buf[a]))
                )
            ]
            stores = [
                pltpu.make_async_copy(src.at[rows], dst.at[rows], store_sem.at[p, q])
                for q, (src, dst) in enumerate(
                    ((m_buf[a], out_first[a]), (v_buf[a], out_second[a]), (d_buf[a], out_dir[a]))
                )
            ]
            work.append((a, at, part, loads, stores))
    for _, _, _, loads, _ in work[:3]:
        for copy in loads:
            copy.start()
    lane = lax.broadcasted_iota(jnp.int32, (8, 128), 1)
    row = lax.broadcasted_iota(jnp.int32, (8, 128), 0)

    def scalar_at(values, r, c):
        return jnp.sum(jnp.where((row == r) & (lane == c), values, 0.0))

    smalls = [ref[...].astype(jnp.float32) for ref in small_sums]
    norm = jnp.sqrt(
        jnp.full((1, 1), scalar_at(sums_ref[...], 0, 0) + sum(square_sum(v) for v in smalls))
    )
    clip = jnp.minimum(1.0, scalar_ref[2] / norm)
    inverse_first = scalar_ref[0]
    inverse_second = scalar_ref[1]

    def adam(weight, grad, first, second):
        scaled = clip * grad
        first_new = beta_first * first + (1.0 - beta_first) * scaled
        second_new = beta_second * second + (1.0 - beta_second) * scaled * scaled
        direction = (first_new * inverse_first) / (
            jnp.sqrt(second_new * inverse_second) + adam_eps
        ) + decay_rate * weight
        return first_new, second_new, direction

    def small_step(group, part, grad):
        w_ref, m_ref, v_ref = small_in[3 * group : 3 * group + 3]
        weight = w_ref[part]
        first_new, second_new, direction = adam(weight, grad, m_ref[part], v_ref[part])
        norms = [jnp.sqrt(jnp.full((1, 1), square_sum(v))) for v in (weight, direction)]
        small_out[3 * group][part] = weight - learn_rate * (norms[0] / norms[1]) * direction
        small_out[3 * group + 1][part] = first_new
        small_out[3 * group + 2][part] = second_new
        return norms

    features, heads = small_in[0].shape[1:]
    small_norms = []
    for layer in range(2):
        small_norms += small_step(0, layer, smalls[layer].T[0:features, 0:heads])
    for t in range(5):
        grad = smalls[2 + t // 2][t % 2 : t % 2 + 1, :]
        small_norms += small_step(1, slice(t, t + 1), grad)
    table = jnp.where((row == 0) & (lane == 0), norm, 0.0)
    for t, value in enumerate(small_norms):
        table = jnp.where((row == 1) & (lane == t), value, table)
    small_norm_ref[...] = table

    sums = [[jnp.float32(0), jnp.float32(0)] for _ in range(n)]
    for p, (a, at, part, loads, stores) in enumerate(work):
        for copy in loads:
            copy.wait()
        if p + 3 < len(work):
            for copy in work[p + 3][3]:
                copy.start()
        g, w, m, v, d = (buf[a].at[pl.ds(at, part)] for buf in (g_buf, w_buf, m_buf, v_buf, d_buf))
        columns = shapes[a][1]
        wide = 256 if columns % 256 == 0 else columns

        def tile(rows, cols, carry):
            weight = w[rows, cols]
            first_new, second_new, direction = adam(
                weight, g[rows, cols].astype(jnp.float32), m[rows, cols], v[rows, cols]
            )
            m[rows, cols] = first_new
            v[rows, cols] = second_new
            d[rows, cols] = direction
            return [carry[0] + weight * weight, carry[1] + direction * direction]

        zero = jnp.zeros((16, wide), jnp.float32)
        done = each_tile(part, columns, tile, [zero, zero])
        for copy in stores:
            copy.start()
        for q in range(2):
            sums[a][q] = sums[a][q] + jnp.sum(done[q])
            if len(done) > 2:
                sums[a][q] = sums[a][q] + done[2 + q]
    section = lax.axis_index("section")
    table = jnp.zeros((8, 128), jnp.float32)
    for a in range(n):
        here = (section if a == 0 else lax.axis_index("replica")) == 0
        place = 0 if a == 0 else 2 * section
        for q in range(2):
            value = jnp.where(here, sums[a][q], 0.0)
            table = jnp.where((row == a) & (lane == place + q), value, table)
    norm_ref[...] = table
    for _, _, _, _, stores in work:
        for copy in stores:
            copy.wait()


def optimizer_step(scalars, sums, small_sums, small, grads, weights, firsts, seconds):
    n = len(grads)
    shapes = [w.shape for w in weights]
    flat = [jax.ShapeDtypeStruct(s, jnp.float32) for s in shapes]
    buffers = lambda kinds: [pltpu.VMEM(s, k) for s, k in zip(shapes, kinds)]
    parts = sum(len(pieces_of(s[0])) for s in shapes)
    out = pl.pallas_call(
        partial(step_kernel, shapes),
        out_shape=flat * 3
        + [jax.ShapeDtypeStruct(s.shape, jnp.float32) for s in small]
        + [jax.ShapeDtypeStruct((8, 128), jnp.float32)] * 2,
        in_specs=[pl.BlockSpec(memory_space=pltpu.SMEM)] + [VMEM] * 12 + [ANY] * (4 * n),
        out_specs=[ANY] * (3 * n) + [VMEM] * 8,
        scratch_shapes=buffers([g.dtype for g in grads])
        + buffers([jnp.float32] * n) * 4
        + [DMA((parts, 4)), DMA((parts, 3))],
        compiler_params=pltpu.CompilerParams(vmem_limit_bytes=60 * 2**20),
        name="optimizer_step",
    )(scalars, sums, *small_sums, *small, *grads, *weights, *firsts, *seconds)
    return out[:n], out[n : 2 * n], out[2 * n : 3 * n], out[3 * n : 3 * n + 6], out[-2], out[-1]


def apply_kernel(shapes, norm_ref, *refs):
    n = len(shapes)
    norms = jnp.sqrt(norm_ref[...])
    lane = lax.broadcasted_iota(jnp.int32, (8, 128), 1)
    row = lax.broadcasted_iota(jnp.int32, (8, 128), 0)

    def norm_at(a, q):
        place = q if a == 0 else 2 * lax.axis_index("section") + q
        return jnp.full((1, 1), jnp.sum(jnp.where((row == a) & (lane == place), norms, 0.0)))

    weights, directions, outs = refs[:n], refs[n : 2 * n], refs[2 * n : 3 * n]
    w_buf, d_buf = refs[3 * n : 4 * n], refs[4 * n : 5 * n]
    load_sem, store_sem = refs[5 * n :]
    work = []
    for a in range(n):
        for at, part in pieces_of(shapes[a][0]):
            rows = pl.ds(at, part)
            p = len(work)
            loads = [
                pltpu.make_async_copy(weights[a].at[rows], w_buf[a].at[rows], load_sem.at[p, 0]),
                pltpu.make_async_copy(directions[a].at[rows], d_buf[a].at[rows], load_sem.at[p, 1]),
            ]
            store = pltpu.make_async_copy(w_buf[a].at[rows], outs[a].at[rows], store_sem.at[p])
            work.append((a, at, part, loads, store))
    for _, _, _, loads, _ in work[:3]:
        for copy in loads:
            copy.start()
    for p, (a, at, part, loads, store) in enumerate(work):
        for copy in loads:
            copy.wait()
        if p + 3 < len(work):
            for copy in work[p + 3][3]:
                copy.start()
        w, d = w_buf[a].at[pl.ds(at, part)], d_buf[a].at[pl.ds(at, part)]
        rate = learn_rate * (norm_at(a, 0) / norm_at(a, 1))

        def tile(rows, cols, carry):
            w[rows, cols] = w[rows, cols] - rate * d[rows, cols]
            return carry

        each_tile(part, shapes[a][1], tile, [jnp.float32(0), jnp.float32(0)])
        store.start()
    for _, _, _, _, store in work:
        store.wait()


def apply_step(norms, weights, directions):
    n = len(weights)
    shapes = [w.shape for w in weights]
    parts = sum(len(pieces_of(s[0])) for s in shapes)
    return pl.pallas_call(
        partial(apply_kernel, shapes),
        out_shape=[jax.ShapeDtypeStruct(s, jnp.float32) for s in shapes],
        in_specs=[VMEM] + [ANY] * (2 * n),
        out_specs=[ANY] * n,
        scratch_shapes=[pltpu.VMEM(s, jnp.float32) for s in shapes] * 2 + [DMA((parts, 2)), DMA((parts,))],
        compiler_params=pltpu.CompilerParams(vmem_limit_bytes=62 * 2**20),
        name="apply_step",
    )(norms, *weights, *directions)


def lower(values):
    return values.astype(jnp.bfloat16)


def product(left, right):
    return jnp.dot(left, right, preferred_element_type=jnp.float32)


def product_left(left, right):
    return lax.dot_general(left, right, (((0,), (0,)), ((), ())), preferred_element_type=jnp.float32)


def product_right(left, right):
    return lax.dot_general(left, right, (((1,), (1,)), ((), ())), preferred_element_type=jnp.float32)


def rms_forward(values, gain):
    inverse = lax.rsqrt(jnp.mean(values * values, axis=-1, keepdims=True) + eps_norm)
    normed = values * inverse
    return (normed * gain, normed, inverse)


def rms_backward(grad_out, normed, inverse, gain):
    grad_normed = grad_out * gain
    grad_in = inverse * (
        grad_normed - normed * jnp.mean(grad_normed * normed, axis=-1, keepdims=True)
    )
    return (grad_in, jnp.sum(grad_out * normed, axis=0))


def path_mask(parent_row, tree_len):
    seg_count = parent_row.shape[0]
    seglen = tree_len // seg_count
    seg_order = jnp.arange(seg_count, dtype=jnp.int32)
    parent_hot = ((parent_row[:, None] == seg_order[None, :]) & (seg_order[:, None] >= 1)).astype(
        jnp.float32
    )
    identity = jnp.eye(seg_count, dtype=jnp.float32)
    power, steps = parent_hot, 1
    reached = identity + parent_hot
    while steps < seg_count:
        reached = jnp.minimum(1.0, jnp.dot(reached, reached))
        steps *= 2
    strict = reached - identity
    seg_of = jnp.arange(tree_len, dtype=jnp.int32) // seglen
    seg_hot = (seg_of[:, None] == seg_order[None, :]).astype(jnp.float32)
    ancestor = jnp.dot(jnp.dot(seg_hot, strict), seg_hot.T)
    places = jnp.arange(tree_len, dtype=jnp.int32)
    inside = (seg_of[:, None] == seg_of[None, :]) & (places[None, :] <= places[:, None])
    return ancestor + inside.astype(jnp.float32)


def square_sum(values):
    return jnp.sum(values * values)


def local(
    tokens,
    parents,
    loss_positions,
    targets,
    teacher_index,
    teacher_probability,
    step_count,
    embed_table,
    table_first,
    table_second,
    attention_in,
    attention_in_first,
    attention_in_second,
    attention_out,
    attention_out_first,
    attention_out_second,
    feedforward_in,
    feedforward_in_first,
    feedforward_in_second,
    feedforward_out,
    feedforward_out_first,
    feedforward_out_second,
    forget_gate,
    forget_first,
    forget_second,
    norm_gains,
    gains_first,
    gains_second,
):
    section_id = lax.axis_index("section")
    replica_id = lax.axis_index("replica")
    shard_id = lax.axis_index("shard")
    sections = lax.axis_size("section")
    replicas = lax.axis_size("replica")
    shards = lax.axis_size("shard")
    group_trees, tree_len = tokens.shape
    rows_each, width = embed_table.shape
    pos_count = loss_positions.shape[1]
    pos_all = group_trees * replicas * pos_count
    owners = replicas * shards
    owner_id = replica_id * shards + shard_id
    own_tree = section_id * shards + shard_id
    table_low = lower(embed_table)

    def own_row(values):
        return lax.dynamic_index_in_dim(values, own_tree, 0, keepdims=False)

    tree_tokens = own_row(tokens)
    token_owner = tree_tokens // rows_each
    token_row = tree_tokens % rows_each
    spots = jnp.arange(tree_len, dtype=jnp.int32)

    def asked(batch):
        earlier = spots[None, :] < spots[:, None]
        same = tree_tokens[:, None] == tree_tokens[None, :]
        is_first = jnp.logical_not(jnp.any(same & earlier, axis=1))
        counted = earlier & (token_owner[:, None] == token_owner[None, :]) & is_first[None, :]
        number_first = jnp.sum(counted.astype(jnp.int32), axis=1)
        number = jnp.sum(jnp.where(same & is_first[None, :], number_first[None, :], 0), axis=1)
        slot = number - batch * batch_rows
        inside = (slot >= 0) & (slot < batch_rows)
        place = jnp.where(inside, token_owner * batch_rows + slot, -1)
        spot_of = jnp.arange(owners * batch_rows, dtype=jnp.int32)
        hot = place[None, :] == spot_of[:, None]
        rows = jnp.max(jnp.where(hot & is_first[None, :], token_row[None, :] + 1, 0), axis=1)
        return rows.reshape(owners, batch_rows), lower(hot)

    def all_devices(part, ident):
        return exchange(part[None], ident, relay=True).reshape((sections, replicas, shards) + part.shape)

    def wanted(batch):
        rows, hot = asked(batch)
        every = all_devices(jnp.pad(rows, ((0, 0), (0, 128 - batch_rows))), 0)
        mine = lax.dynamic_index_in_dim(every, owner_id, 3, keepdims=False)[..., :batch_rows]
        wish = mine.reshape(sections * owners * batch_rows) - 1
        row_of = jnp.arange(rows_each, dtype=jnp.int32)
        return hot, lower(wish[:, None] == row_of[None, :])

    def more_rows(state):
        batch, total_rows = state
        hot_more, pick = wanted(batch)
        own_pick = lax.dynamic_index_in_dim(
            pick.reshape(sections, owners * batch_rows, rows_each), section_id, 0, keepdims=False
        )
        sent = lower(product(own_pick, table_low)).reshape(owners, batch_rows, width)
        got_more = exchange(sent, 1)[0].reshape(owners * batch_rows, width)
        return (batch + 1, total_rows + product_left(hot_more, got_more))

    def more_grads(state):
        batch, total_rows = state
        hot_more, pick = wanted(batch)
        sent = lower(product(hot_more, embed_low)).reshape(owners, batch_rows, width)
        got_more = exchange(sent, 6, relay=True).reshape(sections * owners * batch_rows, width)
        more = product_left(pick, got_more)
        return (batch + 1, total_rows + jnp.pad(more, ((0, width_all - rows_each), (0, 0))))

    def halves(weight):
        return lower(weight).reshape(2, weight.shape[1] // 2, weight.shape[2])

    width_all = -(-rows_each // 128) * 128
    table_wide = jnp.pad(table_low, ((0, width_all - rows_each), (0, 0)))
    layer_weights = (attention_in, attention_out, feedforward_in, feedforward_out)
    entries = 8 * teacher_index.shape[2]
    group_data = [
        teacher_index.reshape(-1, 1, entries),
        teacher_probability.reshape(-1, 1, entries),
        targets.reshape(-1, 1),
    ]
    pair_parts = group_data if replicas == 2 else []
    hot, asks = ask_rows(tree_tokens, token_owner, token_row, owners)
    gathered, group_all, (asked_all, got, *marks) = gather(
        [halves(w) for w in layer_weights], 2, pair_parts, split=True, errand=(asks, table_wide), rows_each=rows_each
    )
    if replicas != 2:
        group_all = [lax.all_gather(part, "replica") for part in group_data]
        marks = [spread_entries((owner_id * rows_each)[None], *group_all, rows_each, width_all)]
    batches = (jnp.max(asked_all[:, :, 0, 127]) + batch_rows - 1) // batch_rows
    embeds = product_left(hot, got.reshape(owners * batch_rows, width))
    _, embeds = lax.while_loop(lambda s: s[0] < batches, more_rows, (jnp.int32(1), embeds))
    mats = [g.reshape(sections, -1, g.shape[-1]) for g in gathered]
    heads = forget_gate.shape[2]
    forget_low = jnp.pad(lower(forget_gate[:, :width]), ((0, 0), (0, 0), (0, 128 - heads)))
    forget_bias = jnp.pad(forget_gate[:, width:], ((0, 0), (0, 0), (0, 128 - heads)))
    gains_of = [jnp.pad(norm_gains[2 * n : 2 * n + 2], ((0, 6), (0, 0))) for n in range(2)]

    allowed = lower(path_mask(own_row(parents), tree_len))
    out_0, *saved_0 = layer_forward(0, False, embeds, allowed, mats, forget_low[0], forget_bias[0], gains_of[0])
    out_1, *saved_1 = layer_forward(1, True, out_0, allowed, mats, forget_low[1], forget_bias[1], gains_of[1])

    positions = own_row(loss_positions)
    position_hot = (positions[:, None] == spots[None, :]).astype(jnp.float32)
    picked = jnp.take(out_1, positions, axis=0)
    final_gain = norm_gains[4]
    head_out, head_normed, head_inverse = rms_forward(picked, final_gain)
    head_rows = jnp.swapaxes(all_devices(lower(head_out), 3), 0, 1).reshape(pos_all, width)

    prob_all = group_all[1].reshape(pos_all, -1)
    marks = marks[0]
    logits, stats = head_forward(rows_each, head_rows, table_wide, marks)
    if replicas == 2:
        stats_all = exchange(stats[None], 4)[0]
    else:
        stats_all = lax.all_gather(lax.all_gather(stats, "replica"), "shard")
    grad_heads, head_table, loss_sum = head_backward(
        head_rows, table_wide, marks, logits, stats_all.reshape(owners, 4, pos_all), prob_all, shards * pos_count, pos_all
    )
    grad_heads = exchange(grad_heads.reshape(owners, pos_count, width), 5)[0]
    grad_heads = jnp.sum(grad_heads.astype(jnp.float32), axis=0)
    grad_picked, grad_final = rms_backward(grad_heads, head_normed, head_inverse, final_gain)
    grad_top = lax.dot_general(
        position_hot, grad_picked, (((0,), (0,)), ((), ())), precision=highest
    )

    grad_mid, forget_1, gains_1, *grads_1 = layer_backward(
        1, True, False, grad_top, out_0, allowed, saved_1, mats, forget_low[1], gains_of[1]
    )
    grad_low, forget_0, gains_0, *grads_0 = layer_backward(
        0, False, True, grad_mid, embeds, allowed, saved_0, mats, forget_low[0], gains_of[0]
    )
    embed_low = lower(grad_low)

    stacked = [
        [g.reshape(shards, 2, -1, g.shape[-1]) for g in pair] for pair in zip(grads_0, grads_1)
    ]
    sent = lower(product(hot, embed_low)).reshape(owners, batch_rows, width)
    small_sums = [forget_0, forget_1, gains_0, gains_1, grad_final[None]]
    layer_grads, (got_grads,) = reduce_parts(stacked, 8, ([], sent))
    if replicas != 2:
        layer_grads = [lax.psum(g * jnp.bfloat16(0.5), "replica") for g in layer_grads]
    _, head_table = lax.while_loop(lambda s: s[0] < batches, more_grads, (jnp.int32(1), head_table))
    table_grad, square = table_gradient(
        rows_each, asked_all, got_grads.reshape(-1, width), head_table, layer_grads
    )
    layer_grads = [g.reshape(w.shape[1:]) for g, w in zip(layer_grads, layer_weights)]
    scalars, *small_sums = total([square, *small_sums], 15)
    loss_total = loss_sum[0, 0] / pos_all
    count_float = step_count.astype(jnp.float32)
    rates = jnp.stack(
        [
            1.0 / (1.0 - jnp.power(beta_first, count_float)),
            1.0 / (1.0 - jnp.power(beta_second, count_float)),
            clip_factor / jnp.sqrt(jnp.float32(pos_all)),
        ]
    )
    small = [forget_gate, forget_first, forget_second, norm_gains, gains_first, gains_second]
    weights = [embed_table] + [w[0] for w in layer_weights]
    firsts = [table_first] + [
        m[0] for m in (attention_in_first, attention_out_first, feedforward_in_first, feedforward_out_first)
    ]
    seconds = [table_second] + [
        m[0] for m in (attention_in_second, attention_out_second, feedforward_in_second, feedforward_out_second)
    ]
    firsts_new, seconds_new, directions, small_new, norms, small_norms = optimizer_step(
        rates, scalars, small_sums, small, [table_grad, *layer_grads], weights, firsts, seconds
    )
    (norms,) = total([norms], 16)
    weights_new = apply_step(norms, weights, directions)
    norms = jnp.sqrt(norms)
    table_norms = norms[0, :2]
    layer_norms = norms[1:5, : 2 * sections].reshape(4 * sections, 2)
    new_table, table_first_new, table_second_new = weights_new[0], firsts_new[0], seconds_new[0]
    new_layers = [(weights_new[n][None], firsts_new[n][None], seconds_new[n][None]) for n in range(1, 5)]
    new_forget, forget_first_new, forget_second_new, new_gains, gains_first_new, gains_second_new = small_new
    layer_count, gain_count = forget_gate.shape[0], norm_gains.shape[0]
    grad_norm = small_norms[0, 0]
    tensor_norms = jnp.concatenate(
        [
            table_norms[None],
            layer_norms,
            small_norms[1, : 2 * (layer_count + gain_count)].reshape(-1, 2),
        ],
        axis=0,
    )
    return (
        new_table,
        table_first_new,
        table_second_new,
        *new_layers[0],
        *new_layers[1],
        *new_layers[2],
        *new_layers[3],
        new_forget,
        forget_first_new,
        forget_second_new,
        new_gains,
        gains_first_new,
        gains_second_new,
        tensor_norms,
        grad_norm,
        loss_total,
    )


def solution(mesh):
    group = P("replica", None)
    table = P(("replica", "shard"), None)
    layer = P("section", "shard", None)
    in_specs = (
        (group,) * 4
        + (P("replica", None, None),) * 2
        + (P(),)
        + (table,) * 3
        + (layer,) * 12
        + (P(),) * 6
    )
    out_specs = (table,) * 3 + (layer,) * 12 + (P(),) * 9
    return jax.shard_map(local, mesh=mesh, in_specs=in_specs, out_specs=out_specs, check_vma=False)
```

```python
from functools import partial

import jax
import jax.numpy as jnp
from jax import lax
from jax.experimental import pallas as pl
from jax.experimental.pallas import tpu as pltpu
from jax.sharding import PartitionSpec as P

MESH = pl.DeviceIdType.MESH
VMEM = pl.BlockSpec(memory_space=pltpu.VMEM)
ANY = pl.BlockSpec(memory_space=pl.ANY)
DMA = pltpu.SemaphoreType.DMA
eps_norm = 1e-06
beta_first = 0.9
beta_second = 0.999
adam_eps = 1e-10
decay_rate = 0.01
learn_rate = 0.2
clip_factor = 8.0
highest = lax.Precision.HIGHEST
masked_score = -1e30
batch_rows = 32
every_axis = ("section", "replica", "shard")


class Place:
    def __init__(self):
        self.sections = lax.axis_size("section")
        self.replicas = lax.axis_size("replica")
        self.shards = lax.axis_size("shard")
        self.nz = min(4, self.shards)
        self.ny = self.shards // self.nz
        self.x = lax.axis_index("section")
        self.rep = lax.axis_index("replica")
        self.shard = lax.axis_index("shard")
        self.core = lax.rem(self.rep, 2)
        self.z = self.shard // self.ny
        self.y = lax.rem(self.shard, self.ny)

    def at(self, section=None, rep=None, z=None, y=None, shard=None):
        if shard is None:
            shard = (self.z if z is None else z) * self.ny + (self.y if y is None else y)
        return {
            "section": self.x if section is None else section,
            "replica": self.rep if rep is None else rep,
            "shard": shard,
        }

    def peer_x(self, i):
        return self.at(section=lax.rem(self.x + i, self.sections))

    def peer_y(self, j):
        return self.at(y=lax.rem(self.y + j, self.ny))

    def line(self, step):
        return self.at(z=self.z + step)

    def partner(self):
        return self.at(rep=self.rep + 1 - 2 * self.core)

    def group(self, p):
        count = self.replicas * self.shards
        place = lax.rem(self.rep * self.shards + self.shard + p, count)
        return place, self.at(rep=place // self.shards, shard=lax.rem(place, self.shards))

    def device(self, i, p):
        place, _ = self.group(p)
        section = lax.rem(self.x + i, self.sections)
        return place, self.at(section=section, rep=place // self.shards, shard=lax.rem(place, self.shards))

    def greet_all(self):
        barrier = pltpu.get_barrier_semaphore()
        peers = self.replicas * self.shards
        for i in range(self.sections):
            for p in range(peers):
                if i or p:
                    pl.semaphore_signal(barrier, inc=1, device_id=self.device(i, p)[1], device_id_type=MESH)
        pl.semaphore_wait(barrier, self.sections * peers - 1)

    def greet_group(self):
        barrier = pltpu.get_barrier_semaphore()
        peers = self.replicas * self.shards
        for p in range(1, peers):
            pl.semaphore_signal(barrier, inc=1, device_id=self.group(p)[1], device_id_type=MESH)
        for i in range(1, self.sections):
            pl.semaphore_signal(barrier, inc=1, device_id=self.peer_x(i), device_id_type=MESH)
        pl.semaphore_wait(barrier, peers + self.sections - 2)

    def inside(self, k):
        if k == 0:
            return None
        return self.z + k < self.nz if k > 0 else self.z + k >= 0

    def greet(self, use_x=True):
        barrier = pltpu.get_barrier_semaphore()

        def signal(device):
            pl.semaphore_signal(barrier, inc=1, device_id=device, device_id_type=MESH)

        count = 1
        if use_x:
            for i in range(1, self.sections):
                signal(self.peer_x(i))
                count += 1
        for j in range(1, self.ny):
            signal(self.peer_y(j))
            count += 1
        signal(self.partner())
        up, down = self.inside(1), self.inside(-1)
        pl.when(up)(lambda: signal(self.line(1)))
        pl.when(down)(lambda: signal(self.line(-1)))
        ends = jnp.minimum(self.z, 1) + jnp.minimum(self.nz - 1 - self.z, 1)
        pl.semaphore_wait(barrier, count + ends)


def when(cond, fn):
    if cond is None:
        fn()
    else:
        pl.when(cond)(fn)


def both(a, b):
    if a is None:
        return b
    if b is None:
        return a
    return jnp.logical_and(a, b)


def remote(src, dst, send, recv, device):
    return pltpu.make_async_remote_copy(
        src_ref=src, dst_ref=dst, send_sem=send, recv_sem=recv, device_id=device, device_id_type=MESH
    )


def rows_errand(me, ask_ref, table_ref, asked_ref, got_ref, hot, found, ask_sem, row_sem, own_sem):
    peers = me.replicas * me.shards
    mine = me.rep * me.shards + me.shard
    width = table_ref.shape[1]
    asks = []
    for i in range(me.sections):
        for p in range(peers):
            place, device = me.device(i, p)
            if i or p:
                asks.append(remote(ask_ref.at[place], asked_ref.at[me.x, mine], ask_sem.at[0, i, p], ask_sem.at[1, i, p], device))
    for copy in asks:
        copy.start()
    own_ask = pltpu.make_async_copy(ask_ref.at[mine], asked_ref.at[me.x, mine], own_sem.at[0])
    own_ask.start()
    rows = [
        remote(found.at[me.group(p)[0]], got_ref.at[mine], row_sem.at[0, p], row_sem.at[1, p], me.group(p)[1])
        for p in range(1, peers)
    ]
    own_rows = pltpu.make_async_copy(found.at[mine], got_ref.at[mine], own_sem.at[1])

    def look_up():
        own_ask.wait()
        for i in range(me.sections):
            for p in range(peers):
                if i or p:
                    source = lax.rem(mine + peers - p, peers)
                    dst = asked_ref.at[lax.rem(me.x + me.sections - i, me.sections), source]
                    remote(dst, dst, ask_sem.at[0, i, p], ask_sem.at[1, i, p], me.partner()).wait_recv()
        wish = asked_ref[me.x].reshape(peers, 128).astype(jnp.float32).T
        column = lax.broadcasted_iota(jnp.int32, (batch_rows, table_ref.shape[0]), 1).astype(jnp.float32) + 1.0
        for s in range(peers):
            ours = wish[0:batch_rows, s : s + 1] == column
            hot[s * batch_rows : (s + 1) * batch_rows, :] = jnp.where(ours, 1.0, 0.0).astype(jnp.bfloat16)

        def take(n, carry):
            at = pl.ds(pl.multiple_of(n * 256, 256), 256)
            values = jnp.dot(hot[...], table_ref[:, at], preferred_element_type=jnp.float32)
            found[:, :, at] = values.reshape(peers, batch_rows, 256).astype(jnp.bfloat16)
            return carry

        lax.fori_loop(0, width // 256, take, 0)
        own_rows.start()
        for copy in rows:
            copy.start()

    def finish():
        for p in range(1, peers):
            source = lax.rem(mine + peers - p, peers)
            dst = got_ref.at[source]
            remote(dst, dst, row_sem.at[0, p], row_sem.at[1, p], me.partner()).wait_recv()
        own_rows.wait()
        for copy in asks + rows:
            copy.wait_send()

    return {1: look_up, "end": finish}


def gather_kernel(count, pairs, split, orders, errand, *refs):
    ins, refs = refs[:count], refs[count:]
    pair_ins, refs = refs[:pairs], refs[pairs:]
    asked = 2 if errand else 0
    errand_in, refs = refs[:asked], refs[asked:]
    outs, refs = refs[:count], refs[count:]
    pair_outs, refs = refs[:pairs], refs[pairs:]
    errand_out, refs = refs[:asked], refs[asked:]
    if errand and pairs:
        marks_ref, refs = refs[0], refs[1:]
    errand_refs = errand_in + errand_out
    send_sem, recv_sem, cross_sem, pair_sem, local_sem = refs[:5]
    me = Place()
    nz, ny, nx = me.nz, me.ny, me.sections
    if "x" not in orders[0][0][0]:
        nx = 1
    hooks = {}
    if errand:
        me.greet_all()
        hooks = rows_errand(me, *errand_refs, *refs[5:])
    else:
        me.greet(use_x=nx > 1)

    def slot(ref, k, j, i, half):
        section = lax.rem(me.x + i, nx) if nx > 1 else 0
        return ref.at[section, (me.z + k) * ny + lax.rem(me.y + j, ny), half]

    locals_ = []
    for a in range(count):
        if split:
            dst = outs[a].at[me.x if nx > 1 else 0, me.shard]
        else:
            dst = outs[a].at[me.x if nx > 1 else 0, me.shard, me.core]
        locals_.append(pltpu.make_async_copy(ins[a], dst, local_sem.at[a]))
    for p in range(pairs):
        locals_.append(
            pltpu.make_async_copy(pair_ins[p], pair_outs[p].at[me.core], local_sem.at[count + p])
        )
    for copy in locals_:
        copy.start()
    pair_copies = [
        remote(pair_ins[p], pair_outs[p].at[me.core], pair_sem.at[0, p], pair_sem.at[1, p], me.partner())
        for p in range(pairs)
    ]

    def run(core, plan):
        sends = []

        def push(cond, src, dst, device, sem):
            copy = remote(src, dst, send_sem.at[len(sends)], sem, device)
            when(cond, copy.start)
            sends.append((cond, copy))

        def sem_of(a, k, j, i):
            return recv_sem.at[a, k + nz - 1, j, i]

        def spread(order, arrays, k, j, i, via):
            cond = me.inside(k)
            own = via is None
            later = order if own else order[order.index(via) + 1 :]
            for a in arrays:
                dst = slot(outs[a], k, j, i, core)
                src = dst
                if own:
                    src = ins[a].at[core] if split else ins[a]
                else:
                    arrival = remote(dst, dst, send_sem.at[0], sem_of(a, k, j, i), me.partner())
                    when(cond, arrival.wait_recv)
                steps = []
                if via == "z":
                    steps = [-1 if k > 0 else 1]
                elif "z" in later:
                    steps = [1, -1]
                for step in steps:
                    push(both(cond, me.inside(step)), src, dst, me.line(step), sem_of(a, k - step, j, i))
                if "y" in later:
                    for p in range(1, ny):
                        push(cond, src, dst, me.peer_y(p), sem_of(a, k, (j - p) % ny, i))
                if "x" in later:
                    for p in range(1, nx):
                        push(cond, src, dst, me.peer_x(p), sem_of(a, k, j, (i - p) % nx))
                if not (own and split):
                    push(cond, src, dst, me.partner(), cross_sem.at[a, k + nz - 1, j, i])

        events = []
        for order, arrays in plan:
            for k in range(1 - nz, nz):
                for j in range(ny):
                    for i in range(nx):
                        via = [d for d in order if {"z": k, "y": j, "x": i}[d] != 0]
                        hops = abs(k) + (j != 0) + (i != 0)
                        stage = order.index(via[-1]) if via else -1
                        events.append((hops, stage, k, j, i, order, arrays, via[-1] if via else None))
        events.sort(key=lambda e: e[:5])
        for n, (hops, stage, k, j, i, order, arrays, via) in enumerate(events):
            spread(order, arrays, k, j, i, via)
            if n + 1 < len(events) and events[n + 1][0] == hops:
                continue
            if hops == 0:
                for copy in pair_copies:
                    copy.start()
            if hops in hooks:
                hooks[hops]()
        for hops, stage, k, j, i, order, arrays, via in events:
            if via is None and split:
                continue
            for a in arrays:
                dst = slot(outs[a], k, j, i, 1 - core)
                arrival = remote(dst, dst, send_sem.at[0], cross_sem.at[a, k + nz - 1, j, i], me.partner())
                when(me.inside(k), arrival.wait_recv)
        for cond, copy in sends:
            when(cond, copy.wait_send)

    if errand and pairs:
        groups = 2 * pair_ins[0].shape[0]
        shift = (me.rep * me.shards + me.shard) * errand
        far_hops = [hops for hops in range(2, nz + 2)]

        def spread_some(n):
            if n == 0:
                for copy in locals_[count:]:
                    copy.wait()
                for p in range(pairs):
                    pair_copies[p].wait_send()
                    remote(
                        pair_ins[p], pair_outs[p].at[1 - me.core], pair_sem.at[0, p], pair_sem.at[1, p], me.partner()
                    ).wait_recv()
            edges = [groups * t // len(far_hops) for t in range(len(far_hops) + 1)]
            spread_range(edges[n], edges[n + 1], shift, errand, *pair_outs, marks_ref)

        for n, hops in enumerate(far_hops):
            hooks[hops] = partial(spread_some, n)

    for core, plan in enumerate(orders):
        pl.when(me.core == core)(partial(run, core, plan))
    if errand:
        hooks["end"]()
    for copy in locals_[:count]:
        copy.wait()


def gather(parts, ident, pair_parts=(), split=False, use_x=True, space=ANY, errand=(), rows_each=0):
    count, pairs = len(parts), len(pair_parts)
    every = list(range(count))
    if not use_x:
        orders = [[(("z", "y"), every)]] * 2
    elif split:
        orders = [[(("z", "y", "x"), every)], [(("x", "z", "y"), every[:-1]), (("x", "y", "z"), every[-1:])]]
    else:
        orders = [[(("z", "y", "x"), every)], [(("x", "z", "y"), every)]]
    shards = lax.axis_size("shard")
    nx = lax.axis_size("section") if use_x else 1
    nz = min(4, shards)
    ny = shards // nz
    lead = (nx, shards) if split else (nx, shards, 2)
    blocks = (2 * nz - 1) * ny * nx
    errand_shapes, errand_scratch = [], []
    if errand:
        asks, table = errand
        peers, wide = asks.shape[0], table.shape[1]
        errand_shapes = [
            jax.ShapeDtypeStruct((nx, peers) + asks.shape[1:], asks.dtype),
            jax.ShapeDtypeStruct((peers, batch_rows, wide), table.dtype),
        ]
        if pairs:
            rows = 2 * pair_parts[2].shape[0]
            errand_shapes.append(jax.ShapeDtypeStruct((rows, table.shape[0]), jnp.float32))
        errand_scratch = [
            pltpu.VMEM((peers * batch_rows, table.shape[0]), table.dtype),
            pltpu.VMEM((peers, batch_rows, wide), table.dtype),
            DMA((2, nx, peers)),
            DMA((2, peers)),
            DMA((2,)),
        ]
    outs = pl.pallas_call(
        partial(gather_kernel, count, pairs, split, orders, rows_each),
        out_shape=[jax.ShapeDtypeStruct(lead + p.shape, p.dtype) for p in parts]
        + [jax.ShapeDtypeStruct((2,) + p.shape, p.dtype) for p in pair_parts]
        + errand_shapes,
        in_specs=[VMEM] * (count + pairs + len(errand)),
        out_specs=[space] * count + [VMEM] * pairs + [VMEM] * len(errand_shapes),
        scratch_shapes=[
            DMA((blocks * count * 4,)),
            DMA((count, 2 * nz - 1, ny, nx)),
            DMA((count, 2 * nz - 1, ny, nx)),
            DMA((2, max(pairs, 1))),
            DMA((count + pairs,)),
        ]
        + errand_scratch,
        compiler_params=pltpu.CompilerParams(collective_id=ident, has_side_effects=True),
        name=f"gather_{ident}",
    )(*parts, *pair_parts, *errand)
    return outs[:count], outs[count : count + pairs], outs[count + pairs :]


def exchange_kernel(relay, src_ref, out_ref, send_sem, recv_sem, relay_send, relay_recv, local_sem):
    me = Place()
    peers = me.replicas * me.shards
    barrier = pltpu.get_barrier_semaphore()
    for p in range(1, peers):
        pl.semaphore_signal(barrier, inc=1, device_id=me.group(p)[1], device_id_type=MESH)
    if relay:
        for i in range(1, me.sections):
            pl.semaphore_signal(barrier, inc=1, device_id=me.peer_x(i), device_id_type=MESH)
    pl.semaphore_wait(barrier, peers - 1 + (me.sections - 1 if relay else 0))
    mine = me.rep * me.shards + me.shard
    section = me.x if relay else 0
    own = pltpu.make_async_copy(
        src_ref.at[mine if src_ref.shape[0] > 1 else 0], out_ref.at[section, mine], local_sem.at[0]
    )
    own.start()
    sends = []
    for p in range(1, peers):
        place, device = me.group(p)
        copy = remote(
            src_ref.at[place if src_ref.shape[0] > 1 else 0], out_ref.at[section, mine], send_sem.at[p], recv_sem.at[p], device
        )
        copy.start()
        sends.append(copy)
    relays = []

    def forward(p, src, dst):
        for i in range(1, me.sections):
            copy = remote(src, dst, relay_send.at[p, i], relay_recv.at[p, i], me.peer_x(i))
            copy.start()
            relays.append(copy)

    if relay:
        forward(0, src_ref.at[mine if src_ref.shape[0] > 1 else 0], out_ref.at[me.x, mine])
    for p in range(1, peers):
        source, device = me.group(peers - p)
        dst = out_ref.at[section, source]
        remote(dst, dst, send_sem.at[p], recv_sem.at[p], device).wait_recv()
        if relay:
            forward(p, dst, dst)
    if relay:
        for p in range(peers):
            source, _ = me.group(peers - p)
            for i in range(1, me.sections):
                dst = out_ref.at[lax.rem(me.x + me.sections - i, me.sections), source]
                remote(dst, dst, relay_send.at[p, i], relay_recv.at[p, i], me.peer_x(i)).wait_recv()
    for copy in sends + relays:
        copy.wait_send()
    own.wait()


def exchange(blocks, ident, relay=False):
    peers = lax.axis_size("replica") * lax.axis_size("shard")
    nx = lax.axis_size("section")
    return pl.pallas_call(
        partial(exchange_kernel, relay),
        out_shape=jax.ShapeDtypeStruct((nx if relay else 1, peers) + blocks.shape[1:], blocks.dtype),
        in_specs=[VMEM],
        out_specs=VMEM,
        scratch_shapes=[DMA((peers,)), DMA((peers,)), DMA((peers, nx)), DMA((peers, nx)), DMA((1,))],
        compiler_params=pltpu.CompilerParams(collective_id=ident, has_side_effects=True),
        name=f"exchange_{ident}",
    )(blocks)


def total_steps(me):
    steps = []
    for axis, size in (("replica", me.replicas), ("section", me.sections), ("shard", me.shards)):
        bit = 1
        while bit < size:
            steps.append((axis, bit))
            bit *= 2
    return steps


def total_kernel(count, *refs):
    ins, refs = refs[:count], refs[count:]
    outs, refs = refs[:count], refs[count:]
    held, refs = refs[:count], refs[count:]
    send_sem, recv_sem = refs
    me = Place()
    steps = total_steps(me)
    position = {"section": me.x, "replica": me.rep, "shard": me.shard}

    def other(axis, bit):
        index = position[axis]
        return {**position, axis: index + bit - 2 * bit * lax.rem(index // bit, 2)}

    barrier = pltpu.get_barrier_semaphore()
    for axis, bit in steps:
        pl.semaphore_signal(barrier, inc=1, device_id=other(axis, bit), device_id_type=MESH)
    pl.semaphore_wait(barrier, len(steps))
    for a in range(count):
        held[a][0] = ins[a][...]
    copies = []
    for n, (axis, bit) in enumerate(steps):
        step_copies = [
            remote(held[a].at[2 * n], held[a].at[2 * n + 1], send_sem.at[n, a], recv_sem.at[n, a], other(axis, bit))
            for a in range(count)
        ]
        for copy in step_copies:
            copy.start()
        copies += step_copies
        for a in range(count):
            step_copies[a].wait_recv()
            summed = (held[a][2 * n].astype(jnp.float32) + held[a][2 * n + 1].astype(jnp.float32)).astype(held[a].dtype)
            if n + 1 < len(steps):
                held[a][2 * n + 2] = summed
            else:
                outs[a][...] = summed
    for copy in copies:
        copy.wait_send()


def total(values, ident):
    count = len(values)
    steps = sum((lax.axis_size(axis) - 1).bit_length() for axis in every_axis)
    return pl.pallas_call(
        partial(total_kernel, count),
        out_shape=[jax.ShapeDtypeStruct(v.shape, v.dtype) for v in values],
        in_specs=[VMEM] * count,
        out_specs=[VMEM] * count,
        scratch_shapes=[pltpu.VMEM((2 * steps,) + v.shape, v.dtype) for v in values]
        + [DMA((steps, count)), DMA((steps, count))],
        compiler_params=pltpu.CompilerParams(collective_id=ident, has_side_effects=True),
        name=f"total_{ident}",
    )(*values)


def add_rows(dst, src):
    rows = dst.shape[0]
    if rows % 16 != 0:
        dst[...] = (dst[...].astype(jnp.float32) + src[...].astype(jnp.float32)).astype(dst.dtype)
        return
    step = 16

    def body(n, carry):
        at = pl.ds(pl.multiple_of(n * step, step), step)
        dst[at, :] = (dst[at, :].astype(jnp.float32) + src[at, :].astype(jnp.float32)).astype(dst.dtype)
        return carry

    lax.fori_loop(0, rows // step, body, 0)


def grads_errand(me, sent, got, sum_in, sum_out, *refs):
    n_sums = len(sum_in)
    held, refs = refs[:n_sums], refs[n_sums:]
    row_sem, relay_sem, own_sem, sum_sem = refs
    peers = me.replicas * me.shards
    mine = me.rep * me.shards + me.shard
    direct = [
        remote(sent.at[me.group(p)[0]], got.at[me.x, mine], row_sem.at[0, p], row_sem.at[1, p], me.group(p)[1])
        for p in range(1, peers)
    ]
    own = pltpu.make_async_copy(sent.at[mine], got.at[me.x, mine], own_sem.at[0])
    relays = []

    def source(p):
        return lax.rem(mine + peers - p, peers)

    def begin():
        own.start()
        for copy in direct:
            copy.start()
        for i in range(1, me.sections):
            copy = remote(sent.at[mine], got.at[me.x, mine], relay_sem.at[0, 0, i], relay_sem.at[1, 0, i], me.peer_x(i))
            copy.start()
            relays.append(copy)

    steps = total_steps(me)
    position = {"section": me.x, "replica": me.rep, "shard": me.shard}

    def other(axis, bit):
        index = position[axis]
        return {**position, axis: index + bit - 2 * bit * lax.rem(index // bit, 2)}

    def sum_copies(n):
        axis, bit = steps[n]
        return [
            remote(held[a].at[2 * n], held[a].at[2 * n + 1], sum_sem.at[0, n, a], sum_sem.at[1, n, a], other(axis, bit))
            for a in range(n_sums)
        ]

    def sum_step(n):
        if n == 0:
            for a in range(n_sums):
                held[a][0] = sum_in[a][...]
        else:
            for a, copy in enumerate(sum_copies(n - 1)):
                copy.wait_recv()
                summed = held[a][2 * n - 2] + held[a][2 * n - 1]
                if n < len(steps):
                    held[a][2 * n] = summed
                else:
                    sum_out[a][...] = summed
        if n < len(steps):
            for copy in sum_copies(n):
                copy.start()

    def relay(first, last):
        for p in range(first, last):
            dst = got.at[me.x, source(p)]
            remote(dst, dst, row_sem.at[0, p], row_sem.at[1, p], me.partner()).wait_recv()
            for i in range(1, me.sections):
                copy = remote(dst, dst, relay_sem.at[0, p, i], relay_sem.at[1, p, i], me.peer_x(i))
                copy.start()
                relays.append(copy)

    def finish():
        for p in range(peers):
            for i in range(1, me.sections):
                dst = got.at[lax.rem(me.x + me.sections - i, me.sections), source(p)]
                remote(dst, dst, relay_sem.at[0, p, i], relay_sem.at[1, p, i], me.partner()).wait_recv()
        for p in range(peers):
            for i in range(1, me.sections):
                dst = got.at[me.x, source(p)]
                remote(dst, dst, relay_sem.at[0, p, i], relay_sem.at[1, p, i], me.peer_x(i)).wait_send()
        for copy in direct:
            copy.wait_send()
        for n in range(len(steps)):
            for copy in sum_copies(n):
                copy.wait_send()
        own.wait()

    early = [begin] + [partial(sum_step, n) for n in range(len(steps) + 1) if n_sums]
    return early, [partial(relay, 1, peers)], [finish]


def reduce_kernel(count, sections, sums, extra, *refs):
    ins, refs = [refs[a * sections : (a + 1) * sections] for a in range(count)], refs[count * sections :]
    sum_in, refs = refs[:sums], refs[sums:]
    if extra:
        sent, refs = refs[0], refs[1:]
    outs, refs = refs[:count], refs[count:]
    sum_out, refs = refs[:sums], refs[sums:]
    if extra:
        got, refs = refs[0], refs[1:]
    acc, refs = refs[:count], refs[count:]
    from_core, refs = refs[:count], refs[count:]
    from_x, refs = refs[:count], refs[count:]
    from_y, refs = refs[:count], refs[count:]
    from_z, refs = refs[:count], refs[count:]
    load_sem, core_send, core_recv, send_sem, x_recv, y_recv, z_recv, last_sem = refs[:8]
    me = Place()
    nz, ny, nx = me.nz, me.ny, me.sections
    hooks = []
    if extra:
        me.greet_group()
        hooks = grads_errand(me, sent, got, sum_in, sum_out, *refs[8 : 8 + sums], *refs[8 + sums :])
    else:
        me.greet()

    far = sorted((k for k in range(1 - nz, nz)), key=lambda k: -abs(k))

    def block(k, j, i):
        return lax.rem(me.x + i, nx), (me.z + k) * ny + lax.rem(me.y + j, ny)

    def order_of(core):
        if core == 0:
            return [(k, j, i) for i in range(nx - 1, -1, -1) for j in range(ny - 1, -1, -1) for k in far]
        return [(k, j, i) for j in range(ny - 1, -1, -1) for k in far for i in range(nx - 1, -1, -1)]

    def run(core):
        other = 1 - core
        sends = []

        def start_core(k, j, i):
            x, s = block(k, j, i)

            def go(layer):
                for a in range(count):
                    remote(
                        ins[a][layer].at[s, other], from_core[a].at[x, s], core_send.at[a, x, s],
                        core_recv.at[a, x, s], me.partner(),
                    ).start()

            for layer in range(nx):
                when(both(me.inside(k), x == layer), partial(go, layer))

        def start_load(k, j, i):
            x, s = block(k, j, i)

            def go(layer):
                for a in range(count):
                    pltpu.make_async_copy(ins[a][layer].at[s, core], acc[a].at[x, s], load_sem.at[a, x, s]).start()

            for layer in range(nx):
                when(both(me.inside(k), x == layer), partial(go, layer))

        for b in order_of(other):
            start_core(*b)
        for b in order_of(core):
            start_load(*b)
        early, late, final = [list(part) for part in hooks] if hooks else ([], [], [])

        def errand(todo, every=False):
            while todo:
                todo.pop(0)()
                if not every:
                    break

        errand(early)

        def push(cond, src, dst, sem, device):
            copy = remote(src, dst, send_sem.at[len(sends)], sem, device)
            when(cond, copy.start)
            sends.append((cond, copy))

        def take(cond, dst, src, sem):
            def go():
                remote(src, src, core_send.at[0, 0, 0], sem, me.partner()).wait_recv()
                add_rows(dst, src)

            when(cond, go)

        def join_core(a, k, j, i):
            x, s = block(k, j, i)

            def go():
                pltpu.make_async_copy(ins[a][0].at[s, core], acc[a].at[x, s], load_sem.at[a, x, s]).wait()

            when(me.inside(k), go)
            take(me.inside(k), acc[a].at[x, s], from_core[a].at[x, s], core_recv.at[a, x, s])

        def join_x(a, k, j):
            x, s = block(k, j, 0)
            for p in range(1, nx):
                take(me.inside(k), acc[a].at[x, s], from_x[a].at[p - 1, s], x_recv.at[a, p - 1, s])

        def join_y(a, k, i):
            x, s = block(k, 0, i)
            for p in range(1, ny):
                take(me.inside(k), acc[a].at[x, s], from_y[a].at[p - 1, x, me.z + k], y_recv.at[a, p - 1, x, me.z + k])

        def join_z(a, k, i):
            x, s = block(k, 0, i)
            if k >= 0:
                take(both(me.inside(k), me.inside(-1)), acc[a].at[x, s], from_z[a].at[x, me.z + k], z_recv.at[a, x, me.z + k])
            if k <= 0:
                place = nz if k == 0 else me.z + k
                take(both(me.inside(k), me.inside(1)), acc[a].at[x, s], from_z[a].at[x, place], z_recv.at[a, x, place])

        def send_x(a, k, j, i):
            x, s = block(k, j, i)
            push(me.inside(k), acc[a].at[x, s], from_x[a].at[i - 1, s], x_recv.at[a, i - 1, s], me.peer_x(i))

        def send_y(a, k, j, i):
            x, s = block(k, j, i)
            push(
                me.inside(k), acc[a].at[x, s], from_y[a].at[j - 1, x, me.z + k],
                y_recv.at[a, j - 1, x, me.z + k], me.peer_y(j),
            )

        def send_z(a, k, i):
            x, s = block(k, 0, i)
            place = nz if k == -1 else me.z + k
            push(
                me.inside(k), acc[a].at[x, s], from_z[a].at[x, place], z_recv.at[a, x, place],
                me.line(1 if k > 0 else -1),
            )

        each = range(count)

        def x_first(arrays):
            first, second, third = [], [], []

            def cross_x(k, j, i):
                for a in arrays:
                    join_core(a, k, j, i)
                    send_x(a, k, j, i)

            def join_own(k, j):
                for a in arrays:
                    join_core(a, k, j, 0)

            def cross_y(k, j):
                for a in arrays:
                    join_x(a, k, j)
                    send_y(a, k, j, 0)

            def along_z(k):
                for a in arrays:
                    join_x(a, k, 0)
                    join_y(a, k, 0)
                    join_z(a, k, 0)
                    if k != 0:
                        send_z(a, k, 0)

            for i in range(nx - 1, 0, -1):
                for j in range(ny - 1, -1, -1):
                    first += [partial(cross_x, k, j, i) for k in far]
            for j in range(ny - 1, -1, -1):
                second += [partial(join_own, k, j) for k in far]
            for j in range(ny - 1, 0, -1):
                second += [partial(cross_y, k, j) for k in far]
            third += [partial(along_z, k) for k in far]
            return first, second, third

        def y_first(arrays):
            def cross_y(k, j, i):
                for a in arrays:
                    join_core(a, k, j, i)
                    send_y(a, k, j, i)

            def join_own(k, i):
                for a in arrays:
                    join_core(a, k, 0, i)

            def along_z(k, i):
                for a in arrays:
                    join_y(a, k, i)
                    join_z(a, k, i)
                    if k != 0:
                        send_z(a, k, i)
                    elif i != 0:
                        send_x(a, 0, 0, i)
                    else:
                        join_x(a, 0, 0)

            slots = range(nx - 1, -1, -1)
            first = [partial(cross_y, k, j, i) for j in range(ny - 1, 0, -1) for k in far for i in slots]
            second = [partial(join_own, k, i) for k in far for i in slots]
            third = [partial(along_z, k, i) for k in far for i in slots]
            return first, second, third

        plans = [x_first(list(each)) if core == 0 else y_first(list(each))]
        for stage in range(3):
            lists = [plan[stage] for plan in plans if plan[stage]]
            longest = max(len(steps) for steps in lists)
            if stage == 1:
                errand(early, every=True)
                errand(late, every=True)
            for n in range(longest):
                for steps in lists:
                    for step in steps[len(steps) * n // longest : len(steps) * (n + 1) // longest]:
                        step()
                errand(early)
        errand(final, every=True)
        finals = []
        for a in each:
            copy = remote(
                acc[a].at[me.x, me.shard], outs[a].at[core], last_sem.at[0, a], last_sem.at[1, a], me.partner()
            )
            copy.start()
            finals.append(copy)
            outs[a][core] = acc[a][me.x, me.shard]
        for a in each:
            remote(outs[a].at[other], outs[a].at[other], last_sem.at[0, a], last_sem.at[1, a], me.partner()).wait_recv()
        for cond, copy in sends:
            when(cond, copy.wait_send)
        for copy in finals:
            copy.wait_send()
        for k, j, i in order_of(other):
            x, s = block(k, j, i)

            def finish():
                for a in each:
                    remote(
                        ins[a][0].at[s, other], from_core[a].at[x, s], core_send.at[a, x, s],
                        core_recv.at[a, x, s], me.partner(),
                    ).wait_send()

            when(me.inside(k), finish)

    pl.when(me.core == 0)(lambda: run(0))
    pl.when(me.core == 1)(lambda: run(1))


def reduce_shards(grads, ident, errand=None):
    count = len(grads)
    nx, shards = lax.axis_size("section"), lax.axis_size("shard")
    nz = min(4, shards)
    ny = shards // nz
    blocks = (2 * nz - 1) * ny * nx

    def scratch(lead):
        return [pltpu.VMEM(lead + g[0].shape[2:], g[0].dtype) for g in grads]

    extra_in, extra_shapes, extra_scratch, sums = [], [], [], 0
    if errand:
        values, sent = errand
        sums, peers = len(values), sent.shape[0]
        steps = sum((lax.axis_size(axis) - 1).bit_length() for axis in every_axis)
        extra_in = [*values, sent]
        extra_shapes = [jax.ShapeDtypeStruct(v.shape, v.dtype) for v in values] + [
            jax.ShapeDtypeStruct((nx,) + sent.shape, sent.dtype)
        ]
        extra_scratch = [pltpu.VMEM((2 * steps,) + v.shape, v.dtype) for v in values] + [
            DMA((2, peers)),
            DMA((2, peers, nx)),
            DMA((1,)),
            DMA((2, steps, max(sums, 1))),
        ]
    return pl.pallas_call(
        partial(reduce_kernel, count, nx, sums, bool(errand)),
        out_shape=[jax.ShapeDtypeStruct(g[0].shape[1:], g[0].dtype) for g in grads] + extra_shapes,
        in_specs=[ANY] * (count * nx) + [VMEM] * sums + [ANY] * bool(errand),
        out_specs=[VMEM] * (count + sums) + [ANY] * bool(errand),
        scratch_shapes=scratch((nx, shards))
        + scratch((nx, shards))
        + scratch((max(nx - 1, 1), shards))
        + scratch((max(ny - 1, 1), nx, nz))
        + scratch((nx, nz + 1))
        + [
            DMA((count, nx, shards)),
            DMA((count, nx, shards)),
            DMA((count, nx, shards)),
            DMA((blocks * count * 2,)),
            DMA((count, max(nx - 1, 1), shards)),
            DMA((count, max(ny - 1, 1), nx, nz)),
            DMA((count, nx, nz + 1)),
            DMA((2, count)),
        ]
        + extra_scratch,
        compiler_params=pltpu.CompilerParams(
            collective_id=ident, has_side_effects=True, vmem_limit_bytes=67043328
        ),
        name=f"reduce_{ident}",
    )(*[layer for g in grads for layer in g], *extra_in)


def reduce_parts(grads, ident, errand):
    nx, shards = lax.axis_size("section"), lax.axis_size("shard")
    ny = shards // min(4, shards)
    slots = 2 * nx * shards + (nx - 1) * shards + (ny - 1) * nx * 4 + nx * 5 + 4
    groups, used = [[]], 0
    for n, grad in enumerate(grads):
        rows, columns = grad[0].shape[2:]
        size = slots * (-(-rows // 16) * 16) * columns * 2
        if used + size > 58 * 2**20 and groups[-1]:
            groups.append([])
            used = 0
        groups[-1].append(n)
        used += size
    out = [None] * len(grads)
    for g, group in enumerate(groups):
        done = reduce_shards([grads[n] for n in group], ident + g, errand if g == 0 else None)
        for n, value in zip(group, done):
            out[n] = value
        if g == 0:
            extra = done[len(group) :]
    return out, extra


def spread_group(columns, values, target, high):
    entries = columns.shape[1]
    each = entries // 8
    row = lax.broadcasted_iota(jnp.int32, (1, entries), 1) // each
    key = jnp.where(columns >= 0, (columns // 128) * 8 + row, -1)
    low_part = jnp.where(columns >= 0, lax.rem(columns, 128), -1)
    left = jnp.where(key == lax.broadcasted_iota(jnp.int32, (high * 8, entries), 0), values, 0.0).astype(jnp.bfloat16)
    right = jnp.where(low_part == lax.broadcasted_iota(jnp.int32, (128, entries), 0), 1.0, 0.0).astype(jnp.bfloat16)
    placed = lax.dot_general(left, right, (((1,), (1,)), ((), ())), preferred_element_type=jnp.float32)
    pieces = []
    for h in range(high):
        one = jnp.where(lax.broadcasted_iota(jnp.int32, (8, 128), 1) + 128 * h == target, 1.0, 0.0)
        pieces.append(placed[h * 8 : (h + 1) * 8] + one)
    return pieces


def spread_range(first, last, shift, rows_each, columns_ref, weight_ref, target_ref, out_ref):
    high = out_ref.shape[1] // 128
    per = columns_ref.shape[1]

    def local_of(ids):
        column = ids - shift
        return jnp.where((column >= 0) & (column < rows_each), column, -1)

    def body(g, carry):
        pair, place = g // per, lax.rem(g, per)
        target = target_ref[pair, pl.ds(pl.multiple_of(place * 8, 8), 8), :]
        pieces = spread_group(local_of(columns_ref[pair, place]), weight_ref[pair, place], local_of(target), high)
        at = pl.ds(pl.multiple_of(g * 8, 8), 8)
        for h in range(high):
            out_ref[at, h * 128 : (h + 1) * 128] = pieces[h]
        return carry

    lax.fori_loop(first, last, body, 0)


def spread_kernel(rows_each, shift_ref, columns_ref, weight_ref, target_ref, out_ref):
    spread_range(
        0, columns_ref.shape[0] * columns_ref.shape[1], shift_ref[0], rows_each, columns_ref, weight_ref, target_ref, out_ref
    )


def spread_entries(shift, columns, values, targets, rows_each, width):
    rows = targets.shape[0] * targets.shape[1]
    return pl.pallas_call(
        partial(spread_kernel, rows_each),
        out_shape=jax.ShapeDtypeStruct((rows, width), jnp.float32),
        in_specs=[pl.BlockSpec(memory_space=pltpu.SMEM)] + [VMEM] * 3,
        out_specs=VMEM,
        name="spread_entries",
    )(shift, columns, values, targets)


def ask_kernel(owners, token_row, token_col, owner_row, owner_col, row_col, hot_ref, ask_ref):
    count = token_row.shape[1]
    i = lax.broadcasted_iota(jnp.int32, (count, count), 0)
    j = lax.broadcasted_iota(jnp.int32, (count, count), 1)
    same = token_col[...] == token_row[...]
    kin = owner_col[...] == owner_row[...]
    first_col = 1.0 - jnp.max(jnp.where(same & (j < i), 1.0, 0.0), axis=1, keepdims=True)
    first_row = 1.0 - jnp.max(jnp.where(same & (i < j), 1.0, 0.0), axis=0, keepdims=True)
    place_col = jnp.sum(jnp.where(kin & (j < i), first_row, 0.0), axis=1, keepdims=True)
    place_row = jnp.sum(jnp.where(kin & (i < j), first_col, 0.0), axis=0, keepdims=True)
    number_col = jnp.sum(jnp.where(same, first_row * place_row, 0.0), axis=1, keepdims=True)
    number_row = jnp.sum(jnp.where(same, first_col * place_col, 0.0), axis=0, keepdims=True)
    size = float(batch_rows)
    slot_row = jnp.where(number_row < size, owner_row[...].astype(jnp.float32) * size + number_row, -1.0)
    slot_col = jnp.where(number_col < size, owner_col[...].astype(jnp.float32) * size + number_col, -1.0)
    spots = owners * batch_rows
    part = 512 if spots % 512 == 0 else spots
    for at in range(0, spots, part):
        line = lax.broadcasted_iota(jnp.int32, (part, count), 0).astype(jnp.float32) + float(at)
        hot_ref[at : at + part, :] = jnp.where(slot_row == line, 1.0, 0.0).astype(jnp.bfloat16)
    most = jnp.max(number_col) + 1.0
    wanted = first_col * (row_col[...].astype(jnp.float32) + 1.0)
    lane = lax.broadcasted_iota(jnp.int32, (1, 128), 1)
    for at in range(0, spots, 128):
        line = lax.broadcasted_iota(jnp.int32, (count, 128), 1).astype(jnp.float32) + float(at)
        rows = jnp.max(jnp.where(slot_col == line, wanted, 0.0), axis=0, keepdims=True)
        for n in range(128 // batch_rows):
            shifted = pltpu.roll(rows, (128 - n * batch_rows) % 128, 1) if n else rows
            values = jnp.where(lane < batch_rows, shifted, jnp.where(lane == 127, most, 0.0))
            ask_ref[at // batch_rows + n] = values.astype(jnp.int32)


def ask_rows(tokens, owner, row, owners):
    count = tokens.shape[0]
    return pl.pallas_call(
        partial(ask_kernel, owners),
        out_shape=[
            jax.ShapeDtypeStruct((owners * batch_rows, count), jnp.bfloat16),
            jax.ShapeDtypeStruct((owners, 1, 128), jnp.int32),
        ],
        in_specs=[VMEM] * 5,
        out_specs=[VMEM] * 2,
        name="ask_rows",
    )(tokens[None], tokens[:, None], owner[None], owner[:, None], row[:, None])


def table_kernel(asked_ref, got_ref, head_ref, *refs):
    layers, table_ref, square_ref = refs[:-2], refs[-2], refs[-1]
    sections, peers = asked_ref.shape[:2]
    each = 128 // batch_rows
    lane = lax.broadcasted_iota(jnp.int32, (1, 128), 1)
    lists = []
    for at in range(0, sections * peers, each):
        wish = jnp.zeros((1, 128), jnp.int32)
        for n in range(each):
            part = asked_ref[(at + n) // peers, (at + n) % peers]
            part = pltpu.roll(part, n * batch_rows, 1) if n else part
            wish = jnp.where((lane >= n * batch_rows) & (lane < (n + 1) * batch_rows), part, wish)
        lists.append(wish)
    wish = jnp.concatenate(lists, axis=1)
    rows = table_ref.shape[0]
    step = 400 if rows % 400 == 0 else rows

    def body(n, square):
        at = pl.ds(pl.multiple_of(n * step, 8), step) if step != rows else slice(0, rows)
        row = lax.broadcasted_iota(jnp.int32, (step, wish.shape[1]), 0) + 1 + n * step
        hot = jnp.where(row == wish, 1.0, 0.0).astype(jnp.bfloat16)
        values = head_ref[at, :] + jnp.dot(hot, got_ref[...], preferred_element_type=jnp.float32)
        table_ref[at, :] = values
        return square + jnp.sum(values * values, axis=0, keepdims=True)

    zero = jnp.zeros((1, table_ref.shape[1]), jnp.float32)
    square = jnp.sum(lax.fori_loop(0, rows // step, body, zero)) if step != rows else jnp.sum(body(0, zero))
    square = jnp.where(lax.axis_index("section") == 0, square, 0.0)
    others = jnp.float32(0)
    for layer in layers:
        for half in range(2):
            values = layer[half].astype(jnp.float32)
            others = others + jnp.sum(values * values)
    square = square + jnp.where(lax.axis_index("replica") == 0, others, 0.0)
    corner = lax.broadcasted_iota(jnp.int32, (8, 128), 0) + lax.broadcasted_iota(jnp.int32, (8, 128), 1)
    square_ref[...] = jnp.where(corner == 0, square, 0.0)


def table_gradient(rows_each, asked, got, head_table, layer_grads):
    width = head_table.shape[1]
    return pl.pallas_call(
        table_kernel,
        out_shape=[
            jax.ShapeDtypeStruct((rows_each, width), jnp.float32),
            jax.ShapeDtypeStruct((8, 128), jnp.float32),
        ],
        in_specs=[VMEM] * (3 + len(layer_grads)),
        out_specs=[VMEM] * 2,
        compiler_params=pltpu.CompilerParams(vmem_limit_bytes=56 * 2**20),
        name="table_gradient",
    )(asked, got, head_table, *layer_grads)
def dims_nt(left, right):
    return lax.dot_general(left, right, (((1,), (1,)), ((), ())), preferred_element_type=jnp.float32)


def dims_tn(left, right):
    return lax.dot_general(left, right, (((0,), (0,)), ((), ())), preferred_element_type=jnp.float32)


def three_parts(values):
    first = lower(values)
    rest = values - first.astype(jnp.float32)
    second = lower(rest)
    return first, second, lower(rest - second.astype(jnp.float32))


def log_sigmoid(values):
    return jnp.minimum(values, 0.0) - jnp.log1p(jnp.exp(-jnp.abs(values)))


def norm_parts(values, gain):
    inverse = lax.rsqrt(jnp.mean(values * values, axis=-1, keepdims=True) + eps_norm)
    normed = values * inverse
    return normed, inverse, lower(normed * gain)


class HeadPair:
    def __init__(self, tree_len, cumul):
        self.lane = lax.broadcasted_iota(jnp.int32, (tree_len, 128), 1)
        self.parts = jnp.concatenate(three_parts(cumul), axis=1)
        self.row = lax.broadcasted_iota(jnp.int32, (384, 128), 0)
        self.column = lax.broadcasted_iota(jnp.int32, (384, 128), 1)

    def augmented(self, head, side, query, key):
        start = 64 - 64 * side
        mine = (self.lane >= 64 * side) & (self.lane < 64 * side + 64)
        wanted = (self.row - 128 * (self.row // 128) == head) & (self.column == self.row // 128 + start)
        placed = product(self.parts, lower(jnp.where(wanted, 1.0, 0.0)))
        wanted = (self.row - 128 * (self.row // 128) == head) & (self.column == self.row // 128 + start + 3)
        negative = product(self.parts, lower(jnp.where(wanted, -1.0, 0.0)))
        ones_q = jnp.where((self.lane >= start + 3) & (self.lane < start + 6), 1.0, 0.0)
        ones_k = jnp.where((self.lane >= start) & (self.lane < start + 3), 1.0, 0.0)
        query = lower(jnp.where(mine, query.astype(jnp.float32) * 0.125, placed + ones_q))
        key = lower(jnp.where(mine, key.astype(jnp.float32), negative + ones_k))
        return query, key, mine


def forward_kernel(layer, round_input, x_ref, allowed_ref, w_in, w_out, w_up, w_down, forget_ref, bias_ref, gain_ref,
                   y_ref, qkv_ref, logit_ref, lse_ref, att_ref, mid_ref, gu_ref,
                   b_in, b_out, b_up, b_down, gu_buf, hidden, mask, sem, gu_sem, in_sem):
    tree_len, width = x_ref.shape
    heads = width // 64
    half = hidden.shape[1]
    loads = [None] + [
        pltpu.make_async_copy(src.at[layer], dst, sem.at[n])
        for n, (src, dst) in enumerate(((w_out, b_out), (w_up, b_up), (w_down, b_down)))
    ]

    def first_load(n):
        at = pl.ds(pl.multiple_of(n * 256, 256), 256)
        return pltpu.make_async_copy(w_in.at[layer, :, at], b_in.at[:, at], in_sem.at[n])

    for n in range(3 * width // 256):
        first_load(n).start()
    for copy in loads[1:]:
        copy.start()
    x = x_ref[...]
    if round_input:
        x = lower(x).astype(jnp.float32)
    _, _, act = norm_parts(x, gain_ref[0:1, :])
    allowed = allowed_ref[...]
    mask[...] = jnp.where(allowed > 0, 0.0, masked_score)
    logit = product(act, forget_ref[...]) + bias_ref[...]
    logit_ref[...] = logit
    cumul = sum(product(allowed, part) for part in three_parts(log_sigmoid(logit)))
    def project(n, carry):
        first_load(n).wait()
        at = pl.ds(pl.multiple_of(n * 256, 256), 256)
        qkv_ref[:, at] = lower(product(act, b_in[:, at]))
        return carry

    lax.fori_loop(0, 3 * width // 256, project, 0)
    pair = HeadPair(tree_len, cumul)
    lse_ref[...] = jnp.zeros_like(lse_ref)

    def attend(p, carry):
        base = pl.multiple_of(p * 128, 128)
        query = qkv_ref[:, pl.ds(base, 128)]
        key = qkv_ref[:, pl.ds(base + width, 128)]
        value = qkv_ref[:, pl.ds(base + 2 * width, 128)]
        outs = []
        for side in range(2):
            q_side, k_side, mine = pair.augmented(2 * p + side, side, query, key)
            scores = dims_nt(q_side, k_side) + mask[...]
            peak = jnp.max(scores, axis=1, keepdims=True)
            probs = jnp.exp(scores - peak)
            count = jnp.sum(probs, axis=1, keepdims=True)
            outs.append(product(lower(probs * (1.0 / count)), value))
            lse_ref[...] = jnp.where(pair.lane == 2 * p + side, peak + jnp.log(count), lse_ref[...])
        att_ref[:, pl.ds(base, 128)] = lower(jnp.where(pair.lane < 64, outs[0], outs[1]))
        return carry

    lax.fori_loop(0, heads // 2, attend, 0, unroll=2)
    loads[1].wait()
    middle = x + product(att_ref[...], b_out[...])
    mid_ref[...] = middle
    _, _, act_b = norm_parts(middle, gain_ref[1:2, :])
    loads[2].wait()

    def stores(n):
        return [
            pltpu.make_async_copy(
                gu_buf.at[:, pl.ds(n * 512 + s * half, 512)], gu_ref.at[:, pl.ds(n * 512 + s * half, 512)], gu_sem.at[n, s]
            )
            for s in range(2)
        ]

    for n in range(half // 512):
        def expand(h, carry):
            at = pl.ds(pl.multiple_of(n * 512 + h * 256, 256), 256)
            at_up = pl.ds(pl.multiple_of(half + n * 512 + h * 256, 256), 256)
            gate = product(act_b, b_up[:, at])
            upper = product(act_b, b_up[:, at_up])
            gu_buf[:, at] = gate
            gu_buf[:, at_up] = upper
            hidden[:, at] = lower(gate / (1.0 + jnp.exp(-gate)) * upper)
            return carry

        lax.fori_loop(0, 2, expand, 0)
        for copy in stores(n):
            copy.start()
    loads[3].wait()

    def contract(n, carry):
        at = pl.ds(pl.multiple_of(n * 256, 256), 256)
        y_ref[:, at] = mid_ref[:, at] + product(hidden[...], b_down[:, at])
        return carry

    lax.fori_loop(0, width // 256, contract, 0)
    for n in range(half // 512):
        for copy in stores(n):
            copy.wait()


def layer_forward(layer, round_input, values, allowed, mats, forget_w, forget_b, gains):
    tree_len, width = values.shape
    w_in, w_out, w_up, w_down = mats
    half = w_down.shape[1]
    f32, b16 = jnp.float32, jnp.bfloat16
    shape = jax.ShapeDtypeStruct
    return pl.pallas_call(
        partial(forward_kernel, layer, round_input),
        out_shape=[
            shape((tree_len, width), f32),
            shape((tree_len, 3 * width), b16),
            shape((tree_len, 128), f32),
            shape((tree_len, 128), f32),
            shape((tree_len, width), b16),
            shape((tree_len, width), f32),
            shape((tree_len, 2 * half), f32),
        ],
        in_specs=[VMEM] * 2 + [ANY] * 4 + [VMEM] * 3,
        out_specs=[VMEM] * 6 + [ANY],
        scratch_shapes=[pltpu.VMEM(w.shape[1:], b16) for w in mats]
        + [
            pltpu.VMEM((tree_len, 2 * half), f32),
            pltpu.VMEM((tree_len, half), b16),
            pltpu.VMEM((tree_len, tree_len), f32),
            DMA((4,)),
            DMA((half // 512, 2)),
            DMA((3 * width // 256,)),
        ],
        compiler_params=pltpu.CompilerParams(vmem_limit_bytes=56 * 2**20),
        name=f"forward_{layer}",
    )(values, allowed, *mats, forget_w, forget_b, gains)


def backward_kernel(layer, round_input, round_grad, dy_ref, x_ref, allowed_ref, qkv_ref, logit_ref, lse_ref, att_ref,
                    mid_ref, forget_ref, gain_ref, gu_hbm, w_in, w_out, w_up, w_down,
                    dx_ref, dforget_ref, dgain_ref, dw_in, dw_out, dw_up, dw_down,
                    b_in, b_out, b_up, b_down, gu, dqkv, act_t, grad_b, mask, dcum,
                    g_in, g_out, g_up, g_down, sem, gu_sem, store_sem):
    tree_len, width = x_ref.shape
    heads = width // 64
    half = b_down.shape[0]
    chunk = 256
    loads = [
        pltpu.make_async_copy(src.at[layer], dst, sem.at[n]) for n, (src, dst) in enumerate(((w_in, b_in), (w_out, b_out)))
    ]
    def feed_loads(n):
        at = pl.ds(pl.multiple_of(n * chunk, chunk), chunk)
        at_up = pl.ds(pl.multiple_of(half + n * chunk, chunk), chunk)
        pairs = ((gu_hbm.at[:, at], gu.at[:, at]), (gu_hbm.at[:, at_up], gu.at[:, at_up]),
                 (w_down.at[layer, at], b_down.at[at]), (w_up.at[layer, :, at], b_up.at[:, at]),
                 (w_up.at[layer, :, at_up], b_up.at[:, at_up]))
        return [pltpu.make_async_copy(src, dst, gu_sem.at[n, s]) for s, (src, dst) in enumerate(pairs)]

    for n in range(half // chunk):
        for copy in feed_loads(n):
            copy.start()
    for n in (1, 0):
        loads[n].start()
    dy = dy_ref[...]
    if round_grad:
        dy = lower(dy).astype(jnp.float32)
    branch = lower(dy)
    normed_b, inverse_b, act_b = norm_parts(mid_ref[...], gain_ref[1:2, :])
    act_t[...] = lower((normed_b * gain_ref[1:2, :]).T)
    grad_b[...] = jnp.zeros_like(grad_b)

    def feed(n, carry):
        for copy in feed_loads(n):
            copy.wait()
        at = pl.ds(pl.multiple_of(n * chunk, chunk), chunk)
        at_up = pl.ds(pl.multiple_of(half + n * chunk, chunk), chunk)
        gate, upper = gu[:, at], gu[:, at_up]
        sigma = 1.0 / (1.0 + jnp.exp(-gate))
        silu = gate * sigma
        hidden = lower(silu * upper)
        grad_hidden = dims_nt(branch, b_down[at, :])
        g_down[at, :] = lower(dims_tn(hidden, branch))
        grad_gate = lower(grad_hidden * upper * sigma * (1.0 + gate * (1.0 - sigma)))
        grad_upper = lower(grad_hidden * silu)
        g_up[:, at] = lower(product(act_t[...], grad_gate))
        g_up[:, at_up] = lower(product(act_t[...], grad_upper))
        grad_b[...] += dims_nt(grad_gate, b_up[:, at]) + dims_nt(grad_upper, b_up[:, at_up])
        return carry

    lax.fori_loop(0, half // chunk, feed, 0)
    stores = [
        pltpu.make_async_copy(src, dst, store_sem.at[n])
        for n, (src, dst) in enumerate(((g_down, dw_down), (g_up, dw_up), (g_out, dw_out), (g_in, dw_in)))
    ]
    stores[0].start()
    stores[1].start()

    def norm_backward(grad, normed, inverse, gain):
        grad_normed = grad * gain
        back = inverse * (grad_normed - normed * jnp.mean(grad_normed * normed, axis=-1, keepdims=True))
        return back, jnp.sum(grad * normed, axis=0, keepdims=True)

    back_b, dgain_b = norm_backward(grad_b[...], normed_b, inverse_b, gain_ref[1:2, :])
    grad_mid = dy + back_b
    branch_a = lower(grad_mid)
    g_out[...] = lower(dims_tn(att_ref[...], branch_a))
    stores[2].start()
    loads[1].wait()
    att_ref_grad = lower(dims_nt(branch_a, b_out[...]))
    x = x_ref[...]
    if round_input:
        x = lower(x).astype(jnp.float32)
    normed_a, inverse_a, act_a = norm_parts(x, gain_ref[0:1, :])
    act_t[...] = lower((normed_a * gain_ref[0:1, :]).T)
    allowed = allowed_ref[...]
    mask[...] = jnp.where(allowed > 0, 0.0, masked_score)
    logit = logit_ref[...]
    cumul = sum(product(allowed, part) for part in three_parts(log_sigmoid(logit)))
    pair = HeadPair(tree_len, cumul)
    dcum[...] = jnp.zeros_like(dcum)
    grad_att = grad_b
    grad_att[...] = att_ref_grad.astype(jnp.float32)

    def attend(p, carry):
        base = pl.multiple_of(p * 128, 128)
        query = qkv_ref[:, pl.ds(base, 128)]
        key = qkv_ref[:, pl.ds(base + width, 128)]
        value = qkv_ref[:, pl.ds(base + 2 * width, 128)]
        grad_out = grad_att[:, pl.ds(base, 128)]
        grad_low = lower(grad_out)
        results = []
        for side in range(2):
            head = 2 * p + side
            start = 64 - 64 * side
            q_side, k_side, mine = pair.augmented(head, side, query, key)
            lse = jnp.sum(jnp.where(pair.lane == head, lse_ref[...], 0.0), axis=1, keepdims=True)
            probs = jnp.exp(dims_nt(q_side, k_side) + (mask[...] - lse))
            grad_probs = dims_nt(lower(jnp.where(mine, grad_out, 0.0)), value)
            weighted = probs * grad_probs
            row = jnp.sum(weighted, axis=1, keepdims=True)
            grad_scores = lower(weighted - probs * row)
            grad_value = dims_tn(lower(probs), grad_low)
            grad_query = product(grad_scores, k_side)
            grad_key = dims_tn(grad_scores, q_side)
            taken = jnp.sum(
                jnp.where(pair.lane == start, grad_query, 0.0) - jnp.where(pair.lane == start + 3, grad_key, 0.0),
                axis=1, keepdims=True,
            )
            dcum[...] = jnp.where(pair.lane == head, taken, dcum[...])
            results.append((grad_query * 0.125, grad_key, grad_value))
        for part in range(3):
            merged = jnp.where(pair.lane < 64, results[0][part], results[1][part])
            dqkv[:, pl.ds(base + part * width, 128)] = lower(merged)
        return carry

    lax.fori_loop(0, heads // 2, attend, 0)
    rising = sum(dims_tn(allowed, part) for part in three_parts(dcum[...]))
    grad_logit = rising / (1.0 + jnp.exp(logit))
    lane = lax.broadcasted_iota(jnp.int32, grad_logit.shape, 1)
    grad_logit = lower(jnp.where(lane < heads, grad_logit, 0.0))
    dforget_ref[:, 0:width] = lower(dims_tn(grad_logit, act_a)[0:16, :])
    bias = dims_tn(grad_logit, jnp.ones((tree_len, 128), jnp.bfloat16))[0:16, :]
    bias = jnp.where(lax.broadcasted_iota(jnp.int32, (16, 128), 1) == 0, bias, 0.0)
    dforget_ref[:, width : width + 128] = lower(bias)

    def weigh(n, carry):
        at = pl.ds(pl.multiple_of(n * 256, 256), 256)
        g_in[:, at] = lower(product(act_t[...], dqkv[:, at]))
        return carry

    lax.fori_loop(0, 3 * width // 256, weigh, 0)
    stores[3].start()
    loads[0].wait()
    grad_b[...] = dims_nt(grad_logit, forget_ref[...])

    def gather_back(n, carry):
        at = pl.ds(pl.multiple_of(n * 256, 256), 256)
        grad_b[...] += dims_nt(dqkv[:, at], b_in[:, at])
        return carry

    lax.fori_loop(0, 3 * width // 256, gather_back, 0)
    back_a, dgain_a = norm_backward(grad_b[...], normed_a, inverse_a, gain_ref[0:1, :])
    dx_ref[...] = grad_mid + back_a
    dgain_ref[...] = jnp.concatenate([dgain_a, dgain_b], axis=0)
    for copy in stores:
        copy.wait()


def layer_backward(layer, round_input, round_grad, grad, values, allowed, saved, mats, forget_w, gains):
    tree_len, width = values.shape
    qkv, logit, lse, att, middle, gate_up = saved
    w_in, w_out, w_up, w_down = mats
    half = w_down.shape[1]
    f32, b16 = jnp.float32, jnp.bfloat16
    shape = jax.ShapeDtypeStruct
    return pl.pallas_call(
        partial(backward_kernel, layer, round_input, round_grad),
        out_shape=[
            shape((tree_len, width), f32),
            shape((16, width + 128), b16),
            shape((2, width), f32),
        ]
        + [shape(w.shape[1:], b16) for w in mats],
        in_specs=[VMEM] * 10 + [ANY] * 5,
        out_specs=[VMEM] * 3 + [ANY] * 4,
        scratch_shapes=[pltpu.VMEM(w.shape[1:], b16) for w in mats]
        + [
            pltpu.VMEM((tree_len, 2 * half), f32),
            pltpu.VMEM((tree_len, 3 * width), b16),
            pltpu.VMEM((width, tree_len), b16),
            pltpu.VMEM((tree_len, width), f32),
            pltpu.VMEM((tree_len, tree_len), f32),
            pltpu.VMEM((tree_len, 128), f32),
        ]
        + [pltpu.VMEM(w.shape[1:], b16) for w in mats]
        + [DMA((4,)), DMA((half // 256, 5)), DMA((4,))],
        compiler_params=pltpu.CompilerParams(vmem_limit_bytes=60 * 2**20),
        name=f"backward_{layer}",
    )(grad, values, allowed, qkv, logit, lse, att, middle, forget_w, gains, gate_up, *mats)
def head_forward_kernel(rows_each, z_ref, table_ref, marks_ref, logits_ref, stats_ref):
    rows = z_ref.shape[0]
    chunk = 256 if table_ref.shape[0] % 256 == 0 else 128
    z = z_ref[...]

    def body(n, carry):
        peak, count, linear = carry
        at = pl.ds(pl.multiple_of(n * chunk, chunk), chunk)
        logits = dims_nt(z, table_ref[at, :])
        column = lax.broadcasted_iota(jnp.int32, (rows, chunk), 1) + n * chunk
        linear = linear + jnp.sum(logits * marks_ref[:, at], axis=1, keepdims=True)
        logits = jnp.where(column < rows_each, logits, masked_score)
        logits_ref[:, at] = logits
        new_peak = jnp.maximum(peak, jnp.max(logits, axis=1, keepdims=True))
        count = count * jnp.exp(peak - new_peak) + jnp.sum(jnp.exp(logits - new_peak), axis=1, keepdims=True)
        return new_peak, count, linear

    start = jnp.full((rows, 1), masked_score, jnp.float32)
    zero = jnp.zeros((rows, 1), jnp.float32)
    peak, count, linear = lax.fori_loop(0, table_ref.shape[0] // chunk, body, (start, zero, zero))
    lane = lax.broadcasted_iota(jnp.int32, (rows, 128), 1)
    stats = jnp.where(lane == 0, peak, jnp.where(lane == 1, count, jnp.where(lane == 2, linear, 0.0)))
    stats_ref[...] = stats.T[0:4, :]


def head_forward(rows_each, z, table, marks):
    rows, width = z.shape[0], table.shape[0]
    return pl.pallas_call(
        partial(head_forward_kernel, rows_each),
        out_shape=[jax.ShapeDtypeStruct((rows, width), jnp.float32), jax.ShapeDtypeStruct((4, rows), jnp.float32)],
        in_specs=[VMEM] * 3,
        out_specs=[VMEM] * 2,
        name="head_forward",
    )(z, table, marks)


def head_backward_kernel(sections, span, pos_all, z_ref, table_ref, marks_ref, logits_ref, stats_ref,
                         prob_ref, dz_ref, dtable_ref, row_ref, grads):
    rows, width = logits_ref.shape
    peak = jnp.max(stats_ref[:, 0, :], axis=0, keepdims=True)
    count = jnp.sum(stats_ref[:, 1, :] * jnp.exp(stats_ref[:, 0, :] - peak), axis=0, keepdims=True)
    log_norm = peak + jnp.log(count)
    prob = prob_ref[...]
    prob_sum = jnp.sum(prob, axis=1, keepdims=True)
    entropy = jnp.sum(prob * jnp.log(prob), axis=1, keepdims=True)
    log_norm = jnp.broadcast_to(log_norm, (128, rows)).T[:, 0:1]
    whole = jnp.sum(log_norm * (1.0 + prob_sum) + entropy) - jnp.sum(stats_ref[:, 2, :])
    row_ref[...] = jnp.full((8, 128), whole)
    chunk = 256 if width % 256 == 0 else 128
    weight = 1.0 + prob_sum

    def body(n, carry):
        at = pl.ds(pl.multiple_of(n * chunk, chunk), chunk)
        grad = (weight * jnp.exp(logits_ref[:, at] - log_norm) - marks_ref[:, at]) * (1.0 / pos_all)
        grads[:, at] = lower(grad)
        dtable_ref[at, :] = dims_tn(lower(grad), z_ref[...])
        return carry

    lax.fori_loop(0, width // chunk, body, 0)
    section = lax.axis_index("section")
    for r in range(rows // (sections * span)):
        at = pl.ds(pl.multiple_of((r * sections + section) * span, span), span)
        dz_ref[r * span : (r + 1) * span, :] = lower(product(grads[at, :], table_ref[...]))


def head_backward(z, table, marks, logits, stats_all, prob, span, pos_all):
    rows, width = logits.shape
    sections = lax.axis_size("section")
    return pl.pallas_call(
        partial(head_backward_kernel, sections, span, pos_all),
        out_shape=[
            jax.ShapeDtypeStruct((rows // sections, z.shape[1]), jnp.bfloat16),
            jax.ShapeDtypeStruct((width, z.shape[1]), jnp.float32),
            jax.ShapeDtypeStruct((8, 128), jnp.float32),
        ],
        in_specs=[VMEM] * 6,
        out_specs=[VMEM] * 3,
        scratch_shapes=[pltpu.VMEM((rows, width), jnp.bfloat16)],
        name="head_backward",
    )(z, table, marks, logits, stats_all, prob)
def pieces_of(rows):
    part = 400 if rows % 400 == 0 else rows
    return [(at, part) for at in range(0, rows, part)]


def each_tile(rows, columns, fn, carry):
    step = 16
    wide = 256 if columns % 256 == 0 else columns

    def body(n, carry):
        at = pl.ds(pl.multiple_of(n * step, step), step)
        for c in range(0, columns, wide):
            carry = fn(at, slice(c, c + wide), carry)
        return carry

    carry = lax.fori_loop(0, rows // step, body, carry)
    if rows % step:
        at = slice(rows // step * step, rows)
        tail = [jnp.zeros((rows % step, wide), jnp.float32)] * 2
        for c in range(0, columns, wide):
            tail = fn(at, slice(c, c + wide), tail)
        carry = [carry[0], carry[1]] + [jnp.sum(t) for t in tail]
    return carry


def step_kernel(shapes, scalar_ref, sums_ref, *refs):
    n = len(shapes)
    small_sums, refs = refs[:5], refs[5:]
    small_in, refs = refs[:6], refs[6:]
    grads, refs = refs[:n], refs[n:]
    weights, refs = refs[:n], refs[n:]
    firsts, refs = refs[:n], refs[n:]
    seconds, refs = refs[:n], refs[n:]
    out_first, refs = refs[:n], refs[n:]
    out_second, refs = refs[:n], refs[n:]
    out_dir, refs = refs[:n], refs[n:]
    small_out, refs = refs[:6], refs[6:]
    norm_ref, small_norm_ref, refs = refs[0], refs[1], refs[2:]
    g_buf, refs = refs[:n], refs[n:]
    w_buf, refs = refs[:n], refs[n:]
    m_buf, refs = refs[:n], refs[n:]
    v_buf, refs = refs[:n], refs[n:]
    d_buf, refs = refs[:n], refs[n:]
    load_sem, store_sem = refs
    work = []
    for a in range(n):
        for at, part in pieces_of(shapes[a][0]):
            rows = pl.ds(at, part)
            p = len(work)
            loads = [
                pltpu.make_async_copy(src.at[rows], dst.at[rows], load_sem.at[p, q])
                for q, (src, dst) in enumerate(
                    ((grads[a], g_buf[a]), (weights[a], w_buf[a]), (firsts[a], m_buf[a]), (seconds[a], v_buf[a]))
                )
            ]
            stores = [
                pltpu.make_async_copy(src.at[rows], dst.at[rows], store_sem.at[p, q])
                for q, (src, dst) in enumerate(
                    ((m_buf[a], out_first[a]), (v_buf[a], out_second[a]), (d_buf[a], out_dir[a]))
                )
            ]
            work.append((a, at, part, loads, stores))
    for _, _, _, loads, _ in work[:3]:
        for copy in loads:
            copy.start()
    lane = lax.broadcasted_iota(jnp.int32, (8, 128), 1)
    row = lax.broadcasted_iota(jnp.int32, (8, 128), 0)

    def scalar_at(values, r, c):
        return jnp.sum(jnp.where((row == r) & (lane == c), values, 0.0))

    smalls = [ref[...].astype(jnp.float32) for ref in small_sums]
    norm = jnp.sqrt(
        jnp.full((1, 1), scalar_at(sums_ref[...], 0, 0) + sum(square_sum(v) for v in smalls))
    )
    clip = jnp.minimum(1.0, scalar_ref[2] / norm)
    inverse_first = scalar_ref[0]
    inverse_second = scalar_ref[1]

    def adam(weight, grad, first, second):
        scaled = clip * grad
        first_new = beta_first * first + (1.0 - beta_first) * scaled
        second_new = beta_second * second + (1.0 - beta_second) * scaled * scaled
        direction = (first_new * inverse_first) / (
            jnp.sqrt(second_new * inverse_second) + adam_eps
        ) + decay_rate * weight
        return first_new, second_new, direction

    def small_step(group, part, grad):
        w_ref, m_ref, v_ref = small_in[3 * group : 3 * group + 3]
        weight = w_ref[part]
        first_new, second_new, direction = adam(weight, grad, m_ref[part], v_ref[part])
        norms = [jnp.sqrt(jnp.full((1, 1), square_sum(v))) for v in (weight, direction)]
        small_out[3 * group][part] = weight - learn_rate * (norms[0] / norms[1]) * direction
        small_out[3 * group + 1][part] = first_new
        small_out[3 * group + 2][part] = second_new
        return norms

    features, heads = small_in[0].shape[1:]
    small_norms = []
    for layer in range(2):
        small_norms += small_step(0, layer, smalls[layer].T[0:features, 0:heads])
    for t in range(5):
        grad = smalls[2 + t // 2][t % 2 : t % 2 + 1, :]
        small_norms += small_step(1, slice(t, t + 1), grad)
    table = jnp.where((row == 0) & (lane == 0), norm, 0.0)
    for t, value in enumerate(small_norms):
        table = jnp.where((row == 1) & (lane == t), value, table)
    small_norm_ref[...] = table

    sums = [[jnp.float32(0), jnp.float32(0)] for _ in range(n)]
    for p, (a, at, part, loads, stores) in enumerate(work):
        for copy in loads:
            copy.wait()
        if p + 3 < len(work):
            for copy in work[p + 3][3]:
                copy.start()
        g, w, m, v, d = (buf[a].at[pl.ds(at, part)] for buf in (g_buf, w_buf, m_buf, v_buf, d_buf))
        columns = shapes[a][1]
        wide = 256 if columns % 256 == 0 else columns

        def tile(rows, cols, carry):
            weight = w[rows, cols]
            first_new, second_new, direction = adam(
                weight, g[rows, cols].astype(jnp.float32), m[rows, cols], v[rows, cols]
            )
            m[rows, cols] = first_new
            v[rows, cols] = second_new
            d[rows, cols] = direction
            return [carry[0] + weight * weight, carry[1] + direction * direction]

        zero = jnp.zeros((16, wide), jnp.float32)
        done = each_tile(part, columns, tile, [zero, zero])
        for copy in stores:
            copy.start()
        for q in range(2):
            sums[a][q] = sums[a][q] + jnp.sum(done[q])
            if len(done) > 2:
                sums[a][q] = sums[a][q] + done[2 + q]
    section = lax.axis_index("section")
    table = jnp.zeros((8, 128), jnp.float32)
    for a in range(n):
        here = (section if a == 0 else lax.axis_index("replica")) == 0
        place = 0 if a == 0 else 2 * section
        for q in range(2):
            value = jnp.where(here, sums[a][q], 0.0)
            table = jnp.where((row == a) & (lane == place + q), value, table)
    norm_ref[...] = table
    for _, _, _, _, stores in work:
        for copy in stores:
            copy.wait()


def optimizer_step(scalars, sums, small_sums, small, grads, weights, firsts, seconds):
    n = len(grads)
    shapes = [w.shape for w in weights]
    flat = [jax.ShapeDtypeStruct(s, jnp.float32) for s in shapes]
    buffers = lambda kinds: [pltpu.VMEM(s, k) for s, k in zip(shapes, kinds)]
    parts = sum(len(pieces_of(s[0])) for s in shapes)
    out = pl.pallas_call(
        partial(step_kernel, shapes),
        out_shape=flat * 3
        + [jax.ShapeDtypeStruct(s.shape, jnp.float32) for s in small]
        + [jax.ShapeDtypeStruct((8, 128), jnp.float32)] * 2,
        in_specs=[pl.BlockSpec(memory_space=pltpu.SMEM)] + [VMEM] * 12 + [ANY] * (4 * n),
        out_specs=[ANY] * (3 * n) + [VMEM] * 8,
        scratch_shapes=buffers([g.dtype for g in grads])
        + buffers([jnp.float32] * n) * 4
        + [DMA((parts, 4)), DMA((parts, 3))],
        compiler_params=pltpu.CompilerParams(vmem_limit_bytes=60 * 2**20),
        name="optimizer_step",
    )(scalars, sums, *small_sums, *small, *grads, *weights, *firsts, *seconds)
    return out[:n], out[n : 2 * n], out[2 * n : 3 * n], out[3 * n : 3 * n + 6], out[-2], out[-1]


def apply_kernel(shapes, norm_ref, *refs):
    n = len(shapes)
    norms = jnp.sqrt(norm_ref[...])
    lane = lax.broadcasted_iota(jnp.int32, (8, 128), 1)
    row = lax.broadcasted_iota(jnp.int32, (8, 128), 0)

    def norm_at(a, q):
        place = q if a == 0 else 2 * lax.axis_index("section") + q
        return jnp.full((1, 1), jnp.sum(jnp.where((row == a) & (lane == place), norms, 0.0)))

    weights, directions, outs = refs[:n], refs[n : 2 * n], refs[2 * n : 3 * n]
    w_buf, d_buf = refs[3 * n : 4 * n], refs[4 * n : 5 * n]
    load_sem, store_sem = refs[5 * n :]
    work = []
    for a in range(n):
        for at, part in pieces_of(shapes[a][0]):
            rows = pl.ds(at, part)
            p = len(work)
            loads = [
                pltpu.make_async_copy(weights[a].at[rows], w_buf[a].at[rows], load_sem.at[p, 0]),
                pltpu.make_async_copy(directions[a].at[rows], d_buf[a].at[rows], load_sem.at[p, 1]),
            ]
            store = pltpu.make_async_copy(w_buf[a].at[rows], outs[a].at[rows], store_sem.at[p])
            work.append((a, at, part, loads, store))
    for _, _, _, loads, _ in work[:3]:
        for copy in loads:
            copy.start()
    for p, (a, at, part, loads, store) in enumerate(work):
        for copy in loads:
            copy.wait()
        if p + 3 < len(work):
            for copy in work[p + 3][3]:
                copy.start()
        w, d = w_buf[a].at[pl.ds(at, part)], d_buf[a].at[pl.ds(at, part)]
        rate = learn_rate * (norm_at(a, 0) / norm_at(a, 1))

        def tile(rows, cols, carry):
            w[rows, cols] = w[rows, cols] - rate * d[rows, cols]
            return carry

        each_tile(part, shapes[a][1], tile, [jnp.float32(0), jnp.float32(0)])
        store.start()
    for _, _, _, _, store in work:
        store.wait()


def apply_step(norms, weights, directions):
    n = len(weights)
    shapes = [w.shape for w in weights]
    parts = sum(len(pieces_of(s[0])) for s in shapes)
    return pl.pallas_call(
        partial(apply_kernel, shapes),
        out_shape=[jax.ShapeDtypeStruct(s, jnp.float32) for s in shapes],
        in_specs=[VMEM] + [ANY] * (2 * n),
        out_specs=[ANY] * n,
        scratch_shapes=[pltpu.VMEM(s, jnp.float32) for s in shapes] * 2 + [DMA((parts, 2)), DMA((parts,))],
        compiler_params=pltpu.CompilerParams(vmem_limit_bytes=62 * 2**20),
        name="apply_step",
    )(norms, *weights, *directions)


def lower(values):
    return values.astype(jnp.bfloat16)


def product(left, right):
    return jnp.dot(left, right, preferred_element_type=jnp.float32)


def product_left(left, right):
    return lax.dot_general(left, right, (((0,), (0,)), ((), ())), preferred_element_type=jnp.float32)


def product_right(left, right):
    return lax.dot_general(left, right, (((1,), (1,)), ((), ())), preferred_element_type=jnp.float32)


def rms_forward(values, gain):
    inverse = lax.rsqrt(jnp.mean(values * values, axis=-1, keepdims=True) + eps_norm)
    normed = values * inverse
    return (normed * gain, normed, inverse)


def rms_backward(grad_out, normed, inverse, gain):
    grad_normed = grad_out * gain
    grad_in = inverse * (
        grad_normed - normed * jnp.mean(grad_normed * normed, axis=-1, keepdims=True)
    )
    return (grad_in, jnp.sum(grad_out * normed, axis=0))


def path_mask(parent_row, tree_len):
    seg_count = parent_row.shape[0]
    seglen = tree_len // seg_count
    seg_order = jnp.arange(seg_count, dtype=jnp.int32)
    parent_hot = ((parent_row[:, None] == seg_order[None, :]) & (seg_order[:, None] >= 1)).astype(
        jnp.float32
    )
    identity = jnp.eye(seg_count, dtype=jnp.float32)
    power, steps = parent_hot, 1
    reached = identity + parent_hot
    while steps < seg_count:
        reached = jnp.minimum(1.0, jnp.dot(reached, reached))
        steps *= 2
    strict = reached - identity
    seg_of = jnp.arange(tree_len, dtype=jnp.int32) // seglen
    seg_hot = (seg_of[:, None] == seg_order[None, :]).astype(jnp.float32)
    ancestor = jnp.dot(jnp.dot(seg_hot, strict), seg_hot.T)
    places = jnp.arange(tree_len, dtype=jnp.int32)
    inside = (seg_of[:, None] == seg_of[None, :]) & (places[None, :] <= places[:, None])
    return ancestor + inside.astype(jnp.float32)


def square_sum(values):
    return jnp.sum(values * values)


def local(
    tokens,
    parents,
    loss_positions,
    targets,
    teacher_index,
    teacher_probability,
    step_count,
    embed_table,
    table_first,
    table_second,
    attention_in,
    attention_in_first,
    attention_in_second,
    attention_out,
    attention_out_first,
    attention_out_second,
    feedforward_in,
    feedforward_in_first,
    feedforward_in_second,
    feedforward_out,
    feedforward_out_first,
    feedforward_out_second,
    forget_gate,
    forget_first,
    forget_second,
    norm_gains,
    gains_first,
    gains_second,
):
    section_id = lax.axis_index("section")
    replica_id = lax.axis_index("replica")
    shard_id = lax.axis_index("shard")
    sections = lax.axis_size("section")
    replicas = lax.axis_size("replica")
    shards = lax.axis_size("shard")
    group_trees, tree_len = tokens.shape
    rows_each, width = embed_table.shape
    pos_count = loss_positions.shape[1]
    pos_all = group_trees * replicas * pos_count
    owners = replicas * shards
    owner_id = replica_id * shards + shard_id
    own_tree = section_id * shards + shard_id

    def own_row(values):
        return lax.dynamic_index_in_dim(values, own_tree, 0, keepdims=False)

    tree_tokens = own_row(tokens)
    token_owner = tree_tokens // rows_each
    token_row = tree_tokens % rows_each
    spots = jnp.arange(tree_len, dtype=jnp.int32)

    def asked(batch):
        earlier = spots[None, :] < spots[:, None]
        same = tree_tokens[:, None] == tree_tokens[None, :]
        is_first = jnp.logical_not(jnp.any(same & earlier, axis=1))
        counted = earlier & (token_owner[:, None] == token_owner[None, :]) & is_first[None, :]
        number_first = jnp.sum(counted.astype(jnp.int32), axis=1)
        number = jnp.sum(jnp.where(same & is_first[None, :], number_first[None, :], 0), axis=1)
        slot = number - batch * batch_rows
        inside = (slot >= 0) & (slot < batch_rows)
        place = jnp.where(inside, token_owner * batch_rows + slot, -1)
        spot_of = jnp.arange(owners * batch_rows, dtype=jnp.int32)
        hot = place[None, :] == spot_of[:, None]
        rows = jnp.max(jnp.where(hot & is_first[None, :], token_row[None, :] + 1, 0), axis=1)
        return rows.reshape(owners, batch_rows), lower(hot)

    def all_devices(part, ident):
        return exchange(part[None], ident, relay=True).reshape((sections, replicas, shards) + part.shape)

    def wanted(batch):
        rows, hot = asked(batch)
        every = all_devices(jnp.pad(rows, ((0, 0), (0, 128 - batch_rows))), 0)
        mine = lax.dynamic_index_in_dim(every, owner_id, 3, keepdims=False)[..., :batch_rows]
        wish = mine.reshape(sections * owners * batch_rows) - 1
        row_of = jnp.arange(rows_each, dtype=jnp.int32)
        return hot, lower(wish[:, None] == row_of[None, :])

    def more_rows(state):
        batch, total_rows = state
        hot_more, pick = wanted(batch)
        own_pick = lax.dynamic_index_in_dim(
            pick.reshape(sections, owners * batch_rows, rows_each), section_id, 0, keepdims=False
        )
        sent = lower(product(own_pick, table_wide[:rows_each])).reshape(owners, batch_rows, width)
        got_more = exchange(sent, 1)[0].reshape(owners * batch_rows, width)
        return (batch + 1, total_rows + product_left(hot_more, got_more))

    def more_grads(state):
        batch, total_rows = state
        hot_more, pick = wanted(batch)
        sent = lower(product(hot_more, embed_low)).reshape(owners, batch_rows, width)
        got_more = exchange(sent, 6, relay=True).reshape(sections * owners * batch_rows, width)
        more = product_left(pick, got_more)
        return (batch + 1, total_rows + jnp.pad(more, ((0, width_all - rows_each), (0, 0))))

    def halves(weight):
        return lower(weight).reshape(2, weight.shape[1] // 2, weight.shape[2])

    width_all = -(-rows_each // 128) * 128
    table_wide = lower(jnp.pad(embed_table, ((0, width_all - rows_each), (0, 0))))
    layer_weights = (attention_in, attention_out, feedforward_in, feedforward_out)
    entries = 8 * teacher_index.shape[2]
    group_data = [
        teacher_index.reshape(-1, 1, entries),
        teacher_probability.reshape(-1, 1, entries),
        targets.reshape(-1, 1),
    ]
    pair_parts = group_data if replicas == 2 else []
    hot, asks = ask_rows(tree_tokens, token_owner, token_row, owners)
    gathered, group_all, (asked_all, got, *marks) = gather(
        [halves(w) for w in layer_weights], 2, pair_parts, split=True, errand=(asks, table_wide), rows_each=rows_each
    )
    if replicas != 2:
        group_all = [lax.all_gather(part, "replica") for part in group_data]
        marks = [spread_entries((owner_id * rows_each)[None], *group_all, rows_each, width_all)]
    batches = (jnp.max(asked_all[:, :, 0, 127]) + batch_rows - 1) // batch_rows
    embeds = product_left(hot, got.reshape(owners * batch_rows, width))
    _, embeds = lax.while_loop(lambda s: s[0] < batches, more_rows, (jnp.int32(1), embeds))
    mats = [g.reshape(sections, -1, g.shape[-1]) for g in gathered]
    heads = forget_gate.shape[2]
    forget_low = jnp.pad(lower(forget_gate[:, :width]), ((0, 0), (0, 0), (0, 128 - heads)))
    forget_bias = jnp.pad(forget_gate[:, width:], ((0, 0), (0, 0), (0, 128 - heads)))
    gains_of = [jnp.pad(norm_gains[2 * n : 2 * n + 2], ((0, 6), (0, 0))) for n in range(2)]

    allowed = lower(path_mask(own_row(parents), tree_len))
    out_0, *saved_0 = layer_forward(0, False, embeds, allowed, mats, forget_low[0], forget_bias[0], gains_of[0])
    out_1, *saved_1 = layer_forward(1, True, out_0, allowed, mats, forget_low[1], forget_bias[1], gains_of[1])

    positions = own_row(loss_positions)
    position_hot = (positions[:, None] == spots[None, :]).astype(jnp.float32)
    picked = jnp.take(out_1, positions, axis=0)
    final_gain = norm_gains[4]
    head_out, head_normed, head_inverse = rms_forward(picked, final_gain)
    head_rows = jnp.swapaxes(all_devices(lower(head_out), 3), 0, 1).reshape(pos_all, width)

    prob_all = group_all[1].reshape(pos_all, -1)
    marks = marks[0]
    logits, stats = head_forward(rows_each, head_rows, table_wide, marks)
    if replicas == 2:
        stats_all = exchange(stats[None], 4)[0]
    else:
        stats_all = lax.all_gather(lax.all_gather(stats, "replica"), "shard")
    grad_heads, head_table, loss_sum = head_backward(
        head_rows, table_wide, marks, logits, stats_all.reshape(owners, 4, pos_all), prob_all, shards * pos_count, pos_all
    )
    grad_heads = exchange(grad_heads.reshape(owners, pos_count, width), 5)[0]
    grad_heads = jnp.sum(grad_heads.astype(jnp.float32), axis=0)
    grad_picked, grad_final = rms_backward(grad_heads, head_normed, head_inverse, final_gain)
    grad_top = lax.dot_general(
        position_hot, grad_picked, (((0,), (0,)), ((), ())), precision=highest
    )

    grad_mid, forget_1, gains_1, *grads_1 = layer_backward(
        1, True, False, grad_top, out_0, allowed, saved_1, mats, forget_low[1], gains_of[1]
    )
    grad_low, forget_0, gains_0, *grads_0 = layer_backward(
        0, False, True, grad_mid, embeds, allowed, saved_0, mats, forget_low[0], gains_of[0]
    )
    embed_low = lower(grad_low)

    stacked = [
        [g.reshape(shards, 2, -1, g.shape[-1]) for g in pair] for pair in zip(grads_0, grads_1)
    ]
    sent = lower(product(hot, embed_low)).reshape(owners, batch_rows, width)
    small_sums = [forget_0, forget_1, gains_0, gains_1, grad_final[None]]
    layer_grads, (got_grads,) = reduce_parts(stacked, 8, ([], sent))
    if replicas != 2:
        layer_grads = [lax.psum(g * jnp.bfloat16(0.5), "replica") for g in layer_grads]
    _, head_table = lax.while_loop(lambda s: s[0] < batches, more_grads, (jnp.int32(1), head_table))
    table_grad, square = table_gradient(
        rows_each, asked_all, got_grads.reshape(-1, width), head_table, layer_grads
    )
    layer_grads = [g.reshape(w.shape[1:]) for g, w in zip(layer_grads, layer_weights)]
    scalars, *small_sums = total([square, *small_sums], 15)
    loss_total = loss_sum[0, 0] / pos_all
    count_float = step_count.astype(jnp.float32)
    rates = jnp.stack(
        [
            1.0 / (1.0 - jnp.power(beta_first, count_float)),
            1.0 / (1.0 - jnp.power(beta_second, count_float)),
            clip_factor / jnp.sqrt(jnp.float32(pos_all)),
        ]
    )
    small = [forget_gate, forget_first, forget_second, norm_gains, gains_first, gains_second]
    weights = [embed_table] + [w[0] for w in layer_weights]
    firsts = [table_first] + [
        m[0] for m in (attention_in_first, attention_out_first, feedforward_in_first, feedforward_out_first)
    ]
    seconds = [table_second] + [
        m[0] for m in (attention_in_second, attention_out_second, feedforward_in_second, feedforward_out_second)
    ]
    firsts_new, seconds_new, directions, small_new, norms, small_norms = optimizer_step(
        rates, scalars, small_sums, small, [table_grad, *layer_grads], weights, firsts, seconds
    )
    (norms,) = total([norms], 16)
    weights_new = apply_step(norms, weights, directions)
    norms = jnp.sqrt(norms)
    table_norms = norms[0, :2]
    layer_norms = norms[1:5, : 2 * sections].reshape(4 * sections, 2)
    new_table, table_first_new, table_second_new = weights_new[0], firsts_new[0], seconds_new[0]
    new_layers = [(weights_new[n][None], firsts_new[n][None], seconds_new[n][None]) for n in range(1, 5)]
    new_forget, forget_first_new, forget_second_new, new_gains, gains_first_new, gains_second_new = small_new
    layer_count, gain_count = forget_gate.shape[0], norm_gains.shape[0]
    grad_norm = small_norms[0, 0]
    tensor_norms = jnp.concatenate(
        [
            table_norms[None],
            layer_norms,
            small_norms[1, : 2 * (layer_count + gain_count)].reshape(-1, 2),
        ],
        axis=0,
    )
    return (
        new_table,
        table_first_new,
        table_second_new,
        *new_layers[0],
        *new_layers[1],
        *new_layers[2],
        *new_layers[3],
        new_forget,
        forget_first_new,
        forget_second_new,
        new_gains,
        gains_first_new,
        gains_second_new,
        tensor_norms,
        grad_norm,
        loss_total,
    )


def solution(mesh):
    group = P("replica", None)
    table = P(("replica", "shard"), None)
    layer = P("section", "shard", None)
    in_specs = (
        (group,) * 4
        + (P("replica", None, None),) * 2
        + (P(),)
        + (table,) * 3
        + (layer,) * 12
        + (P(),) * 6
    )
    out_specs = (table,) * 3 + (layer,) * 12 + (P(),) * 9
    return jax.shard_map(local, mesh=mesh, in_specs=in_specs, out_specs=out_specs, check_vma=False)
```
